128 devices in a mesh: dp: 1, ep: 128 (over z, y, x, core).
Axes of the slice: x: 4, y: 4, z: 4, core: 2. Of those that a mesh axis runs over, the one named last changes fastest.
Arguments:
- hidden: bfloat16 [128, 256, 2048], P(('dp', 'ep'))
- expert_ids: int32 [128, 256, 8], P(('dp', 'ep'))
- slot_ids: int32 [128, 256, 8], P(('dp', 'ep'))
- attn_norm: bfloat16 [2048], replicated
- w_query: bfloat16 [2048, 4096], replicated
- w_key: bfloat16 [2048, 512], replicated
- w_value: bfloat16 [2048, 512], replicated
- w_out: bfloat16 [32, 128, 2048], replicated
- ffn_norm: bfloat16 [2048], replicated
- ffn_gate: bfloat16 [2048, 6144], replicated
- ffn_up: bfloat16 [2048, 6144], replicated
- ffn_down: bfloat16 [6144, 2048], replicated
- moe_norm: bfloat16 [2048], replicated
- w_router: bfloat16 [2048, 128], replicated
- exp_gate: bfloat16 [128, 2048, 768], P('ep')
- exp_up: bfloat16 [128, 2048, 768], P('ep')
- exp_down: bfloat16 [128, 768, 2048], P('ep')
Outputs:
- output: bfloat16 [128, 256, 2048], P(('dp', 'ep'))
All inputs are finite; a program needn't handle non-finite values.
Results may differ from the reference program's by a relative error of at most 0.0109522.
Values are sent between devices in bfloat16 or wider.
A program may use at most 1 GiB of HBM per device.

```python
import jax
import jax.numpy as jnp
from jax import lax

D_MODEL = 2048
N_HEADS = 32
KV_HEADS = 4
HEAD_DIM = 128
FF_DIM = 6144
N_EXPERTS = 128
TOP_K = 8
EXPERT_FF = 768
SEQ_LEN = 256
BATCH_DEV = 1
GROUP_SIZE = 128

N_SEQS = GROUP_SIZE * BATCH_DEV
TOKENS_DEV = BATCH_DEV * SEQ_LEN
TOKENS = GROUP_SIZE * TOKENS_DEV
LOCAL_EXPERTS = N_EXPERTS // GROUP_SIZE
CAPACITY = 3 * TOKENS_DEV * TOP_K // N_EXPERTS
HOT_DEVICES = max(1, GROUP_SIZE // 8)
Q_PER_KV = N_HEADS // KV_HEADS
RMS_EPS = 1e-6
ROPE_BASE = 10000.0


def draw_routing(route_key):
    key_devs, key_rows = jax.random.split(route_key)
    mean_load = TOKENS_DEV * TOP_K // N_EXPERTS
    hot_count = HOT_DEVICES * LOCAL_EXPERTS
    cold_count = N_EXPERTS - hot_count
    cold_total = N_EXPERTS * mean_load - hot_count * CAPACITY
    cold_base = cold_total // cold_count
    cold_extra = cold_total - cold_base * cold_count
    expert_rank = jnp.arange(N_EXPERTS, dtype=jnp.int32)
    rank_load = jnp.where(expert_rank < hot_count, CAPACITY, cold_base + (expert_rank - hot_count < cold_extra).astype(jnp.int32))
    rank_start = jnp.cumsum(rank_load) - rank_load
    copy_rank = jnp.repeat(expert_rank, rank_load, total_repeat_length=TOKENS_DEV * TOP_K)
    copy_slot = jnp.arange(TOKENS_DEV * TOP_K, dtype=jnp.int32) - rank_start[copy_rank]
    dev_order = jax.random.permutation(key_devs, GROUP_SIZE)
    expert_of_rank = (dev_order[:, None] * LOCAL_EXPERTS + jnp.arange(LOCAL_EXPERTS)[None, :]).reshape(N_EXPERTS)
    base_ids = expert_of_rank[copy_rank].reshape(TOP_K, TOKENS_DEV).T
    base_slots = copy_slot.reshape(TOP_K, TOKENS_DEV).T

    def one_device(dev_key):
        key_perm, key_shift = jax.random.split(dev_key)
        row_order = jax.random.permutation(key_perm, TOKENS_DEV)
        col_shift = jax.random.randint(key_shift, (TOKENS_DEV, 1), 0, TOP_K)
        col_index = (jnp.arange(TOP_K)[None, :] + col_shift) % TOP_K
        dev_ids = jnp.take_along_axis(base_ids[row_order], col_index, axis=1)
        dev_slots = jnp.take_along_axis(base_slots[row_order], col_index, axis=1)
        return dev_ids, dev_slots

    dev_ids, dev_slots = jax.vmap(one_device)(jax.random.split(key_rows, GROUP_SIZE))
    return (dev_ids.astype(jnp.int32).reshape(N_SEQS, SEQ_LEN, TOP_K), dev_slots.astype(jnp.int32).reshape(N_SEQS, SEQ_LEN, TOP_K))


def draw_normal(draw_key, shape, std):
    return (jax.random.normal(draw_key, shape, jnp.float32) * std).astype(jnp.bfloat16)


def draw_gain(gain_key):
    return (1.0 + 0.4 * jax.random.normal(gain_key, (D_MODEL,), jnp.float32)).astype(jnp.bfloat16)


def setup_inputs(seed: int = 0, part: int = 0) -> dict:
    shared = jax.random.split(jax.random.key(seed), 14)
    part_key = jax.random.fold_in(jax.random.key(seed + 1), part)
    expert_ids, slot_ids = draw_routing(jax.random.fold_in(part_key, 3))
    q_width = N_HEADS * HEAD_DIM
    kv_width = KV_HEADS * HEAD_DIM
    return {
        'hidden': draw_normal(jax.random.fold_in(part_key, 1), (N_SEQS, SEQ_LEN, D_MODEL), 1.0),
        'expert_ids': expert_ids,
        'slot_ids': slot_ids,
        'attn_norm': draw_gain(shared[0]),
        'w_query': draw_normal(shared[1], (D_MODEL, q_width), 2.0 * D_MODEL ** -0.5),
        'w_key': draw_normal(shared[2], (D_MODEL, kv_width), D_MODEL ** -0.5),
        'w_value': draw_normal(shared[3], (D_MODEL, kv_width), D_MODEL ** -0.5),
        'w_out': draw_normal(shared[4], (N_HEADS, HEAD_DIM, D_MODEL), 2.0 * q_width ** -0.5),
        'ffn_norm': draw_gain(shared[5]),
        'ffn_gate': draw_normal(shared[6], (D_MODEL, FF_DIM), D_MODEL ** -0.5),
        'ffn_up': draw_normal(shared[7], (D_MODEL, FF_DIM), D_MODEL ** -0.5),
        'ffn_down': draw_normal(shared[8], (FF_DIM, D_MODEL), FF_DIM ** -0.5),
        'moe_norm': draw_gain(shared[9]),
        'w_router': draw_normal(shared[10], (D_MODEL, N_EXPERTS), 1.5 * D_MODEL ** -0.5),
        'exp_gate': draw_normal(shared[11], (N_EXPERTS, D_MODEL, EXPERT_FF), D_MODEL ** -0.5),
        'exp_up': draw_normal(shared[12], (N_EXPERTS, D_MODEL, EXPERT_FF), D_MODEL ** -0.5),
        'exp_down': draw_normal(shared[13], (N_EXPERTS, EXPERT_FF, D_MODEL), 2.0 * EXPERT_FF ** -0.5),
    }


def rms_norm(row_vals, norm_scale):
    as_float = row_vals.astype(jnp.float32)
    inv_rms = lax.rsqrt(jnp.mean(as_float * as_float, axis=-1, keepdims=True) + RMS_EPS)
    return (as_float * inv_rms * norm_scale.astype(jnp.float32)).astype(jnp.bfloat16)


def rotary(head_vals):
    half_dim = HEAD_DIM // 2
    inv_freq = ROPE_BASE ** (-2.0 * jnp.arange(half_dim, dtype=jnp.float32) / HEAD_DIM)
    angles = jnp.arange(SEQ_LEN, dtype=jnp.float32)[:, None] * inv_freq[None, :]
    cos_t = jnp.cos(angles)[:, None, :]
    sin_t = jnp.sin(angles)[:, None, :]
    first_half = head_vals[..., :half_dim]
    second_half = head_vals[..., half_dim:]
    return jnp.concatenate([first_half * cos_t - second_half * sin_t, second_half * cos_t + first_half * sin_t], axis=-1)


def reference(hidden, expert_ids, slot_ids, attn_norm, w_query, w_key, w_value, w_out, ffn_norm, ffn_gate, ffn_up, ffn_down, moe_norm, w_router, exp_gate, exp_up, exp_down):
    causal = jnp.arange(SEQ_LEN)[:, None] >= jnp.arange(SEQ_LEN)[None, :]
    out_mat = w_out.reshape(N_HEADS * HEAD_DIM, D_MODEL)

    def dense_seq(seq_rows):
        normed = rms_norm(seq_rows, attn_norm)
        queries = rotary(jnp.dot(normed, w_query, preferred_element_type=jnp.float32).reshape(SEQ_LEN, N_HEADS, HEAD_DIM)).astype(jnp.bfloat16)
        key_vals = rotary(jnp.dot(normed, w_key, preferred_element_type=jnp.float32).reshape(SEQ_LEN, KV_HEADS, HEAD_DIM)).astype(jnp.bfloat16)
        values = jnp.dot(normed, w_value, preferred_element_type=jnp.float32).astype(jnp.bfloat16).reshape(SEQ_LEN, KV_HEADS, HEAD_DIM)
        grouped = queries.reshape(SEQ_LEN, KV_HEADS, Q_PER_KV, HEAD_DIM)
        scores = jnp.einsum('sgrd,tgd->grst', grouped.astype(jnp.float32), key_vals.astype(jnp.float32)) * HEAD_DIM ** -0.5
        scores = jnp.where(causal, scores, -jnp.inf)
        attn_prob = jax.nn.softmax(scores, axis=-1).astype(jnp.bfloat16)
        context = jnp.einsum('grst,tgd->sgrd', attn_prob.astype(jnp.float32), values.astype(jnp.float32)).astype(jnp.bfloat16)
        attn_out = (seq_rows.astype(jnp.float32) + jnp.dot(context.reshape(SEQ_LEN, N_HEADS * HEAD_DIM), out_mat, preferred_element_type=jnp.float32)).astype(jnp.bfloat16)
        normed_ffn = rms_norm(attn_out, ffn_norm)
        hidden_act = (jax.nn.silu(jnp.dot(normed_ffn, ffn_gate, preferred_element_type=jnp.float32)) * jnp.dot(normed_ffn, ffn_up, preferred_element_type=jnp.float32)).astype(jnp.bfloat16)
        return attn_out.astype(jnp.float32) + jnp.dot(hidden_act, ffn_down, preferred_element_type=jnp.float32)

    dense_out = lax.map(dense_seq, hidden).reshape(TOKENS, D_MODEL)

    token_rows = hidden.reshape(TOKENS, D_MODEL)
    choice_ids = expert_ids.reshape(TOKENS, TOP_K)
    choice_slots = slot_ids.reshape(TOKENS, TOP_K)
    normed = rms_norm(token_rows, moe_norm)
    logits = jnp.dot(normed, w_router, preferred_element_type=jnp.float32)
    gate_vals = jax.nn.softmax(jnp.take_along_axis(logits, choice_ids, axis=1), axis=-1)
    src_dev = jnp.arange(TOKENS, dtype=jnp.int32) // TOKENS_DEV
    buf_pos = (choice_ids * GROUP_SIZE + src_dev[:, None]) * CAPACITY + choice_slots
    buf_rows = N_EXPERTS * GROUP_SIZE * CAPACITY
    owner_copy = jnp.full((buf_rows,), TOKENS * TOP_K, jnp.int32).at[buf_pos.reshape(-1)].set(jnp.arange(TOKENS * TOP_K, dtype=jnp.int32))
    padded = jnp.concatenate([normed, jnp.zeros((1, D_MODEL), jnp.bfloat16)], axis=0)
    gate_ext = jnp.concatenate([gate_vals.reshape(-1), jnp.zeros((1,), jnp.float32)])

    def one_expert(moe_acc, operands):
        copy_index, gate_w, up_w, down_w = operands
        token_index = copy_index // TOP_K
        expert_rows = padded[token_index]
        z_gate = jnp.dot(expert_rows, gate_w, preferred_element_type=jnp.float32)
        z_up = jnp.dot(expert_rows, up_w, preferred_element_type=jnp.float32)
        hidden_act = (jax.nn.silu(z_gate) * z_up).astype(jnp.bfloat16)
        expert_y = jnp.dot(hidden_act, down_w, preferred_element_type=jnp.float32).astype(jnp.bfloat16)
        weighted = gate_ext[copy_index][:, None] * expert_y.astype(jnp.float32)
        return moe_acc.at[token_index].add(weighted), None

    moe_acc = lax.scan(one_expert, jnp.zeros((TOKENS + 1, D_MODEL), jnp.float32), (owner_copy.reshape(N_EXPERTS, GROUP_SIZE * CAPACITY), exp_gate, exp_up, exp_down))[0]
    moe_out = moe_acc[:TOKENS]
    return (dense_out + moe_out).astype(jnp.bfloat16).reshape(N_SEQS, SEQ_LEN, D_MODEL)
```

```python
import functools
import math

import jax
import jax.numpy as jnp
from jax import lax
from jax.experimental import pallas as pl
from jax.experimental.pallas import tpu as pltpu
from jax.sharding import PartitionSpec as P

RMS_EPS = 1e-6
ROPE_BASE = 10000.0
CAP_FACTOR = 3
N_CHUNKS = 3
MESH = pl.DeviceIdType.MESH

BF16, F32, I32 = jnp.bfloat16, jnp.float32, jnp.int32

AXES = ('z', 'y', 'x', 'c')
LINE = ('z', 'x', 'y')
PLANE = (('y', 'x'), ('z', 'y'), ('z', 'x'))


def rms_norm(row_vals, norm_scale):
    as_float = row_vals.astype(F32)
    inv_rms = lax.rsqrt(jnp.mean(as_float * as_float, axis=-1, keepdims=True) + RMS_EPS)
    return (as_float * inv_rms * norm_scale.astype(F32)).astype(BF16)


def rotary(head_vals):
    seq_len, _, head_dim = head_vals.shape
    half_dim = head_dim // 2
    inv_freq = ROPE_BASE ** (-2.0 * jnp.arange(half_dim, dtype=F32) / head_dim)
    angles = jnp.arange(seq_len, dtype=F32)[:, None] * inv_freq[None, :]
    cos_t = jnp.cos(angles)[:, None, :]
    sin_t = jnp.sin(angles)[:, None, :]
    first_half = head_vals[..., :half_dim]
    second_half = head_vals[..., half_dim:]
    return jnp.concatenate([first_half * cos_t - second_half * sin_t, second_half * cos_t + first_half * sin_t], axis=-1)


def dense_sequence(rows, attn_norm, w_query, w_key, w_value, w_out, ffn_norm, ffn_gate, ffn_up, ffn_down):
    seq_len, model_dim = rows.shape
    n_heads, head_dim = w_out.shape[0], w_out.shape[1]
    kv_heads = w_key.shape[1] // head_dim
    q_per_kv = n_heads // kv_heads
    normed = rms_norm(rows, attn_norm)
    q_flat, k_flat, v_flat = lax.optimization_barrier(
        (
            jnp.dot(normed, w_query, preferred_element_type=F32),
            jnp.dot(normed, w_key, preferred_element_type=F32),
            jnp.dot(normed, w_value, preferred_element_type=F32).astype(BF16),
        )
    )
    queries = rotary(q_flat.reshape(seq_len, n_heads, head_dim)).astype(BF16).reshape(seq_len, kv_heads, q_per_kv, head_dim)
    key_vals = rotary(k_flat.reshape(seq_len, kv_heads, head_dim)).astype(BF16)
    values = v_flat.reshape(seq_len, kv_heads, head_dim)
    scores = jnp.einsum('sgrd,tgd->grst', queries, key_vals, preferred_element_type=F32) * head_dim ** -0.5
    causal = jnp.arange(seq_len)[:, None] >= jnp.arange(seq_len)[None, :]
    attn_prob = jax.nn.softmax(jnp.where(causal, scores, -jnp.inf), axis=-1).astype(BF16)
    context = jnp.einsum('grst,tgd->sgrd', attn_prob, values, preferred_element_type=F32).astype(BF16)
    context = context.reshape(seq_len, n_heads * head_dim)
    attn_out = (rows.astype(F32) + jnp.dot(context, w_out.reshape(n_heads * head_dim, model_dim), preferred_element_type=F32)).astype(BF16)
    normed_ffn = rms_norm(attn_out, ffn_norm)
    hidden_act = (jax.nn.silu(jnp.dot(normed_ffn, ffn_gate, preferred_element_type=F32)) * jnp.dot(normed_ffn, ffn_up, preferred_element_type=F32)).astype(BF16)
    return attn_out.astype(F32) + jnp.dot(hidden_act, ffn_down, preferred_element_type=F32)


def torus_of(n_devices):
    side = round((n_devices // 2) ** (1 / 3))
    assert side ** 3 * 2 == n_devices
    return side


def column_parts(model):
    lanes = model // 128
    first = -(-lanes // 3)
    second = -(-(lanes - first) // 2)
    ends = (0, first * 128, (first + second) * 128, model)
    return tuple((ends[p], ends[p + 1]) for p in range(3))


def expert_index(p, member, line_pos, side):
    pair, core = member // 2, member % 2
    a, b = pair // side, pair % side
    place = {PLANE[p][0]: a, PLANE[p][1]: b, LINE[p]: line_pos}
    return ((place['z'] * side + place['y']) * side + place['x']) * 2 + core


def slot_keys(p, shape, dim, chunk, line_pos, side, capacity):
    slots = capacity // N_CHUNKS
    row = lax.broadcasted_iota(I32, shape, dim)
    return expert_index(p, row // slots, line_pos, side) * capacity + chunk * slots + row % slots


def pick_kernel(place_ref, *refs, side, capacity):
    tokens_refs, key_refs, out_refs = refs[:3], refs[3:6], refs[6:]
    chunk = pl.program_id(1)
    for p in range(3):
        rows, n_tokens = out_refs[p].shape[0], tokens_refs[p].shape[1]
        wanted = slot_keys(p, (rows, n_tokens), 0, chunk, place_ref[p], side, capacity)
        keys = key_refs[p][0]
        hit = wanted == keys[0:1, :]
        for j in range(1, keys.shape[0]):
            hit = jnp.logical_or(hit, wanted == keys[j : j + 1, :])
        pick = jnp.where(hit, 1.0, 0.0).astype(BF16)
        out_refs[p][...] = jnp.dot(pick, tokens_refs[p][0], preferred_element_type=F32).astype(BF16)


def pick_rows(place, tokens, keys_t, side, capacity):
    members, slots = side * side * 2, capacity // N_CHUNKS
    rows = members * slots
    return pl.pallas_call(
        functools.partial(pick_kernel, side=side, capacity=capacity),
        out_shape=[jax.ShapeDtypeStruct((N_CHUNKS * side * rows, t.shape[2]), BF16) for t in tokens],
        grid=(side, N_CHUNKS),
        in_specs=[pl.BlockSpec(memory_space=pltpu.SMEM)]
        + [pl.BlockSpec((1,) + t.shape[1:], lambda d, k: (d, 0, 0)) for t in tokens]
        + [pl.BlockSpec((1,) + t.shape[1:], lambda d, k: (d, 0, 0)) for t in keys_t],
        out_specs=[pl.BlockSpec((rows, t.shape[2]), lambda d, k: (k * side + d, 0)) for t in tokens],
        compiler_params=pltpu.CompilerParams(vmem_limit_bytes=40 * 1024 * 1024),
        cost_estimate=pl.CostEstimate(
            flops=sum(2 * N_CHUNKS * side * rows * t.shape[1] * t.shape[2] for t in tokens),
            bytes_accessed=sum(2 * N_CHUNKS * side * rows * t.shape[2] for t in tokens),
            transcendentals=0,
        ),
    )(place, *tokens, *keys_t)


def weigh_kernel(place_ref, *refs, side, capacity):
    row_refs, key_refs, gate_refs, out_refs = refs[:3], refs[3:6], refs[6:9], refs[9:]
    chunk = pl.program_id(1)
    for p in range(3):
        rows, n_tokens = row_refs[p].shape[0], out_refs[p].shape[1]
        held = slot_keys(p, (n_tokens, rows), 1, chunk, place_ref[p], side, capacity)
        keys, gates = key_refs[p][0], gate_refs[p][0]
        weight = jnp.zeros((n_tokens, rows), F32)
        for j in range(keys.shape[1]):
            weight = jnp.where(held == keys[:, j : j + 1], gates[:, j : j + 1], weight)
        high = weight.astype(BF16)
        rest = weight - high.astype(F32)
        middle = rest.astype(BF16)
        low = (rest - middle.astype(F32)).astype(BF16)
        y = row_refs[p][...]
        total = jnp.dot(high, y, preferred_element_type=F32) + (
            jnp.dot(middle, y, preferred_element_type=F32) + jnp.dot(low, y, preferred_element_type=F32)
        )

        @pl.when(chunk == 0)
        def _():
            out_refs[p][0] = total

        @pl.when(chunk > 0)
        def _():
            out_refs[p][0] += total


def weigh_rows(place, rows, keys, gates, side, capacity):
    block = side * side * 2 * capacity // N_CHUNKS
    n_tokens = keys[0].shape[1]
    by_source = lambda a: pl.BlockSpec((1,) + a.shape[1:], lambda d, k: (d, 0, 0))
    return pl.pallas_call(
        functools.partial(weigh_kernel, side=side, capacity=capacity),
        out_shape=[jax.ShapeDtypeStruct((side, n_tokens, r.shape[1]), F32) for r in rows],
        grid=(side, N_CHUNKS),
        in_specs=[pl.BlockSpec(memory_space=pltpu.SMEM)]
        + [pl.BlockSpec((block, r.shape[1]), lambda d, k: (k * side + d, 0)) for r in rows]
        + [by_source(a) for a in keys]
        + [by_source(a) for a in gates],
        out_specs=[pl.BlockSpec((1, n_tokens, r.shape[1]), lambda d, k: (d, 0, 0)) for r in rows],
        compiler_params=pltpu.CompilerParams(
            dimension_semantics=("arbitrary", "arbitrary"), vmem_limit_bytes=40 * 1024 * 1024
        ),
        cost_estimate=pl.CostEstimate(
            flops=sum(6 * r.shape[0] * n_tokens * r.shape[1] for r in rows),
            bytes_accessed=sum(2 * r.size for r in rows),
            transcendentals=0,
        ),
    )(place, *rows, *keys, *gates)


def expert_kernel(*refs, side, slots, parts, f_chunk, d_chunk):
    sends, weights_hbm = refs[0:3], refs[3:6]
    results, arrivals, outputs = refs[6:9], refs[9:12], refs[12:15]
    weights, bounces = refs[15:18], refs[18:21]
    x_buf, act_buf, y_buf, go_send, go_recv, back_send, back_recv, own_sem, weight_sem, in_sem, out_sem = refs[21:]
    members = side * side * 2
    me = {axis: lax.axis_index(axis) for axis in AXES}

    def member(p, place):
        return (place[PLANE[p][0]] * side + place[PLANE[p][1]]) * 2 + place['c']

    def rows_of(ref, p, chunk, place):
        spot = [pl.ds(0, side) if axis == LINE[p] else place[axis] for axis in ('y', 'x', 'c', 'z')]
        return ref.at[tuple([chunk] + spot)]

    def peer(p, offset):
        first, second = PLANE[p]
        place = dict(me)
        place[first] = lax.rem(me[first] + offset // (2 * side), side)
        place[second] = lax.rem(me[second] + lax.rem(offset // 2, side), side)
        place['c'] = lax.rem(me['c'] + lax.rem(offset, 2), 2)
        return place

    def go(chunk, p, place):
        return pltpu.make_async_remote_copy(
            src_ref=sends[p].at[chunk, pl.ds(0, side), member(p, place)],
            dst_ref=rows_of(arrivals[p], p, chunk, me),
            send_sem=go_send.at[chunk, p],
            recv_sem=go_recv.at[chunk, p],
            device_id=tuple(place[axis] for axis in AXES),
            device_id_type=MESH,
        )

    def back(chunk, p, place):
        return pltpu.make_async_remote_copy(
            src_ref=rows_of(outputs[p], p, chunk, place),
            dst_ref=results[p].at[chunk, pl.ds(0, side), member(p, me)],
            send_sem=back_send.at[chunk, p],
            recv_sem=back_recv.at[chunk, p],
            device_id=tuple(place[axis] for axis in AXES),
            device_id_type=MESH,
        )

    def send_all(copy, chunk):
        def one(offset, carry):
            for p in range(3):
                copy(chunk, p, peer(p, offset)).start()
            return carry

        lax.fori_loop(1, members, one, 0)

    def wait_bytes(ref, sem):
        pltpu.make_async_copy(ref, ref, sem).wait()

    loads = [pltpu.make_async_copy(weights_hbm[i], weights[i], weight_sem.at[i]) for i in range(3)]
    for load in loads:
        load.start()
    for chunk in range(N_CHUNKS):
        send_all(go, chunk)
    for p in range(3):
        for chunk in range(N_CHUNKS):
            pltpu.make_async_copy(sends[p].at[chunk, pl.ds(0, side), member(p, me)], bounces[p].at[chunk], own_sem.at[chunk, p]).start()
    for p in range(3):
        for chunk in range(N_CHUNKS):
            pltpu.make_async_copy(sends[p].at[chunk, pl.ds(0, side), member(p, me)], bounces[p].at[chunk], own_sem.at[chunk, p]).wait()
            pltpu.make_async_copy(bounces[p].at[chunk], rows_of(arrivals[p], p, chunk, me), go_recv.at[chunk, p]).start()
    for load in loads:
        load.wait()

    def fetch(chunk, y, slot):
        return [
            pltpu.make_async_copy(arrivals[p].at[chunk, y], x_buf.at[slot, :, :, :, :, pl.ds(lo, hi - lo)], in_sem.at[slot, p])
            for p, (lo, hi) in enumerate(parts)
        ]

    def flush(chunk, y, slot):
        return [
            pltpu.make_async_copy(y_buf.at[slot, :, :, :, :, pl.ds(lo, hi - lo)], outputs[p].at[chunk, y], out_sem.at[slot, p])
            for p, (lo, hi) in enumerate(parts)
        ]

    width, model = act_buf.shape[1], x_buf.shape[-1]
    group = x_buf.shape[1:-1]
    rows = math.prod(group)
    gate_ref, up_ref, down_ref = weights

    def one_chunk(chunk, carry):
        for p in range(3):
            wait_bytes(arrivals[p].at[chunk], go_recv.at[chunk, p])
        for copy in fetch(chunk, 0, 0):
            copy.start()

        def one_tile(y, carry):
            slot = lax.rem(y, 2)

            @pl.when(y + 1 < side)
            def _():
                for copy in fetch(chunk, y + 1, 1 - slot):
                    copy.start()

            for copy in fetch(chunk, y, slot):
                copy.wait()

            @pl.when(y >= 2)
            def _():
                for copy in flush(chunk, y - 2, slot):
                    copy.wait()

            x = x_buf[slot].reshape(rows, model)
            for lo in range(0, width, f_chunk):
                cols = slice(lo, lo + f_chunk)
                z = jnp.dot(x, gate_ref[:, cols], preferred_element_type=F32)
                u = jnp.dot(x, up_ref[:, cols], preferred_element_type=F32)
                act_buf[:, cols] = (jax.nn.silu(z) * u).astype(BF16)
            act = act_buf[...]
            for lo in range(0, model, d_chunk):
                cols = slice(lo, lo + d_chunk)
                y_rows = jnp.dot(act, down_ref[:, cols], preferred_element_type=F32).astype(BF16)
                y_buf[slot, :, :, :, :, cols] = y_rows.reshape(group + (d_chunk,))
            for copy in flush(chunk, y, slot):
                copy.start()
            return carry

        lax.fori_loop(0, side, one_tile, 0)
        for y in range(max(side - 2, 0), side):
            for copy in flush(chunk, y, y % 2):
                copy.wait()
        send_all(back, chunk)
        for p in range(3):
            pltpu.make_async_copy(rows_of(outputs[p], p, chunk, me), bounces[p].at[chunk], own_sem.at[chunk, p]).start()
        for p in range(3):
            pltpu.make_async_copy(rows_of(outputs[p], p, chunk, me), bounces[p].at[chunk], own_sem.at[chunk, p]).wait()
            pltpu.make_async_copy(bounces[p].at[chunk], results[p].at[chunk, pl.ds(0, side), member(p, me)], back_recv.at[chunk, p]).start()
        return carry

    for chunk in range(N_CHUNKS):
        one_chunk(chunk, 0)
    for chunk in range(N_CHUNKS):
        for p in range(3):
            wait_bytes(results[p].at[chunk], back_recv.at[chunk, p])
            wait_bytes(sends[p].at[chunk, pl.ds(0, side), pl.ds(0, members - 1)], go_send.at[chunk, p])
            wait_bytes(sends[p].at[chunk, pl.ds(0, side), pl.ds(0, members - 1)], back_send.at[chunk, p])


def exchange_experts(sends, gate, up, down, side, capacity):
    slots = capacity // N_CHUNKS
    model, width = gate.shape
    parts = column_parts(model)
    members = side * side * 2
    widths = [hi - lo for lo, hi in parts]
    there = [jax.ShapeDtypeStruct((N_CHUNKS, side, side, 2, side, slots, w), BF16) for w in widths]
    home = [jax.ShapeDtypeStruct((N_CHUNKS, side, members, slots, w), BF16) for w in widths]
    group = (side, 2, side, slots)
    anywhere = pl.BlockSpec(memory_space=pl.ANY)
    total = members * side * capacity
    out = pl.pallas_call(
        functools.partial(
            expert_kernel, side=side, slots=slots, parts=parts, f_chunk=min(256, width), d_chunk=min(512, model)
        ),
        out_shape=home + there + there,
        in_specs=[anywhere] * 6,
        out_specs=[anywhere] * 9,
        scratch_shapes=[
            pltpu.VMEM((model, width), BF16),
            pltpu.VMEM((model, width), BF16),
            pltpu.VMEM((width, model), BF16),
            *[pltpu.VMEM((N_CHUNKS, side, slots, w), BF16) for w in widths],
            pltpu.VMEM((2,) + group + (model,), BF16),
            pltpu.VMEM((math.prod(group), width), BF16),
            pltpu.VMEM((2,) + group + (model,), BF16),
            *[pltpu.SemaphoreType.DMA((N_CHUNKS, 3)) for _ in range(5)],
            pltpu.SemaphoreType.DMA((3,)),
            pltpu.SemaphoreType.DMA((2, 3)),
            pltpu.SemaphoreType.DMA((2, 3)),
        ],
        compiler_params=pltpu.CompilerParams(has_side_effects=True, vmem_limit_bytes=56 * 1024 * 1024),
        cost_estimate=pl.CostEstimate(flops=6 * total * model * width, bytes_accessed=8 * total * model, transcendentals=0),
    )(*[s.reshape(N_CHUNKS, side, members, slots, s.shape[1]) for s in sends], gate, up, down)
    return [r.reshape(-1, r.shape[-1]) for r in out[:3]]


def moe_branch(rows, choice_ids, slots, moe_norm, w_router, exp_gate, exp_up, exp_down, side):
    tokens, model = rows.shape
    top_k = choice_ids.shape[1]
    n_experts = side ** 3 * 2
    capacity = CAP_FACTOR * tokens * top_k // n_experts
    parts = column_parts(model)
    keys = choice_ids * capacity + slots
    normed = rms_norm(rows, moe_norm)
    logits = jnp.dot(normed, w_router, preferred_element_type=F32)
    chosen = choice_ids[:, :, None] == jnp.arange(n_experts, dtype=I32)
    gates = jax.nn.softmax(jnp.sum(jnp.where(chosen, logits[:, None, :], 0.0), axis=-1), axis=-1)
    place = jnp.stack([lax.axis_index(axis) for axis in LINE]).astype(I32)
    keys_t = keys.T
    line_tokens = [lax.all_gather(normed[:, lo:hi], axis) for axis, (lo, hi) in zip(LINE, parts)]
    line_keys_t = [lax.all_gather(keys_t, axis) for axis in LINE]
    line_keys = [k.transpose(0, 2, 1) for k in line_keys_t]
    line_gates = [lax.all_gather(gates, axis) for axis in LINE]
    sends = pick_rows(place, line_tokens, line_keys_t, side, capacity)
    returned = exchange_experts(sends, exp_gate, exp_up, exp_down, side, capacity)
    partial = weigh_rows(place, returned, line_keys, line_gates, side, capacity)
    return jnp.concatenate([lax.psum_scatter(m, axis, scatter_dimension=0) for m, axis in zip(partial, LINE)], axis=-1)


def solution(mesh):
    group_size = mesh.shape['ep']
    side = torus_of(group_size)
    torus = jax.sharding.Mesh(mesh.devices.reshape(side, side, side, 2), AXES)
    row_spec = P(AXES, None, None)
    vec_spec = P(None)
    mat_spec = P(None, None)
    cube_spec = P(None, None, None)
    expert_spec = P(AXES, None, None)

    def per_device(hidden, expert_ids, slot_ids, attn_norm, w_query, w_key, w_value, w_out, ffn_norm, ffn_gate, ffn_up, ffn_down, moe_norm, w_router, exp_gate, exp_up, exp_down):
        n_seqs, seq_len, model = hidden.shape
        assert n_seqs == 1 and exp_gate.shape[0] == 1
        rows = hidden[0]
        moe = moe_branch(rows, expert_ids[0], slot_ids[0], moe_norm, w_router, exp_gate[0], exp_up[0], exp_down[0], side)
        dense = dense_sequence(rows, attn_norm, w_query, w_key, w_value, w_out, ffn_norm, ffn_gate, ffn_up, ffn_down)
        return (dense + moe).astype(BF16).reshape(hidden.shape)

    return jax.shard_map(per_device, mesh=torus, in_specs=(row_spec, row_spec, row_spec, vec_spec, mat_spec, mat_spec, mat_spec, cube_spec, vec_spec, mat_spec, mat_spec, mat_spec, vec_spec, mat_spec, expert_spec, expert_spec, expert_spec), out_specs=row_spec, check_vma=False)
```

```python
import functools
import math
import types

import jax
import jax.numpy as jnp
from jax import lax
from jax.experimental import pallas as pl
from jax.experimental.pallas import tpu as pltpu
from jax.sharding import PartitionSpec as P

RMS_EPS = 1e-6
ROPE_BASE = 10000.0
CAP_FACTOR = 3
N_CHUNKS = 3
RING = 6
TILE = 256
MESH = pl.DeviceIdType.MESH

BF16, F32, I32 = jnp.bfloat16, jnp.float32, jnp.int32

AXES = ('z', 'y', 'x', 'c')
LINE = ('z', 'x', 'y')
PLANE = (('y', 'x'), ('z', 'y'), ('x', 'z'))
ROW_AXES = ('y', 'x', 'c', 'z')


def torus_side(n_devices):
    side = round((n_devices // 2) ** (1 / 3))
    assert side ** 3 * 2 == n_devices
    return side


def column_parts(model):
    lanes = model // 128
    first = -(-lanes // 3)
    second = -(-(lanes - first) // 2)
    ends = (0, first * 128, (first + second) * 128, model)
    return tuple((ends[p], ends[p + 1]) for p in range(3))


def steps(total, size):
    return [(lo, min(size, total - lo)) for lo in range(0, total, size)]


def rms_rows(rows, scale):
    as_float = rows.astype(F32)
    inv_rms = lax.rsqrt(jnp.mean(as_float * as_float, axis=-1, keepdims=True) + RMS_EPS)
    return (as_float * inv_rms * scale.astype(F32)).astype(BF16)


def dot(a, b):
    return jnp.dot(a, b, preferred_element_type=F32)


def kernel(*refs, names, side, parts, capacity, head_dim, f_chunk, d_chunk):
    r = types.SimpleNamespace(**dict(zip(names, refs)))
    each = lambda name: [getattr(r, name + str(p)) for p in range(3)]
    slots = capacity // N_CHUNKS
    members = side * side * 2
    mates = side * 2
    rows_block = members * slots
    tokens, model = r.hidden.shape
    me = {axis: lax.axis_index(axis) for axis in AXES}


    def member(p, place):
        return (place[PLANE[p][0]] * side + place[PLANE[p][1]]) * 2 + place['c']

    def rows_of(ref, p, chunk, place):
        spot = [pl.ds(0, side) if axis == LINE[p] else place[axis] for axis in ROW_AXES]
        return ref.at[tuple([chunk] + spot)]

    def gathered_rows_of(ref, p, chunk, place):
        free = (LINE[p], PLANE[p][0])
        spot = [pl.ds(0, side) if axis in free else place[axis] for axis in ROW_AXES]
        return ref.at[tuple([chunk] + spot)]

    def source_index(p, i, d):
        where = {PLANE[p][0]: i, LINE[p]: d}
        return tuple(where[axis] for axis in ROW_AXES if axis in where)

    def device(place):
        return tuple(place[axis] for axis in AXES)

    def plane_peer(p, offset):
        first, second = PLANE[p]
        place = dict(me)
        place[first] = lax.rem(me[first] + offset // (2 * side), side)
        place[second] = lax.rem(me[second] + lax.rem(offset // 2, side), side)
        place['c'] = lax.rem(me['c'] + lax.rem(offset, 2), 2)
        return place

    def axis_peer(axis, offset):
        return {**me, axis: lax.rem(me[axis] + offset, side)}

    def line_peer(p, offset):
        return axis_peer(LINE[p], offset)

    def remote(src, dst, send_sem, recv_sem, place):
        return pltpu.make_async_remote_copy(
            src_ref=src, dst_ref=dst, send_sem=send_sem, recv_sem=recv_sem, device_id=device(place), device_id_type=MESH
        )

    def wait_bytes(ref, sem):
        pltpu.make_async_copy(ref, ref, sem).wait()

    def expert_key(place, core, slot):
        return (((place['z'] * side + place['y']) * side + place['x']) * 2 + core) * capacity + slot

    def plane_keys(p, shape, chunk):
        row = lax.broadcasted_iota(I32, shape, 1)
        which, slot = row // slots, lax.rem(row, slots)
        pair = which // 2
        place = {PLANE[p][0]: pair // side, PLANE[p][1]: lax.rem(pair, side), LINE[p]: me[LINE[p]]}
        return expert_key(place, lax.rem(which, 2), slot + chunk * slots)

    def mate_keys(p, shape):
        row = lax.broadcasted_iota(I32, shape, 0)
        block, slot = row // slots, lax.rem(row, slots)
        chunk, mate = block // mates, lax.rem(block, mates)
        place = {**me, PLANE[p][1]: mate // 2}
        return expert_key(place, lax.rem(mate, 2), slot + chunk * slots)

    tok, far, sends, arrivals, outputs = each('tok'), each('far'), each('send'), each('arrive'), each('output')
    results, sums, others, bounce = each('result'), each('sum'), each('other'), each('bounce')
    widths = [hi - lo for lo, hi in parts]


    band = min(32, tokens)

    def bands(body):
        lax.fori_loop(0, tokens // band, lambda i, c: (body(pl.ds(pl.multiple_of(i * band, band), band)), c)[1], 0)

    def norm_both(here):
        normed = rms_rows(r.hidden[here, :], r.moe_norm[...])
        for p, (lo, hi) in enumerate(parts):
            tok[p][me[LINE[p]], here, :] = normed[:, lo:hi]
        r.rows[here, :] = rms_rows(r.hidden[here, :], r.attn_norm[...])

    bands(norm_both)
    for p in range(3):
        r.all_keys[p, me[PLANE[p][0]], me[LINE[p]]] = r.keys_t[...]
    pairs = ((r.gate_hbm, r.gate), (r.up_hbm, r.up), (r.down_hbm, r.down))
    loads = [pltpu.make_async_copy(src, dst, r.weight_sem.at[i]) for i, (src, dst) in enumerate(pairs)]
    for load in loads:
        load.start()
    for offset in range(1, side):
        for p in range(3):
            spot, place = me[LINE[p]], line_peer(p, offset)
            remote(tok[p].at[spot], tok[p].at[spot], r.tok_send.at[p], r.tok_recv.at[p], place).start()
            remote(
                r.keys_t, r.all_keys.at[p, me[PLANE[p][0]], spot], r.key_send.at[p], r.key_recv.at[p], place
            ).start()


    ring = r.ring
    ring_sem = r.ring_sem

    def stream(n_steps, group, source, body):
        ahead = RING // group * group - group

        def copy(i, s):
            slot = lax.rem(i * group + s, RING // group * group)
            return pltpu.make_async_copy(source(i, s), ring.at[slot], ring_sem.at[slot])

        for i in range(min(ahead // group, n_steps)):
            for s in range(group):
                copy(i, s).start()

        def step(i, carry):
            @pl.when(i + ahead // group < n_steps)
            def _():
                for s in range(group):
                    copy(i + ahead // group, s).start()

            for s in range(group):
                copy(i, s).wait()
            body(i, [ring.at[lax.rem(i * group + s, RING // group * group)] for s in range(group)])
            return carry

        lax.fori_loop(0, n_steps, step, 0)

    def col_tile(i):
        return pl.ds(pl.multiple_of(i * TILE, TILE), TILE)

    def turned(y):
        return y * r.cos[...] + pltpu.roll(y, head_dim // 2, 1) * r.sin[...]

    def project(weight, out, rotary):
        def body(i, tiles):
            y = dot(r.rows[...], tiles[0][...])
            if rotary:
                y = jnp.concatenate([turned(y[:, lo : lo + head_dim]) for lo in range(0, TILE, head_dim)], axis=1)
            out[:, col_tile(i)] = y.astype(BF16)

        stream(weight.shape[1] // TILE, 1, lambda i, s: weight.at[:, col_tile(i)], body)

    project(r.w_query, r.query, True)
    project(r.w_key, r.key, True)
    project(r.w_value, r.value, False)


    logits = sum(dot(tok[p][me[LINE[p]]], r.w_router[lo:hi, :]) for p, (lo, hi) in enumerate(parts))
    lane = lax.broadcasted_iota(I32, logits.shape, 1)
    top_k = r.ids.shape[1]
    ids = r.ids[...]
    picked = [jnp.sum(jnp.where(lane == ids[:, j : j + 1], logits, 0.0), axis=1, keepdims=True) for j in range(top_k)]
    peak = functools.reduce(jnp.maximum, picked)
    powers = [jnp.exp(v - peak) for v in picked]
    norm = functools.reduce(jnp.add, powers)
    mine = r.keys_f[...]
    lane = lax.broadcasted_iota(I32, mine.shape, 1)
    for j in range(top_k):
        mine = jnp.where(lane == top_k + j, powers[j] / norm, mine)
    r.my_gates[...] = mine
    for p in range(3):
        r.line_gates[p, me[LINE[p]]] = mine


    for p in range(3):
        wait_bytes(r.all_keys.at[p, 0, pl.ds(0, side - 1)], r.key_recv.at[p])
        wait_bytes(tok[p].at[pl.ds(0, side - 1)], r.tok_recv.at[p])
    for offset in range(1, side):
        for p in range(3):
            spot, place = me[PLANE[p][0]], axis_peer(PLANE[p][0], offset)
            remote(
                r.all_keys.at[p, spot], r.all_keys.at[p, spot], r.far_key_send.at[p], r.far_key_recv.at[p], place
            ).start()
            remote(tok[p], far[p].at[spot], r.far_send.at[p], r.far_recv.at[p], place).start()
    for offset in range(1, side):
        for p in range(3):
            spot = me[LINE[p]]
            remote(
                r.my_gates, r.line_gates.at[p, spot], r.gate_send.at[p], r.gate_recv.at[p], line_peer(p, offset)
            ).start()


    n_heads = r.query.shape[1] // head_dim
    per_key = r.query.shape[1] // r.key.shape[1]
    causal = lax.broadcasted_iota(I32, (tokens, tokens), 0) >= lax.broadcasted_iota(I32, (tokens, tokens), 1)

    def one_head(h, carry):
        cols = pl.ds(pl.multiple_of(h * head_dim, head_dim), head_dim)
        key_cols = pl.ds(pl.multiple_of(h // per_key * head_dim, head_dim), head_dim)
        scores = lax.dot_general(
            r.query[:, cols], r.key[:, key_cols], (((1,), (1,)), ((), ())), preferred_element_type=F32
        )
        scores = jnp.where(causal, scores * head_dim ** -0.5, -jnp.inf)
        power = jnp.exp(scores - jnp.max(scores, axis=1, keepdims=True))
        prob = (power / jnp.sum(power, axis=1, keepdims=True)).astype(BF16)
        r.query[:, cols] = dot(prob, r.value[:, key_cols]).astype(BF16)
        return carry

    lax.fori_loop(0, n_heads, one_head, 0)


    stage = r.stage
    blocks = N_CHUNKS * mates
    my_mate = {p: me[PLANE[p][1]] * 2 + me['c'] for p in range(3)}

    def pick_rows(p, i, d, slot, source):
        wanted = mate_keys(p, (blocks * slots, tokens))
        keys = r.all_keys[p, i, d]
        hit = wanted == keys[0:1, :]
        for j in range(1, top_k):
            hit = jnp.logical_or(hit, wanted == keys[j : j + 1, :])
        pick = jnp.where(hit, 1.0, 0.0).astype(BF16)
        for lo, n in steps(widths[p], TILE):
            found = dot(pick, source[:, lo : lo + n]).astype(BF16)
            stage[slot, 0:blocks, :, lo : lo + n] = found.reshape(blocks, slots, n)

    def flush(p, i, d, slot):
        a, b = source_index(p, i, d)
        return pltpu.make_async_copy(
            stage.at[slot, pl.ds(0, blocks), :, pl.ds(0, widths[p])],
            sends[p].at[pl.ds(0, blocks), a, b],
            r.stage_sem.at[slot],
        )

    def keep(p, i, d, slot, chunk):
        spot = {**me, PLANE[p][0]: i, LINE[p]: d}
        return pltpu.make_async_copy(
            stage.at[slot, chunk * mates + my_mate[p], :, pl.ds(0, widths[p])],
            arrivals[p].at[tuple([chunk] + [spot[axis] for axis in ROW_AXES])],
            r.keep_sem.at[slot, chunk],
        )

    for p in range(3):
        sources = side * side
        near = me[PLANE[p][0]]
        wait_bytes(r.all_keys.at[p, pl.ds(0, side - 1)], r.far_key_recv.at[p])
        wait_bytes(far[p].at[pl.ds(0, side - 1)], r.far_recv.at[p])

        def place_of(n):
            return lax.rem(near + n // side, side), lax.rem(n, side)

        def load(n, slot):
            i, d = place_of(n)
            return pltpu.make_async_copy(far[p].at[i, d], r.source.at[slot, :, pl.ds(0, widths[p])], r.source_sem.at[slot])

        def one_source(n, c):
            slot = lax.rem(n, 2)
            i, d = place_of(n)

            @pl.when(jnp.logical_and(n + 1 >= side, n + 1 < sources))
            def _():
                load(n + 1, 1 - slot).start()

            @pl.when(n >= side)
            def _():
                load(n, slot).wait()

            @pl.when(n < side)
            def _():
                r.source[slot, :, 0 : widths[p]] = tok[p][d]

            @pl.when(n >= 2)
            def _():
                i2, d2 = place_of(n - 2)
                flush(p, i2, d2, slot).wait()
                for chunk in range(N_CHUNKS):
                    keep(p, i2, d2, slot, chunk).wait()

            pick_rows(p, i, d, slot, r.source.at[slot])
            flush(p, i, d, slot).start()
            for chunk in range(N_CHUNKS):
                keep(p, i, d, slot, chunk).start()
            return c

        lax.fori_loop(0, sources, one_source, 0)
        for n in range(sources - 2, sources):
            i, d = place_of(n)
            flush(p, i, d, n % 2).wait()
            for chunk in range(N_CHUNKS):
                keep(p, i, d, n % 2, chunk).wait()

        def go_chunk(chunk, c):
            def one_mate(offset, c2):
                axis = PLANE[p][1]
                place = {
                    **me,
                    axis: lax.rem(me[axis] + offset // 2, side),
                    'c': lax.rem(me['c'] + lax.rem(offset, 2), 2),
                }
                remote(
                    sends[p].at[chunk * mates + place[axis] * 2 + place['c']],
                    gathered_rows_of(arrivals[p], p, chunk, me),
                    r.go_send.at[chunk, p],
                    r.go_recv.at[chunk, p],
                    place,
                ).start()
                return c2

            return lax.fori_loop(1, mates, one_mate, c)

        lax.fori_loop(0, N_CHUNKS, go_chunk, 0)


    out_split = n_heads * head_dim // model

    def out_body(i, tiles):
        total = r.hidden[:, col_tile(i)].astype(F32)
        attended = dot(r.query[:, 0:model], tiles[0][...])
        for s in range(1, out_split):
            attended += dot(r.query[:, s * model : (s + 1) * model], tiles[s][...])
        r.attended[:, col_tile(i)] = (total + attended).astype(BF16)

    stream(model // TILE, out_split, lambda i, s: r.w_out.at[pl.ds(s * model, model), col_tile(i)], out_body)

    def norm_attended(here):
        r.rows[here, :] = rms_rows(r.attended[here, :], r.ffn_norm[...])

    bands(norm_attended)

    def act_body(i, tiles):
        z = dot(r.rows[...], tiles[0][...])
        u = dot(r.rows[...], tiles[1][...])
        r.act[:, col_tile(i)] = (jax.nn.silu(z) * u).astype(BF16)

    ff_dim = r.ffn_gate.shape[1]
    stream(
        ff_dim // TILE, 2, lambda i, s: (r.ffn_gate, r.ffn_up)[s].at[:, col_tile(i)], act_body
    )
    down_split = ff_dim // model

    def down_body(i, tiles):
        total = dot(r.act[:, 0:model], tiles[0][...])
        for s in range(1, down_split):
            total += dot(r.act[:, s * model : (s + 1) * model], tiles[s][...])
        r.dense[:, col_tile(i)] = r.attended[:, col_tile(i)].astype(F32) + total

    stream(model // TILE, down_split, lambda i, s: r.ffn_down.at[pl.ds(s * model, model), col_tile(i)], down_body)


    for load in loads:
        load.wait()
    x_buf, y_buf, hidden_buf = r.x_buf, r.y_buf, r.hidden_buf
    group = x_buf.shape[1:-1]
    rows = math.prod(group)
    width = hidden_buf.shape[1]

    def fetch(chunk, y, slot):
        return [
            pltpu.make_async_copy(
                arrivals[p].at[chunk, y], x_buf.at[slot, :, :, :, :, pl.ds(lo, hi - lo)], r.in_sem.at[slot, p]
            )
            for p, (lo, hi) in enumerate(parts)
        ]

    def put(chunk, y, slot):
        return [
            pltpu.make_async_copy(
                y_buf.at[slot, :, :, :, :, pl.ds(lo, hi - lo)], outputs[p].at[chunk, y], r.out_sem.at[slot, p]
            )
            for p, (lo, hi) in enumerate(parts)
        ]

    def expert_chunk(chunk, carry):
        for p in range(3):
            wait_bytes(sends[p].at[pl.ds(0, mates - 1)], r.go_recv.at[chunk, p])
        for copy in fetch(chunk, 0, 0):
            copy.start()

        def one_tile(y, c):
            slot = lax.rem(y, 2)

            @pl.when(y + 1 < side)
            def _():
                for copy in fetch(chunk, y + 1, 1 - slot):
                    copy.start()

            for copy in fetch(chunk, y, slot):
                copy.wait()

            @pl.when(y >= 2)
            def _():
                for copy in put(chunk, y - 2, slot):
                    copy.wait()

            for lo in range(0, width, f_chunk):
                cols = slice(lo, lo + f_chunk)
                z = dot(x_buf[slot].reshape(rows, model), r.gate[:, cols])
                u = dot(x_buf[slot].reshape(rows, model), r.up[:, cols])
                hidden_buf[:, cols] = (jax.nn.silu(z) * u).astype(BF16)
            for lo in range(0, model, d_chunk):
                cols = slice(lo, lo + d_chunk)
                y_rows = dot(hidden_buf[...], r.down[:, cols]).astype(BF16)
                y_buf[slot, :, :, :, :, cols] = y_rows.reshape(group + (d_chunk,))
            for copy in put(chunk, y, slot):
                copy.start()
            return c

        lax.fori_loop(0, side, one_tile, 0)
        for y in range(max(side - 2, 0), side):
            for copy in put(chunk, y, y % 2):
                copy.wait()

        def one_peer(offset, c):
            for p in range(3):
                place = plane_peer(p, offset)
                remote(
                    rows_of(outputs[p], p, chunk, place),
                    results[p].at[chunk, pl.ds(0, side), member(p, me)],
                    r.back_send.at[chunk, p],
                    r.back_recv.at[chunk, p],
                    place,
                ).start()
            return c

        lax.fori_loop(1, members, one_peer, 0)
        own = [
            pltpu.make_async_copy(rows_of(outputs[p], p, chunk, me), bounce[p].at[chunk], r.own_sem.at[p])
            for p in range(3)
        ]
        for copy in own:
            copy.start()
        for p, copy in enumerate(own):
            copy.wait()
            pltpu.make_async_copy(
                bounce[p].at[chunk], results[p].at[chunk, pl.ds(0, side), member(p, me)], r.back_recv.at[chunk, p]
            ).start()
        return carry

    lax.fori_loop(0, N_CHUNKS, expert_chunk, 0)


    for p in range(3):
        wait_bytes(r.line_gates.at[p, pl.ds(0, side - 1)], r.gate_recv.at[p])
    split = r.split
    lanes = min(128, rows_block)

    def weigh_chunk(chunk, carry):
        for p in range(3):
            wait_bytes(results[p].at[chunk], r.back_recv.at[chunk, p])

        for p in range(3):

            def load(d, slot):
                return pltpu.make_async_copy(
                    results[p].at[chunk, d],
                    stage.at[slot, pl.ds(0, members), :, pl.ds(0, widths[p])],
                    r.stage_sem.at[slot],
                )

            load(0, 0).start()

            def one_source(d, c):
                slot = lax.rem(d, 2)

                @pl.when(d + 1 < side)
                def _():
                    load(d + 1, 1 - slot).start()

                info = r.line_gates[p, d]
                keys = [jnp.broadcast_to(info[:, j : j + 1], (tokens, lanes)) for j in range(top_k)]
                gates = [jnp.broadcast_to(info[:, top_k + j : top_k + j + 1], (tokens, lanes)) for j in range(top_k)]
                held = plane_keys(p, (tokens, rows_block), chunk)
                for lo in range(0, rows_block, lanes):
                    here = held[:, lo : lo + lanes].astype(F32)
                    weight = jnp.zeros((tokens, lanes), F32)
                    for j in range(top_k):
                        weight = jnp.where(here == keys[j], gates[j], weight)
                    high = weight.astype(BF16)
                    rest = weight - high.astype(F32)
                    middle = rest.astype(BF16)
                    low = (rest - middle.astype(F32)).astype(BF16)
                    split[0:tokens, lo : lo + lanes] = high
                    split[tokens : 2 * tokens, lo : lo + lanes] = middle
                    split[2 * tokens : 3 * tokens, lo : lo + lanes] = low
                load(d, slot).wait()
                for lo, n in steps(widths[p], TILE):
                    y = stage[slot, 0:members, :, lo : lo + n].reshape(rows_block, n)
                    both = dot(split[...], y)
                    total = both[0:tokens] + (both[tokens : 2 * tokens] + both[2 * tokens : 3 * tokens])

                    @pl.when(chunk == 0)
                    def _():
                        sums[p][d, :, lo : lo + n] = total

                    @pl.when(chunk > 0)
                    def _():
                        sums[p][d, :, lo : lo + n] += total

                return c

            lax.fori_loop(0, side, one_source, 0)

            @pl.when(chunk == N_CHUNKS - 1)
            def _():
                for offset in range(1, side):
                    place = line_peer(p, offset)
                    remote(
                        sums[p].at[place[LINE[p]]],
                        others[p].at[offset - 1],
                        r.sum_send.at[p],
                        r.sum_recv.at[p],
                        place,
                    ).start()

        return carry

    lax.fori_loop(0, N_CHUNKS, weigh_chunk, 0)
    for p, (lo, hi) in enumerate(parts):
        wait_bytes(others[p], r.sum_recv.at[p])

        def finish(here):
            moe = sums[p][me[LINE[p]], here, :]
            for offset in range(1, side):
                moe += others[p][offset - 1, here, :]
            r.out[here, lo:hi] = (r.dense[here, lo:hi] + moe).astype(BF16)

        bands(finish)


    for p in range(3):
        wait_bytes(tok[p].at[pl.ds(0, side - 1)], r.tok_send.at[p])
        wait_bytes(r.all_keys.at[p, 0, pl.ds(0, side - 1)], r.key_send.at[p])
        wait_bytes(far[p].at[pl.ds(0, side - 1)], r.far_send.at[p])
        wait_bytes(r.all_keys.at[p, pl.ds(0, side - 1)], r.far_key_send.at[p])
        wait_bytes(r.line_gates.at[p, pl.ds(0, side - 1)], r.gate_send.at[p])
        wait_bytes(others[p], r.sum_send.at[p])
        for chunk in range(N_CHUNKS):
            wait_bytes(sends[p].at[pl.ds(0, mates - 1)], r.go_send.at[chunk, p])
            wait_bytes(results[p].at[chunk, pl.ds(0, side), pl.ds(0, members - 1)], r.back_send.at[chunk, p])


def layer_pair(small, large, side, capacity, head_dim):
    tokens, model = small['hidden'].shape
    top_k, width = small['ids'].shape[1], large['gate_hbm'].shape[1]
    key_dim, ff_dim = large['w_key'].shape[1], large['ffn_gate'].shape[1]
    parts = column_parts(model)
    widths = [hi - lo for lo, hi in parts]
    slots, members, mates = capacity // N_CHUNKS, side * side * 2, side * 2
    group = (side, 2, side, slots)
    rows = math.prod(group)
    sds, vmem = jax.ShapeDtypeStruct, pltpu.VMEM
    dma = lambda *shape: pltpu.SemaphoreType.DMA(shape)
    outs = dict(out=sds((tokens, model), BF16))
    scratch = dict(
        rows=vmem((tokens, model), BF16),
        query=vmem((tokens, large['w_query'].shape[1]), BF16),
        key=vmem((tokens, key_dim), BF16),
        value=vmem((tokens, key_dim), BF16),
        attended=vmem((tokens, model), BF16),
        act=vmem((tokens, ff_dim), BF16),
        dense=vmem((tokens, model), F32),
        ring=vmem((RING, model, TILE), BF16),
        all_keys=vmem((3, side, side, top_k, tokens), I32),
        my_gates=vmem((tokens, 128), F32),
        line_gates=vmem((3, side, tokens, 128), F32),
        source=vmem((2, tokens, max(widths)), BF16),
        stage=vmem((2, max(members, N_CHUNKS * mates), slots, max(widths)), BF16),
        split=vmem((3 * tokens, members * slots), BF16),
        gate=vmem((model, width), BF16),
        up=vmem((model, width), BF16),
        down=vmem((width, model), BF16),
        x_buf=vmem((2,) + group + (model,), BF16),
        y_buf=vmem((2,) + group + (model,), BF16),
        hidden_buf=vmem((rows, width), BF16),
        weight_sem=dma(3),
        ring_sem=dma(RING),
        source_sem=dma(2),
        stage_sem=dma(2),
        keep_sem=dma(2, N_CHUNKS),
        in_sem=dma(2, 3),
        out_sem=dma(2, 3),
        own_sem=dma(3),
        tok_send=dma(3),
        tok_recv=dma(3),
        key_send=dma(3),
        key_recv=dma(3),
        far_send=dma(3),
        far_recv=dma(3),
        far_key_send=dma(3),
        far_key_recv=dma(3),
        gate_send=dma(3),
        gate_recv=dma(3),
        sum_send=dma(3),
        sum_recv=dma(3),
        go_send=dma(N_CHUNKS, 3),
        go_recv=dma(N_CHUNKS, 3),
        back_send=dma(N_CHUNKS, 3),
        back_recv=dma(N_CHUNKS, 3),
    )
    for p, w in enumerate(widths):
        there = sds((N_CHUNKS, side, side, 2, side, slots, w), BF16)
        outs['far' + str(p)] = sds((side, side, tokens, w), BF16)
        outs['send' + str(p)] = sds((N_CHUNKS * mates, side, side, slots, w), BF16)
        outs['arrive' + str(p)] = there
        outs['output' + str(p)] = there
        outs['result' + str(p)] = sds((N_CHUNKS, side, members, slots, w), BF16)
        scratch['tok' + str(p)] = vmem((side, tokens, w), BF16)
        scratch['bounce' + str(p)] = vmem((N_CHUNKS, side, slots, w), BF16)
        scratch['sum' + str(p)] = vmem((side, tokens, w), F32)
        scratch['other' + str(p)] = vmem((side - 1, tokens, w), F32)
    anywhere = pl.BlockSpec(memory_space=pl.ANY)
    local = pl.BlockSpec(memory_space=pltpu.VMEM)
    n_rows = members * side * capacity
    return pl.pallas_call(
        functools.partial(
            kernel,
            names=tuple(small) + tuple(large) + tuple(outs) + tuple(scratch),
            side=side,
            parts=parts,
            capacity=capacity,
            head_dim=head_dim,
            f_chunk=min(256, width),
            d_chunk=min(512, model),
        ),
        out_shape=list(outs.values()),
        in_specs=[local] * len(small) + [anywhere] * len(large),
        out_specs=[local] + [anywhere] * (len(outs) - 1),
        scratch_shapes=list(scratch.values()),
        compiler_params=pltpu.CompilerParams(has_side_effects=True, vmem_limit_bytes=67043328),
        cost_estimate=pl.CostEstimate(flops=6 * n_rows * model * width, bytes_accessed=8 * n_rows * model, transcendentals=0),
    )(*small.values(), *large.values())[0]


def solution(mesh):
    group_size = mesh.shape['ep']
    side = torus_side(group_size)
    torus = jax.sharding.Mesh(mesh.devices.reshape(side, side, side, 2), AXES)
    row_spec = P(AXES, None, None)
    vec_spec = P(None)
    mat_spec = P(None, None)
    cube_spec = P(None, None, None)
    expert_spec = P(AXES, None, None)

    def per_device(hidden, expert_ids, slot_ids, attn_norm, w_query, w_key, w_value, w_out, ffn_norm, ffn_gate, ffn_up, ffn_down, moe_norm, w_router, exp_gate, exp_up, exp_down):
        n_seqs, tokens, model = hidden.shape
        assert n_seqs == 1 and exp_gate.shape[0] == 1
        n_heads, head_dim = w_out.shape[0], w_out.shape[1]
        ids = expert_ids[0]
        capacity = CAP_FACTOR * tokens * ids.shape[1] // group_size
        keys = ids * capacity + slot_ids[0]
        inv_freq = ROPE_BASE ** (-2.0 * jnp.arange(head_dim // 2, dtype=F32) / head_dim)
        angles = jnp.arange(tokens, dtype=F32)[:, None] * inv_freq[None, :]
        cos, sin = jnp.cos(angles), jnp.sin(angles)
        small = dict(
            hidden=hidden[0],
            attn_norm=attn_norm.reshape(1, model),
            moe_norm=moe_norm.reshape(1, model),
            ffn_norm=ffn_norm.reshape(1, model),
            keys_t=keys.T,
            keys_f=jnp.pad(keys.astype(F32), ((0, 0), (0, 128 - keys.shape[1]))),
            ids=ids,
            w_router=w_router,
            cos=jnp.concatenate([cos, cos], axis=1),
            sin=jnp.concatenate([-sin, sin], axis=1),
        )
        large = dict(
            w_query=w_query,
            w_key=w_key,
            w_value=w_value,
            w_out=w_out.reshape(n_heads * head_dim, model),
            ffn_gate=ffn_gate,
            ffn_up=ffn_up,
            ffn_down=ffn_down,
            gate_hbm=exp_gate[0],
            up_hbm=exp_up[0],
            down_hbm=exp_down[0],
        )
        return layer_pair(small, large, side, capacity, head_dim).reshape(hidden.shape)

    return jax.shard_map(per_device, mesh=torus, in_specs=(row_spec, row_spec, row_spec, vec_spec, mat_spec, mat_spec, mat_spec, cube_spec, vec_spec, mat_spec, mat_spec, mat_spec, vec_spec, mat_spec, expert_spec, expert_spec, expert_spec), out_specs=row_spec, check_vma=False)
```

```python
import functools
import math
import types

import jax
import jax.numpy as jnp
import numpy as np
from jax import lax
from jax.experimental import pallas as pl
from jax.experimental.pallas import tpu as pltpu
from jax.sharding import PartitionSpec as P

RMS_EPS = 1e-6
ROPE_BASE = 10000.0
CAP_FACTOR = 3
N_CHUNKS = 3
RING = 6
TILE = 256
MESH = pl.DeviceIdType.MESH

BF16, F32, I32 = jnp.bfloat16, jnp.float32, jnp.int32

AXES = ('z', 'y', 'x', 'c')
LINE = ('z', 'x', 'y')
PLANE = (('y', 'x'), ('z', 'y'), ('x', 'z'))
ROW_AXES = ('y', 'x', 'c', 'z')


def torus_side(n_devices):
    side = round((n_devices // 2) ** (1 / 3))
    assert side ** 3 * 2 == n_devices
    return side


def column_parts(model):
    lanes = model // 128
    first = -(-lanes // 3)
    second = -(-(lanes - first) // 2)
    ends = (0, first * 128, (first + second) * 128, model)
    return tuple((ends[p], ends[p + 1]) for p in range(3))


def steps(total, size):
    return [(lo, min(size, total - lo)) for lo in range(0, total, size)]


def rms_rows(rows, scale):
    as_float = rows.astype(F32)
    inv_rms = lax.rsqrt(jnp.mean(as_float * as_float, axis=-1, keepdims=True) + RMS_EPS)
    return (as_float * inv_rms * scale.astype(F32)).astype(BF16)


def dot(a, b):
    return jnp.dot(a, b, preferred_element_type=F32)


def kernel(*refs, names, side, parts, capacity, head_dim, f_chunk, d_chunk):
    r = types.SimpleNamespace(**dict(zip(names, refs)))
    each = lambda name: [getattr(r, name + str(p)) for p in range(3)]
    slots = capacity // N_CHUNKS
    members = side * side * 2
    mates = side * 2
    rows_block = members * slots
    tokens, model = r.hidden.shape
    me = {axis: lax.axis_index(axis) for axis in AXES}


    def gathered_rows_of(ref, p, chunk, place):
        free = (LINE[p], PLANE[p][0])
        spot = [pl.ds(0, side) if axis in free else place[axis] for axis in ROW_AXES]
        return ref.at[tuple([chunk] + spot)]

    def source_index(p, i, d):
        where = {PLANE[p][0]: i, LINE[p]: d}
        return tuple(where[axis] for axis in ROW_AXES if axis in where)

    def device(place):
        return tuple(place[axis] for axis in AXES)

    def axis_peer(axis, offset):
        return {**me, axis: lax.rem(me[axis] + offset, side)}

    def line_peer(p, offset):
        return axis_peer(LINE[p], offset)

    def mate_peer(p, offset):
        axis = PLANE[p][1]
        return {
            **me,
            axis: lax.rem(me[axis] + offset // 2, side),
            'c': lax.rem(me['c'] + lax.rem(offset, 2), 2),
        }

    def remote(src, dst, send_sem, recv_sem, place):
        return pltpu.make_async_remote_copy(
            src_ref=src, dst_ref=dst, send_sem=send_sem, recv_sem=recv_sem, device_id=device(place), device_id_type=MESH
        )

    def wait_bytes(ref, sem):
        pltpu.make_async_copy(ref, ref, sem).wait()

    def expert_key(place, core, slot):
        return (((place['z'] * side + place['y']) * side + place['x']) * 2 + core) * capacity + slot

    def plane_keys(p, shape, chunk):
        row = lax.broadcasted_iota(I32, shape, 1)
        which, slot = row // slots, lax.rem(row, slots)
        pair = which // 2
        place = {PLANE[p][0]: pair // side, PLANE[p][1]: lax.rem(pair, side), LINE[p]: me[LINE[p]]}
        return expert_key(place, lax.rem(which, 2), slot + chunk * slots)

    def mate_keys(p, shape):
        row = lax.broadcasted_iota(I32, shape, 0)
        block, slot = row // slots, lax.rem(row, slots)
        chunk, mate = block // mates, lax.rem(block, mates)
        place = {**me, PLANE[p][1]: mate // 2}
        return expert_key(place, lax.rem(mate, 2), slot + chunk * slots)

    tok, far, sends, arrivals, outputs = each('tok'), each('far'), each('send'), each('arrive'), each('output')
    middles, results, sums, others = each('middle'), each('result'), each('sum'), each('other')
    widths = [hi - lo for lo, hi in parts]


    band = min(32, tokens)

    def bands(body):
        lax.fori_loop(0, tokens // band, lambda i, c: (body(pl.ds(pl.multiple_of(i * band, band), band)), c)[1], 0)

    def one_row(scale):
        lines = scale[...].astype(F32)
        return jnp.concatenate([lines[i : i + 1, :] for i in range(lines.shape[0])], axis=1)

    def norm_both(here):
        normed = rms_rows(r.hidden[here, :], one_row(r.moe_scale))
        for p, (lo, hi) in enumerate(parts):
            tok[p][me[LINE[p]], here, :] = normed[:, lo:hi]
        r.rows[here, :] = rms_rows(r.hidden[here, :], one_row(r.attn_scale))

    bands(norm_both)
    keys_t = r.ids_t[...] * capacity + r.slots_t[...]
    for p in range(3):
        r.all_keys[p, me[PLANE[p][0]], me[LINE[p]]] = keys_t
    pairs = ((r.gate_hbm, r.gate), (r.up_hbm, r.up), (r.down_hbm, r.down))
    loads = [pltpu.make_async_copy(src, dst, r.weight_sem.at[i]) for i, (src, dst) in enumerate(pairs)]
    for load in loads:
        load.start()

    def send_far(p, d):
        for offset in range(1, side):
            here = me[PLANE[p][0]]
            remote(
                tok[p].at[d], far[p].at[here, d], r.far_send.at[p], r.far_recv.at[p], axis_peer(PLANE[p][0], offset)
            ).start()

    for offset in range(1, side):
        for p in range(3):
            spot, place = me[LINE[p]], line_peer(p, offset)
            remote(
                tok[p].at[spot], tok[p].at[spot], r.tok_send.at[p, offset - 1], r.tok_recv.at[p, offset - 1], place
            ).start()
            keys = r.all_keys.at[p, me[PLANE[p][0]], spot]
            remote(keys, keys, r.key_send.at[p], r.key_recv.at[p], place).start()
    for p in range(3):
        send_far(p, me[LINE[p]])


    ring = r.ring
    ring_sem = r.ring_sem

    def stream(n_steps, group, source, body):
        ahead = RING // group * group - group

        def copy(i, s):
            slot = lax.rem(i * group + s, RING // group * group)
            return pltpu.make_async_copy(source(i, s), ring.at[slot], ring_sem.at[slot])

        for i in range(min(ahead // group, n_steps)):
            for s in range(group):
                copy(i, s).start()

        def step(i, carry):
            @pl.when(i + ahead // group < n_steps)
            def _():
                for s in range(group):
                    copy(i + ahead // group, s).start()

            for s in range(group):
                copy(i, s).wait()
            body(i, [ring.at[lax.rem(i * group + s, RING // group * group)] for s in range(group)])
            return carry

        lax.fori_loop(0, n_steps, step, 0)

    def col_tile(i):
        return pl.ds(pl.multiple_of(i * TILE, TILE), TILE)

    def turned(y):
        return y * r.cos[...] + pltpu.roll(y, head_dim // 2, 1) * r.sin[...]

    def project(weight, out, rotary):
        def body(i, tiles):
            y = dot(r.rows[...], tiles[0][...])
            if rotary:
                y = jnp.concatenate([turned(y[:, lo : lo + head_dim]) for lo in range(0, TILE, head_dim)], axis=1)
            out[:, col_tile(i)] = y.astype(BF16)

        stream(weight.shape[1] // TILE, 1, lambda i, s: weight.at[:, col_tile(i)], body)

    project(r.w_query, r.query, True)
    project(r.w_key, r.key, True)
    project(r.w_value, r.value, False)


    logits = sum(dot(tok[p][me[LINE[p]]], r.w_router[lo:hi, :]) for p, (lo, hi) in enumerate(parts))
    top_k = r.ids_t.shape[0]
    gap = jnp.zeros((128 - 3 * top_k, tokens), F32)
    blank = jnp.zeros((top_k, tokens), F32)
    info = jnp.concatenate([keys_t.astype(F32), blank, r.ids_t[...].astype(F32), gap], axis=0).T
    lane = lax.broadcasted_iota(I32, logits.shape, 1).astype(F32)
    picked = [
        jnp.sum(jnp.where(lane == info[:, 2 * top_k + j : 2 * top_k + j + 1], logits, 0.0), axis=1, keepdims=True)
        for j in range(top_k)
    ]
    peak = functools.reduce(jnp.maximum, picked)
    powers = [jnp.exp(v - peak) for v in picked]
    norm = functools.reduce(jnp.add, powers)
    lane = lax.broadcasted_iota(I32, info.shape, 1)
    for j in range(top_k):
        info = jnp.where(lane == top_k + j, powers[j] / norm, info)
    r.my_gates[...] = info
    for p in range(3):
        r.line_gates[p, me[LINE[p]]] = info


    for offset in range(1, side):
        for p in range(3):
            d = lax.rem(me[LINE[p]] + side - offset, side)
            wait_bytes(tok[p].at[d], r.tok_recv.at[p, offset - 1])
            send_far(p, d)
    for p in range(3):
        wait_bytes(r.all_keys.at[p, 0, pl.ds(0, side - 1)], r.key_recv.at[p])
        for offset in range(1, side):
            keys = r.all_keys.at[p, me[PLANE[p][0]]]
            remote(keys, keys, r.far_key_send.at[p], r.far_key_recv.at[p], axis_peer(PLANE[p][0], offset)).start()
    for offset in range(1, side):
        for p in range(3):
            spot = me[LINE[p]]
            remote(
                r.my_gates, r.line_gates.at[p, spot], r.gate_send.at[p], r.gate_recv.at[p], line_peer(p, offset)
            ).start()


    n_heads = r.query.shape[1] // head_dim
    per_key = r.query.shape[1] // r.key.shape[1]
    causal = lax.broadcasted_iota(I32, (tokens, tokens), 0) >= lax.broadcasted_iota(I32, (tokens, tokens), 1)

    def one_head(h, carry):
        cols = pl.ds(pl.multiple_of(h * head_dim, head_dim), head_dim)
        key_cols = pl.ds(pl.multiple_of(h // per_key * head_dim, head_dim), head_dim)
        scores = lax.dot_general(
            r.query[:, cols], r.key[:, key_cols], (((1,), (1,)), ((), ())), preferred_element_type=F32
        )
        scores = jnp.where(causal, scores * head_dim ** -0.5, -jnp.inf)
        power = jnp.exp(scores - jnp.max(scores, axis=1, keepdims=True))
        prob = (power / jnp.sum(power, axis=1, keepdims=True)).astype(BF16)
        r.query[:, cols] = dot(prob, r.value[:, key_cols]).astype(BF16)
        return carry

    lax.fori_loop(0, n_heads, one_head, 0)


    stage = r.stage
    blocks = N_CHUNKS * mates
    my_mate = {p: me[PLANE[p][1]] * 2 + me['c'] for p in range(3)}

    def pick_rows(p, i, d, slot, source, wanted):
        keys = r.all_keys[p, i, d]
        for lo, n in steps(tokens, 128):
            hit = wanted[:, 0:n] == keys[0:1, lo : lo + n]
            for j in range(1, top_k):
                hit = jnp.logical_or(hit, wanted[:, 0:n] == keys[j : j + 1, lo : lo + n])
            r.split[0 : blocks * slots, lo : lo + n] = jnp.where(hit, 1.0, 0.0).astype(BF16)
        for lo, n in steps(widths[p], TILE):
            found = dot(r.split[0 : blocks * slots, 0:tokens], source[:, lo : lo + n]).astype(BF16)
            stage[slot, 0:blocks, :, lo : lo + n] = found.reshape(blocks, slots, n)

    def flush(p, i, d, slot):
        a, b = source_index(p, i, d)
        return pltpu.make_async_copy(
            stage.at[slot, pl.ds(0, blocks), :, pl.ds(0, widths[p])],
            sends[p].at[pl.ds(0, blocks), a, b],
            r.stage_sem.at[slot],
        )

    def keep(p, i, d, slot, chunk):
        spot = {**me, PLANE[p][0]: i, LINE[p]: d}
        return pltpu.make_async_copy(
            stage.at[slot, chunk * mates + my_mate[p], :, pl.ds(0, widths[p])],
            arrivals[p].at[tuple([chunk] + [spot[axis] for axis in ROW_AXES])],
            r.keep_sem.at[slot, chunk],
        )

    for p in range(3):
        sources = side * side
        near = me[PLANE[p][0]]
        wanted = mate_keys(p, (blocks * slots, min(128, tokens)))
        wait_bytes(r.all_keys.at[p, pl.ds(0, side - 1)], r.far_key_recv.at[p])
        wait_bytes(far[p].at[pl.ds(0, side - 1)], r.far_recv.at[p])

        def place_of(n):
            return lax.rem(near + n // side, side), lax.rem(n, side)

        def load(n, slot):
            i, d = place_of(n)
            return pltpu.make_async_copy(far[p].at[i, d], r.source.at[slot, :, pl.ds(0, widths[p])], r.source_sem.at[slot])

        def one_source(n, c):
            slot = lax.rem(n, 2)
            i, d = place_of(n)

            @pl.when(jnp.logical_and(n + 1 >= side, n + 1 < sources))
            def _():
                load(n + 1, 1 - slot).start()

            @pl.when(n >= side)
            def _():
                load(n, slot).wait()

            @pl.when(n < side)
            def _():
                r.source[slot, :, 0 : widths[p]] = tok[p][d]

            @pl.when(n >= 2)
            def _():
                i2, d2 = place_of(n - 2)
                flush(p, i2, d2, slot).wait()
                for chunk in range(N_CHUNKS):
                    keep(p, i2, d2, slot, chunk).wait()

            pick_rows(p, i, d, slot, r.source.at[slot], wanted)
            flush(p, i, d, slot).start()
            for chunk in range(N_CHUNKS):
                keep(p, i, d, slot, chunk).start()
            return c

        lax.fori_loop(0, sources, one_source, 0)
        for n in range(sources - 2, sources):
            i, d = place_of(n)
            flush(p, i, d, n % 2).wait()
            for chunk in range(N_CHUNKS):
                keep(p, i, d, n % 2, chunk).wait()

        def go_chunk(chunk, c):
            def one_mate(offset, c2):
                place = mate_peer(p, offset)
                remote(
                    sends[p].at[chunk * mates + place[PLANE[p][1]] * 2 + place['c']],
                    gathered_rows_of(arrivals[p], p, chunk, me),
                    r.go_send.at[chunk, p],
                    r.go_recv.at[chunk, p],
                    place,
                ).start()
                return c2

            return lax.fori_loop(1, mates, one_mate, c)

        lax.fori_loop(0, N_CHUNKS, go_chunk, 0)


    out_split = n_heads * head_dim // model

    def out_body(i, tiles):
        total = r.hidden[:, col_tile(i)].astype(F32)
        attended = dot(r.query[:, 0:model], tiles[0][...])
        for s in range(1, out_split):
            attended += dot(r.query[:, s * model : (s + 1) * model], tiles[s][...])
        r.attended[:, col_tile(i)] = (total + attended).astype(BF16)

    stream(model // TILE, out_split, lambda i, s: r.w_out.at[pl.ds(s * model, model), col_tile(i)], out_body)

    def norm_attended(here):
        r.rows[here, :] = rms_rows(r.attended[here, :], one_row(r.ffn_scale))

    bands(norm_attended)

    def act_body(i, tiles):
        z = dot(r.rows[...], tiles[0][...])
        u = dot(r.rows[...], tiles[1][...])
        r.act[:, col_tile(i)] = (jax.nn.silu(z) * u).astype(BF16)

    ff_dim = r.ffn_gate.shape[1]
    stream(
        ff_dim // TILE, 2, lambda i, s: (r.ffn_gate, r.ffn_up)[s].at[:, col_tile(i)], act_body
    )
    down_split = ff_dim // model

    def down_body(i, tiles):
        total = dot(r.act[:, 0:model], tiles[0][...])
        for s in range(1, down_split):
            total += dot(r.act[:, s * model : (s + 1) * model], tiles[s][...])
        r.dense[:, col_tile(i)] = r.attended[:, col_tile(i)].astype(F32) + total

    stream(model // TILE, down_split, lambda i, s: r.ffn_down.at[pl.ds(s * model, model), col_tile(i)], down_body)


    for load in loads:
        load.wait()
    x_buf, y_buf, hidden_buf = r.x_buf, r.y_buf, r.hidden_buf
    group = x_buf.shape[1:-1]
    rows = math.prod(group)
    width = hidden_buf.shape[1]

    def fetch(chunk, y, slot):
        return [
            pltpu.make_async_copy(
                arrivals[p].at[chunk, y], x_buf.at[slot, :, :, :, :, pl.ds(lo, hi - lo)], r.in_sem.at[slot, p]
            )
            for p, (lo, hi) in enumerate(parts)
        ]

    def put(chunk, y, slot):
        return [
            pltpu.make_async_copy(
                y_buf.at[slot, :, :, :, :, pl.ds(lo, hi - lo)], outputs[p].at[chunk, y], r.out_sem.at[slot, p]
            )
            for p, (lo, hi) in enumerate(parts)
        ]

    def keep_own(chunk, y, slot, p):
        lo, hi = parts[p]
        free = (LINE[p], PLANE[p][0])
        spot = [pl.ds(0, side) if axis in free else me[axis] for axis in ROW_AXES[1:]]
        along = {axis: y if axis == 'y' else pl.ds(0, side) for axis in free}
        mine = pltpu.make_async_copy(
            y_buf.at[tuple([slot] + spot + [pl.ds(0, slots), pl.ds(lo, hi - lo)])],
            middles[p].at[tuple([chunk] + [along[axis] for axis in ROW_AXES if axis in free] + [my_mate[p]])],
            r.own_sem.at[slot, p],
        )
        return mine, (None if 'y' in free else y == me['y'])

    def start_put(chunk, y, slot):
        for copy in put(chunk, y, slot):
            copy.start()
        for p in range(3):
            copy, when = keep_own(chunk, y, slot, p)
            if when is None:
                copy.start()
            else:
                pl.when(when)(copy.start)

    def wait_put(chunk, y, slot):
        for copy in put(chunk, y, slot):
            copy.wait()
        for p in range(3):
            copy, when = keep_own(chunk, y, slot, p)
            if when is None:
                copy.wait()
            else:
                pl.when(when)(copy.wait)

    def expert_chunk(chunk):
        for p in range(3):
            wait_bytes(sends[p].at[pl.ds(0, mates - 1)], r.go_recv.at[chunk, p])
        for copy in fetch(chunk, 0, 0):
            copy.start()

        def one_tile(y, c):
            slot = lax.rem(y, 2)

            @pl.when(y + 1 < side)
            def _():
                for copy in fetch(chunk, y + 1, 1 - slot):
                    copy.start()

            for copy in fetch(chunk, y, slot):
                copy.wait()

            @pl.when(y >= 2)
            def _():
                wait_put(chunk, y - 2, slot)

            for lo in range(0, width, f_chunk):
                cols = slice(lo, lo + f_chunk)
                z = dot(x_buf[slot].reshape(rows, model), r.gate[:, cols])
                u = dot(x_buf[slot].reshape(rows, model), r.up[:, cols])
                hidden_buf[:, cols] = (jax.nn.silu(z) * u).astype(BF16)
            for lo in range(0, model, d_chunk):
                cols = slice(lo, lo + d_chunk)
                y_rows = dot(hidden_buf[...], r.down[:, cols]).astype(BF16)
                y_buf[slot, :, :, :, :, cols] = y_rows.reshape(group + (d_chunk,))
            start_put(chunk, y, slot)
            return c

        lax.fori_loop(0, side, one_tile, 0)
        for y in range(side - 2, side):
            wait_put(chunk, y, y % 2)

        def one_mate(offset, c):
            for p in range(3):
                place = mate_peer(p, offset)
                remote(
                    gathered_rows_of(outputs[p], p, chunk, place),
                    middles[p].at[chunk, pl.ds(0, side), pl.ds(0, side), my_mate[p]],
                    r.back_send.at[chunk, p],
                    r.back_recv.at[chunk, p],
                    place,
                ).start()
            return c

        lax.fori_loop(1, mates, one_mate, 0)

    def middle_rows(p, chunk, i, d):
        a, b = source_index(p, i, d)
        return middles[p].at[chunk, a, b]

    def pass_on(chunk):
        for p in range(3):
            wait_bytes(middles[p].at[chunk, pl.ds(0, side), pl.ds(0, side), pl.ds(0, mates - 1)], r.back_recv.at[chunk, p])
            for offset in range(1, side):
                place = axis_peer(PLANE[p][0], offset)
                remote(
                    middle_rows(p, chunk, place[PLANE[p][0]], pl.ds(0, side)),
                    results[p].at[chunk, pl.ds(0, side), me[PLANE[p][0]]],
                    r.home_send.at[chunk, p],
                    r.home_recv.at[chunk, p],
                    place,
                ).start()


    split = r.split
    lanes = min(128, rows_block)

    def weigh_chunk(chunk):
        for p in range(3):
            wait_bytes(results[p].at[chunk, pl.ds(0, side), pl.ds(0, side - 1)], r.home_recv.at[chunk, p])
            held = plane_keys(p, (1, rows_block), chunk).astype(F32)

            def load(d, slot):
                copies = []
                for offset in range(side):
                    i = lax.rem(me[PLANE[p][0]] + offset, side)
                    copies.append(
                        pltpu.make_async_copy(
                            results[p].at[chunk, d, i] if offset else middle_rows(p, chunk, i, d),
                            stage.at[slot, pl.ds(i * mates, mates), :, pl.ds(0, widths[p])],
                            r.load_sem.at[slot, offset],
                        )
                    )
                return copies

            for copy in load(0, 0):
                copy.start()

            def one_source(d, c):
                slot = lax.rem(d, 2)

                @pl.when(d + 1 < side)
                def _():
                    for copy in load(d + 1, 1 - slot):
                        copy.start()

                info = r.line_gates[p, d]
                keys = [jnp.broadcast_to(info[:, j : j + 1], (tokens, lanes)) for j in range(top_k)]
                gates = [jnp.broadcast_to(info[:, top_k + j : top_k + j + 1], (tokens, lanes)) for j in range(top_k)]
                for lo in range(0, rows_block, lanes):
                    here = held[:, lo : lo + lanes]
                    weight = jnp.zeros((tokens, lanes), F32)
                    for j in range(top_k):
                        weight = jnp.where(here == keys[j], gates[j], weight)
                    high = weight.astype(BF16)
                    rest = weight - high.astype(F32)
                    middle = rest.astype(BF16)
                    low = (rest - middle.astype(F32)).astype(BF16)
                    split[0:tokens, lo : lo + lanes] = high
                    split[tokens : 2 * tokens, lo : lo + lanes] = middle
                    split[2 * tokens : 3 * tokens, lo : lo + lanes] = low
                for copy in load(d, slot):
                    copy.wait()
                for lo, n in steps(widths[p], TILE):
                    y = stage[slot, 0:members, :, lo : lo + n].reshape(rows_block, n)
                    both = dot(split[...], y)
                    total = both[0:tokens] + (both[tokens : 2 * tokens] + both[2 * tokens : 3 * tokens])

                    if chunk == 0:
                        sums[p][d, :, lo : lo + n] = total
                    else:
                        sums[p][d, :, lo : lo + n] += total

                return c

            lax.fori_loop(0, side, one_source, 0)

            if chunk == N_CHUNKS - 1:
                for offset in range(1, side):
                    place = line_peer(p, offset)
                    remote(
                        sums[p].at[place[LINE[p]]],
                        others[p].at[offset - 1],
                        r.sum_send.at[p],
                        r.sum_recv.at[p],
                        place,
                    ).start()


    expert_chunk(0)
    for chunk in range(1, N_CHUNKS):
        expert_chunk(chunk)
        pass_on(chunk - 1)
    for p in range(3):
        wait_bytes(r.line_gates.at[p, pl.ds(0, side - 1)], r.gate_recv.at[p])
    weigh_chunk(0)
    pass_on(N_CHUNKS - 1)
    for chunk in range(1, N_CHUNKS):
        weigh_chunk(chunk)
    for p, (lo, hi) in enumerate(parts):
        wait_bytes(others[p], r.sum_recv.at[p])

        def finish(here):
            moe = sums[p][me[LINE[p]], here, :]
            for offset in range(1, side):
                moe += others[p][offset - 1, here, :]
            r.out[here, lo:hi] = (r.dense[here, lo:hi] + moe).astype(BF16)

        bands(finish)


    for p in range(3):
        for offset in range(1, side):
            wait_bytes(tok[p].at[0], r.tok_send.at[p, offset - 1])
        wait_bytes(r.all_keys.at[p, 0, pl.ds(0, side - 1)], r.key_send.at[p])
        wait_bytes(far[p].at[pl.ds(0, side - 1)], r.far_send.at[p])
        wait_bytes(r.all_keys.at[p, pl.ds(0, side - 1)], r.far_key_send.at[p])
        wait_bytes(r.line_gates.at[p, pl.ds(0, side - 1)], r.gate_send.at[p])
        wait_bytes(others[p], r.sum_send.at[p])
        for chunk in range(N_CHUNKS):
            wait_bytes(sends[p].at[pl.ds(0, mates - 1)], r.go_send.at[chunk, p])
            wait_bytes(middles[p].at[chunk, pl.ds(0, side), pl.ds(0, side), pl.ds(0, mates - 1)], r.back_send.at[chunk, p])
            wait_bytes(results[p].at[chunk, pl.ds(0, side), pl.ds(0, side - 1)], r.home_send.at[chunk, p])


def layer_pair(small, large, side, capacity, head_dim):
    tokens, model = small['hidden'].shape
    top_k, width = small['ids_t'].shape[0], large['gate_hbm'].shape[1]
    key_dim, ff_dim = large['w_key'].shape[1], large['ffn_gate'].shape[1]
    parts = column_parts(model)
    widths = [hi - lo for lo, hi in parts]
    slots, members, mates = capacity // N_CHUNKS, side * side * 2, side * 2
    group = (side, 2, side, slots)
    rows = math.prod(group)
    sds, vmem = jax.ShapeDtypeStruct, pltpu.VMEM
    dma = lambda *shape: pltpu.SemaphoreType.DMA(shape)
    outs = dict(out=sds((tokens, model), BF16))
    scratch = dict(
        rows=vmem((tokens, model), BF16),
        query=vmem((tokens, large['w_query'].shape[1]), BF16),
        key=vmem((tokens, key_dim), BF16),
        value=vmem((tokens, key_dim), BF16),
        attended=vmem((tokens, model), BF16),
        act=vmem((tokens, ff_dim), BF16),
        dense=vmem((tokens, model), F32),
        ring=vmem((RING, model, TILE), BF16),
        all_keys=vmem((3, side, side, top_k, tokens), I32),
        my_gates=vmem((tokens, 128), F32),
        line_gates=vmem((3, side, tokens, 128), F32),
        source=vmem((2, tokens, max(widths)), BF16),
        stage=vmem((2, max(members, N_CHUNKS * mates), slots, max(widths)), BF16),
        split=vmem((3 * tokens, members * slots), BF16),
        gate=vmem((model, width), BF16),
        up=vmem((model, width), BF16),
        down=vmem((width, model), BF16),
        x_buf=vmem((2,) + group + (model,), BF16),
        y_buf=vmem((2,) + group + (model,), BF16),
        hidden_buf=vmem((rows, width), BF16),
        weight_sem=dma(3),
        ring_sem=dma(RING),
        source_sem=dma(2),
        stage_sem=dma(2),
        keep_sem=dma(2, N_CHUNKS),
        in_sem=dma(2, 3),
        out_sem=dma(2, 3),
        own_sem=dma(2, 3),
        load_sem=dma(2, side),
        tok_send=dma(3, side - 1),
        tok_recv=dma(3, side - 1),
        key_send=dma(3),
        key_recv=dma(3),
        far_send=dma(3),
        far_recv=dma(3),
        far_key_send=dma(3),
        far_key_recv=dma(3),
        gate_send=dma(3),
        gate_recv=dma(3),
        sum_send=dma(3),
        sum_recv=dma(3),
        go_send=dma(N_CHUNKS, 3),
        go_recv=dma(N_CHUNKS, 3),
        back_send=dma(N_CHUNKS, 3),
        back_recv=dma(N_CHUNKS, 3),
        home_send=dma(N_CHUNKS, 3),
        home_recv=dma(N_CHUNKS, 3),
    )
    for p, w in enumerate(widths):
        there = sds((N_CHUNKS, side, side, 2, side, slots, w), BF16)
        outs['far' + str(p)] = sds((side, side, tokens, w), BF16)
        outs['send' + str(p)] = sds((N_CHUNKS * mates, side, side, slots, w), BF16)
        outs['arrive' + str(p)] = there
        outs['output' + str(p)] = there
        outs['middle' + str(p)] = sds((N_CHUNKS, side, side, mates, slots, w), BF16)
        outs['result' + str(p)] = sds((N_CHUNKS, side, side, mates, slots, w), BF16)
        scratch['tok' + str(p)] = vmem((side, tokens, w), BF16)
        scratch['sum' + str(p)] = vmem((side, tokens, w), F32)
        scratch['other' + str(p)] = vmem((side - 1, tokens, w), F32)
    anywhere = pl.BlockSpec(memory_space=pl.ANY)
    local = pl.BlockSpec(memory_space=pltpu.VMEM)
    n_rows = members * side * capacity
    return pl.pallas_call(
        functools.partial(
            kernel,
            names=tuple(small) + tuple(large) + tuple(outs) + tuple(scratch),
            side=side,
            parts=parts,
            capacity=capacity,
            head_dim=head_dim,
            f_chunk=min(256, width),
            d_chunk=min(512, model),
        ),
        out_shape=list(outs.values()),
        in_specs=[local] * len(small) + [anywhere] * len(large),
        out_specs=[local] + [anywhere] * (len(outs) - 1),
        scratch_shapes=list(scratch.values()),
        compiler_params=pltpu.CompilerParams(has_side_effects=True, vmem_limit_bytes=67043328),
        cost_estimate=pl.CostEstimate(flops=6 * n_rows * model * width, bytes_accessed=8 * n_rows * model, transcendentals=0),
    )(*small.values(), *large.values())[0]


def solution(mesh):
    group_size = mesh.shape['ep']
    side = torus_side(group_size)
    torus = jax.sharding.Mesh(mesh.devices.reshape(side, side, side, 2), AXES)
    row_spec = P(AXES, None, None)
    vec_spec = P(None)
    mat_spec = P(None, None)
    cube_spec = P(None, None, None)
    expert_spec = P(AXES, None, None)

    def per_device(hidden, expert_ids, slot_ids, attn_norm, w_query, w_key, w_value, w_out, ffn_norm, ffn_gate, ffn_up, ffn_down, moe_norm, w_router, exp_gate, exp_up, exp_down):
        n_seqs, tokens, model = hidden.shape
        assert n_seqs == 1 and exp_gate.shape[0] == 1
        n_heads, head_dim = w_out.shape[0], w_out.shape[1]
        top_k = expert_ids.shape[2]
        capacity = CAP_FACTOR * tokens * top_k // group_size
        inv_freq = np.float32(ROPE_BASE) ** (np.float32(-2.0) * np.arange(head_dim // 2, dtype=np.float32) / head_dim)
        angles = np.arange(tokens, dtype=np.float32)[:, None] * inv_freq[None, :]
        cos, sin = np.cos(angles), np.sin(angles)
        small = dict(
            hidden=hidden[0],
            attn_scale=attn_norm.reshape(-1, 128),
            moe_scale=moe_norm.reshape(-1, 128),
            ffn_scale=ffn_norm.reshape(-1, 128),
            ids_t=expert_ids[0].T,
            slots_t=slot_ids[0].T,
            w_router=w_router,
            cos=np.concatenate([cos, cos], axis=1).astype(np.float32),
            sin=np.concatenate([-sin, sin], axis=1).astype(np.float32),
        )
        large = dict(
            w_query=w_query,
            w_key=w_key,
            w_value=w_value,
            w_out=w_out.reshape(n_heads * head_dim, model),
            ffn_gate=ffn_gate,
            ffn_up=ffn_up,
            ffn_down=ffn_down,
            gate_hbm=exp_gate[0],
            up_hbm=exp_up[0],
            down_hbm=exp_down[0],
        )
        return layer_pair(small, large, side, capacity, head_dim).reshape(hidden.shape)

    return jax.shard_map(per_device, mesh=torus, in_specs=(row_spec, row_spec, row_spec, vec_spec, mat_spec, mat_spec, mat_spec, cube_spec, vec_spec, mat_spec, mat_spec, mat_spec, vec_spec, mat_spec, expert_spec, expert_spec, expert_spec), out_specs=row_spec, check_vma=False)
```

```python
import functools
import math
import types

import jax
import jax.numpy as jnp
import numpy as np
from jax import lax
from jax.experimental import pallas as pl
from jax.experimental.pallas import tpu as pltpu
from jax.sharding import PartitionSpec as P

RMS_EPS = 1e-6
ROPE_BASE = 10000.0
CAP_FACTOR = 3
N_CHUNKS = 3
RING = 6
TILE = 256
MESH = pl.DeviceIdType.MESH

BF16, F32, I32 = jnp.bfloat16, jnp.float32, jnp.int32

AXES = ('z', 'y', 'x', 'c')
LINE = ('z', 'x', 'y')
PLANE = (('y', 'x'), ('z', 'y'), ('x', 'z'))
ROW_AXES = ('y', 'x', 'c', 'z')


def torus_side(n_devices):
    side = round((n_devices // 2) ** (1 / 3))
    assert side ** 3 * 2 == n_devices
    return side


def column_parts(model):
    lanes = model // 128
    first = -(-lanes // 3)
    second = -(-(lanes - first) // 2)
    ends = (0, first * 128, (first + second) * 128, model)
    return tuple((ends[p], ends[p + 1]) for p in range(3))


def steps(total, size):
    return [(lo, min(size, total - lo)) for lo in range(0, total, size)]


def rms_rows(rows, scale):
    as_float = rows.astype(F32)
    inv_rms = lax.rsqrt(jnp.mean(as_float * as_float, axis=-1, keepdims=True) + RMS_EPS)
    return (as_float * inv_rms * scale.astype(F32)).astype(BF16)


def dot(a, b):
    return jnp.dot(a, b, preferred_element_type=F32)


def kernel(*refs, names, side, parts, capacity, head_dim, f_chunk, d_chunk):
    r = types.SimpleNamespace(**dict(zip(names, refs)))
    each = lambda name: [getattr(r, name + str(p)) for p in range(3)]
    slots = capacity // N_CHUNKS
    members = side * side * 2
    mates = side * 2
    rows_block = members * slots
    tokens, model = r.hidden.shape
    me = {axis: lax.axis_index(axis) for axis in AXES}


    def rows_of(ref, p, chunk, place, free):
        spot = [pl.ds(0, side) if axis in free else place[axis] for axis in ROW_AXES]
        return ref.at[tuple([chunk] + spot)]

    def gathered_rows_of(ref, p, chunk, place):
        return rows_of(ref, p, chunk, place, (LINE[p], PLANE[p][0]))

    def source_index(p, i, d):
        where = {PLANE[p][0]: i, LINE[p]: d}
        return tuple(where[axis] for axis in ROW_AXES if axis in where)

    def device(place):
        return tuple(place[axis] for axis in AXES)

    def axis_peer(axis, offset):
        return {**me, axis: lax.rem(me[axis] + offset, side)}

    def line_peer(p, offset):
        return axis_peer(LINE[p], offset)

    def mate_peer(p, offset):
        axis = PLANE[p][1]
        return {
            **me,
            axis: lax.rem(me[axis] + offset // 2, side),
            'c': lax.rem(me['c'] + lax.rem(offset, 2), 2),
        }

    def remote(src, dst, send_sem, recv_sem, place):
        return pltpu.make_async_remote_copy(
            src_ref=src, dst_ref=dst, send_sem=send_sem, recv_sem=recv_sem, device_id=device(place), device_id_type=MESH
        )

    def wait_bytes(ref, sem):
        pltpu.make_async_copy(ref, ref, sem).wait()

    def expert_key(place, core, slot):
        return (((place['z'] * side + place['y']) * side + place['x']) * 2 + core) * capacity + slot

    def plane_keys(p, shape, chunk):
        row = lax.broadcasted_iota(I32, shape, 1)
        which, slot = row // slots, lax.rem(row, slots)
        pair = which // 2
        place = {PLANE[p][0]: pair // side, PLANE[p][1]: lax.rem(pair, side), LINE[p]: me[LINE[p]]}
        return expert_key(place, lax.rem(which, 2), slot + chunk * slots)

    def mate_keys(p, shape):
        row = lax.broadcasted_iota(I32, shape, 0)
        block, slot = row // slots, lax.rem(row, slots)
        chunk, mate = block // mates, lax.rem(block, mates)
        place = {**me, PLANE[p][1]: mate // 2}
        return expert_key(place, lax.rem(mate, 2), slot + chunk * slots)

    tok, far, sends, arrivals, outputs = each('tok'), each('far'), each('send'), each('arrive'), each('output')
    middles, results, sums, others = each('middle'), each('result'), each('sum'), each('other')
    widths = [hi - lo for lo, hi in parts]


    band = min(32, tokens)

    def bands(body):
        lax.fori_loop(0, tokens // band, lambda i, c: (body(pl.ds(pl.multiple_of(i * band, band), band)), c)[1], 0)

    def one_row(scale):
        lines = scale[...].astype(F32)
        return jnp.concatenate([lines[i : i + 1, :] for i in range(lines.shape[0])], axis=1)

    def norm_both(here):
        normed = rms_rows(r.hidden[here, :], one_row(r.moe_scale))
        for p, (lo, hi) in enumerate(parts):
            tok[p][me[LINE[p]], here, :] = normed[:, lo:hi]
        r.rows[here, :] = rms_rows(r.hidden[here, :], one_row(r.attn_scale))

    bands(norm_both)
    keys_t = r.ids_t[...] * capacity + r.slots_t[...]
    for p in range(3):
        r.all_keys[p, me[PLANE[p][0]], me[LINE[p]]] = keys_t
    pairs = ((r.gate_hbm, r.gate), (r.up_hbm, r.up), (r.down_hbm, r.down))
    loads = [pltpu.make_async_copy(src, dst, r.weight_sem.at[i]) for i, (src, dst) in enumerate(pairs)]
    for load in loads:
        load.start()

    def send_far(p, d):
        for offset in range(1, side):
            here = me[PLANE[p][0]]
            remote(
                tok[p].at[d],
                far[p].at[here, d],
                r.far_send.at[p],
                r.far_recv.at[p, offset - 1],
                axis_peer(PLANE[p][0], offset),
            ).start()

    for offset in range(1, side):
        for p in range(3):
            spot, place = me[LINE[p]], line_peer(p, offset)
            remote(
                tok[p].at[spot], tok[p].at[spot], r.tok_send.at[p, offset - 1], r.tok_recv.at[p, offset - 1], place
            ).start()
            keys = r.all_keys.at[p, me[PLANE[p][0]], spot]
            remote(keys, keys, r.key_send.at[p], r.key_recv.at[p], place).start()
    for p in range(3):
        send_far(p, me[LINE[p]])


    ring = r.ring
    ring_sem = r.ring_sem

    def stream(n_steps, group, source, body):
        ahead = RING // group * group - group

        def copy(i, s):
            slot = lax.rem(i * group + s, RING // group * group)
            return pltpu.make_async_copy(source(i, s), ring.at[slot], ring_sem.at[slot])

        for i in range(min(ahead // group, n_steps)):
            for s in range(group):
                copy(i, s).start()

        def step(i, carry):
            @pl.when(i + ahead // group < n_steps)
            def _():
                for s in range(group):
                    copy(i + ahead // group, s).start()

            for s in range(group):
                copy(i, s).wait()
            body(i, [ring.at[lax.rem(i * group + s, RING // group * group)] for s in range(group)])
            return carry

        lax.fori_loop(0, n_steps, step, 0)

    def col_tile(i):
        return pl.ds(pl.multiple_of(i * TILE, TILE), TILE)

    def turned(y):
        return y * r.cos[...] + pltpu.roll(y, head_dim // 2, 1) * r.sin[...]

    def project(weight, out, rotary):
        def body(i, tiles):
            y = dot(r.rows[...], tiles[0][...])
            if rotary:
                y = jnp.concatenate([turned(y[:, lo : lo + head_dim]) for lo in range(0, TILE, head_dim)], axis=1)
            out[:, col_tile(i)] = y.astype(BF16)

        stream(weight.shape[1] // TILE, 1, lambda i, s: weight.at[:, col_tile(i)], body)

    project(r.w_query, r.query, True)
    project(r.w_key, r.key, True)
    project(r.w_value, r.value, False)


    logits = sum(dot(tok[p][me[LINE[p]]], r.w_router[lo:hi, :]) for p, (lo, hi) in enumerate(parts))
    top_k = r.ids_t.shape[0]
    gap = jnp.zeros((128 - 3 * top_k, tokens), F32)
    blank = jnp.zeros((top_k, tokens), F32)
    info = jnp.concatenate([keys_t.astype(F32), blank, r.ids_t[...].astype(F32), gap], axis=0).T
    lane = lax.broadcasted_iota(I32, logits.shape, 1).astype(F32)
    picked = [
        jnp.sum(jnp.where(lane == info[:, 2 * top_k + j : 2 * top_k + j + 1], logits, 0.0), axis=1, keepdims=True)
        for j in range(top_k)
    ]
    peak = functools.reduce(jnp.maximum, picked)
    powers = [jnp.exp(v - peak) for v in picked]
    norm = functools.reduce(jnp.add, powers)
    lane = lax.broadcasted_iota(I32, info.shape, 1)
    for j in range(top_k):
        info = jnp.where(lane == top_k + j, powers[j] / norm, info)
    r.my_gates[...] = info
    for p in range(3):
        r.line_gates[p, me[LINE[p]]] = info


    def hand_on(offset):
        for p in range(3):
            d = lax.rem(me[LINE[p]] + side - offset, side)
            wait_bytes(tok[p].at[d], r.tok_recv.at[p, offset - 1])
            send_far(p, d)

    for offset in range(1, side):
        hand_on(offset)
    for p in range(3):
        wait_bytes(r.all_keys.at[p, 0, pl.ds(0, side - 1)], r.key_recv.at[p])
        for offset in range(1, side):
            keys = r.all_keys.at[p, me[PLANE[p][0]]]
            remote(
                keys, keys, r.far_key_send.at[p], r.far_key_recv.at[p, offset - 1], axis_peer(PLANE[p][0], offset)
            ).start()
    for offset in range(1, side):
        for p in range(3):
            spot = me[LINE[p]]
            remote(
                r.my_gates, r.line_gates.at[p, spot], r.gate_send.at[p], r.gate_recv.at[p], line_peer(p, offset)
            ).start()


    n_heads = r.query.shape[1] // head_dim
    per_key = r.query.shape[1] // r.key.shape[1]
    causal = lax.broadcasted_iota(I32, (tokens, tokens), 0) >= lax.broadcasted_iota(I32, (tokens, tokens), 1)

    def one_head(h, carry):
        cols = pl.ds(pl.multiple_of(h * head_dim, head_dim), head_dim)
        key_cols = pl.ds(pl.multiple_of(h // per_key * head_dim, head_dim), head_dim)
        scores = lax.dot_general(
            r.query[:, cols], r.key[:, key_cols], (((1,), (1,)), ((), ())), preferred_element_type=F32
        )
        scores = jnp.where(causal, scores * head_dim ** -0.5, -jnp.inf)
        power = jnp.exp(scores - jnp.max(scores, axis=1, keepdims=True))
        prob = (power / jnp.sum(power, axis=1, keepdims=True)).astype(BF16)
        r.query[:, cols] = dot(prob, r.value[:, key_cols]).astype(BF16)
        return carry


    stage = r.stage
    blocks = N_CHUNKS * mates
    my_mate = {p: me[PLANE[p][1]] * 2 + me['c'] for p in range(3)}

    def pick_rows(p, i, d, slot, source, wanted):
        keys = r.all_keys[p, i, d]
        for lo, n in steps(tokens, 128):
            hit = wanted[:, 0:n] == keys[0:1, lo : lo + n]
            for j in range(1, top_k):
                hit = jnp.logical_or(hit, wanted[:, 0:n] == keys[j : j + 1, lo : lo + n])
            r.split[0 : blocks * slots, lo : lo + n] = jnp.where(hit, 1.0, 0.0).astype(BF16)
        for lo, n in steps(widths[p], TILE):
            found = dot(r.split[0 : blocks * slots, 0:tokens], source[:, lo : lo + n]).astype(BF16)
            stage[slot, 0:blocks, :, lo : lo + n] = found.reshape(blocks, slots, n)

    def flush(p, i, d, slot):
        a, b = source_index(p, i, d)
        return pltpu.make_async_copy(
            stage.at[slot, pl.ds(0, blocks), :, pl.ds(0, widths[p])],
            sends[p].at[pl.ds(0, blocks), a, b],
            r.stage_sem.at[slot],
        )

    def keep(p, i, d, slot, chunk):
        spot = {**me, PLANE[p][0]: i, LINE[p]: d}
        return pltpu.make_async_copy(
            stage.at[slot, chunk * mates + my_mate[p], :, pl.ds(0, widths[p])],
            arrivals[p].at[tuple([chunk] + [spot[axis] for axis in ROW_AXES])],
            r.keep_sem.at[slot, chunk],
        )

    wanted = [mate_keys(p, (blocks * slots, min(128, tokens))) for p in range(3)]

    def send_rows(p, chunk, i):
        free = (LINE[p],) if i is not None else (LINE[p], PLANE[p][0])
        a, b = source_index(p, pl.ds(0, side) if i is None else i, pl.ds(0, side))
        group_place = me if i is None else {**me, PLANE[p][0]: i}

        def one_mate(offset, c):
            place = mate_peer(p, offset)
            remote(
                sends[p].at[chunk * mates + place[PLANE[p][1]] * 2 + place['c'], a, b],
                rows_of(arrivals[p], p, chunk, group_place, free),
                r.go_send.at[chunk, p],
                r.go_recv.at[chunk, p],
                place,
            ).start()
            return c

        lax.fori_loop(1, mates, one_mate, 0)

    def pick_group(offset):
        for p in range(3):
            i = lax.rem(me[PLANE[p][0]] + side - offset, side)
            if offset:
                wait_bytes(r.all_keys.at[p, 0], r.far_key_recv.at[p, offset - 1])
                wait_bytes(far[p].at[0], r.far_recv.at[p, offset - 1])

            def load(d, slot):
                return pltpu.make_async_copy(
                    far[p].at[i, d], r.source.at[slot, :, pl.ds(0, widths[p])], r.source_sem.at[slot]
                )

            if offset:
                load(0, 0).start()

            def one_source(d, c):
                slot = lax.rem(d, 2)
                if offset:

                    @pl.when(d + 1 < side)
                    def _():
                        load(d + 1, 1 - slot).start()

                    load(d, slot).wait()

                @pl.when(d >= 2)
                def _():
                    flush(p, i, d - 2, slot).wait()
                    for chunk in range(N_CHUNKS):
                        keep(p, i, d - 2, slot, chunk).wait()

                pick_rows(p, i, d, slot, r.source.at[slot] if offset else tok[p].at[d], wanted[p])
                flush(p, i, d, slot).start()
                for chunk in range(N_CHUNKS):
                    keep(p, i, d, slot, chunk).start()
                return c

            lax.fori_loop(0, side, one_source, 0)
            for d in range(side - 2, side):
                flush(p, i, d, d % 2).wait()
                for chunk in range(N_CHUNKS):
                    keep(p, i, d, d % 2, chunk).wait()
            send_rows(p, 0, i)

    def heads(part, n_parts):
        lax.fori_loop(n_heads * part // n_parts, n_heads * (part + 1) // n_parts, one_head, 0)

    heads(0, 2)
    pick_group(0)
    for offset in range(1, side):
        heads(side - 2 + offset, 2 * (side - 1))
        pick_group(offset)
    for chunk in range(1, N_CHUNKS):
        for p in range(3):
            send_rows(p, chunk, None)


    out_split = n_heads * head_dim // model

    def out_body(i, tiles):
        total = r.hidden[:, col_tile(i)].astype(F32)
        attended = dot(r.query[:, 0:model], tiles[0][...])
        for s in range(1, out_split):
            attended += dot(r.query[:, s * model : (s + 1) * model], tiles[s][...])
        r.attended[:, col_tile(i)] = (total + attended).astype(BF16)

    stream(model // TILE, out_split, lambda i, s: r.w_out.at[pl.ds(s * model, model), col_tile(i)], out_body)

    def norm_attended(here):
        r.rows[here, :] = rms_rows(r.attended[here, :], one_row(r.ffn_scale))

    bands(norm_attended)

    def act_body(i, tiles):
        z = dot(r.rows[...], tiles[0][...])
        u = dot(r.rows[...], tiles[1][...])
        r.act[:, col_tile(i)] = (jax.nn.silu(z) * u).astype(BF16)

    ff_dim = r.ffn_gate.shape[1]
    stream(
        ff_dim // TILE, 2, lambda i, s: (r.ffn_gate, r.ffn_up)[s].at[:, col_tile(i)], act_body
    )
    down_split = ff_dim // model

    def down_body(i, tiles):
        total = dot(r.act[:, 0:model], tiles[0][...])
        for s in range(1, down_split):
            total += dot(r.act[:, s * model : (s + 1) * model], tiles[s][...])
        r.dense[:, col_tile(i)] = r.attended[:, col_tile(i)].astype(F32) + total

    stream(model // TILE, down_split, lambda i, s: r.ffn_down.at[pl.ds(s * model, model), col_tile(i)], down_body)


    for load in loads:
        load.wait()
    x_buf, y_buf, hidden_buf = r.x_buf, r.y_buf, r.hidden_buf
    group = x_buf.shape[1:-1]
    rows = math.prod(group)
    width = hidden_buf.shape[1]

    def fetch(chunk, y, slot):
        return [
            pltpu.make_async_copy(
                arrivals[p].at[chunk, y], x_buf.at[slot, :, :, :, :, pl.ds(lo, hi - lo)], r.in_sem.at[slot, p]
            )
            for p, (lo, hi) in enumerate(parts)
        ]

    def put(chunk, y, slot):
        return [
            pltpu.make_async_copy(
                y_buf.at[slot, :, :, :, :, pl.ds(lo, hi - lo)], outputs[p].at[chunk, y], r.out_sem.at[slot, p]
            )
            for p, (lo, hi) in enumerate(parts)
        ]

    def keep_own(chunk, y, slot, p):
        lo, hi = parts[p]
        free = (LINE[p], PLANE[p][0])
        spot = [pl.ds(0, side) if axis in free else me[axis] for axis in ROW_AXES[1:]]
        along = {axis: y if axis == 'y' else pl.ds(0, side) for axis in free}
        mine = pltpu.make_async_copy(
            y_buf.at[tuple([slot] + spot + [pl.ds(0, slots), pl.ds(lo, hi - lo)])],
            middles[p].at[tuple([chunk] + [along[axis] for axis in ROW_AXES if axis in free] + [my_mate[p]])],
            r.own_sem.at[slot, p],
        )
        return mine, (None if 'y' in free else y == me['y'])

    def start_put(chunk, y, slot):
        for copy in put(chunk, y, slot):
            copy.start()
        for p in range(3):
            copy, when = keep_own(chunk, y, slot, p)
            if when is None:
                copy.start()
            else:
                pl.when(when)(copy.start)

    def wait_put(chunk, y, slot):
        for copy in put(chunk, y, slot):
            copy.wait()
        for p in range(3):
            copy, when = keep_own(chunk, y, slot, p)
            if when is None:
                copy.wait()
            else:
                pl.when(when)(copy.wait)

    def expert_chunk(chunk):
        for p in range(3):
            wait_bytes(sends[p].at[pl.ds(0, mates - 1)], r.go_recv.at[chunk, p])
        for copy in fetch(chunk, 0, 0):
            copy.start()

        def one_tile(y, c):
            slot = lax.rem(y, 2)

            @pl.when(y + 1 < side)
            def _():
                for copy in fetch(chunk, y + 1, 1 - slot):
                    copy.start()

            for copy in fetch(chunk, y, slot):
                copy.wait()

            @pl.when(y >= 2)
            def _():
                wait_put(chunk, y - 2, slot)

            for lo in range(0, width, f_chunk):
                cols = slice(lo, lo + f_chunk)
                z = dot(x_buf[slot].reshape(rows, model), r.gate[:, cols])
                u = dot(x_buf[slot].reshape(rows, model), r.up[:, cols])
                hidden_buf[:, cols] = (jax.nn.silu(z) * u).astype(BF16)
            for lo in range(0, model, d_chunk):
                cols = slice(lo, lo + d_chunk)
                y_rows = dot(hidden_buf[...], r.down[:, cols]).astype(BF16)
                y_buf[slot, :, :, :, :, cols] = y_rows.reshape(group + (d_chunk,))
            start_put(chunk, y, slot)
            return c

        lax.fori_loop(0, side, one_tile, 0)
        for y in range(side - 2, side):
            wait_put(chunk, y, y % 2)

        def one_mate(offset, c):
            for p in range(3):
                place = mate_peer(p, offset)
                remote(
                    gathered_rows_of(outputs[p], p, chunk, place),
                    middles[p].at[chunk, pl.ds(0, side), pl.ds(0, side), my_mate[p]],
                    r.back_send.at[chunk, p],
                    r.back_recv.at[chunk, p],
                    place,
                ).start()
            return c

        lax.fori_loop(1, mates, one_mate, 0)

    def middle_rows(p, chunk, i, d):
        a, b = source_index(p, i, d)
        return middles[p].at[chunk, a, b]

    def pass_on(chunk):
        for p in range(3):
            wait_bytes(middles[p].at[chunk, pl.ds(0, side), pl.ds(0, side), pl.ds(0, mates - 1)], r.back_recv.at[chunk, p])
            for offset in range(1, side):
                place = axis_peer(PLANE[p][0], offset)
                remote(
                    middle_rows(p, chunk, place[PLANE[p][0]], pl.ds(0, side)),
                    results[p].at[chunk, pl.ds(0, side), me[PLANE[p][0]]],
                    r.home_send.at[chunk, p],
                    r.home_recv.at[chunk, p],
                    place,
                ).start()


    split = r.split
    lanes = min(128, rows_block)

    def weigh_chunk(chunk, carry):
        @pl.when(chunk == 1)
        def _():
            pass_on(N_CHUNKS - 1)

        for p in range(3):
            wait_bytes(results[p].at[chunk, pl.ds(0, side), pl.ds(0, side - 1)], r.home_recv.at[chunk, p])

        def source_of(p, n):
            return lax.rem(me[LINE[p]] + 1 + n, side)

        def load(p, n, slot):
            copies = []
            for offset in range(side):
                i, d = lax.rem(me[PLANE[p][0]] + offset, side), source_of(p, n)
                copies.append(
                    pltpu.make_async_copy(
                        results[p].at[chunk, d, i] if offset else middle_rows(p, chunk, i, d),
                        stage.at[slot, pl.ds(i * mates, mates), :, pl.ds(0, widths[p])],
                        r.load_sem.at[slot, offset],
                    )
                )
            return copies

        for copy in load(0, 0, 0):
            copy.start()

        def one_source(n, c):
            for p in range(3):
                d = source_of(p, n)
                slot = lax.rem(n + p, 2)

                @pl.when(n + p // 2 < side)
                def _():
                    for copy in load((p + 1) % 3, n + p // 2, 1 - slot):
                        copy.start()

                held = plane_keys(p, (1, rows_block), chunk).astype(F32)
                info = r.line_gates[p, d]
                keys = [jnp.broadcast_to(info[:, j : j + 1], (tokens, lanes)) for j in range(top_k)]
                gates = [jnp.broadcast_to(info[:, top_k + j : top_k + j + 1], (tokens, lanes)) for j in range(top_k)]
                for lo in range(0, rows_block, lanes):
                    here = held[:, lo : lo + lanes]
                    weight = jnp.zeros((tokens, lanes), F32)
                    for j in range(top_k):
                        weight = jnp.where(here == keys[j], gates[j], weight)
                    high = weight.astype(BF16)
                    rest = weight - high.astype(F32)
                    middle = rest.astype(BF16)
                    low = (rest - middle.astype(F32)).astype(BF16)
                    split[0:tokens, lo : lo + lanes] = high
                    split[tokens : 2 * tokens, lo : lo + lanes] = middle
                    split[2 * tokens : 3 * tokens, lo : lo + lanes] = low
                for copy in load(p, n, slot):
                    copy.wait()
                for lo, size in steps(widths[p], TILE):
                    y = stage[slot, 0:members, :, lo : lo + size].reshape(rows_block, size)
                    both = dot(split[...], y)
                    total = both[0:tokens] + (both[tokens : 2 * tokens] + both[2 * tokens : 3 * tokens])

                    @pl.when(chunk == 0)
                    def _():
                        sums[p][d, :, lo : lo + size] = total

                    @pl.when(chunk > 0)
                    def _():
                        sums[p][d, :, lo : lo + size] += total

                @pl.when(jnp.logical_and(chunk == N_CHUNKS - 1, n < side - 1))
                def _():
                    remote(
                        sums[p].at[d], others[p].at[n], r.sum_send.at[p], r.sum_recv.at[p], {**me, LINE[p]: d}
                    ).start()

            return c

        return lax.fori_loop(0, side, one_source, carry)


    def experts_and_back(chunk, carry):
        expert_chunk(chunk)
        pl.when(chunk >= 1)(lambda: pass_on(chunk - 1))
        return carry

    lax.fori_loop(0, N_CHUNKS, experts_and_back, 0)
    for p in range(3):
        wait_bytes(r.line_gates.at[p, pl.ds(0, side - 1)], r.gate_recv.at[p])
    lax.fori_loop(0, N_CHUNKS, weigh_chunk, 0)
    for p, (lo, hi) in enumerate(parts):
        wait_bytes(others[p], r.sum_recv.at[p])

        def finish(here):
            moe = sums[p][me[LINE[p]], here, :]
            for offset in range(1, side):
                moe += others[p][offset - 1, here, :]
            r.out[here, lo:hi] = (r.dense[here, lo:hi] + moe).astype(BF16)

        bands(finish)


    for p in range(3):
        for offset in range(1, side):
            wait_bytes(tok[p].at[0], r.tok_send.at[p, offset - 1])
        wait_bytes(r.all_keys.at[p, 0, pl.ds(0, side - 1)], r.key_send.at[p])
        wait_bytes(far[p].at[pl.ds(0, side - 1)], r.far_send.at[p])
        wait_bytes(r.all_keys.at[p, pl.ds(0, side - 1)], r.far_key_send.at[p])
        wait_bytes(r.line_gates.at[p, pl.ds(0, side - 1)], r.gate_send.at[p])
        wait_bytes(others[p], r.sum_send.at[p])
        for chunk in range(N_CHUNKS):
            wait_bytes(sends[p].at[pl.ds(0, mates - 1)], r.go_send.at[chunk, p])
            wait_bytes(middles[p].at[chunk, pl.ds(0, side), pl.ds(0, side), pl.ds(0, mates - 1)], r.back_send.at[chunk, p])
            wait_bytes(results[p].at[chunk, pl.ds(0, side), pl.ds(0, side - 1)], r.home_send.at[chunk, p])


def layer_pair(small, large, side, capacity, head_dim):
    tokens, model = small['hidden'].shape
    top_k, width = small['ids_t'].shape[0], large['gate_hbm'].shape[1]
    key_dim, ff_dim = large['w_key'].shape[1], large['ffn_gate'].shape[1]
    parts = column_parts(model)
    widths = [hi - lo for lo, hi in parts]
    slots, members, mates = capacity // N_CHUNKS, side * side * 2, side * 2
    group = (side, 2, side, slots)
    rows = math.prod(group)
    sds, vmem = jax.ShapeDtypeStruct, pltpu.VMEM
    dma = lambda *shape: pltpu.SemaphoreType.DMA(shape)
    outs = dict(out=sds((tokens, model), BF16))
    scratch = dict(
        rows=vmem((tokens, model), BF16),
        query=vmem((tokens, large['w_query'].shape[1]), BF16),
        key=vmem((tokens, key_dim), BF16),
        value=vmem((tokens, key_dim), BF16),
        attended=vmem((tokens, model), BF16),
        act=vmem((tokens, ff_dim), BF16),
        dense=vmem((tokens, model), F32),
        ring=vmem((RING, model, TILE), BF16),
        all_keys=vmem((3, side, side, top_k, tokens), I32),
        my_gates=vmem((tokens, 128), F32),
        line_gates=vmem((3, side, tokens, 128), F32),
        source=vmem((2, tokens, max(widths)), BF16),
        stage=vmem((2, max(members, N_CHUNKS * mates), slots, max(widths)), BF16),
        split=vmem((3 * tokens, members * slots), BF16),
        gate=vmem((model, width), BF16),
        up=vmem((model, width), BF16),
        down=vmem((width, model), BF16),
        x_buf=vmem((2,) + group + (model,), BF16),
        y_buf=vmem((2,) + group + (model,), BF16),
        hidden_buf=vmem((rows, width), BF16),
        weight_sem=dma(3),
        ring_sem=dma(RING),
        source_sem=dma(2),
        stage_sem=dma(2),
        keep_sem=dma(2, N_CHUNKS),
        in_sem=dma(2, 3),
        out_sem=dma(2, 3),
        own_sem=dma(2, 3),
        load_sem=dma(2, side),
        tok_send=dma(3, side - 1),
        tok_recv=dma(3, side - 1),
        key_send=dma(3),
        key_recv=dma(3),
        far_send=dma(3),
        far_recv=dma(3, side - 1),
        far_key_send=dma(3),
        far_key_recv=dma(3, side - 1),
        gate_send=dma(3),
        gate_recv=dma(3),
        sum_send=dma(3),
        sum_recv=dma(3),
        go_send=dma(N_CHUNKS, 3),
        go_recv=dma(N_CHUNKS, 3),
        back_send=dma(N_CHUNKS, 3),
        back_recv=dma(N_CHUNKS, 3),
        home_send=dma(N_CHUNKS, 3),
        home_recv=dma(N_CHUNKS, 3),
    )
    for p, w in enumerate(widths):
        there = sds((N_CHUNKS, side, side, 2, side, slots, w), BF16)
        outs['far' + str(p)] = sds((side, side, tokens, w), BF16)
        outs['send' + str(p)] = sds((N_CHUNKS * mates, side, side, slots, w), BF16)
        outs['arrive' + str(p)] = there
        outs['output' + str(p)] = there
        outs['middle' + str(p)] = sds((N_CHUNKS, side, side, mates, slots, w), BF16)
        outs['result' + str(p)] = sds((N_CHUNKS, side, side, mates, slots, w), BF16)
        scratch['tok' + str(p)] = vmem((side, tokens, w), BF16)
        scratch['sum' + str(p)] = vmem((side, tokens, w), F32)
        scratch['other' + str(p)] = vmem((side - 1, tokens, w), F32)
    anywhere = pl.BlockSpec(memory_space=pl.ANY)
    local = pl.BlockSpec(memory_space=pltpu.VMEM)
    n_rows = members * side * capacity
    return pl.pallas_call(
        functools.partial(
            kernel,
            names=tuple(small) + tuple(large) + tuple(outs) + tuple(scratch),
            side=side,
            parts=parts,
            capacity=capacity,
            head_dim=head_dim,
            f_chunk=min(256, width),
            d_chunk=min(512, model),
        ),
        out_shape=list(outs.values()),
        in_specs=[local] * len(small) + [anywhere] * len(large),
        out_specs=[local] + [anywhere] * (len(outs) - 1),
        scratch_shapes=list(scratch.values()),
        compiler_params=pltpu.CompilerParams(has_side_effects=True, vmem_limit_bytes=67043328),
        cost_estimate=pl.CostEstimate(flops=6 * n_rows * model * width, bytes_accessed=8 * n_rows * model, transcendentals=0),
    )(*small.values(), *large.values())[0]


def solution(mesh):
    group_size = mesh.shape['ep']
    side = torus_side(group_size)
    torus = jax.sharding.Mesh(mesh.devices.reshape(side, side, side, 2), AXES)
    row_spec = P(AXES, None, None)
    vec_spec = P(None)
    mat_spec = P(None, None)
    cube_spec = P(None, None, None)
    expert_spec = P(AXES, None, None)

    def per_device(hidden, expert_ids, slot_ids, attn_norm, w_query, w_key, w_value, w_out, ffn_norm, ffn_gate, ffn_up, ffn_down, moe_norm, w_router, exp_gate, exp_up, exp_down):
        n_seqs, tokens, model = hidden.shape
        assert n_seqs == 1 and exp_gate.shape[0] == 1
        n_heads, head_dim = w_out.shape[0], w_out.shape[1]
        top_k = expert_ids.shape[2]
        capacity = CAP_FACTOR * tokens * top_k // group_size
        inv_freq = np.float32(ROPE_BASE) ** (np.float32(-2.0) * np.arange(head_dim // 2, dtype=np.float32) / head_dim)
        angles = np.arange(tokens, dtype=np.float32)[:, None] * inv_freq[None, :]
        cos, sin = np.cos(angles), np.sin(angles)
        small = dict(
            hidden=hidden[0],
            attn_scale=attn_norm.reshape(-1, 128),
            moe_scale=moe_norm.reshape(-1, 128),
            ffn_scale=ffn_norm.reshape(-1, 128),
            ids_t=expert_ids[0].T,
            slots_t=slot_ids[0].T,
            w_router=w_router,
            cos=np.concatenate([cos, cos], axis=1).astype(np.float32),
            sin=np.concatenate([-sin, sin], axis=1).astype(np.float32),
        )
        large = dict(
            w_query=w_query,
            w_key=w_key,
            w_value=w_value,
            w_out=w_out.reshape(n_heads * head_dim, model),
            ffn_gate=ffn_gate,
            ffn_up=ffn_up,
            ffn_down=ffn_down,
            gate_hbm=exp_gate[0],
            up_hbm=exp_up[0],
            down_hbm=exp_down[0],
        )
        return layer_pair(small, large, side, capacity, head_dim).reshape(hidden.shape)

    return jax.shard_map(per_device, mesh=torus, in_specs=(row_spec, row_spec, row_spec, vec_spec, mat_spec, mat_spec, mat_spec, cube_spec, vec_spec, mat_spec, mat_spec, mat_spec, vec_spec, mat_spec, expert_spec, expert_spec, expert_spec), out_specs=row_spec, check_vma=False)
```

```python
import functools
import math
import types

import jax
import jax.numpy as jnp
import numpy as np
from jax import lax
from jax.experimental import pallas as pl
from jax.experimental.pallas import tpu as pltpu
from jax.sharding import PartitionSpec as P

RMS_EPS = 1e-6
ROPE_BASE = 10000.0
CAP_FACTOR = 3
N_CHUNKS = 3
RING = 6
TILE = 256
MESH = pl.DeviceIdType.MESH

BF16, F32, I32 = jnp.bfloat16, jnp.float32, jnp.int32

AXES = ('z', 'y', 'x', 'c')
OUT = (('z', 'y', 'x'), ('x', 'z', 'y'), ('y', 'x', 'z'))
BACK = (('y', 'z', 'x'), ('z', 'x', 'y'), ('x', 'y', 'z'))
ROW_AXES = ('y', 'x', 'c', 'z')


def torus_side(n_devices):
    side = round((n_devices // 2) ** (1 / 3))
    assert side ** 3 * 2 == n_devices
    return side


def column_parts(model):
    lanes = model // 128
    first = -(-lanes // 3)
    second = -(-(lanes - first) // 2)
    ends = (0, first * 128, (first + second) * 128, model)
    return tuple((ends[p], ends[p + 1]) for p in range(3))


def steps(total, size):
    return [(lo, min(size, total - lo)) for lo in range(0, total, size)]


def rms_rows(rows, scale):
    as_float = rows.astype(F32)
    inv_rms = lax.rsqrt(jnp.mean(as_float * as_float, axis=-1, keepdims=True) + RMS_EPS)
    return (as_float * inv_rms * scale.astype(F32)).astype(BF16)


def dot(a, b):
    return jnp.dot(a, b, preferred_element_type=F32)


def kernel(*refs, names, side, parts, capacity, head_dim, f_chunk, d_chunk):
    r = types.SimpleNamespace(**dict(zip(names, refs)))
    each = lambda name: [getattr(r, name + str(p)) for p in range(3)]
    slots = capacity // N_CHUNKS
    members = side * side * 2
    mates = side * 2
    rows_block = members * slots
    tokens, model = r.hidden.shape
    me = {axis: lax.axis_index(axis) for axis in AXES}


    def rows_of(ref, p, chunk, place, free):
        spot = [pl.ds(0, side) if axis in free else place[axis] for axis in ROW_AXES]
        return ref.at[tuple([chunk] + spot)]

    def ordered(where):
        return tuple(where[axis] for axis in ROW_AXES if axis in where)

    def device(place):
        return tuple(place[axis] for axis in AXES)

    def axis_peer(axis, offset):
        return {**me, axis: lax.rem(me[axis] + offset, side)}

    def mate_peer(axis, offset):
        return {
            **me,
            axis: lax.rem(me[axis] + offset // 2, side),
            'c': lax.rem(me['c'] + lax.rem(offset, 2), 2),
        }

    def remote(src, dst, send_sem, recv_sem, place):
        return pltpu.make_async_remote_copy(
            src_ref=src, dst_ref=dst, send_sem=send_sem, recv_sem=recv_sem, device_id=device(place), device_id_type=MESH
        )

    def wait_bytes(ref, sem):
        pltpu.make_async_copy(ref, ref, sem).wait()

    def expert_key(place, core, slot):
        return (((place['z'] * side + place['y']) * side + place['x']) * 2 + core) * capacity + slot

    def plane_keys(p, shape, chunk):
        first, second, _ = BACK[p]
        row = lax.broadcasted_iota(I32, shape, 1)
        which, slot = row // slots, lax.rem(row, slots)
        pair = which // 2
        place = {**me, second: pair // side, first: lax.rem(pair, side)}
        return expert_key(place, lax.rem(which, 2), slot + chunk * slots)

    def mate_keys(p, shape):
        row = lax.broadcasted_iota(I32, shape, 0)
        block, slot = row // slots, lax.rem(row, slots)
        chunk, mate = block // mates, lax.rem(block, mates)
        place = {**me, OUT[p][2]: mate // 2}
        return expert_key(place, lax.rem(mate, 2), slot + chunk * slots)

    tok, far, sends, arrivals, outputs = each('tok'), each('far'), each('send'), each('arrive'), each('output')
    middles, results, sums, others = each('middle'), each('result'), each('sum'), each('other')
    widths = [hi - lo for lo, hi in parts]


    band = min(32, tokens)

    def bands(body):
        lax.fori_loop(0, tokens // band, lambda i, c: (body(pl.ds(pl.multiple_of(i * band, band), band)), c)[1], 0)

    def one_row(scale):
        lines = scale[...].astype(F32)
        return jnp.concatenate([lines[i : i + 1, :] for i in range(lines.shape[0])], axis=1)

    def norm_both(here):
        normed = rms_rows(r.hidden[here, :], one_row(r.moe_scale))
        for p, (lo, hi) in enumerate(parts):
            tok[p][me[OUT[p][0]], here, :] = normed[:, lo:hi]
        r.rows[here, :] = rms_rows(r.hidden[here, :], one_row(r.attn_scale))

    bands(norm_both)
    keys_t = r.ids_t[...] * capacity + r.slots_t[...]
    for p in range(3):
        r.all_keys[p, me[OUT[p][1]], me[OUT[p][0]]] = keys_t
    pairs = ((r.gate_hbm, r.gate), (r.up_hbm, r.up), (r.down_hbm, r.down))
    loads = [pltpu.make_async_copy(src, dst, r.weight_sem.at[i]) for i, (src, dst) in enumerate(pairs)]
    for load in loads:
        load.start()

    def send_far(p, d):
        for offset in range(1, side):
            here = me[OUT[p][1]]
            remote(
                tok[p].at[d],
                far[p].at[here, d],
                r.far_send.at[p],
                r.far_recv.at[p, offset - 1],
                axis_peer(OUT[p][1], offset),
            ).start()

    for offset in range(1, side):
        for p in range(3):
            spot, place = me[OUT[p][0]], axis_peer(OUT[p][0], offset)
            remote(
                tok[p].at[spot], tok[p].at[spot], r.tok_send.at[p, offset - 1], r.tok_recv.at[p, offset - 1], place
            ).start()
            keys = r.all_keys.at[p, me[OUT[p][1]], spot]
            remote(keys, keys, r.key_send.at[p], r.key_recv.at[p], place).start()
    for p in range(3):
        send_far(p, me[OUT[p][0]])


    ring = r.ring
    ring_sem = r.ring_sem

    def stream(n_steps, group, source, body):
        ahead = RING // group * group - group

        def copy(i, s):
            slot = lax.rem(i * group + s, RING // group * group)
            return pltpu.make_async_copy(source(i, s), ring.at[slot], ring_sem.at[slot])

        for i in range(min(ahead // group, n_steps)):
            for s in range(group):
                copy(i, s).start()

        def step(i, carry):
            @pl.when(i + ahead // group < n_steps)
            def _():
                for s in range(group):
                    copy(i + ahead // group, s).start()

            for s in range(group):
                copy(i, s).wait()
            body(i, [ring.at[lax.rem(i * group + s, RING // group * group)] for s in range(group)])
            return carry

        lax.fori_loop(0, n_steps, step, 0)

    def col_tile(i):
        return pl.ds(pl.multiple_of(i * TILE, TILE), TILE)

    def turned(y):
        return y * r.cos[...] + pltpu.roll(y, head_dim // 2, 1) * r.sin[...]

    def project(weight, out, rotary):
        def body(i, tiles):
            y = dot(r.rows[...], tiles[0][...])
            if rotary:
                y = jnp.concatenate([turned(y[:, lo : lo + head_dim]) for lo in range(0, TILE, head_dim)], axis=1)
            out[:, col_tile(i)] = y.astype(BF16)

        stream(weight.shape[1] // TILE, 1, lambda i, s: weight.at[:, col_tile(i)], body)

    project(r.w_query, r.query, True)
    project(r.w_key, r.key, True)
    project(r.w_value, r.value, False)


    logits = sum(dot(tok[p][me[OUT[p][0]]], r.w_router[lo:hi, :]) for p, (lo, hi) in enumerate(parts))
    top_k = r.ids_t.shape[0]
    gap = jnp.zeros((128 - 3 * top_k, tokens), F32)
    blank = jnp.zeros((top_k, tokens), F32)
    info = jnp.concatenate([keys_t.astype(F32), blank, r.ids_t[...].astype(F32), gap], axis=0).T
    lane = lax.broadcasted_iota(I32, logits.shape, 1).astype(F32)
    picked = [
        jnp.sum(jnp.where(lane == info[:, 2 * top_k + j : 2 * top_k + j + 1], logits, 0.0), axis=1, keepdims=True)
        for j in range(top_k)
    ]
    peak = functools.reduce(jnp.maximum, picked)
    powers = [jnp.exp(v - peak) for v in picked]
    norm = functools.reduce(jnp.add, powers)
    lane = lax.broadcasted_iota(I32, info.shape, 1)
    for j in range(top_k):
        info = jnp.where(lane == top_k + j, powers[j] / norm, info)
    r.my_gates[...] = info
    for p in range(3):
        r.line_gates[p, me[BACK[p][2]]] = info


    def hand_on(offset):
        for p in range(3):
            d = lax.rem(me[OUT[p][0]] + side - offset, side)
            wait_bytes(tok[p].at[d], r.tok_recv.at[p, offset - 1])
            send_far(p, d)

    for offset in range(1, side):
        hand_on(offset)
    for p in range(3):
        wait_bytes(r.all_keys.at[p, 0, pl.ds(0, side - 1)], r.key_recv.at[p])
        for offset in range(1, side):
            keys = r.all_keys.at[p, me[OUT[p][1]]]
            remote(
                keys, keys, r.far_key_send.at[p], r.far_key_recv.at[p, offset - 1], axis_peer(OUT[p][1], offset)
            ).start()
    for offset in range(1, side):
        for p in range(3):
            axis = BACK[p][2]
            remote(
                r.my_gates, r.line_gates.at[p, me[axis]], r.gate_send.at[p], r.gate_recv.at[p], axis_peer(axis, offset)
            ).start()


    n_heads = r.query.shape[1] // head_dim
    per_key = r.query.shape[1] // r.key.shape[1]
    causal = lax.broadcasted_iota(I32, (tokens, tokens), 0) >= lax.broadcasted_iota(I32, (tokens, tokens), 1)

    def one_head(h, carry):
        cols = pl.ds(pl.multiple_of(h * head_dim, head_dim), head_dim)
        key_cols = pl.ds(pl.multiple_of(h // per_key * head_dim, head_dim), head_dim)
        scores = lax.dot_general(
            r.query[:, cols], r.key[:, key_cols], (((1,), (1,)), ((), ())), preferred_element_type=F32
        )
        scores = jnp.where(causal, scores * head_dim ** -0.5, -jnp.inf)
        power = jnp.exp(scores - jnp.max(scores, axis=1, keepdims=True))
        prob = (power / jnp.sum(power, axis=1, keepdims=True)).astype(BF16)
        r.query[:, cols] = dot(prob, r.value[:, key_cols]).astype(BF16)
        return carry


    stage = r.stage
    blocks = N_CHUNKS * mates
    out_mate = [me[OUT[p][2]] * 2 + me['c'] for p in range(3)]
    back_mate = [me[BACK[p][0]] * 2 + me['c'] for p in range(3)]

    def pick_rows(p, i, d, slot, source, wanted):
        keys = r.all_keys[p, i, d]
        for lo, n in steps(tokens, 128):
            hit = wanted[:, 0:n] == keys[0:1, lo : lo + n]
            for j in range(1, top_k):
                hit = jnp.logical_or(hit, wanted[:, 0:n] == keys[j : j + 1, lo : lo + n])
            r.split[0 : blocks * slots, lo : lo + n] = jnp.where(hit, 1.0, 0.0).astype(BF16)
        for lo, n in steps(widths[p], TILE):
            found = dot(r.split[0 : blocks * slots, 0:tokens], source[:, lo : lo + n]).astype(BF16)
            stage[slot, 0:blocks, :, lo : lo + n] = found.reshape(blocks, slots, n)

    def flush(p, i, d, slot):
        a, b = ordered({OUT[p][1]: i, OUT[p][0]: d})
        return pltpu.make_async_copy(
            stage.at[slot, pl.ds(0, blocks), :, pl.ds(0, widths[p])],
            sends[p].at[pl.ds(0, blocks), a, b],
            r.stage_sem.at[slot],
        )

    def keep(p, i, d, slot, chunk):
        spot = {**me, OUT[p][1]: i, OUT[p][0]: d}
        return pltpu.make_async_copy(
            stage.at[slot, chunk * mates + out_mate[p], :, pl.ds(0, widths[p])],
            arrivals[p].at[(chunk,) + ordered(spot)],
            r.keep_sem.at[slot, chunk],
        )

    wanted = [mate_keys(p, (blocks * slots, min(128, tokens))) for p in range(3)]

    def send_rows(p, chunk, i):
        near, far_axis, axis = OUT[p]
        free = (near,) if i is not None else (near, far_axis)
        a, b = ordered({far_axis: pl.ds(0, side) if i is None else i, near: pl.ds(0, side)})
        group_place = me if i is None else {**me, far_axis: i}

        def one_mate(offset, c):
            place = mate_peer(axis, offset)
            remote(
                sends[p].at[chunk * mates + place[axis] * 2 + place['c'], a, b],
                rows_of(arrivals[p], p, chunk, group_place, free),
                r.go_send.at[chunk, p],
                r.go_recv.at[chunk, p],
                place,
            ).start()
            return c

        lax.fori_loop(1, mates, one_mate, 0)

    def pick_group(offset):
        for p in range(3):
            i = lax.rem(me[OUT[p][1]] + side - offset, side)
            if offset:
                wait_bytes(r.all_keys.at[p, 0], r.far_key_recv.at[p, offset - 1])
                wait_bytes(far[p].at[0], r.far_recv.at[p, offset - 1])

            def load(d, slot):
                return pltpu.make_async_copy(
                    far[p].at[i, d], r.source.at[slot, :, pl.ds(0, widths[p])], r.source_sem.at[slot]
                )

            if offset:
                load(0, 0).start()

            def one_source(d, c):
                slot = lax.rem(d, 2)
                if offset:

                    @pl.when(d + 1 < side)
                    def _():
                        load(d + 1, 1 - slot).start()

                    load(d, slot).wait()

                @pl.when(d >= 2)
                def _():
                    flush(p, i, d - 2, slot).wait()
                    for chunk in range(N_CHUNKS):
                        keep(p, i, d - 2, slot, chunk).wait()

                pick_rows(p, i, d, slot, r.source.at[slot] if offset else tok[p].at[d], wanted[p])
                flush(p, i, d, slot).start()
                for chunk in range(N_CHUNKS):
                    keep(p, i, d, slot, chunk).start()
                return c

            lax.fori_loop(0, side, one_source, 0)
            for d in range(side - 2, side):
                flush(p, i, d, d % 2).wait()
                for chunk in range(N_CHUNKS):
                    keep(p, i, d, d % 2, chunk).wait()
            send_rows(p, 0, i)

    def heads(part, n_parts):
        lax.fori_loop(n_heads * part // n_parts, n_heads * (part + 1) // n_parts, one_head, 0)

    heads(0, 2)
    pick_group(0)
    for offset in range(1, side):
        heads(side - 2 + offset, 2 * (side - 1))
        pick_group(offset)
    for chunk in range(1, N_CHUNKS):
        for p in range(3):
            send_rows(p, chunk, None)


    out_split = n_heads * head_dim // model

    def out_body(i, tiles):
        total = r.hidden[:, col_tile(i)].astype(F32)
        attended = dot(r.query[:, 0:model], tiles[0][...])
        for s in range(1, out_split):
            attended += dot(r.query[:, s * model : (s + 1) * model], tiles[s][...])
        r.attended[:, col_tile(i)] = (total + attended).astype(BF16)

    stream(model // TILE, out_split, lambda i, s: r.w_out.at[pl.ds(s * model, model), col_tile(i)], out_body)

    def norm_attended(here):
        r.rows[here, :] = rms_rows(r.attended[here, :], one_row(r.ffn_scale))

    bands(norm_attended)

    def act_body(i, tiles):
        z = dot(r.rows[...], tiles[0][...])
        u = dot(r.rows[...], tiles[1][...])
        r.act[:, col_tile(i)] = (jax.nn.silu(z) * u).astype(BF16)

    ff_dim = r.ffn_gate.shape[1]
    stream(
        ff_dim // TILE, 2, lambda i, s: (r.ffn_gate, r.ffn_up)[s].at[:, col_tile(i)], act_body
    )
    down_split = ff_dim // model

    def down_body(i, tiles):
        total = dot(r.act[:, 0:model], tiles[0][...])
        for s in range(1, down_split):
            total += dot(r.act[:, s * model : (s + 1) * model], tiles[s][...])
        r.dense[:, col_tile(i)] = r.attended[:, col_tile(i)].astype(F32) + total

    stream(model // TILE, down_split, lambda i, s: r.ffn_down.at[pl.ds(s * model, model), col_tile(i)], down_body)


    for load in loads:
        load.wait()
    x_buf, y_buf, hidden_buf = r.x_buf, r.y_buf, r.hidden_buf
    group = x_buf.shape[1:-1]
    rows = math.prod(group)
    width = hidden_buf.shape[1]

    def fetch(chunk, y, slot):
        return [
            pltpu.make_async_copy(
                arrivals[p].at[chunk, y], x_buf.at[slot, :, :, :, :, pl.ds(lo, hi - lo)], r.in_sem.at[slot, p]
            )
            for p, (lo, hi) in enumerate(parts)
        ]

    def put(chunk, y, slot):
        return [
            pltpu.make_async_copy(
                y_buf.at[slot, :, :, :, :, pl.ds(lo, hi - lo)], outputs[p].at[chunk, y], r.out_sem.at[slot, p]
            )
            for p, (lo, hi) in enumerate(parts)
        ]

    def keep_own(chunk, y, slot, p):
        lo, hi = parts[p]
        free = BACK[p][1:]
        spot = [pl.ds(0, side) if axis in free else me[axis] for axis in ROW_AXES[1:]]
        mine = pltpu.make_async_copy(
            y_buf.at[tuple([slot] + spot + [pl.ds(0, slots), pl.ds(lo, hi - lo)])],
            middles[p].at[
                (chunk,) + ordered({axis: y if axis == 'y' else pl.ds(0, side) for axis in free}) + (back_mate[p],)
            ],
            r.own_sem.at[slot, p],
        )
        return mine, (None if 'y' in free else y == me['y'])

    def start_put(chunk, y, slot):
        for copy in put(chunk, y, slot):
            copy.start()
        for p in range(3):
            copy, when = keep_own(chunk, y, slot, p)
            if when is None:
                copy.start()
            else:
                pl.when(when)(copy.start)

    def wait_put(chunk, y, slot):
        for copy in put(chunk, y, slot):
            copy.wait()
        for p in range(3):
            copy, when = keep_own(chunk, y, slot, p)
            if when is None:
                copy.wait()
            else:
                pl.when(when)(copy.wait)

    def expert_chunk(chunk):
        for p in range(3):
            wait_bytes(sends[p].at[pl.ds(0, mates - 1)], r.go_recv.at[chunk, p])
        for copy in fetch(chunk, 0, 0):
            copy.start()

        def one_tile(y, c):
            slot = lax.rem(y, 2)

            @pl.when(y + 1 < side)
            def _():
                for copy in fetch(chunk, y + 1, 1 - slot):
                    copy.start()

            for copy in fetch(chunk, y, slot):
                copy.wait()

            @pl.when(y >= 2)
            def _():
                wait_put(chunk, y - 2, slot)

            for lo in range(0, width, f_chunk):
                cols = slice(lo, lo + f_chunk)
                z = dot(x_buf[slot].reshape(rows, model), r.gate[:, cols])
                u = dot(x_buf[slot].reshape(rows, model), r.up[:, cols])
                hidden_buf[:, cols] = (jax.nn.silu(z) * u).astype(BF16)
            for lo in range(0, model, d_chunk):
                cols = slice(lo, lo + d_chunk)
                y_rows = dot(hidden_buf[...], r.down[:, cols]).astype(BF16)
                y_buf[slot, :, :, :, :, cols] = y_rows.reshape(group + (d_chunk,))
            start_put(chunk, y, slot)
            return c

        lax.fori_loop(0, side, one_tile, 0)
        for y in range(side - 2, side):
            wait_put(chunk, y, y % 2)

        def one_mate(offset, c):
            for p in range(3):
                place = mate_peer(BACK[p][0], offset)
                remote(
                    rows_of(outputs[p], p, chunk, place, BACK[p][1:]),
                    middles[p].at[chunk, pl.ds(0, side), pl.ds(0, side), back_mate[p]],
                    r.back_send.at[chunk, p],
                    r.back_recv.at[chunk, p],
                    place,
                ).start()
            return c

        lax.fori_loop(1, mates, one_mate, 0)

    def middle_rows(p, chunk, i, d):
        return middles[p].at[(chunk,) + ordered({BACK[p][1]: i, BACK[p][2]: d})]

    def pass_on(chunk):
        for p in range(3):
            wait_bytes(middles[p].at[chunk, pl.ds(0, side), pl.ds(0, side), pl.ds(0, mates - 1)], r.back_recv.at[chunk, p])
            for offset in range(1, side):
                axis = BACK[p][1]
                place = axis_peer(axis, offset)
                remote(
                    middle_rows(p, chunk, place[axis], pl.ds(0, side)),
                    results[p].at[chunk, pl.ds(0, side), me[axis]],
                    r.home_send.at[chunk, p],
                    r.home_recv.at[chunk, p],
                    place,
                ).start()


    split = r.split
    lanes = min(128, rows_block)

    def weigh_chunk(chunk, carry):
        @pl.when(chunk == 1)
        def _():
            pass_on(N_CHUNKS - 1)

        for p in range(3):
            wait_bytes(results[p].at[chunk, pl.ds(0, side), pl.ds(0, side - 1)], r.home_recv.at[chunk, p])

        def source_of(p, n):
            return lax.rem(me[BACK[p][2]] + 1 + n, side)

        def load(p, n, slot):
            copies = []
            for offset in range(side):
                i, d = lax.rem(me[BACK[p][1]] + offset, side), source_of(p, n)
                copies.append(
                    pltpu.make_async_copy(
                        results[p].at[chunk, d, i] if offset else middle_rows(p, chunk, i, d),
                        stage.at[slot, pl.ds(i * mates, mates), :, pl.ds(0, widths[p])],
                        r.load_sem.at[slot, offset],
                    )
                )
            return copies

        for copy in load(0, 0, 0):
            copy.start()

        def one_source(n, c):
            for p in range(3):
                d = source_of(p, n)
                slot = lax.rem(n + p, 2)

                @pl.when(n + p // 2 < side)
                def _():
                    for copy in load((p + 1) % 3, n + p // 2, 1 - slot):
                        copy.start()

                held = plane_keys(p, (1, rows_block), chunk).astype(F32)
                info = r.line_gates[p, d]
                keys = [jnp.broadcast_to(info[:, j : j + 1], (tokens, lanes)) for j in range(top_k)]
                gates = [jnp.broadcast_to(info[:, top_k + j : top_k + j + 1], (tokens, lanes)) for j in range(top_k)]
                for lo in range(0, rows_block, lanes):
                    here = held[:, lo : lo + lanes]
                    weight = jnp.zeros((tokens, lanes), F32)
                    for j in range(top_k):
                        weight = jnp.where(here == keys[j], gates[j], weight)
                    high = weight.astype(BF16)
                    rest = weight - high.astype(F32)
                    middle = rest.astype(BF16)
                    low = (rest - middle.astype(F32)).astype(BF16)
                    split[0:tokens, lo : lo + lanes] = high
                    split[tokens : 2 * tokens, lo : lo + lanes] = middle
                    split[2 * tokens : 3 * tokens, lo : lo + lanes] = low
                for copy in load(p, n, slot):
                    copy.wait()
                for lo, size in steps(widths[p], TILE):
                    y = stage[slot, 0:members, :, lo : lo + size].reshape(rows_block, size)
                    both = dot(split[...], y)
                    total = both[0:tokens] + (both[tokens : 2 * tokens] + both[2 * tokens : 3 * tokens])

                    @pl.when(chunk == 0)
                    def _():
                        sums[p][d, :, lo : lo + size] = total

                    @pl.when(chunk > 0)
                    def _():
                        sums[p][d, :, lo : lo + size] += total

                @pl.when(jnp.logical_and(chunk == N_CHUNKS - 1, n < side - 1))
                def _():
                    remote(
                        sums[p].at[d], others[p].at[n], r.sum_send.at[p], r.sum_recv.at[p], {**me, BACK[p][2]: d}
                    ).start()

            return c

        return lax.fori_loop(0, side, one_source, carry)


    def experts_and_back(chunk, carry):
        expert_chunk(chunk)
        pl.when(chunk >= 1)(lambda: pass_on(chunk - 1))
        return carry

    lax.fori_loop(0, N_CHUNKS, experts_and_back, 0)
    for p in range(3):
        wait_bytes(r.line_gates.at[p, pl.ds(0, side - 1)], r.gate_recv.at[p])
    lax.fori_loop(0, N_CHUNKS, weigh_chunk, 0)
    for p, (lo, hi) in enumerate(parts):
        wait_bytes(others[p], r.sum_recv.at[p])

        def finish(here):
            moe = sums[p][me[BACK[p][2]], here, :]
            for offset in range(1, side):
                moe += others[p][offset - 1, here, :]
            r.out[here, lo:hi] = (r.dense[here, lo:hi] + moe).astype(BF16)

        bands(finish)


    for p in range(3):
        for offset in range(1, side):
            wait_bytes(tok[p].at[0], r.tok_send.at[p, offset - 1])
        wait_bytes(r.all_keys.at[p, 0, pl.ds(0, side - 1)], r.key_send.at[p])
        wait_bytes(far[p].at[pl.ds(0, side - 1)], r.far_send.at[p])
        wait_bytes(r.all_keys.at[p, pl.ds(0, side - 1)], r.far_key_send.at[p])
        wait_bytes(r.line_gates.at[p, pl.ds(0, side - 1)], r.gate_send.at[p])
        wait_bytes(others[p], r.sum_send.at[p])
        for chunk in range(N_CHUNKS):
            wait_bytes(sends[p].at[pl.ds(0, mates - 1)], r.go_send.at[chunk, p])
            wait_bytes(middles[p].at[chunk, pl.ds(0, side), pl.ds(0, side), pl.ds(0, mates - 1)], r.back_send.at[chunk, p])
            wait_bytes(results[p].at[chunk, pl.ds(0, side), pl.ds(0, side - 1)], r.home_send.at[chunk, p])


def layer_pair(small, large, side, capacity, head_dim):
    tokens, model = small['hidden'].shape
    top_k, width = small['ids_t'].shape[0], large['gate_hbm'].shape[1]
    key_dim, ff_dim = large['w_key'].shape[1], large['ffn_gate'].shape[1]
    parts = column_parts(model)
    widths = [hi - lo for lo, hi in parts]
    slots, members, mates = capacity // N_CHUNKS, side * side * 2, side * 2
    group = (side, 2, side, slots)
    rows = math.prod(group)
    sds, vmem = jax.ShapeDtypeStruct, pltpu.VMEM
    dma = lambda *shape: pltpu.SemaphoreType.DMA(shape)
    outs = dict(out=sds((tokens, model), BF16))
    scratch = dict(
        rows=vmem((tokens, model), BF16),
        query=vmem((tokens, large['w_query'].shape[1]), BF16),
        key=vmem((tokens, key_dim), BF16),
        value=vmem((tokens, key_dim), BF16),
        attended=vmem((tokens, model), BF16),
        act=vmem((tokens, ff_dim), BF16),
        dense=vmem((tokens, model), F32),
        ring=vmem((RING, model, TILE), BF16),
        all_keys=vmem((3, side, side, top_k, tokens), I32),
        my_gates=vmem((tokens, 128), F32),
        line_gates=vmem((3, side, tokens, 128), F32),
        source=vmem((2, tokens, max(widths)), BF16),
        stage=vmem((2, max(members, N_CHUNKS * mates), slots, max(widths)), BF16),
        split=vmem((3 * tokens, members * slots), BF16),
        gate=vmem((model, width), BF16),
        up=vmem((model, width), BF16),
        down=vmem((width, model), BF16),
        x_buf=vmem((2,) + group + (model,), BF16),
        y_buf=vmem((2,) + group + (model,), BF16),
        hidden_buf=vmem((rows, width), BF16),
        weight_sem=dma(3),
        ring_sem=dma(RING),
        source_sem=dma(2),
        stage_sem=dma(2),
        keep_sem=dma(2, N_CHUNKS),
        in_sem=dma(2, 3),
        out_sem=dma(2, 3),
        own_sem=dma(2, 3),
        load_sem=dma(2, side),
        tok_send=dma(3, side - 1),
        tok_recv=dma(3, side - 1),
        key_send=dma(3),
        key_recv=dma(3),
        far_send=dma(3),
        far_recv=dma(3, side - 1),
        far_key_send=dma(3),
        far_key_recv=dma(3, side - 1),
        gate_send=dma(3),
        gate_recv=dma(3),
        sum_send=dma(3),
        sum_recv=dma(3),
        go_send=dma(N_CHUNKS, 3),
        go_recv=dma(N_CHUNKS, 3),
        back_send=dma(N_CHUNKS, 3),
        back_recv=dma(N_CHUNKS, 3),
        home_send=dma(N_CHUNKS, 3),
        home_recv=dma(N_CHUNKS, 3),
    )
    for p, w in enumerate(widths):
        there = sds((N_CHUNKS, side, side, 2, side, slots, w), BF16)
        outs['far' + str(p)] = sds((side, side, tokens, w), BF16)
        outs['send' + str(p)] = sds((N_CHUNKS * mates, side, side, slots, w), BF16)
        outs['arrive' + str(p)] = there
        outs['output' + str(p)] = there
        outs['middle' + str(p)] = sds((N_CHUNKS, side, side, mates, slots, w), BF16)
        outs['result' + str(p)] = sds((N_CHUNKS, side, side, mates, slots, w), BF16)
        scratch['tok' + str(p)] = vmem((side, tokens, w), BF16)
        scratch['sum' + str(p)] = vmem((side, tokens, w), F32)
        scratch['other' + str(p)] = vmem((side - 1, tokens, w), F32)
    anywhere = pl.BlockSpec(memory_space=pl.ANY)
    local = pl.BlockSpec(memory_space=pltpu.VMEM)
    n_rows = members * side * capacity
    return pl.pallas_call(
        functools.partial(
            kernel,
            names=tuple(small) + tuple(large) + tuple(outs) + tuple(scratch),
            side=side,
            parts=parts,
            capacity=capacity,
            head_dim=head_dim,
            f_chunk=min(256, width),
            d_chunk=min(512, model),
        ),
        out_shape=list(outs.values()),
        in_specs=[local] * len(small) + [anywhere] * len(large),
        out_specs=[local] + [anywhere] * (len(outs) - 1),
        scratch_shapes=list(scratch.values()),
        compiler_params=pltpu.CompilerParams(has_side_effects=True, vmem_limit_bytes=67043328),
        cost_estimate=pl.CostEstimate(flops=6 * n_rows * model * width, bytes_accessed=8 * n_rows * model, transcendentals=0),
    )(*small.values(), *large.values())[0]


def solution(mesh):
    group_size = mesh.shape['ep']
    side = torus_side(group_size)
    torus = jax.sharding.Mesh(mesh.devices.reshape(side, side, side, 2), AXES)
    row_spec = P(AXES, None, None)
    vec_spec = P(None)
    mat_spec = P(None, None)
    cube_spec = P(None, None, None)
    expert_spec = P(AXES, None, None)

    def per_device(hidden, expert_ids, slot_ids, attn_norm, w_query, w_key, w_value, w_out, ffn_norm, ffn_gate, ffn_up, ffn_down, moe_norm, w_router, exp_gate, exp_up, exp_down):
        n_seqs, tokens, model = hidden.shape
        assert n_seqs == 1 and exp_gate.shape[0] == 1
        n_heads, head_dim = w_out.shape[0], w_out.shape[1]
        top_k = expert_ids.shape[2]
        capacity = CAP_FACTOR * tokens * top_k // group_size
        inv_freq = np.float32(ROPE_BASE) ** (np.float32(-2.0) * np.arange(head_dim // 2, dtype=np.float32) / head_dim)
        angles = np.arange(tokens, dtype=np.float32)[:, None] * inv_freq[None, :]
        cos, sin = np.cos(angles), np.sin(angles)
        small = dict(
            hidden=hidden[0],
            attn_scale=attn_norm.reshape(-1, 128),
            moe_scale=moe_norm.reshape(-1, 128),
            ffn_scale=ffn_norm.reshape(-1, 128),
            ids_t=expert_ids[0].T,
            slots_t=slot_ids[0].T,
            w_router=w_router,
            cos=np.concatenate([cos, cos], axis=1).astype(np.float32),
            sin=np.concatenate([-sin, sin], axis=1).astype(np.float32),
        )
        large = dict(
            w_query=w_query,
            w_key=w_key,
            w_value=w_value,
            w_out=w_out.reshape(n_heads * head_dim, model),
            ffn_gate=ffn_gate,
            ffn_up=ffn_up,
            ffn_down=ffn_down,
            gate_hbm=exp_gate[0],
            up_hbm=exp_up[0],
            down_hbm=exp_down[0],
        )
        return layer_pair(small, large, side, capacity, head_dim).reshape(hidden.shape)

    return jax.shard_map(per_device, mesh=torus, in_specs=(row_spec, row_spec, row_spec, vec_spec, mat_spec, mat_spec, mat_spec, cube_spec, vec_spec, mat_spec, mat_spec, mat_spec, vec_spec, mat_spec, expert_spec, expert_spec, expert_spec), out_specs=row_spec, check_vma=False)
```

```python
import functools
import math
import types

import jax
import jax.numpy as jnp
import numpy as np
from jax import lax
from jax.experimental import pallas as pl
from jax.experimental.pallas import tpu as pltpu
from jax.sharding import PartitionSpec as P

RMS_EPS = 1e-6
ROPE_BASE = 10000.0
CAP_FACTOR = 3
N_CHUNKS = 3
RING = 6
TILE = 256
MESH = pl.DeviceIdType.MESH

BF16, F32, I32 = jnp.bfloat16, jnp.float32, jnp.int32

AXES = ('z', 'y', 'x', 'c')
OUT = (('z', 'y', 'x'), ('x', 'z', 'y'), ('y', 'x', 'z'))
BACK = (('y', 'z', 'x'), ('z', 'x', 'y'), ('x', 'y', 'z'))
ROW_AXES = ('y', 'x', 'c', 'z')


def torus_side(n_devices):
    side = round((n_devices // 2) ** (1 / 3))
    assert side ** 3 * 2 == n_devices
    return side


def column_parts(model):
    lanes = model // 128
    first = -(-lanes // 3)
    second = -(-(lanes - first) // 2)
    ends = (0, first * 128, (first + second) * 128, model)
    return tuple((ends[p], ends[p + 1]) for p in range(3))


def steps(total, size):
    return [(lo, min(size, total - lo)) for lo in range(0, total, size)]


def rms_rows(rows, scale):
    as_float = rows.astype(F32)
    inv_rms = lax.rsqrt(jnp.mean(as_float * as_float, axis=-1, keepdims=True) + RMS_EPS)
    return (as_float * inv_rms * scale.astype(F32)).astype(BF16)


def dot(a, b):
    return jnp.dot(a, b, preferred_element_type=F32)


def kernel(*refs, names, side, parts, capacity, head_dim, f_chunk, d_chunk):
    r = types.SimpleNamespace(**dict(zip(names, refs)))
    each = lambda name: [getattr(r, name + str(p)) for p in range(3)]
    slots = capacity // N_CHUNKS
    members = side * side * 2
    mates = side * 2
    assert side in (2, 4)
    relay = side == 4
    strides = (1, side - 1) if relay else (1,)
    order = (0, side - 1, 1, 2) if relay else (0, 1)
    rows_block = members * slots
    tokens, model = r.hidden.shape
    me = {axis: lax.axis_index(axis) for axis in AXES}


    def rows_of(ref, p, chunk, place, free):
        spot = [pl.ds(0, side) if axis in free else place[axis] for axis in ROW_AXES]
        return ref.at[tuple([chunk] + spot)]

    def ordered(where):
        return tuple(where[axis] for axis in ROW_AXES if axis in where)

    def device(place):
        return tuple(place[axis] for axis in AXES)

    def axis_peer(axis, offset):
        return {**me, axis: lax.rem(me[axis] + offset, side)}

    def mate_peer(axis, offset):
        return {
            **me,
            axis: lax.rem(me[axis] + offset // 2, side),
            'c': lax.rem(me['c'] + lax.rem(offset, 2), 2),
        }

    def remote(src, dst, send_sem, recv_sem, place):
        return pltpu.make_async_remote_copy(
            src_ref=src, dst_ref=dst, send_sem=send_sem, recv_sem=recv_sem, device_id=device(place), device_id_type=MESH
        )

    def wait_bytes(ref, sem):
        pltpu.make_async_copy(ref, ref, sem).wait()

    def expert_key(place, core, slot):
        return (((place['z'] * side + place['y']) * side + place['x']) * 2 + core) * capacity + slot

    def plane_keys(p, shape, chunk):
        first, second, _ = BACK[p]
        row = lax.broadcasted_iota(I32, shape, 1)
        which, slot = row // slots, lax.rem(row, slots)
        pair = which // 2
        place = {**me, second: pair // side, first: lax.rem(pair, side)}
        return expert_key(place, lax.rem(which, 2), slot + chunk * slots)

    def mate_keys(p, shape):
        row = lax.broadcasted_iota(I32, shape, 0)
        block, slot = row // slots, lax.rem(row, slots)
        chunk, mate = block // mates, lax.rem(block, mates)
        place = {**me, OUT[p][2]: mate // 2}
        return expert_key(place, lax.rem(mate, 2), slot + chunk * slots)

    tok, far, sends, arrivals, outputs = each('tok'), each('far'), each('send'), each('arrive'), each('output')
    middles, results, sums, others = each('middle'), each('result'), each('sum'), each('other')
    widths = [hi - lo for lo, hi in parts]


    band = min(32, tokens)

    def bands(body):
        lax.fori_loop(0, tokens // band, lambda i, c: (body(pl.ds(pl.multiple_of(i * band, band), band)), c)[1], 0)

    def one_row(scale):
        lines = scale[...].astype(F32)
        return jnp.concatenate([lines[i : i + 1, :] for i in range(lines.shape[0])], axis=1)

    def norm_both(here):
        normed = rms_rows(r.hidden[here, :], one_row(r.moe_scale))
        for p, (lo, hi) in enumerate(parts):
            tok[p][me[OUT[p][0]], here, :] = normed[:, lo:hi]
        r.rows[here, :] = rms_rows(r.hidden[here, :], one_row(r.attn_scale))

    bands(norm_both)
    keys_t = r.ids_t[...] * capacity + r.slots_t[...]
    for p in range(3):
        r.all_keys[p, me[OUT[p][1]], me[OUT[p][0]]] = keys_t
    pairs = ((r.gate_hbm, r.gate), (r.up_hbm, r.up), (r.down_hbm, r.down))
    loads = [pltpu.make_async_copy(src, dst, r.weight_sem.at[i]) for i, (src, dst) in enumerate(pairs)]
    for load in loads:
        load.start()

    half = tokens // 2
    halves = (pl.ds(0, half), pl.ds(half, half))

    def neighbour(axis, k):
        return lax.rem(me[axis] + side - strides[k], side)

    def send_far(p, n):
        near, axis, _ = OUT[p]
        d = lax.rem(me[near] + order[n], side)
        for k, stride in enumerate(strides):
            remote(
                tok[p].at[d], far[p].at[me[axis], d], r.far_send.at[p], r.far_recv.at[p, k, n], axis_peer(axis, stride)
            ).start()

    def pass_far(n):
        for k, stride in enumerate(strides):
            for p in range(3):
                near, axis, _ = OUT[p]
                d = lax.rem(me[near] + order[n], side)
                wait_bytes(tok[p].at[0], r.far_recv.at[p, k, n])
                if relay:
                    block = far[p].at[neighbour(axis, k), d, halves[k]]
                    remote(block, block, r.far_send.at[p], r.far_half.at[p, k, n], axis_peer(axis, stride)).start()

    for k, stride in enumerate(strides):
        for p in range(3):
            axis = OUT[p][0]
            block = tok[p].at[me[axis]]
            remote(block, block, r.tok_send.at[p], r.tok_recv.at[p, k], axis_peer(axis, stride)).start()
    for p in range(3):
        send_far(p, 0)
    for offset in range(1, side):
        for p in range(3):
            axis = OUT[p][0]
            keys = r.all_keys.at[p, me[OUT[p][1]], me[axis]]
            remote(keys, keys, r.key_send.at[p], r.key_recv.at[p], axis_peer(axis, offset)).start()


    ring = r.ring
    ring_sem = r.ring_sem

    def stream(n_steps, group, source, body):
        ahead = RING // group * group - group

        def copy(i, s):
            slot = lax.rem(i * group + s, RING // group * group)
            return pltpu.make_async_copy(source(i, s), ring.at[slot], ring_sem.at[slot])

        for i in range(min(ahead // group, n_steps)):
            for s in range(group):
                copy(i, s).start()

        def step(i, carry):
            @pl.when(i + ahead // group < n_steps)
            def _():
                for s in range(group):
                    copy(i + ahead // group, s).start()

            for s in range(group):
                copy(i, s).wait()
            body(i, [ring.at[lax.rem(i * group + s, RING // group * group)] for s in range(group)])
            return carry

        lax.fori_loop(0, n_steps, step, 0)

    def col_tile(i):
        return pl.ds(pl.multiple_of(i * TILE, TILE), TILE)

    def turned(y):
        return y * r.cos[...] + pltpu.roll(y, head_dim // 2, 1) * r.sin[...]

    def project(weight, out, rotary):
        def body(i, tiles):
            y = dot(r.rows[...], tiles[0][...])
            if rotary:
                y = jnp.concatenate([turned(y[:, lo : lo + head_dim]) for lo in range(0, TILE, head_dim)], axis=1)
            out[:, col_tile(i)] = y.astype(BF16)

        stream(weight.shape[1] // TILE, 1, lambda i, s: weight.at[:, col_tile(i)], body)

    project(r.w_query, r.query, True)
    project(r.w_key, r.key, True)
    project(r.w_value, r.value, False)


    logits = sum(dot(tok[p][me[OUT[p][0]]], r.w_router[lo:hi, :]) for p, (lo, hi) in enumerate(parts))
    top_k = r.ids_t.shape[0]
    gap = jnp.zeros((128 - 3 * top_k, tokens), F32)
    blank = jnp.zeros((top_k, tokens), F32)
    info = jnp.concatenate([keys_t.astype(F32), blank, r.ids_t[...].astype(F32), gap], axis=0).T
    lane = lax.broadcasted_iota(I32, logits.shape, 1).astype(F32)
    picked = [
        jnp.sum(jnp.where(lane == info[:, 2 * top_k + j : 2 * top_k + j + 1], logits, 0.0), axis=1, keepdims=True)
        for j in range(top_k)
    ]
    peak = functools.reduce(jnp.maximum, picked)
    powers = [jnp.exp(v - peak) for v in picked]
    norm = functools.reduce(jnp.add, powers)
    lane = lax.broadcasted_iota(I32, info.shape, 1)
    for j in range(top_k):
        info = jnp.where(lane == top_k + j, powers[j] / norm, info)
    r.my_gates[...] = info
    for p in range(3):
        r.line_gates[p, me[BACK[p][2]]] = info


    for k, stride in enumerate(strides):
        for p in range(3):
            axis = OUT[p][0]
            wait_bytes(tok[p].at[0], r.tok_recv.at[p, k])
            if relay:
                block = tok[p].at[neighbour(axis, k), halves[k]]
                remote(block, block, r.tok_send.at[p], r.tok_half.at[p, k], axis_peer(axis, stride)).start()
            send_far(p, 1 + k)
    pass_far(0)
    if relay:
        for p in range(3):
            for k in range(2):
                wait_bytes(tok[p].at[0, halves[k]], r.tok_half.at[p, k])
            send_far(p, 3)
    for p in range(3):
        wait_bytes(r.all_keys.at[p, 0, pl.ds(0, side - 1)], r.key_recv.at[p])
        for offset in range(1, side):
            keys = r.all_keys.at[p, me[OUT[p][1]]]
            remote(
                keys, keys, r.far_key_send.at[p], r.far_key_recv.at[p, offset - 1], axis_peer(OUT[p][1], offset)
            ).start()
    for offset in range(1, side):
        for p in range(3):
            axis = BACK[p][2]
            remote(
                r.my_gates, r.line_gates.at[p, me[axis]], r.gate_send.at[p], r.gate_recv.at[p], axis_peer(axis, offset)
            ).start()


    n_heads = r.query.shape[1] // head_dim
    per_key = r.query.shape[1] // r.key.shape[1]
    causal = lax.broadcasted_iota(I32, (tokens, tokens), 0) >= lax.broadcasted_iota(I32, (tokens, tokens), 1)

    def one_head(h, carry):
        cols = pl.ds(pl.multiple_of(h * head_dim, head_dim), head_dim)
        key_cols = pl.ds(pl.multiple_of(h // per_key * head_dim, head_dim), head_dim)
        scores = lax.dot_general(
            r.query[:, cols], r.key[:, key_cols], (((1,), (1,)), ((), ())), preferred_element_type=F32
        )
        scores = jnp.where(causal, scores * head_dim ** -0.5, -jnp.inf)
        power = jnp.exp(scores - jnp.max(scores, axis=1, keepdims=True))
        prob = (power / jnp.sum(power, axis=1, keepdims=True)).astype(BF16)
        r.query[:, cols] = dot(prob, r.value[:, key_cols]).astype(BF16)
        return carry


    stage = r.stage
    blocks = N_CHUNKS * mates
    out_mate = [me[OUT[p][2]] * 2 + me['c'] for p in range(3)]
    back_mate = [me[BACK[p][0]] * 2 + me['c'] for p in range(3)]

    def pick_rows(p, i, d, slot, source, wanted):
        keys = r.all_keys[p, i, d]
        for lo, n in steps(tokens, 128):
            hit = wanted[:, 0:n] == keys[0:1, lo : lo + n]
            for j in range(1, top_k):
                hit = jnp.logical_or(hit, wanted[:, 0:n] == keys[j : j + 1, lo : lo + n])
            r.split[0 : blocks * slots, lo : lo + n] = jnp.where(hit, 1.0, 0.0).astype(BF16)
        for lo, n in steps(widths[p], TILE):
            found = dot(r.split[0 : blocks * slots, 0:tokens], source[:, lo : lo + n]).astype(BF16)
            stage[slot, 0:blocks, :, lo : lo + n] = found.reshape(blocks, slots, n)

    def flush(p, i, d, slot):
        a, b = ordered({OUT[p][1]: i, OUT[p][0]: d})
        return pltpu.make_async_copy(
            stage.at[slot, pl.ds(0, blocks), :, pl.ds(0, widths[p])],
            sends[p].at[pl.ds(0, blocks), a, b],
            r.stage_sem.at[slot],
        )

    def keep(p, i, d, slot, chunk):
        spot = {**me, OUT[p][1]: i, OUT[p][0]: d}
        return pltpu.make_async_copy(
            stage.at[slot, chunk * mates + out_mate[p], :, pl.ds(0, widths[p])],
            arrivals[p].at[(chunk,) + ordered(spot)],
            r.keep_sem.at[slot, chunk],
        )

    wanted = [mate_keys(p, (blocks * slots, min(128, tokens))) for p in range(3)]

    def send_rows(p, chunk, i):
        near, far_axis, axis = OUT[p]
        free = (near,) if i is not None else (near, far_axis)
        a, b = ordered({far_axis: pl.ds(0, side) if i is None else i, near: pl.ds(0, side)})
        group_place = me if i is None else {**me, far_axis: i}

        def one_mate(offset, c):
            place = mate_peer(axis, offset)
            remote(
                sends[p].at[chunk * mates + place[axis] * 2 + place['c'], a, b],
                rows_of(arrivals[p], p, chunk, group_place, free),
                r.go_send.at[chunk, p],
                r.go_recv.at[chunk, p],
                place,
            ).start()
            return c

        lax.fori_loop(1, mates, one_mate, 0)

    def pick_group(offset):
        for p in range(3):
            i = lax.rem(me[OUT[p][1]] + side - offset, side)
            if offset:
                wait_bytes(r.all_keys.at[p, 0], r.far_key_recv.at[p, offset - 1])
            if relay and offset == 2:
                for n in range(side):
                    for k in range(2):
                        wait_bytes(tok[p].at[0, halves[k]], r.far_half.at[p, k, n])

            def load(d, slot):
                return pltpu.make_async_copy(
                    far[p].at[i, d], r.source.at[slot, :, pl.ds(0, widths[p])], r.source_sem.at[slot]
                )

            if offset:
                load(0, 0).start()

            def one_source(d, c):
                slot = lax.rem(d, 2)
                if offset:

                    @pl.when(d + 1 < side)
                    def _():
                        load(d + 1, 1 - slot).start()

                    load(d, slot).wait()

                @pl.when(d >= 2)
                def _():
                    flush(p, i, d - 2, slot).wait()
                    for chunk in range(N_CHUNKS):
                        keep(p, i, d - 2, slot, chunk).wait()

                pick_rows(p, i, d, slot, r.source.at[slot] if offset else tok[p].at[d], wanted[p])
                flush(p, i, d, slot).start()
                for chunk in range(N_CHUNKS):
                    keep(p, i, d, slot, chunk).start()
                return c

            lax.fori_loop(0, side, one_source, 0)
            for d in range(side - 2, side):
                flush(p, i, d, d % 2).wait()
                for chunk in range(N_CHUNKS):
                    keep(p, i, d, d % 2, chunk).wait()
            send_rows(p, 0, i)

    def heads(part, n_parts):
        lax.fori_loop(n_heads * part // n_parts, n_heads * (part + 1) // n_parts, one_head, 0)

    pick_group(0)
    for n in range(1, side):
        pass_far(n)
        heads(n - 1, side - 1)
    for offset in (1, 3, 2) if relay else (1,):
        pick_group(offset)
    for chunk in range(1, N_CHUNKS):
        for p in range(3):
            send_rows(p, chunk, None)


    out_split = n_heads * head_dim // model

    def out_body(i, tiles):
        total = r.hidden[:, col_tile(i)].astype(F32)
        attended = dot(r.query[:, 0:model], tiles[0][...])
        for s in range(1, out_split):
            attended += dot(r.query[:, s * model : (s + 1) * model], tiles[s][...])
        r.attended[:, col_tile(i)] = (total + attended).astype(BF16)

    stream(model // TILE, out_split, lambda i, s: r.w_out.at[pl.ds(s * model, model), col_tile(i)], out_body)

    def norm_attended(here):
        r.rows[here, :] = rms_rows(r.attended[here, :], one_row(r.ffn_scale))

    bands(norm_attended)

    def act_body(i, tiles):
        z = dot(r.rows[...], tiles[0][...])
        u = dot(r.rows[...], tiles[1][...])
        r.act[:, col_tile(i)] = (jax.nn.silu(z) * u).astype(BF16)

    ff_dim = r.ffn_gate.shape[1]
    stream(
        ff_dim // TILE, 2, lambda i, s: (r.ffn_gate, r.ffn_up)[s].at[:, col_tile(i)], act_body
    )
    down_split = ff_dim // model

    def down_body(i, tiles):
        total = dot(r.act[:, 0:model], tiles[0][...])
        for s in range(1, down_split):
            total += dot(r.act[:, s * model : (s + 1) * model], tiles[s][...])
        r.dense[:, col_tile(i)] = r.attended[:, col_tile(i)].astype(F32) + total

    stream(model // TILE, down_split, lambda i, s: r.ffn_down.at[pl.ds(s * model, model), col_tile(i)], down_body)


    for load in loads:
        load.wait()
    x_buf, y_buf, hidden_buf = r.x_buf, r.y_buf, r.hidden_buf
    group = x_buf.shape[1:-1]
    rows = math.prod(group)
    width = hidden_buf.shape[1]

    def fetch(chunk, y, slot):
        return [
            pltpu.make_async_copy(
                arrivals[p].at[chunk, y], x_buf.at[slot, :, :, :, :, pl.ds(lo, hi - lo)], r.in_sem.at[slot, p]
            )
            for p, (lo, hi) in enumerate(parts)
        ]

    def put(chunk, y, slot):
        return [
            pltpu.make_async_copy(
                y_buf.at[slot, :, :, :, :, pl.ds(lo, hi - lo)], outputs[p].at[chunk, y], r.out_sem.at[slot, p]
            )
            for p, (lo, hi) in enumerate(parts)
        ]

    def keep_own(chunk, y, slot, p):
        lo, hi = parts[p]
        free = BACK[p][1:]
        spot = [pl.ds(0, side) if axis in free else me[axis] for axis in ROW_AXES[1:]]
        mine = pltpu.make_async_copy(
            y_buf.at[tuple([slot] + spot + [pl.ds(0, slots), pl.ds(lo, hi - lo)])],
            middles[p].at[
                (chunk,) + ordered({axis: y if axis == 'y' else pl.ds(0, side) for axis in free}) + (back_mate[p],)
            ],
            r.own_sem.at[slot, p],
        )
        return mine, (None if 'y' in free else y == me['y'])

    def start_put(chunk, y, slot):
        for copy in put(chunk, y, slot):
            copy.start()
        for p in range(3):
            copy, when = keep_own(chunk, y, slot, p)
            if when is None:
                copy.start()
            else:
                pl.when(when)(copy.start)

    def wait_put(chunk, y, slot):
        for copy in put(chunk, y, slot):
            copy.wait()
        for p in range(3):
            copy, when = keep_own(chunk, y, slot, p)
            if when is None:
                copy.wait()
            else:
                pl.when(when)(copy.wait)

    def expert_chunk(chunk):
        for p in range(3):
            wait_bytes(sends[p].at[pl.ds(0, mates - 1)], r.go_recv.at[chunk, p])
        for copy in fetch(chunk, 0, 0):
            copy.start()

        def one_tile(y, c):
            slot = lax.rem(y, 2)

            @pl.when(y + 1 < side)
            def _():
                for copy in fetch(chunk, y + 1, 1 - slot):
                    copy.start()

            for copy in fetch(chunk, y, slot):
                copy.wait()

            @pl.when(y >= 2)
            def _():
                wait_put(chunk, y - 2, slot)

            for lo in range(0, width, f_chunk):
                cols = slice(lo, lo + f_chunk)
                z = dot(x_buf[slot].reshape(rows, model), r.gate[:, cols])
                u = dot(x_buf[slot].reshape(rows, model), r.up[:, cols])
                hidden_buf[:, cols] = (jax.nn.silu(z) * u).astype(BF16)
            for lo in range(0, model, d_chunk):
                cols = slice(lo, lo + d_chunk)
                y_rows = dot(hidden_buf[...], r.down[:, cols]).astype(BF16)
                y_buf[slot, :, :, :, :, cols] = y_rows.reshape(group + (d_chunk,))
            start_put(chunk, y, slot)
            return c

        lax.fori_loop(0, side, one_tile, 0)
        for y in range(side - 2, side):
            wait_put(chunk, y, y % 2)

        def one_mate(offset, c):
            for p in range(3):
                place = mate_peer(BACK[p][0], offset)
                remote(
                    rows_of(outputs[p], p, chunk, place, BACK[p][1:]),
                    middles[p].at[chunk, pl.ds(0, side), pl.ds(0, side), back_mate[p]],
                    r.back_send.at[chunk, p],
                    r.back_recv.at[chunk, p],
                    place,
                ).start()
            return c

        lax.fori_loop(1, mates, one_mate, 0)

    def middle_rows(p, chunk, i, d):
        return middles[p].at[(chunk,) + ordered({BACK[p][1]: i, BACK[p][2]: d})]

    def pass_on(chunk):
        for p in range(3):
            wait_bytes(middles[p].at[chunk, pl.ds(0, side), pl.ds(0, side), pl.ds(0, mates - 1)], r.back_recv.at[chunk, p])
            for offset in range(1, side):
                axis = BACK[p][1]
                place = axis_peer(axis, offset)
                remote(
                    middle_rows(p, chunk, place[axis], pl.ds(0, side)),
                    results[p].at[chunk, pl.ds(0, side), me[axis]],
                    r.home_send.at[chunk, p],
                    r.home_recv.at[chunk, p],
                    place,
                ).start()


    split = r.split
    lanes = min(128, rows_block)

    def weigh_chunk(chunk, carry):
        @pl.when(chunk == 1)
        def _():
            pass_on(N_CHUNKS - 1)

        for p in range(3):
            wait_bytes(results[p].at[chunk, pl.ds(0, side), pl.ds(0, side - 1)], r.home_recv.at[chunk, p])

        def source_of(p, n):
            ahead = 2 * side - 2 - 2 * n + 3 * (n // 2) if relay else 1 - n
            return lax.rem(me[BACK[p][2]] + ahead, side)

        def load(p, n, slot):
            copies = []
            for offset in range(side):
                i, d = lax.rem(me[BACK[p][1]] + offset, side), source_of(p, n)
                copies.append(
                    pltpu.make_async_copy(
                        results[p].at[chunk, d, i] if offset else middle_rows(p, chunk, i, d),
                        stage.at[slot, pl.ds(i * mates, mates), :, pl.ds(0, widths[p])],
                        r.load_sem.at[slot, offset],
                    )
                )
            return copies

        for copy in load(0, 0, 0):
            copy.start()

        def one_source(n, c):
            for p in range(3):
                d = source_of(p, n)
                slot = lax.rem(n + p, 2)

                @pl.when(n + p // 2 < side)
                def _():
                    for copy in load((p + 1) % 3, n + p // 2, 1 - slot):
                        copy.start()

                held = plane_keys(p, (1, rows_block), chunk).astype(F32)
                info = r.line_gates[p, d]
                keys = [jnp.broadcast_to(info[:, j : j + 1], (tokens, lanes)) for j in range(top_k)]
                gates = [jnp.broadcast_to(info[:, top_k + j : top_k + j + 1], (tokens, lanes)) for j in range(top_k)]
                for lo in range(0, rows_block, lanes):
                    here = held[:, lo : lo + lanes]
                    weight = jnp.zeros((tokens, lanes), F32)
                    for j in range(top_k):
                        weight = jnp.where(here == keys[j], gates[j], weight)
                    high = weight.astype(BF16)
                    rest = weight - high.astype(F32)
                    middle = rest.astype(BF16)
                    low = (rest - middle.astype(F32)).astype(BF16)
                    split[0:tokens, lo : lo + lanes] = high
                    split[tokens : 2 * tokens, lo : lo + lanes] = middle
                    split[2 * tokens : 3 * tokens, lo : lo + lanes] = low
                for copy in load(p, n, slot):
                    copy.wait()
                for lo, size in steps(widths[p], TILE):
                    y = stage[slot, 0:members, :, lo : lo + size].reshape(rows_block, size)
                    both = dot(split[...], y)
                    total = both[0:tokens] + (both[tokens : 2 * tokens] + both[2 * tokens : 3 * tokens])

                    @pl.when(chunk == 0)
                    def _():
                        sums[p][d, :, lo : lo + size] = total

                    @pl.when(chunk > 0)
                    def _():
                        sums[p][d, :, lo : lo + size] += total

                last = chunk == N_CHUNKS - 1
                axis = BACK[p][2]

                @pl.when(jnp.logical_and(last, n == 0))
                def _():
                    for k, stride in enumerate(strides):
                        part, spot, arrived = sums[p].at[d], others[p].at[0], r.sum_recv.at[p, 0]
                        if relay:
                            part = sums[p].at[d, halves[k]]
                            spot, arrived = others[p].at[2, halves[k]], r.sum_half.at[p, k]
                        remote(part, spot, r.sum_send.at[p], arrived, axis_peer(axis, stride)).start()

                for k in range(2 if relay else 0):

                    @pl.when(jnp.logical_and(last, n == 2 + k))
                    def _():
                        wait_bytes(others[p].at[2, halves[k]], r.sum_half.at[p, k])
                        sums[p][d, halves[k], :] += others[p][2, halves[k], :]
                        remote(
                            sums[p].at[d], others[p].at[k], r.sum_send.at[p], r.sum_recv.at[p, k], axis_peer(axis, strides[k])
                        ).start()

            return c

        return lax.fori_loop(0, side, one_source, carry)


    def experts_and_back(chunk, carry):
        expert_chunk(chunk)
        pl.when(chunk >= 1)(lambda: pass_on(chunk - 1))
        return carry

    lax.fori_loop(0, N_CHUNKS, experts_and_back, 0)
    for p in range(3):
        wait_bytes(r.line_gates.at[p, pl.ds(0, side - 1)], r.gate_recv.at[p])
    lax.fori_loop(0, N_CHUNKS, weigh_chunk, 0)
    for p, (lo, hi) in enumerate(parts):
        for k in range(len(strides)):
            wait_bytes(others[p].at[k], r.sum_recv.at[p, k])

        def finish(here):
            moe = sums[p][me[BACK[p][2]], here, :]
            for k in range(len(strides)):
                moe += others[p][k, here, :]
            r.out[here, lo:hi] = (r.dense[here, lo:hi] + moe).astype(BF16)

        bands(finish)


    for p in range(3):
        wait_bytes(tok[p].at[pl.ds(0, side - 1)], r.tok_send.at[p])
        wait_bytes(r.all_keys.at[p, 0, pl.ds(0, side - 1)], r.key_send.at[p])
        wait_bytes(far[p].at[pl.ds(0, side - 1)], r.far_send.at[p])
        wait_bytes(r.all_keys.at[p, pl.ds(0, side - 1)], r.far_key_send.at[p])
        wait_bytes(r.line_gates.at[p, pl.ds(0, side - 1)], r.gate_send.at[p])
        wait_bytes(others[p], r.sum_send.at[p])
        for chunk in range(N_CHUNKS):
            wait_bytes(sends[p].at[pl.ds(0, mates - 1)], r.go_send.at[chunk, p])
            wait_bytes(middles[p].at[chunk, pl.ds(0, side), pl.ds(0, side), pl.ds(0, mates - 1)], r.back_send.at[chunk, p])
            wait_bytes(results[p].at[chunk, pl.ds(0, side), pl.ds(0, side - 1)], r.home_send.at[chunk, p])


def layer_pair(small, large, side, capacity, head_dim):
    tokens, model = small['hidden'].shape
    top_k, width = small['ids_t'].shape[0], large['gate_hbm'].shape[1]
    key_dim, ff_dim = large['w_key'].shape[1], large['ffn_gate'].shape[1]
    parts = column_parts(model)
    widths = [hi - lo for lo, hi in parts]
    slots, members, mates = capacity // N_CHUNKS, side * side * 2, side * 2
    group = (side, 2, side, slots)
    rows = math.prod(group)
    sds, vmem = jax.ShapeDtypeStruct, pltpu.VMEM
    dma = lambda *shape: pltpu.SemaphoreType.DMA(shape)
    outs = dict(out=sds((tokens, model), BF16))
    scratch = dict(
        rows=vmem((tokens, model), BF16),
        query=vmem((tokens, large['w_query'].shape[1]), BF16),
        key=vmem((tokens, key_dim), BF16),
        value=vmem((tokens, key_dim), BF16),
        attended=vmem((tokens, model), BF16),
        act=vmem((tokens, ff_dim), BF16),
        dense=vmem((tokens, model), F32),
        ring=vmem((RING, model, TILE), BF16),
        all_keys=vmem((3, side, side, top_k, tokens), I32),
        my_gates=vmem((tokens, 128), F32),
        line_gates=vmem((3, side, tokens, 128), F32),
        source=vmem((2, tokens, max(widths)), BF16),
        stage=vmem((2, max(members, N_CHUNKS * mates), slots, max(widths)), BF16),
        split=vmem((3 * tokens, members * slots), BF16),
        gate=vmem((model, width), BF16),
        up=vmem((model, width), BF16),
        down=vmem((width, model), BF16),
        x_buf=vmem((2,) + group + (model,), BF16),
        y_buf=vmem((2,) + group + (model,), BF16),
        hidden_buf=vmem((rows, width), BF16),
        weight_sem=dma(3),
        ring_sem=dma(RING),
        source_sem=dma(2),
        stage_sem=dma(2),
        keep_sem=dma(2, N_CHUNKS),
        in_sem=dma(2, 3),
        out_sem=dma(2, 3),
        own_sem=dma(2, 3),
        load_sem=dma(2, side),
        tok_send=dma(3),
        tok_recv=dma(3, 2),
        tok_half=dma(3, 2),
        key_send=dma(3),
        key_recv=dma(3),
        far_send=dma(3),
        far_recv=dma(3, 2, side),
        far_half=dma(3, 2, side),
        far_key_send=dma(3),
        far_key_recv=dma(3, side - 1),
        gate_send=dma(3),
        gate_recv=dma(3),
        sum_send=dma(3),
        sum_recv=dma(3, 2),
        sum_half=dma(3, 2),
        go_send=dma(N_CHUNKS, 3),
        go_recv=dma(N_CHUNKS, 3),
        back_send=dma(N_CHUNKS, 3),
        back_recv=dma(N_CHUNKS, 3),
        home_send=dma(N_CHUNKS, 3),
        home_recv=dma(N_CHUNKS, 3),
    )
    for p, w in enumerate(widths):
        there = sds((N_CHUNKS, side, side, 2, side, slots, w), BF16)
        outs['far' + str(p)] = sds((side, side, tokens, w), BF16)
        outs['send' + str(p)] = sds((N_CHUNKS * mates, side, side, slots, w), BF16)
        outs['arrive' + str(p)] = there
        outs['output' + str(p)] = there
        outs['middle' + str(p)] = sds((N_CHUNKS, side, side, mates, slots, w), BF16)
        outs['result' + str(p)] = sds((N_CHUNKS, side, side, mates, slots, w), BF16)
        scratch['tok' + str(p)] = vmem((side, tokens, w), BF16)
        scratch['sum' + str(p)] = vmem((side, tokens, w), F32)
        scratch['other' + str(p)] = vmem((side - 1, tokens, w), F32)
    anywhere = pl.BlockSpec(memory_space=pl.ANY)
    local = pl.BlockSpec(memory_space=pltpu.VMEM)
    n_rows = members * side * capacity
    return pl.pallas_call(
        functools.partial(
            kernel,
            names=tuple(small) + tuple(large) + tuple(outs) + tuple(scratch),
            side=side,
            parts=parts,
            capacity=capacity,
            head_dim=head_dim,
            f_chunk=min(256, width),
            d_chunk=min(512, model),
        ),
        out_shape=list(outs.values()),
        in_specs=[local] * len(small) + [anywhere] * len(large),
        out_specs=[local] + [anywhere] * (len(outs) - 1),
        scratch_shapes=list(scratch.values()),
        compiler_params=pltpu.CompilerParams(has_side_effects=True, vmem_limit_bytes=67043328),
        cost_estimate=pl.CostEstimate(flops=6 * n_rows * model * width, bytes_accessed=8 * n_rows * model, transcendentals=0),
    )(*small.values(), *large.values())[0]


def solution(mesh):
    group_size = mesh.shape['ep']
    side = torus_side(group_size)
    torus = jax.sharding.Mesh(mesh.devices.reshape(side, side, side, 2), AXES)
    row_spec = P(AXES, None, None)
    vec_spec = P(None)
    mat_spec = P(None, None)
    cube_spec = P(None, None, None)
    expert_spec = P(AXES, None, None)

    def per_device(hidden, expert_ids, slot_ids, attn_norm, w_query, w_key, w_value, w_out, ffn_norm, ffn_gate, ffn_up, ffn_down, moe_norm, w_router, exp_gate, exp_up, exp_down):
        n_seqs, tokens, model = hidden.shape
        assert n_seqs == 1 and exp_gate.shape[0] == 1
        n_heads, head_dim = w_out.shape[0], w_out.shape[1]
        top_k = expert_ids.shape[2]
        capacity = CAP_FACTOR * tokens * top_k // group_size
        inv_freq = np.float32(ROPE_BASE) ** (np.float32(-2.0) * np.arange(head_dim // 2, dtype=np.float32) / head_dim)
        angles = np.arange(tokens, dtype=np.float32)[:, None] * inv_freq[None, :]
        cos, sin = np.cos(angles), np.sin(angles)
        small = dict(
            hidden=hidden[0],
            attn_scale=attn_norm.reshape(-1, 128),
            moe_scale=moe_norm.reshape(-1, 128),
            ffn_scale=ffn_norm.reshape(-1, 128),
            ids_t=expert_ids[0].T,
            slots_t=slot_ids[0].T,
            w_router=w_router,
            cos=np.concatenate([cos, cos], axis=1).astype(np.float32),
            sin=np.concatenate([-sin, sin], axis=1).astype(np.float32),
        )
        large = dict(
            w_query=w_query,
            w_key=w_key,
            w_value=w_value,
            w_out=w_out.reshape(n_heads * head_dim, model),
            ffn_gate=ffn_gate,
            ffn_up=ffn_up,
            ffn_down=ffn_down,
            gate_hbm=exp_gate[0],
            up_hbm=exp_up[0],
            down_hbm=exp_down[0],
        )
        return layer_pair(small, large, side, capacity, head_dim).reshape(hidden.shape)

    return jax.shard_map(per_device, mesh=torus, in_specs=(row_spec, row_spec, row_spec, vec_spec, mat_spec, mat_spec, mat_spec, cube_spec, vec_spec, mat_spec, mat_spec, mat_spec, vec_spec, mat_spec, expert_spec, expert_spec, expert_spec), out_specs=row_spec, check_vma=False)
```

```python
import functools
import math
import types

import jax
import jax.numpy as jnp
import numpy as np
from jax import lax
from jax.experimental import pallas as pl
from jax.experimental.pallas import tpu as pltpu
from jax.sharding import PartitionSpec as P

RMS_EPS = 1e-6
ROPE_BASE = 10000.0
CAP_FACTOR = 3
N_CHUNKS = 3
RING = 6
TILE = 256
MESH = pl.DeviceIdType.MESH

BF16, F32, I32 = jnp.bfloat16, jnp.float32, jnp.int32

AXES = ('z', 'y', 'x', 'c')
OUT = (('z', 'y', 'x'), ('x', 'z', 'y'), ('y', 'x', 'z'))
BACK = (('y', 'z', 'x'), ('z', 'x', 'y'), ('x', 'y', 'z'))
ROW_AXES = ('y', 'x', 'c', 'z')


def torus_side(n_devices):
    side = round((n_devices // 2) ** (1 / 3))
    assert side ** 3 * 2 == n_devices
    return side


def column_parts(model):
    lanes = model // 128
    first = -(-lanes // 3)
    second = -(-(lanes - first) // 2)
    ends = (0, first * 128, (first + second) * 128, model)
    return tuple((ends[p], ends[p + 1]) for p in range(3))


def steps(total, size):
    return [(lo, min(size, total - lo)) for lo in range(0, total, size)]


def rms_rows(rows, scale):
    as_float = rows.astype(F32)
    inv_rms = lax.rsqrt(jnp.mean(as_float * as_float, axis=-1, keepdims=True) + RMS_EPS)
    return (as_float * inv_rms * scale.astype(F32)).astype(BF16)


def dot(a, b):
    return jnp.dot(a, b, preferred_element_type=F32)


def kernel(*refs, names, side, parts, capacity, head_dim, f_chunk, d_chunk):
    r = types.SimpleNamespace(**dict(zip(names, refs)))
    each = lambda name: [getattr(r, name + str(p)) for p in range(3)]
    slots = capacity // N_CHUNKS
    members = side * side * 2
    mates = side * 2
    assert side in (2, 4)
    relay = side == 4
    strides = (1, side - 1) if relay else (1,)
    order = (0, side - 1, 1, 2) if relay else (0, 1)
    rows_block = members * slots
    tokens, model = r.hidden.shape
    me = {axis: lax.axis_index(axis) for axis in AXES}


    def rows_of(ref, p, chunk, place, free):
        spot = [pl.ds(0, side) if axis in free else place[axis] for axis in ROW_AXES]
        return ref.at[tuple([chunk] + spot)]

    def ordered(where):
        return tuple(where[axis] for axis in ROW_AXES if axis in where)

    def device(place):
        return tuple(place[axis] for axis in AXES)

    def axis_peer(axis, offset):
        return {**me, axis: lax.rem(me[axis] + offset, side)}

    def mate_peer(axis, offset):
        return {
            **me,
            axis: lax.rem(me[axis] + offset // 2, side),
            'c': lax.rem(me['c'] + lax.rem(offset, 2), 2),
        }

    def remote(src, dst, send_sem, recv_sem, place):
        return pltpu.make_async_remote_copy(
            src_ref=src, dst_ref=dst, send_sem=send_sem, recv_sem=recv_sem, device_id=device(place), device_id_type=MESH
        )

    def wait_bytes(ref, sem):
        pltpu.make_async_copy(ref, ref, sem).wait()

    def expert_key(place, core, slot):
        return (((place['z'] * side + place['y']) * side + place['x']) * 2 + core) * capacity + slot

    def plane_keys(p, shape, chunk):
        first, second, _ = BACK[p]
        row = lax.broadcasted_iota(I32, shape, 1)
        which, slot = row // slots, lax.rem(row, slots)
        pair = which // 2
        place = {**me, second: pair // side, first: lax.rem(pair, side)}
        return expert_key(place, lax.rem(which, 2), slot + chunk * slots)

    def mate_keys(p, shape):
        row = lax.broadcasted_iota(I32, shape, 0)
        block, slot = row // slots, lax.rem(row, slots)
        chunk, mate = block // mates, lax.rem(block, mates)
        place = {**me, OUT[p][2]: mate // 2}
        return expert_key(place, lax.rem(mate, 2), slot + chunk * slots)

    tok, far, sends, arrivals, outputs = each('tok'), each('far'), each('send'), each('arrive'), each('output')
    middles, results, sums, others = each('middle'), each('result'), each('sum'), each('other')
    widths = [hi - lo for lo, hi in parts]


    band = min(32, tokens)

    def bands(body):
        lax.fori_loop(0, tokens // band, lambda i, c: (body(pl.ds(pl.multiple_of(i * band, band), band)), c)[1], 0)

    def one_row(scale):
        lines = scale[...].astype(F32)
        return jnp.concatenate([lines[i : i + 1, :] for i in range(lines.shape[0])], axis=1)

    def norm_both(here):
        normed = rms_rows(r.hidden[here, :], one_row(r.moe_scale))
        for p, (lo, hi) in enumerate(parts):
            tok[p][me[OUT[p][0]], here, :] = normed[:, lo:hi]
        r.rows[here, :] = rms_rows(r.hidden[here, :], one_row(r.attn_scale))

    bands(norm_both)
    keys_t = r.ids_t[...] * capacity + r.slots_t[...]
    for p in range(3):
        r.all_keys[p, me[OUT[p][1]], me[OUT[p][0]]] = keys_t
    pairs = ((r.gate_hbm, r.gate), (r.up_hbm, r.up), (r.down_hbm, r.down))
    loads = [pltpu.make_async_copy(src, dst, r.weight_sem.at[i]) for i, (src, dst) in enumerate(pairs)]
    for load in loads:
        load.start()

    half = tokens // 2
    halves = (pl.ds(0, half), pl.ds(half, half))

    def neighbour(axis, k):
        return lax.rem(me[axis] + side - strides[k], side)

    def send_far(p, n):
        near, axis, _ = OUT[p]
        d = lax.rem(me[near] + order[n], side)
        for k, stride in enumerate(strides):
            remote(
                tok[p].at[d], far[p].at[me[axis], d], r.far_send.at[p], r.far_recv.at[p, k, n], axis_peer(axis, stride)
            ).start()

    def pass_far(n):
        for k, stride in enumerate(strides):
            for p in range(3):
                near, axis, _ = OUT[p]
                d = lax.rem(me[near] + order[n], side)
                wait_bytes(tok[p].at[0], r.far_recv.at[p, k, n])
                if relay:
                    block = far[p].at[neighbour(axis, k), d, halves[k]]
                    remote(block, block, r.far_send.at[p], r.far_half.at[p, k, n], axis_peer(axis, stride)).start()

    for k, stride in enumerate(strides):
        for p in range(3):
            axis = OUT[p][0]
            block = tok[p].at[me[axis]]
            remote(block, block, r.tok_send.at[p], r.tok_recv.at[p, k], axis_peer(axis, stride)).start()
    for p in range(3):
        send_far(p, 0)
    for offset in range(1, side):
        for p in range(3):
            axis = OUT[p][0]
            keys = r.all_keys.at[p, me[OUT[p][1]], me[axis]]
            remote(keys, keys, r.key_send.at[p], r.key_recv.at[p], axis_peer(axis, offset)).start()


    ring = r.ring
    ring_sem = r.ring_sem

    def stream(n_steps, group, source, body):
        ahead = RING // group * group - group

        def copy(i, s):
            slot = lax.rem(i * group + s, RING // group * group)
            return pltpu.make_async_copy(source(i, s), ring.at[slot], ring_sem.at[slot])

        for i in range(min(ahead // group, n_steps)):
            for s in range(group):
                copy(i, s).start()

        def step(i, carry):
            @pl.when(i + ahead // group < n_steps)
            def _():
                for s in range(group):
                    copy(i + ahead // group, s).start()

            for s in range(group):
                copy(i, s).wait()
            body(i, [ring.at[lax.rem(i * group + s, RING // group * group)] for s in range(group)])
            return carry

        lax.fori_loop(0, n_steps, step, 0)

    def col_tile(i):
        return pl.ds(pl.multiple_of(i * TILE, TILE), TILE)

    def turned(y):
        return y * r.cos[...] + pltpu.roll(y, head_dim // 2, 1) * r.sin[...]

    def project(weight, out, rotary):
        def body(i, tiles):
            y = dot(r.rows[...], tiles[0][...])
            if rotary:
                y = jnp.concatenate([turned(y[:, lo : lo + head_dim]) for lo in range(0, TILE, head_dim)], axis=1)
            out[:, col_tile(i)] = y.astype(BF16)

        stream(weight.shape[1] // TILE, 1, lambda i, s: weight.at[:, col_tile(i)], body)

    project(r.w_query, r.query, True)
    project(r.w_key, r.key, True)
    project(r.w_value, r.value, False)


    logits = sum(dot(tok[p][me[OUT[p][0]]], r.w_router[lo:hi, :]) for p, (lo, hi) in enumerate(parts))
    top_k = r.ids_t.shape[0]
    gap = jnp.zeros((128 - 3 * top_k, tokens), F32)
    blank = jnp.zeros((top_k, tokens), F32)
    info = jnp.concatenate([keys_t.astype(F32), blank, r.ids_t[...].astype(F32), gap], axis=0).T
    lane = lax.broadcasted_iota(I32, logits.shape, 1).astype(F32)
    picked = [
        jnp.sum(jnp.where(lane == info[:, 2 * top_k + j : 2 * top_k + j + 1], logits, 0.0), axis=1, keepdims=True)
        for j in range(top_k)
    ]
    peak = functools.reduce(jnp.maximum, picked)
    powers = [jnp.exp(v - peak) for v in picked]
    norm = functools.reduce(jnp.add, powers)
    lane = lax.broadcasted_iota(I32, info.shape, 1)
    for j in range(top_k):
        info = jnp.where(lane == top_k + j, powers[j] / norm, info)
    r.my_gates[...] = info
    for p in range(3):
        r.line_gates[p, me[BACK[p][2]]] = info


    for k, stride in enumerate(strides):
        for p in range(3):
            axis = OUT[p][0]
            wait_bytes(tok[p].at[0], r.tok_recv.at[p, k])
            if relay:
                block = tok[p].at[neighbour(axis, k), halves[k]]
                remote(block, block, r.tok_send.at[p], r.tok_half.at[p, k], axis_peer(axis, stride)).start()
            send_far(p, 1 + k)
    pass_far(0)
    if relay:
        for p in range(3):
            for k in range(2):
                wait_bytes(tok[p].at[0, halves[k]], r.tok_half.at[p, k])
            send_far(p, 3)
    for p in range(3):
        wait_bytes(r.all_keys.at[p, 0, pl.ds(0, side - 1)], r.key_recv.at[p])
        for offset in range(1, side):
            keys = r.all_keys.at[p, me[OUT[p][1]]]
            remote(
                keys, keys, r.far_key_send.at[p], r.far_key_recv.at[p, offset - 1], axis_peer(OUT[p][1], offset)
            ).start()
    for offset in range(1, side):
        for p in range(3):
            axis = BACK[p][2]
            remote(
                r.my_gates, r.line_gates.at[p, me[axis]], r.gate_send.at[p], r.gate_recv.at[p], axis_peer(axis, offset)
            ).start()


    n_heads = r.query.shape[1] // head_dim
    per_key = r.query.shape[1] // r.key.shape[1]
    causal = lax.broadcasted_iota(I32, (tokens, tokens), 0) >= lax.broadcasted_iota(I32, (tokens, tokens), 1)

    def one_head(h, carry):
        cols = pl.ds(pl.multiple_of(h * head_dim, head_dim), head_dim)
        key_cols = pl.ds(pl.multiple_of(h // per_key * head_dim, head_dim), head_dim)
        scores = lax.dot_general(
            r.query[:, cols], r.key[:, key_cols], (((1,), (1,)), ((), ())), preferred_element_type=F32
        )
        scores = jnp.where(causal, scores * head_dim ** -0.5, -jnp.inf)
        power = jnp.exp(scores - jnp.max(scores, axis=1, keepdims=True))
        prob = (power / jnp.sum(power, axis=1, keepdims=True)).astype(BF16)
        r.query[:, cols] = dot(prob, r.value[:, key_cols]).astype(BF16)
        return carry


    stage = r.stage
    blocks = N_CHUNKS * mates
    out_mate = [me[OUT[p][2]] * 2 + me['c'] for p in range(3)]
    back_mate = [me[BACK[p][0]] * 2 + me['c'] for p in range(3)]

    def pick_rows(p, i, d, slot, source, wanted):
        keys = r.all_keys[p, i, d]
        for lo, n in steps(tokens, 128):
            hit = wanted[:, 0:n] == keys[0:1, lo : lo + n]
            for j in range(1, top_k):
                hit = jnp.logical_or(hit, wanted[:, 0:n] == keys[j : j + 1, lo : lo + n])
            r.split[0 : blocks * slots, lo : lo + n] = jnp.where(hit, 1.0, 0.0).astype(BF16)
        for lo, n in steps(widths[p], TILE):
            found = dot(r.split[0 : blocks * slots, 0:tokens], source[:, lo : lo + n]).astype(BF16)
            stage[slot, 0:blocks, :, lo : lo + n] = found.reshape(blocks, slots, n)

    def flush(p, i, d, slot):
        a, b = ordered({OUT[p][1]: i, OUT[p][0]: d})
        return pltpu.make_async_copy(
            stage.at[slot, pl.ds(0, blocks), :, pl.ds(0, widths[p])],
            sends[p].at[pl.ds(0, blocks), a, b],
            r.stage_sem.at[slot],
        )

    def keep(p, i, d, slot, chunk):
        spot = {**me, OUT[p][1]: i, OUT[p][0]: d}
        return pltpu.make_async_copy(
            stage.at[slot, chunk * mates + out_mate[p], :, pl.ds(0, widths[p])],
            arrivals[p].at[(chunk,) + ordered(spot)],
            r.keep_sem.at[slot, chunk],
        )

    wanted = [mate_keys(p, (blocks * slots, min(128, tokens))) for p in range(3)]

    def send_rows(p, chunk, i):
        near, far_axis, axis = OUT[p]
        free = (near,) if i is not None else (near, far_axis)
        a, b = ordered({far_axis: pl.ds(0, side) if i is None else i, near: pl.ds(0, side)})
        group_place = me if i is None else {**me, far_axis: i}

        def one_mate(offset, c):
            place = mate_peer(axis, offset)
            remote(
                sends[p].at[chunk * mates + place[axis] * 2 + place['c'], a, b],
                rows_of(arrivals[p], p, chunk, group_place, free),
                r.go_send.at[chunk, p],
                r.go_recv.at[chunk, p],
                place,
            ).start()
            return c

        lax.fori_loop(1, mates, one_mate, 0)

    def pick_group(offset):
        for p in range(3):
            i = lax.rem(me[OUT[p][1]] + side - offset, side)
            if offset:
                wait_bytes(r.all_keys.at[p, 0], r.far_key_recv.at[p, offset - 1])
            if relay and offset == 2:
                for n in range(side):
                    for k in range(2):
                        wait_bytes(tok[p].at[0, halves[k]], r.far_half.at[p, k, n])

            def load(d, slot):
                return pltpu.make_async_copy(
                    far[p].at[i, d], r.source.at[slot, :, pl.ds(0, widths[p])], r.source_sem.at[slot]
                )

            if offset:
                load(0, 0).start()

            def one_source(d, c):
                slot = lax.rem(d, 2)
                if offset:

                    @pl.when(d + 1 < side)
                    def _():
                        load(d + 1, 1 - slot).start()

                    load(d, slot).wait()

                @pl.when(d >= 2)
                def _():
                    flush(p, i, d - 2, slot).wait()
                    for chunk in range(N_CHUNKS):
                        keep(p, i, d - 2, slot, chunk).wait()

                pick_rows(p, i, d, slot, r.source.at[slot] if offset else tok[p].at[d], wanted[p])
                flush(p, i, d, slot).start()
                for chunk in range(N_CHUNKS):
                    keep(p, i, d, slot, chunk).start()
                return c

            lax.fori_loop(0, side, one_source, 0)
            for d in range(side - 2, side):
                flush(p, i, d, d % 2).wait()
                for chunk in range(N_CHUNKS):
                    keep(p, i, d, d % 2, chunk).wait()
            send_rows(p, 0, i)

    def heads(part, n_parts):
        lax.fori_loop(n_heads * part // n_parts, n_heads * (part + 1) // n_parts, one_head, 0)

    pick_group(0)
    for n in range(1, side):
        pass_far(n)
        heads(n - 1, side - 1)
    for offset in (1, 3, 2) if relay else (1,):
        pick_group(offset)
    for chunk in range(1, N_CHUNKS):
        for p in range(3):
            send_rows(p, chunk, None)


    out_split = n_heads * head_dim // model

    def out_body(i, tiles):
        total = r.hidden[:, col_tile(i)].astype(F32)
        attended = dot(r.query[:, 0:model], tiles[0][...])
        for s in range(1, out_split):
            attended += dot(r.query[:, s * model : (s + 1) * model], tiles[s][...])
        r.attended[:, col_tile(i)] = (total + attended).astype(BF16)

    stream(model // TILE, out_split, lambda i, s: r.w_out.at[pl.ds(s * model, model), col_tile(i)], out_body)

    def norm_attended(here):
        r.rows[here, :] = rms_rows(r.attended[here, :], one_row(r.ffn_scale))

    bands(norm_attended)

    def act_body(i, tiles):
        z = dot(r.rows[...], tiles[0][...])
        u = dot(r.rows[...], tiles[1][...])
        r.act[:, col_tile(i)] = (jax.nn.silu(z) * u).astype(BF16)

    ff_dim = r.ffn_gate.shape[1]
    stream(
        ff_dim // TILE, 2, lambda i, s: (r.ffn_gate, r.ffn_up)[s].at[:, col_tile(i)], act_body
    )
    down_split = ff_dim // model

    def down_body(i, tiles):
        total = dot(r.act[:, 0:model], tiles[0][...])
        for s in range(1, down_split):
            total += dot(r.act[:, s * model : (s + 1) * model], tiles[s][...])
        r.dense[:, col_tile(i)] = r.attended[:, col_tile(i)].astype(F32) + total

    stream(model // TILE, down_split, lambda i, s: r.ffn_down.at[pl.ds(s * model, model), col_tile(i)], down_body)


    for load in loads:
        load.wait()
    x_buf, y_buf, hidden_buf = r.x_buf, r.y_buf, r.hidden_buf
    group = x_buf.shape[1:-1]
    rows = math.prod(group)
    width = hidden_buf.shape[1]

    def fetch(chunk, y, slot):
        return [
            pltpu.make_async_copy(
                arrivals[p].at[chunk, y], x_buf.at[slot, :, :, :, :, pl.ds(lo, hi - lo)], r.in_sem.at[slot, p]
            )
            for p, (lo, hi) in enumerate(parts)
        ]

    def put(chunk, y, slot):
        return [
            pltpu.make_async_copy(
                y_buf.at[slot, :, :, :, :, pl.ds(lo, hi - lo)], outputs[p].at[chunk, y], r.out_sem.at[slot, p]
            )
            for p, (lo, hi) in enumerate(parts)
        ]

    def keep_own(chunk, y, slot, p):
        lo, hi = parts[p]
        free = BACK[p][1:]
        spot = [pl.ds(0, side) if axis in free else me[axis] for axis in ROW_AXES[1:]]
        mine = pltpu.make_async_copy(
            y_buf.at[tuple([slot] + spot + [pl.ds(0, slots), pl.ds(lo, hi - lo)])],
            middles[p].at[
                (chunk,) + ordered({axis: y if axis == 'y' else pl.ds(0, side) for axis in free}) + (back_mate[p],)
            ],
            r.own_sem.at[slot, p],
        )
        return mine, (None if 'y' in free else y == me['y'])

    def start_put(chunk, y, slot):
        for copy in put(chunk, y, slot):
            copy.start()
        for p in range(3):
            copy, when = keep_own(chunk, y, slot, p)
            if when is None:
                copy.start()
            else:
                pl.when(when)(copy.start)

    def wait_put(chunk, y, slot):
        for copy in put(chunk, y, slot):
            copy.wait()
        for p in range(3):
            copy, when = keep_own(chunk, y, slot, p)
            if when is None:
                copy.wait()
            else:
                pl.when(when)(copy.wait)

    def expert_chunk(chunk):
        for p in range(3):
            wait_bytes(sends[p].at[pl.ds(0, mates - 1)], r.go_recv.at[chunk, p])
        for copy in fetch(chunk, 0, 0):
            copy.start()

        def one_tile(y, c):
            slot = lax.rem(y, 2)

            @pl.when(y + 1 < side)
            def _():
                for copy in fetch(chunk, y + 1, 1 - slot):
                    copy.start()

            for copy in fetch(chunk, y, slot):
                copy.wait()

            @pl.when(y >= 2)
            def _():
                wait_put(chunk, y - 2, slot)

            for lo in range(0, width, f_chunk):
                cols = slice(lo, lo + f_chunk)
                z = dot(x_buf[slot].reshape(rows, model), r.gate[:, cols])
                u = dot(x_buf[slot].reshape(rows, model), r.up[:, cols])
                hidden_buf[:, cols] = (jax.nn.silu(z) * u).astype(BF16)
            for lo in range(0, model, d_chunk):
                cols = slice(lo, lo + d_chunk)
                y_rows = dot(hidden_buf[...], r.down[:, cols]).astype(BF16)
                y_buf[slot, :, :, :, :, cols] = y_rows.reshape(group + (d_chunk,))
            start_put(chunk, y, slot)
            return c

        lax.fori_loop(0, side, one_tile, 0)
        for y in range(side - 2, side):
            wait_put(chunk, y, y % 2)

        def one_mate(offset, c):
            for p in range(3):
                place = mate_peer(BACK[p][0], offset)
                remote(
                    rows_of(outputs[p], p, chunk, place, BACK[p][1:]),
                    middles[p].at[chunk, pl.ds(0, side), pl.ds(0, side), back_mate[p]],
                    r.back_send.at[chunk, p],
                    r.back_recv.at[chunk, p],
                    place,
                ).start()
            return c

        lax.fori_loop(1, mates, one_mate, 0)

    def middle_rows(p, chunk, i, d):
        return middles[p].at[(chunk,) + ordered({BACK[p][1]: i, BACK[p][2]: d})]

    def source_of(p, n):
        ahead = 2 * side - 2 - 2 * n + 3 * (n // 2) if relay else 1 - n
        return lax.rem(me[BACK[p][2]] + ahead, side)

    def pass_on(chunk):
        for p in range(3):
            wait_bytes(middles[p].at[chunk, pl.ds(0, side), pl.ds(0, side), pl.ds(0, mates - 1)], r.back_recv.at[chunk, p])
        for n in range(side):
            for p in range(3):
                axis, d = BACK[p][1], source_of(p, n)
                for offset in range(1, side):
                    place = axis_peer(axis, offset)
                    remote(
                        middle_rows(p, chunk, place[axis], d),
                        results[p].at[chunk, d, me[axis]],
                        r.home_send.at[chunk, p],
                        r.home_recv.at[chunk, p, n],
                        place,
                    ).start()


    split = r.split
    lanes = min(128, rows_block)

    def weigh_chunk(chunk, carry):
        def load(p, n, slot):
            copies = []
            for offset in range(side):
                i, d = lax.rem(me[BACK[p][1]] + offset, side), source_of(p, n)
                copies.append(
                    pltpu.make_async_copy(
                        results[p].at[chunk, d, i] if offset else middle_rows(p, chunk, i, d),
                        stage.at[slot, pl.ds(i * mates, mates), :, pl.ds(0, widths[p])],
                        r.load_sem.at[slot, offset],
                    )
                )
            return copies

        def one_source(n, c):
            for p in range(3):
                wait_bytes(results[p].at[chunk, 0, pl.ds(0, side - 1)], r.home_recv.at[chunk, p, n])
            for copy in load(0, n, 0):
                copy.start()
            for p in range(3):
                d, slot = source_of(p, n), p % 2
                for copy in load(p + 1, n, 1 - slot) if p < 2 else ():
                    copy.start()
                held = plane_keys(p, (1, rows_block), chunk).astype(F32)
                info = r.line_gates[p, d]
                keys = [jnp.broadcast_to(info[:, j : j + 1], (tokens, lanes)) for j in range(top_k)]
                gates = [jnp.broadcast_to(info[:, top_k + j : top_k + j + 1], (tokens, lanes)) for j in range(top_k)]
                for lo in range(0, rows_block, lanes):
                    here = held[:, lo : lo + lanes]
                    weight = jnp.zeros((tokens, lanes), F32)
                    for j in range(top_k):
                        weight = jnp.where(here == keys[j], gates[j], weight)
                    high = weight.astype(BF16)
                    rest = weight - high.astype(F32)
                    middle = rest.astype(BF16)
                    low = (rest - middle.astype(F32)).astype(BF16)
                    split[0:tokens, lo : lo + lanes] = high
                    split[tokens : 2 * tokens, lo : lo + lanes] = middle
                    split[2 * tokens : 3 * tokens, lo : lo + lanes] = low
                for copy in load(p, n, slot):
                    copy.wait()
                for lo, size in steps(widths[p], TILE):
                    y = stage[slot, 0:members, :, lo : lo + size].reshape(rows_block, size)
                    both = dot(split[...], y)
                    total = both[0:tokens] + (both[tokens : 2 * tokens] + both[2 * tokens : 3 * tokens])

                    @pl.when(chunk == 0)
                    def _():
                        sums[p][d, :, lo : lo + size] = total

                    @pl.when(chunk > 0)
                    def _():
                        sums[p][d, :, lo : lo + size] += total

                last = chunk == N_CHUNKS - 1
                axis = BACK[p][2]

                @pl.when(jnp.logical_and(last, n == 0))
                def _():
                    for k, stride in enumerate(strides):
                        part, spot, arrived = sums[p].at[d], others[p].at[0], r.sum_recv.at[p, 0]
                        if relay:
                            part = sums[p].at[d, halves[k]]
                            spot, arrived = others[p].at[2, halves[k]], r.sum_half.at[p, k]
                        remote(part, spot, r.sum_send.at[p], arrived, axis_peer(axis, stride)).start()

            return c

        return lax.fori_loop(0, side, one_source, carry)


    def experts_and_back(chunk, carry):
        expert_chunk(chunk)
        pl.when(chunk >= 1)(lambda: pass_on(chunk - 1))
        return carry

    lax.fori_loop(0, N_CHUNKS, experts_and_back, 0)
    pass_on(N_CHUNKS - 1)
    for p in range(3):
        wait_bytes(r.line_gates.at[p, pl.ds(0, side - 1)], r.gate_recv.at[p])
    lax.fori_loop(0, N_CHUNKS, weigh_chunk, 0)
    for k in range(2 if relay else 0):
        for p in range(3):
            axis, d = BACK[p][2], source_of(p, 2 + k)
            wait_bytes(others[p].at[2, halves[k]], r.sum_half.at[p, k])
            sums[p][d, halves[k], :] += others[p][2, halves[k], :]
            remote(
                sums[p].at[d], others[p].at[k], r.sum_send.at[p], r.sum_recv.at[p, k], axis_peer(axis, strides[k])
            ).start()
    for p, (lo, hi) in enumerate(parts):
        for k in range(len(strides)):
            wait_bytes(others[p].at[k], r.sum_recv.at[p, k])

        def finish(here):
            moe = sums[p][me[BACK[p][2]], here, :]
            for k in range(len(strides)):
                moe += others[p][k, here, :]
            r.out[here, lo:hi] = (r.dense[here, lo:hi] + moe).astype(BF16)

        bands(finish)


    for p in range(3):
        wait_bytes(tok[p].at[pl.ds(0, side - 1)], r.tok_send.at[p])
        wait_bytes(r.all_keys.at[p, 0, pl.ds(0, side - 1)], r.key_send.at[p])
        wait_bytes(far[p].at[pl.ds(0, side - 1)], r.far_send.at[p])
        wait_bytes(r.all_keys.at[p, pl.ds(0, side - 1)], r.far_key_send.at[p])
        wait_bytes(r.line_gates.at[p, pl.ds(0, side - 1)], r.gate_send.at[p])
        wait_bytes(others[p], r.sum_send.at[p])
        for chunk in range(N_CHUNKS):
            wait_bytes(sends[p].at[pl.ds(0, mates - 1)], r.go_send.at[chunk, p])
            wait_bytes(middles[p].at[chunk, pl.ds(0, side), pl.ds(0, side), pl.ds(0, mates - 1)], r.back_send.at[chunk, p])
            wait_bytes(results[p].at[chunk, pl.ds(0, side), pl.ds(0, side - 1)], r.home_send.at[chunk, p])


def layer_pair(small, large, side, capacity, head_dim):
    tokens, model = small['hidden'].shape
    top_k, width = small['ids_t'].shape[0], large['gate_hbm'].shape[1]
    key_dim, ff_dim = large['w_key'].shape[1], large['ffn_gate'].shape[1]
    parts = column_parts(model)
    widths = [hi - lo for lo, hi in parts]
    slots, members, mates = capacity // N_CHUNKS, side * side * 2, side * 2
    group = (side, 2, side, slots)
    rows = math.prod(group)
    sds, vmem = jax.ShapeDtypeStruct, pltpu.VMEM
    dma = lambda *shape: pltpu.SemaphoreType.DMA(shape)
    outs = dict(out=sds((tokens, model), BF16))
    scratch = dict(
        rows=vmem((tokens, model), BF16),
        query=vmem((tokens, large['w_query'].shape[1]), BF16),
        key=vmem((tokens, key_dim), BF16),
        value=vmem((tokens, key_dim), BF16),
        attended=vmem((tokens, model), BF16),
        act=vmem((tokens, ff_dim), BF16),
        dense=vmem((tokens, model), F32),
        ring=vmem((RING, model, TILE), BF16),
        all_keys=vmem((3, side, side, top_k, tokens), I32),
        my_gates=vmem((tokens, 128), F32),
        line_gates=vmem((3, side, tokens, 128), F32),
        source=vmem((2, tokens, max(widths)), BF16),
        stage=vmem((2, max(members, N_CHUNKS * mates), slots, max(widths)), BF16),
        split=vmem((3 * tokens, members * slots), BF16),
        gate=vmem((model, width), BF16),
        up=vmem((model, width), BF16),
        down=vmem((width, model), BF16),
        x_buf=vmem((2,) + group + (model,), BF16),
        y_buf=vmem((2,) + group + (model,), BF16),
        hidden_buf=vmem((rows, width), BF16),
        weight_sem=dma(3),
        ring_sem=dma(RING),
        source_sem=dma(2),
        stage_sem=dma(2),
        keep_sem=dma(2, N_CHUNKS),
        in_sem=dma(2, 3),
        out_sem=dma(2, 3),
        own_sem=dma(2, 3),
        load_sem=dma(2, side),
        tok_send=dma(3),
        tok_recv=dma(3, 2),
        tok_half=dma(3, 2),
        key_send=dma(3),
        key_recv=dma(3),
        far_send=dma(3),
        far_recv=dma(3, 2, side),
        far_half=dma(3, 2, side),
        far_key_send=dma(3),
        far_key_recv=dma(3, side - 1),
        gate_send=dma(3),
        gate_recv=dma(3),
        sum_send=dma(3),
        sum_recv=dma(3, 2),
        sum_half=dma(3, 2),
        go_send=dma(N_CHUNKS, 3),
        go_recv=dma(N_CHUNKS, 3),
        back_send=dma(N_CHUNKS, 3),
        back_recv=dma(N_CHUNKS, 3),
        home_send=dma(N_CHUNKS, 3),
        home_recv=dma(N_CHUNKS, 3, side),
    )
    for p, w in enumerate(widths):
        there = sds((N_CHUNKS, side, side, 2, side, slots, w), BF16)
        outs['far' + str(p)] = sds((side, side, tokens, w), BF16)
        outs['send' + str(p)] = sds((N_CHUNKS * mates, side, side, slots, w), BF16)
        outs['arrive' + str(p)] = there
        outs['output' + str(p)] = there
        outs['middle' + str(p)] = sds((N_CHUNKS, side, side, mates, slots, w), BF16)
        outs['result' + str(p)] = sds((N_CHUNKS, side, side, mates, slots, w), BF16)
        scratch['tok' + str(p)] = vmem((side, tokens, w), BF16)
        scratch['sum' + str(p)] = vmem((side, tokens, w), F32)
        scratch['other' + str(p)] = vmem((side - 1, tokens, w), F32)
    anywhere = pl.BlockSpec(memory_space=pl.ANY)
    local = pl.BlockSpec(memory_space=pltpu.VMEM)
    n_rows = members * side * capacity
    return pl.pallas_call(
        functools.partial(
            kernel,
            names=tuple(small) + tuple(large) + tuple(outs) + tuple(scratch),
            side=side,
            parts=parts,
            capacity=capacity,
            head_dim=head_dim,
            f_chunk=min(256, width),
            d_chunk=min(512, model),
        ),
        out_shape=list(outs.values()),
        in_specs=[local] * len(small) + [anywhere] * len(large),
        out_specs=[local] + [anywhere] * (len(outs) - 1),
        scratch_shapes=list(scratch.values()),
        compiler_params=pltpu.CompilerParams(has_side_effects=True, vmem_limit_bytes=67043328),
        cost_estimate=pl.CostEstimate(flops=6 * n_rows * model * width, bytes_accessed=8 * n_rows * model, transcendentals=0),
    )(*small.values(), *large.values())[0]


def solution(mesh):
    group_size = mesh.shape['ep']
    side = torus_side(group_size)
    torus = jax.sharding.Mesh(mesh.devices.reshape(side, side, side, 2), AXES)
    row_spec = P(AXES, None, None)
    vec_spec = P(None)
    mat_spec = P(None, None)
    cube_spec = P(None, None, None)
    expert_spec = P(AXES, None, None)

    def per_device(hidden, expert_ids, slot_ids, attn_norm, w_query, w_key, w_value, w_out, ffn_norm, ffn_gate, ffn_up, ffn_down, moe_norm, w_router, exp_gate, exp_up, exp_down):
        n_seqs, tokens, model = hidden.shape
        assert n_seqs == 1 and exp_gate.shape[0] == 1
        n_heads, head_dim = w_out.shape[0], w_out.shape[1]
        top_k = expert_ids.shape[2]
        capacity = CAP_FACTOR * tokens * top_k // group_size
        inv_freq = np.float32(ROPE_BASE) ** (np.float32(-2.0) * np.arange(head_dim // 2, dtype=np.float32) / head_dim)
        angles = np.arange(tokens, dtype=np.float32)[:, None] * inv_freq[None, :]
        cos, sin = np.cos(angles), np.sin(angles)
        small = dict(
            hidden=hidden[0],
            attn_scale=attn_norm.reshape(-1, 128),
            moe_scale=moe_norm.reshape(-1, 128),
            ffn_scale=ffn_norm.reshape(-1, 128),
            ids_t=expert_ids[0].T,
            slots_t=slot_ids[0].T,
            w_router=w_router,
            cos=np.concatenate([cos, cos], axis=1).astype(np.float32),
            sin=np.concatenate([-sin, sin], axis=1).astype(np.float32),
        )
        large = dict(
            w_query=w_query,
            w_key=w_key,
            w_value=w_value,
            w_out=w_out.reshape(n_heads * head_dim, model),
            ffn_gate=ffn_gate,
            ffn_up=ffn_up,
            ffn_down=ffn_down,
            gate_hbm=exp_gate[0],
            up_hbm=exp_up[0],
            down_hbm=exp_down[0],
        )
        return layer_pair(small, large, side, capacity, head_dim).reshape(hidden.shape)

    return jax.shard_map(per_device, mesh=torus, in_specs=(row_spec, row_spec, row_spec, vec_spec, mat_spec, mat_spec, mat_spec, cube_spec, vec_spec, mat_spec, mat_spec, mat_spec, vec_spec, mat_spec, expert_spec, expert_spec, expert_spec), out_specs=row_spec, check_vma=False)
```

```python
import functools
import math
import types

import jax
import jax.numpy as jnp
import numpy as np
from jax import lax
from jax.experimental import pallas as pl
from jax.experimental.pallas import tpu as pltpu
from jax.sharding import PartitionSpec as P

RMS_EPS = 1e-6
ROPE_BASE = 10000.0
CAP_FACTOR = 3
N_CHUNKS = 3
RING = 6
TILE = 256
MESH = pl.DeviceIdType.MESH

BF16, F32, I32 = jnp.bfloat16, jnp.float32, jnp.int32

AXES = ('z', 'y', 'x', 'c')
OUT = (('z', 'y', 'x'), ('x', 'z', 'y'), ('y', 'x', 'z'))
BACK = (('y', 'z', 'x'), ('z', 'x', 'y'), ('x', 'y', 'z'))
ROW_AXES = ('y', 'x', 'c', 'z')


def torus_side(n_devices):
    side = round((n_devices // 2) ** (1 / 3))
    assert side ** 3 * 2 == n_devices
    return side


def column_parts(model):
    lanes = model // 128
    first = -(-lanes // 3)
    second = -(-(lanes - first) // 2)
    ends = (0, first * 128, (first + second) * 128, model)
    return tuple((ends[p], ends[p + 1]) for p in range(3))


def steps(total, size):
    return [(lo, min(size, total - lo)) for lo in range(0, total, size)]


def rms_rows(rows, scale):
    as_float = rows.astype(F32)
    inv_rms = lax.rsqrt(jnp.mean(as_float * as_float, axis=-1, keepdims=True) + RMS_EPS)
    return (as_float * inv_rms * scale.astype(F32)).astype(BF16)


def dot(a, b):
    return jnp.dot(a, b, preferred_element_type=F32)


def kernel(*refs, names, side, parts, capacity, head_dim, f_chunk, d_chunk):
    r = types.SimpleNamespace(**dict(zip(names, refs)))
    each = lambda name: [getattr(r, name + str(p)) for p in range(3)]
    slots = capacity // N_CHUNKS
    members = side * side * 2
    mates = side * 2
    assert side in (2, 4)
    relay = side == 4
    strides = (1, side - 1) if relay else (1,)
    order = (0, side - 1, 1, 2) if relay else (0, 1)
    rows_block = members * slots
    tokens, model = r.hidden.shape
    me = {axis: lax.axis_index(axis) for axis in AXES}


    def rows_of(ref, p, chunk, place, free):
        spot = [pl.ds(0, side) if axis in free else place[axis] for axis in ROW_AXES]
        return ref.at[tuple([chunk] + spot)]

    def ordered(where):
        return tuple(where[axis] for axis in ROW_AXES if axis in where)

    def device(place):
        return tuple(place[axis] for axis in AXES)

    def axis_peer(axis, offset):
        return {**me, axis: lax.rem(me[axis] + offset, side)}

    def mate_peer(axis, offset):
        return {
            **me,
            axis: lax.rem(me[axis] + offset // 2, side),
            'c': lax.rem(me['c'] + lax.rem(offset, 2), 2),
        }

    def remote(src, dst, send_sem, recv_sem, place):
        return pltpu.make_async_remote_copy(
            src_ref=src, dst_ref=dst, send_sem=send_sem, recv_sem=recv_sem, device_id=device(place), device_id_type=MESH
        )

    def wait_bytes(ref, sem):
        pltpu.make_async_copy(ref, ref, sem).wait()

    def expert_key(place, core, slot):
        return (((place['z'] * side + place['y']) * side + place['x']) * 2 + core) * capacity + slot

    def plane_keys(p, shape, chunk):
        first, second, _ = BACK[p]
        row = lax.broadcasted_iota(I32, shape, 1)
        which, slot = row // slots, lax.rem(row, slots)
        pair = which // 2
        place = {**me, second: pair // side, first: lax.rem(pair, side)}
        return expert_key(place, lax.rem(which, 2), slot + chunk * slots)

    def mate_keys(p, shape):
        row = lax.broadcasted_iota(I32, shape, 0)
        block, slot = row // slots, lax.rem(row, slots)
        mate, chunk = block // N_CHUNKS, lax.rem(block, N_CHUNKS)
        place = {**me, OUT[p][2]: mate // 2}
        return expert_key(place, lax.rem(mate, 2), slot + chunk * slots)

    tok, far, sends, arrivals, outputs = each('tok'), each('far'), each('send'), each('arrive'), each('output')
    middles, results, sums, others = each('middle'), each('result'), each('sum'), each('other')
    widths = [hi - lo for lo, hi in parts]


    band = min(32, tokens)

    def bands(body):
        lax.fori_loop(0, tokens // band, lambda i, c: (body(pl.ds(pl.multiple_of(i * band, band), band)), c)[1], 0)

    def one_row(scale):
        lines = scale[...].astype(F32)
        return jnp.concatenate([lines[i : i + 1, :] for i in range(lines.shape[0])], axis=1)

    def norm_both(here):
        normed = rms_rows(r.hidden[here, :], one_row(r.moe_scale))
        for p, (lo, hi) in enumerate(parts):
            tok[p][me[OUT[p][0]], here, :] = normed[:, lo:hi]
        r.rows[here, :] = rms_rows(r.hidden[here, :], one_row(r.attn_scale))

    bands(norm_both)
    keys_t = r.ids_t[...] * capacity + r.slots_t[...]
    for p in range(3):
        r.all_keys[p, me[OUT[p][1]], me[OUT[p][0]]] = keys_t
    pairs = ((r.gate_hbm, r.gate), (r.up_hbm, r.up), (r.down_hbm, r.down))
    loads = [pltpu.make_async_copy(src, dst, r.weight_sem.at[i]) for i, (src, dst) in enumerate(pairs)]
    for load in loads:
        load.start()

    half = tokens // 2
    halves = (pl.ds(0, half), pl.ds(half, half))

    def neighbour(axis, k):
        return lax.rem(me[axis] + side - strides[k], side)

    def send_far(p, n):
        near, axis, _ = OUT[p]
        d = lax.rem(me[near] + order[n], side)
        for k, stride in enumerate(strides):
            remote(
                tok[p].at[d], far[p].at[me[axis], d], r.far_send.at[p], r.far_recv.at[p, k, n], axis_peer(axis, stride)
            ).start()

    def pass_far(n):
        for k, stride in enumerate(strides):
            for p in range(3):
                near, axis, _ = OUT[p]
                d = lax.rem(me[near] + order[n], side)
                wait_bytes(tok[p].at[0], r.far_recv.at[p, k, n])
                if relay:
                    block = far[p].at[neighbour(axis, k), d, halves[k]]
                    remote(block, block, r.far_send.at[p], r.far_half.at[p, k, n], axis_peer(axis, stride)).start()

    for k, stride in enumerate(strides):
        for p in range(3):
            axis = OUT[p][0]
            block = tok[p].at[me[axis]]
            remote(block, block, r.tok_send.at[p], r.tok_recv.at[p, k], axis_peer(axis, stride)).start()
    for p in range(3):
        send_far(p, 0)
    for offset in range(1, side):
        for p in range(3):
            axis = OUT[p][0]
            keys = r.all_keys.at[p, me[OUT[p][1]], me[axis]]
            remote(keys, keys, r.key_send.at[p], r.key_recv.at[p], axis_peer(axis, offset)).start()


    ring = r.ring
    ring_sem = r.ring_sem

    def stream(n_steps, group, source, body):
        ahead = RING // group * group - group

        def copy(i, s):
            slot = lax.rem(i * group + s, RING // group * group)
            return pltpu.make_async_copy(source(i, s), ring.at[slot], ring_sem.at[slot])

        for i in range(min(ahead // group, n_steps)):
            for s in range(group):
                copy(i, s).start()

        def step(i, carry):
            @pl.when(i + ahead // group < n_steps)
            def _():
                for s in range(group):
                    copy(i + ahead // group, s).start()

            for s in range(group):
                copy(i, s).wait()
            body(i, [ring.at[lax.rem(i * group + s, RING // group * group)] for s in range(group)])
            return carry

        lax.fori_loop(0, n_steps, step, 0)

    def col_tile(i):
        return pl.ds(pl.multiple_of(i * TILE, TILE), TILE)

    def turned(y):
        return y * r.cos[...] + pltpu.roll(y, head_dim // 2, 1) * r.sin[...]

    def project(weight, out, rotary):
        def body(i, tiles):
            y = dot(r.rows[...], tiles[0][...])
            if rotary:
                y = jnp.concatenate([turned(y[:, lo : lo + head_dim]) for lo in range(0, TILE, head_dim)], axis=1)
            out[:, col_tile(i)] = y.astype(BF16)

        stream(weight.shape[1] // TILE, 1, lambda i, s: weight.at[:, col_tile(i)], body)

    project(r.w_query, r.query, True)
    project(r.w_key, r.key, True)
    project(r.w_value, r.value, False)


    logits = sum(dot(tok[p][me[OUT[p][0]]], r.w_router[lo:hi, :]) for p, (lo, hi) in enumerate(parts))
    top_k = r.ids_t.shape[0]
    gap = jnp.zeros((128 - 3 * top_k, tokens), F32)
    blank = jnp.zeros((top_k, tokens), F32)
    info = jnp.concatenate([keys_t.astype(F32), blank, r.ids_t[...].astype(F32), gap], axis=0).T
    lane = lax.broadcasted_iota(I32, logits.shape, 1).astype(F32)
    picked = [
        jnp.sum(jnp.where(lane == info[:, 2 * top_k + j : 2 * top_k + j + 1], logits, 0.0), axis=1, keepdims=True)
        for j in range(top_k)
    ]
    peak = functools.reduce(jnp.maximum, picked)
    powers = [jnp.exp(v - peak) for v in picked]
    norm = functools.reduce(jnp.add, powers)
    lane = lax.broadcasted_iota(I32, info.shape, 1)
    for j in range(top_k):
        info = jnp.where(lane == top_k + j, powers[j] / norm, info)
    r.my_gates[...] = info.T[0 : 2 * top_k, :]
    for p in range(3):
        r.line_gates[p, me[BACK[p][2]]] = r.my_gates[...]


    for k, stride in enumerate(strides):
        for p in range(3):
            axis = OUT[p][0]
            wait_bytes(tok[p].at[0], r.tok_recv.at[p, k])
            if relay:
                block = tok[p].at[neighbour(axis, k), halves[k]]
                remote(block, block, r.tok_send.at[p], r.tok_half.at[p, k], axis_peer(axis, stride)).start()
            send_far(p, 1 + k)
    pass_far(0)
    if relay:
        for p in range(3):
            for k in range(2):
                wait_bytes(tok[p].at[0, halves[k]], r.tok_half.at[p, k])
            send_far(p, 3)
    for p in range(3):
        wait_bytes(r.all_keys.at[p, 0, pl.ds(0, side - 1)], r.key_recv.at[p])
        for offset in range(1, side):
            keys = r.all_keys.at[p, me[OUT[p][1]]]
            remote(
                keys, keys, r.far_key_send.at[p], r.far_key_recv.at[p, offset - 1], axis_peer(OUT[p][1], offset)
            ).start()
    for offset in range(1, side):
        for p in range(3):
            axis = BACK[p][2]
            remote(
                r.my_gates, r.line_gates.at[p, me[axis]], r.gate_send.at[p], r.gate_recv.at[p], axis_peer(axis, offset)
            ).start()


    n_heads = r.query.shape[1] // head_dim
    per_key = r.query.shape[1] // r.key.shape[1]
    causal = lax.broadcasted_iota(I32, (tokens, tokens), 0) >= lax.broadcasted_iota(I32, (tokens, tokens), 1)

    def one_head(h, carry):
        cols = pl.ds(pl.multiple_of(h * head_dim, head_dim), head_dim)
        key_cols = pl.ds(pl.multiple_of(h // per_key * head_dim, head_dim), head_dim)
        scores = lax.dot_general(
            r.query[:, cols], r.key[:, key_cols], (((1,), (1,)), ((), ())), preferred_element_type=F32
        )
        scores = jnp.where(causal, scores * head_dim ** -0.5, -jnp.inf)
        power = jnp.exp(scores - jnp.max(scores, axis=1, keepdims=True))
        prob = (power / jnp.sum(power, axis=1, keepdims=True)).astype(BF16)
        r.query[:, cols] = dot(prob, r.value[:, key_cols]).astype(BF16)
        return carry


    stage = r.stage
    blocks = N_CHUNKS * mates
    out_mate = [me[OUT[p][2]] * 2 + me['c'] for p in range(3)]
    back_mate = [me[BACK[p][0]] * 2 + me['c'] for p in range(3)]

    def pick_rows(p, i, d, slot, source, wanted):
        keys = r.all_keys[p, i, d]
        for lo, n in steps(tokens, 128):
            hit = wanted[:, 0:n] == keys[0:1, lo : lo + n]
            for j in range(1, top_k):
                hit = jnp.logical_or(hit, wanted[:, 0:n] == keys[j : j + 1, lo : lo + n])
            r.split[0 : blocks * slots, lo : lo + n] = jnp.where(hit, 1.0, 0.0).astype(BF16)
        for lo, n in steps(widths[p], TILE):
            found = dot(r.split[0 : blocks * slots, 0:tokens], source[:, lo : lo + n]).astype(BF16)
            stage[slot, 0:blocks, :, lo : lo + n] = found.reshape(blocks, slots, n)

    def flush(p, i, d, slot):
        a, b = ordered({OUT[p][1]: i, OUT[p][0]: d})
        return pltpu.make_async_copy(
            stage.at[slot, pl.ds(0, blocks), :, pl.ds(0, widths[p])],
            sends[p].at[pl.ds(0, blocks), a, b],
            r.stage_sem.at[slot],
        )

    def keep(p, i, d, slot, chunk):
        spot = {**me, OUT[p][1]: i, OUT[p][0]: d}
        return pltpu.make_async_copy(
            stage.at[slot, out_mate[p] * N_CHUNKS + chunk, :, pl.ds(0, widths[p])],
            arrivals[p].at[(chunk,) + ordered(spot)],
            r.keep_sem.at[slot, chunk],
        )

    wanted = [mate_keys(p, (blocks * slots, min(128, tokens))) for p in range(3)]

    def send_rows(p, first, count):
        near, far_axis, axis = OUT[p]

        def one_mate(offset, c):
            place = mate_peer(axis, offset)
            mate = place[axis] * 2 + place['c']
            remote(
                sends[p].at[pl.ds(mate * N_CHUNKS + first, count)],
                rows_of(arrivals[p], p, pl.ds(first, count), me, (near, far_axis)),
                r.go_send.at[min(first, 1), p],
                r.go_recv.at[min(first, 1), p],
                place,
            ).start()
            return c

        lax.fori_loop(1, mates, one_mate, 0)

    def pick_group(offset):
        for p in range(3):
            i = lax.rem(me[OUT[p][1]] + side - offset, side)
            if offset:
                wait_bytes(r.all_keys.at[p, 0], r.far_key_recv.at[p, offset - 1])
            if relay and offset == 2:
                for n in range(side):
                    for k in range(2):
                        wait_bytes(tok[p].at[0, halves[k]], r.far_half.at[p, k, n])

            def load(d, slot):
                return pltpu.make_async_copy(
                    far[p].at[i, d], r.source.at[slot, :, pl.ds(0, widths[p])], r.source_sem.at[slot]
                )

            if offset:
                load(0, 0).start()

            def one_source(d, c):
                slot = lax.rem(d, 2)
                if offset:

                    @pl.when(d + 1 < side)
                    def _():
                        load(d + 1, 1 - slot).start()

                    load(d, slot).wait()

                @pl.when(d >= 2)
                def _():
                    flush(p, i, d - 2, slot).wait()
                    for chunk in range(N_CHUNKS):
                        keep(p, i, d - 2, slot, chunk).wait()

                pick_rows(p, i, d, slot, r.source.at[slot] if offset else tok[p].at[d], wanted[p])
                flush(p, i, d, slot).start()
                for chunk in range(N_CHUNKS):
                    keep(p, i, d, slot, chunk).start()
                return c

            lax.fori_loop(0, side, one_source, 0)
            for d in range(side - 2, side):
                flush(p, i, d, d % 2).wait()
                for chunk in range(N_CHUNKS):
                    keep(p, i, d, d % 2, chunk).wait()

    def heads(part, n_parts):
        lax.fori_loop(n_heads * part // n_parts, n_heads * (part + 1) // n_parts, one_head, 0)

    pick_group(0)
    for n in range(1, side):
        pass_far(n)
        heads(n - 1, side - 1)
    for offset in (1, 3, 2) if relay else (1,):
        pick_group(offset)
    for first, count in ((0, 1), (1, N_CHUNKS - 1)):
        for p in range(3):
            send_rows(p, first, count)


    out_split = n_heads * head_dim // model

    def out_body(i, tiles):
        total = r.hidden[:, col_tile(i)].astype(F32)
        attended = dot(r.query[:, 0:model], tiles[0][...])
        for s in range(1, out_split):
            attended += dot(r.query[:, s * model : (s + 1) * model], tiles[s][...])
        r.attended[:, col_tile(i)] = (total + attended).astype(BF16)

    stream(model // TILE, out_split, lambda i, s: r.w_out.at[pl.ds(s * model, model), col_tile(i)], out_body)

    def norm_attended(here):
        r.rows[here, :] = rms_rows(r.attended[here, :], one_row(r.ffn_scale))

    bands(norm_attended)

    def act_body(i, tiles):
        z = dot(r.rows[...], tiles[0][...])
        u = dot(r.rows[...], tiles[1][...])
        r.act[:, col_tile(i)] = (jax.nn.silu(z) * u).astype(BF16)

    ff_dim = r.ffn_gate.shape[1]
    stream(
        ff_dim // TILE, 2, lambda i, s: (r.ffn_gate, r.ffn_up)[s].at[:, col_tile(i)], act_body
    )
    down_split = ff_dim // model

    def down_body(i, tiles):
        total = dot(r.act[:, 0:model], tiles[0][...])
        for s in range(1, down_split):
            total += dot(r.act[:, s * model : (s + 1) * model], tiles[s][...])
        r.dense[:, col_tile(i)] = r.attended[:, col_tile(i)].astype(F32) + total

    stream(model // TILE, down_split, lambda i, s: r.ffn_down.at[pl.ds(s * model, model), col_tile(i)], down_body)


    for load in loads:
        load.wait()
    x_buf, y_buf, hidden_buf = r.x_buf, r.y_buf, r.hidden_buf
    group = x_buf.shape[1:-1]
    rows = math.prod(group)
    width = hidden_buf.shape[1]

    def fetch(chunk, y, slot):
        return [
            pltpu.make_async_copy(
                arrivals[p].at[chunk, y], x_buf.at[slot, :, :, :, :, pl.ds(lo, hi - lo)], r.in_sem.at[slot, p]
            )
            for p, (lo, hi) in enumerate(parts)
        ]

    def put(chunk, y, slot):
        return [
            pltpu.make_async_copy(
                y_buf.at[slot, :, :, :, :, pl.ds(lo, hi - lo)], outputs[p].at[chunk, y], r.out_sem.at[slot, p]
            )
            for p, (lo, hi) in enumerate(parts)
        ]

    def keep_own(chunk, y, slot, p):
        lo, hi = parts[p]
        free = BACK[p][1:]
        spot = [pl.ds(0, side) if axis in free else me[axis] for axis in ROW_AXES[1:]]
        mine = pltpu.make_async_copy(
            y_buf.at[tuple([slot] + spot + [pl.ds(0, slots), pl.ds(lo, hi - lo)])],
            middles[p].at[
                (chunk,) + ordered({axis: y if axis == 'y' else pl.ds(0, side) for axis in free}) + (back_mate[p],)
            ],
            r.own_sem.at[slot, p],
        )
        return mine, (None if 'y' in free else y == me['y'])

    def start_put(chunk, y, slot):
        for copy in put(chunk, y, slot):
            copy.start()
        for p in range(3):
            copy, when = keep_own(chunk, y, slot, p)
            if when is None:
                copy.start()
            else:
                pl.when(when)(copy.start)

    def wait_put(chunk, y, slot):
        for copy in put(chunk, y, slot):
            copy.wait()
        for p in range(3):
            copy, when = keep_own(chunk, y, slot, p)
            if when is None:
                copy.wait()
            else:
                pl.when(when)(copy.wait)

    def expert_chunk(chunk):
        for first, count in ((0, 1), (1, N_CHUNKS - 1)):

            @pl.when(chunk == first)
            def _():
                for p in range(3):
                    wait_bytes(sends[p].at[pl.ds(0, count * (mates - 1))], r.go_recv.at[first, p])

        for copy in fetch(chunk, 0, 0):
            copy.start()

        def one_tile(y, c):
            slot = lax.rem(y, 2)

            @pl.when(y + 1 < side)
            def _():
                for copy in fetch(chunk, y + 1, 1 - slot):
                    copy.start()

            for copy in fetch(chunk, y, slot):
                copy.wait()

            @pl.when(y >= 2)
            def _():
                wait_put(chunk, y - 2, slot)

            for lo in range(0, width, f_chunk):
                cols = slice(lo, lo + f_chunk)
                z = dot(x_buf[slot].reshape(rows, model), r.gate[:, cols])
                u = dot(x_buf[slot].reshape(rows, model), r.up[:, cols])
                hidden_buf[:, cols] = (jax.nn.silu(z) * u).astype(BF16)
            for lo in range(0, model, d_chunk):
                cols = slice(lo, lo + d_chunk)
                y_rows = dot(hidden_buf[...], r.down[:, cols]).astype(BF16)
                y_buf[slot, :, :, :, :, cols] = y_rows.reshape(group + (d_chunk,))
            start_put(chunk, y, slot)
            return c

        lax.fori_loop(0, side, one_tile, 0)
        for y in range(side - 2, side):
            wait_put(chunk, y, y % 2)

        def one_mate(offset, c):
            for p in range(3):
                place = mate_peer(BACK[p][0], offset)
                remote(
                    rows_of(outputs[p], p, chunk, place, BACK[p][1:]),
                    middles[p].at[chunk, pl.ds(0, side), pl.ds(0, side), back_mate[p]],
                    r.back_send.at[chunk, p],
                    r.back_recv.at[chunk, p],
                    place,
                ).start()
            return c

        lax.fori_loop(1, mates, one_mate, 0)

    def middle_rows(p, chunk, i, d):
        return middles[p].at[(chunk,) + ordered({BACK[p][1]: i, BACK[p][2]: d})]

    def pass_on(chunk):
        for p in range(3):
            wait_bytes(middles[p].at[chunk, pl.ds(0, side), pl.ds(0, side), pl.ds(0, mates - 1)], r.back_recv.at[chunk, p])
            for offset in range(1, side):
                axis = BACK[p][1]
                place = axis_peer(axis, offset)
                remote(
                    middle_rows(p, chunk, place[axis], pl.ds(0, side)),
                    results[p].at[chunk, pl.ds(0, side), me[axis]],
                    r.home_send.at[chunk, p],
                    r.home_recv.at[chunk, p],
                    place,
                ).start()


    split = r.split
    lanes = min(128, rows_block)

    def weigh_chunk(chunk, carry):
        @pl.when(chunk == 1)
        def _():
            pass_on(N_CHUNKS - 1)

        for p in range(3):
            wait_bytes(results[p].at[chunk, pl.ds(0, side), pl.ds(0, side - 1)], r.home_recv.at[chunk, p])

        def source_of(p, n):
            ahead = 2 * side - 2 - 2 * n + 3 * (n // 2) if relay else 1 - n
            return lax.rem(me[BACK[p][2]] + ahead, side)

        def load(p, n, slot):
            copies = []
            for offset in range(side):
                i, d = lax.rem(me[BACK[p][1]] + offset, side), source_of(p, n)
                copies.append(
                    pltpu.make_async_copy(
                        results[p].at[chunk, d, i] if offset else middle_rows(p, chunk, i, d),
                        stage.at[slot, pl.ds(i * mates, mates), :, pl.ds(0, widths[p])],
                        r.load_sem.at[slot, offset],
                    )
                )
            return copies

        for copy in load(0, 0, 0):
            copy.start()

        def one_source(n, c):
            for p in range(3):
                d = source_of(p, n)
                slot = lax.rem(n + p, 2)

                @pl.when(n + p // 2 < side)
                def _():
                    for copy in load((p + 1) % 3, n + p // 2, 1 - slot):
                        copy.start()

                held = plane_keys(p, (1, rows_block), chunk).astype(F32)
                info = r.line_info[p, d]
                keys = [jnp.broadcast_to(info[:, j : j + 1], (tokens, lanes)) for j in range(top_k)]
                gates = [jnp.broadcast_to(info[:, top_k + j : top_k + j + 1], (tokens, lanes)) for j in range(top_k)]
                for lo in range(0, rows_block, lanes):
                    here = held[:, lo : lo + lanes]
                    weight = jnp.zeros((tokens, lanes), F32)
                    for j in range(top_k):
                        weight = jnp.where(here == keys[j], gates[j], weight)
                    high = weight.astype(BF16)
                    rest = weight - high.astype(F32)
                    middle = rest.astype(BF16)
                    low = (rest - middle.astype(F32)).astype(BF16)
                    split[0:tokens, lo : lo + lanes] = high
                    split[tokens : 2 * tokens, lo : lo + lanes] = middle
                    split[2 * tokens : 3 * tokens, lo : lo + lanes] = low
                for copy in load(p, n, slot):
                    copy.wait()
                for lo, size in steps(widths[p], TILE):
                    y = stage[slot, 0:members, :, lo : lo + size].reshape(rows_block, size)
                    both = dot(split[...], y)
                    total = both[0:tokens] + (both[tokens : 2 * tokens] + both[2 * tokens : 3 * tokens])

                    @pl.when(chunk == 0)
                    def _():
                        sums[p][d, :, lo : lo + size] = total

                    @pl.when(chunk > 0)
                    def _():
                        sums[p][d, :, lo : lo + size] += total

                last = chunk == N_CHUNKS - 1
                axis = BACK[p][2]

                @pl.when(jnp.logical_and(last, n == 0))
                def _():
                    for k, stride in enumerate(strides):
                        part, spot, arrived = sums[p].at[d], others[p].at[0], r.sum_recv.at[p, 0]
                        if relay:
                            part = sums[p].at[d, halves[k]]
                            spot, arrived = others[p].at[2, halves[k]], r.sum_half.at[p, k]
                        remote(part, spot, r.sum_send.at[p], arrived, axis_peer(axis, stride)).start()

                for k in range(2 if relay else 0):

                    @pl.when(jnp.logical_and(last, n == 2 + k))
                    def _():
                        wait_bytes(others[p].at[2, halves[k]], r.sum_half.at[p, k])
                        sums[p][d, halves[k], :] += others[p][2, halves[k], :]
                        remote(
                            sums[p].at[d], others[p].at[k], r.sum_send.at[p], r.sum_recv.at[p, k], axis_peer(axis, strides[k])
                        ).start()

            return c

        return lax.fori_loop(0, side, one_source, carry)


    def experts_and_back(chunk, carry):
        expert_chunk(chunk)
        pl.when(chunk >= 1)(lambda: pass_on(chunk - 1))
        return carry

    lax.fori_loop(0, N_CHUNKS, experts_and_back, 0)
    gap = jnp.zeros((128 - 2 * top_k, tokens), F32)
    for p in range(3):
        wait_bytes(r.line_gates.at[p, pl.ds(0, side - 1)], r.gate_recv.at[p])
        for d in range(side):
            r.line_info[p, d] = jnp.concatenate([r.line_gates[p, d], gap], axis=0).T
    lax.fori_loop(0, N_CHUNKS, weigh_chunk, 0)
    for p, (lo, hi) in enumerate(parts):
        for k in range(len(strides)):
            wait_bytes(others[p].at[k], r.sum_recv.at[p, k])

        def finish(here):
            moe = sums[p][me[BACK[p][2]], here, :]
            for k in range(len(strides)):
                moe += others[p][k, here, :]
            r.out[here, lo:hi] = (r.dense[here, lo:hi] + moe).astype(BF16)

        bands(finish)


    for p in range(3):
        wait_bytes(tok[p].at[pl.ds(0, side - 1)], r.tok_send.at[p])
        wait_bytes(r.all_keys.at[p, 0, pl.ds(0, side - 1)], r.key_send.at[p])
        wait_bytes(far[p].at[pl.ds(0, side - 1)], r.far_send.at[p])
        wait_bytes(r.all_keys.at[p, pl.ds(0, side - 1)], r.far_key_send.at[p])
        wait_bytes(r.line_gates.at[p, pl.ds(0, side - 1)], r.gate_send.at[p])
        wait_bytes(others[p], r.sum_send.at[p])
        for first, count in ((0, 1), (1, N_CHUNKS - 1)):
            wait_bytes(sends[p].at[pl.ds(0, count * (mates - 1))], r.go_send.at[first, p])
        for chunk in range(N_CHUNKS):
            wait_bytes(middles[p].at[chunk, pl.ds(0, side), pl.ds(0, side), pl.ds(0, mates - 1)], r.back_send.at[chunk, p])
            wait_bytes(results[p].at[chunk, pl.ds(0, side), pl.ds(0, side - 1)], r.home_send.at[chunk, p])


def layer_pair(small, large, side, capacity, head_dim):
    tokens, model = small['hidden'].shape
    top_k, width = small['ids_t'].shape[0], large['gate_hbm'].shape[1]
    key_dim, ff_dim = large['w_key'].shape[1], large['ffn_gate'].shape[1]
    parts = column_parts(model)
    widths = [hi - lo for lo, hi in parts]
    slots, members, mates = capacity // N_CHUNKS, side * side * 2, side * 2
    group = (side, 2, side, slots)
    rows = math.prod(group)
    sds, vmem = jax.ShapeDtypeStruct, pltpu.VMEM
    dma = lambda *shape: pltpu.SemaphoreType.DMA(shape)
    outs = dict(out=sds((tokens, model), BF16))
    scratch = dict(
        rows=vmem((tokens, model), BF16),
        query=vmem((tokens, large['w_query'].shape[1]), BF16),
        key=vmem((tokens, key_dim), BF16),
        value=vmem((tokens, key_dim), BF16),
        attended=vmem((tokens, model), BF16),
        act=vmem((tokens, ff_dim), BF16),
        dense=vmem((tokens, model), F32),
        ring=vmem((RING, model, TILE), BF16),
        all_keys=vmem((3, side, side, top_k, tokens), I32),
        my_gates=vmem((2 * top_k, tokens), F32),
        line_gates=vmem((3, side, 2 * top_k, tokens), F32),
        line_info=vmem((3, side, tokens, 128), F32),
        source=vmem((2, tokens, max(widths)), BF16),
        stage=vmem((2, max(members, N_CHUNKS * mates), slots, max(widths)), BF16),
        split=vmem((3 * tokens, members * slots), BF16),
        gate=vmem((model, width), BF16),
        up=vmem((model, width), BF16),
        down=vmem((width, model), BF16),
        x_buf=vmem((2,) + group + (model,), BF16),
        y_buf=vmem((2,) + group + (model,), BF16),
        hidden_buf=vmem((rows, width), BF16),
        weight_sem=dma(3),
        ring_sem=dma(RING),
        source_sem=dma(2),
        stage_sem=dma(2),
        keep_sem=dma(2, N_CHUNKS),
        in_sem=dma(2, 3),
        out_sem=dma(2, 3),
        own_sem=dma(2, 3),
        load_sem=dma(2, side),
        tok_send=dma(3),
        tok_recv=dma(3, 2),
        tok_half=dma(3, 2),
        key_send=dma(3),
        key_recv=dma(3),
        far_send=dma(3),
        far_recv=dma(3, 2, side),
        far_half=dma(3, 2, side),
        far_key_send=dma(3),
        far_key_recv=dma(3, side - 1),
        gate_send=dma(3),
        gate_recv=dma(3),
        sum_send=dma(3),
        sum_recv=dma(3, 2),
        sum_half=dma(3, 2),
        go_send=dma(2, 3),
        go_recv=dma(2, 3),
        back_send=dma(N_CHUNKS, 3),
        back_recv=dma(N_CHUNKS, 3),
        home_send=dma(N_CHUNKS, 3),
        home_recv=dma(N_CHUNKS, 3),
    )
    for p, w in enumerate(widths):
        there = sds((N_CHUNKS, side, side, 2, side, slots, w), BF16)
        outs['far' + str(p)] = sds((side, side, tokens, w), BF16)
        outs['send' + str(p)] = sds((N_CHUNKS * mates, side, side, slots, w), BF16)
        outs['arrive' + str(p)] = there
        outs['output' + str(p)] = there
        outs['middle' + str(p)] = sds((N_CHUNKS, side, side, mates, slots, w), BF16)
        outs['result' + str(p)] = sds((N_CHUNKS, side, side, mates, slots, w), BF16)
        scratch['tok' + str(p)] = vmem((side, tokens, w), BF16)
        scratch['sum' + str(p)] = vmem((side, tokens, w), F32)
        scratch['other' + str(p)] = vmem((side - 1, tokens, w), F32)
    anywhere = pl.BlockSpec(memory_space=pl.ANY)
    local = pl.BlockSpec(memory_space=pltpu.VMEM)
    n_rows = members * side * capacity
    return pl.pallas_call(
        functools.partial(
            kernel,
            names=tuple(small) + tuple(large) + tuple(outs) + tuple(scratch),
            side=side,
            parts=parts,
            capacity=capacity,
            head_dim=head_dim,
            f_chunk=min(256, width),
            d_chunk=min(512, model),
        ),
        out_shape=list(outs.values()),
        in_specs=[local] * len(small) + [anywhere] * len(large),
        out_specs=[local] + [anywhere] * (len(outs) - 1),
        scratch_shapes=list(scratch.values()),
        compiler_params=pltpu.CompilerParams(has_side_effects=True, vmem_limit_bytes=67043328),
        cost_estimate=pl.CostEstimate(flops=6 * n_rows * model * width, bytes_accessed=8 * n_rows * model, transcendentals=0),
    )(*small.values(), *large.values())[0]


def solution(mesh):
    group_size = mesh.shape['ep']
    side = torus_side(group_size)
    torus = jax.sharding.Mesh(mesh.devices.reshape(side, side, side, 2), AXES)
    row_spec = P(AXES, None, None)
    vec_spec = P(None)
    mat_spec = P(None, None)
    cube_spec = P(None, None, None)
    expert_spec = P(AXES, None, None)

    def per_device(hidden, expert_ids, slot_ids, attn_norm, w_query, w_key, w_value, w_out, ffn_norm, ffn_gate, ffn_up, ffn_down, moe_norm, w_router, exp_gate, exp_up, exp_down):
        n_seqs, tokens, model = hidden.shape
        assert n_seqs == 1 and exp_gate.shape[0] == 1
        n_heads, head_dim = w_out.shape[0], w_out.shape[1]
        top_k = expert_ids.shape[2]
        capacity = CAP_FACTOR * tokens * top_k // group_size
        inv_freq = np.float32(ROPE_BASE) ** (np.float32(-2.0) * np.arange(head_dim // 2, dtype=np.float32) / head_dim)
        angles = np.arange(tokens, dtype=np.float32)[:, None] * inv_freq[None, :]
        cos, sin = np.cos(angles), np.sin(angles)
        small = dict(
            hidden=hidden[0],
            attn_scale=attn_norm.reshape(-1, 128),
            moe_scale=moe_norm.reshape(-1, 128),
            ffn_scale=ffn_norm.reshape(-1, 128),
            ids_t=expert_ids[0].T,
            slots_t=slot_ids[0].T,
            w_router=w_router,
            cos=np.concatenate([cos, cos], axis=1).astype(np.float32),
            sin=np.concatenate([-sin, sin], axis=1).astype(np.float32),
        )
        large = dict(
            w_query=w_query,
            w_key=w_key,
            w_value=w_value,
            w_out=w_out.reshape(n_heads * head_dim, model),
            ffn_gate=ffn_gate,
            ffn_up=ffn_up,
            ffn_down=ffn_down,
            gate_hbm=exp_gate[0],
            up_hbm=exp_up[0],
            down_hbm=exp_down[0],
        )
        return layer_pair(small, large, side, capacity, head_dim).reshape(hidden.shape)

    return jax.shard_map(per_device, mesh=torus, in_specs=(row_spec, row_spec, row_spec, vec_spec, mat_spec, mat_spec, mat_spec, cube_spec, vec_spec, mat_spec, mat_spec, mat_spec, vec_spec, mat_spec, expert_spec, expert_spec, expert_spec), out_specs=row_spec, check_vma=False)
```

```python
import functools
import math
import types

import jax
import jax.numpy as jnp
import numpy as np
from jax import lax
from jax.experimental import pallas as pl
from jax.experimental.pallas import tpu as pltpu
from jax.sharding import PartitionSpec as P

RMS_EPS = 1e-6
ROPE_BASE = 10000.0
CAP_FACTOR = 3
N_CHUNKS = 3
RING = 6
TILE = 256
MESH = pl.DeviceIdType.MESH

BF16, F32, I32 = jnp.bfloat16, jnp.float32, jnp.int32

AXES = ('z', 'y', 'x', 'c')
OUT = (('z', 'y', 'x'), ('x', 'z', 'y'), ('y', 'x', 'z'))
BACK = (('y', 'z', 'x'), ('z', 'x', 'y'), ('x', 'y', 'z'))
ROW_AXES = ('y', 'x', 'c', 'z')


def torus_side(n_devices):
    side = round((n_devices // 2) ** (1 / 3))
    assert side ** 3 * 2 == n_devices
    return side


def column_parts(model):
    lanes = model // 128
    first = -(-lanes // 3)
    second = -(-(lanes - first) // 2)
    ends = (0, first * 128, (first + second) * 128, model)
    return tuple((ends[p], ends[p + 1]) for p in range(3))


def steps(total, size):
    return [(lo, min(size, total - lo)) for lo in range(0, total, size)]


def rms_rows(rows, scale):
    as_float = rows.astype(F32)
    inv_rms = lax.rsqrt(jnp.mean(as_float * as_float, axis=-1, keepdims=True) + RMS_EPS)
    return (as_float * inv_rms * scale.astype(F32)).astype(BF16)


def dot(a, b):
    return jnp.dot(a, b, preferred_element_type=F32)


def kernel(*refs, names, side, parts, capacity, head_dim, f_chunk, d_chunk):
    r = types.SimpleNamespace(**dict(zip(names, refs)))
    each = lambda name: [getattr(r, name + str(p)) for p in range(3)]
    slots = capacity // N_CHUNKS
    members = side * side * 2
    mates = side * 2
    assert side in (2, 4)
    relay = side == 4
    strides = (1, side - 1) if relay else (1,)
    order = (0, side - 1, 1, 2) if relay else (0, 1)
    rows_block = members * slots
    tokens, model = r.hidden.shape
    me = {axis: lax.axis_index(axis) for axis in AXES}


    def rows_of(ref, p, chunk, place, free):
        spot = [pl.ds(0, side) if axis in free else place[axis] for axis in ROW_AXES]
        return ref.at[tuple([chunk] + spot)]

    def ordered(where):
        return tuple(where[axis] for axis in ROW_AXES if axis in where)

    def device(place):
        return tuple(place[axis] for axis in AXES)

    def axis_peer(axis, offset):
        return {**me, axis: lax.rem(me[axis] + offset, side)}

    def mate_peer(axis, offset):
        return {
            **me,
            axis: lax.rem(me[axis] + offset // 2, side),
            'c': lax.rem(me['c'] + lax.rem(offset, 2), 2),
        }

    def remote(src, dst, send_sem, recv_sem, place):
        return pltpu.make_async_remote_copy(
            src_ref=src, dst_ref=dst, send_sem=send_sem, recv_sem=recv_sem, device_id=device(place), device_id_type=MESH
        )

    def wait_bytes(ref, sem):
        pltpu.make_async_copy(ref, ref, sem).wait()

    def expert_key(place, core, slot):
        return (((place['z'] * side + place['y']) * side + place['x']) * 2 + core) * capacity + slot

    def plane_keys(p, shape, chunk):
        first, second, _ = BACK[p]
        row = lax.broadcasted_iota(I32, shape, 1)
        which, slot = row // slots, lax.rem(row, slots)
        pair = which // 2
        place = {**me, second: pair // side, first: lax.rem(pair, side)}
        return expert_key(place, lax.rem(which, 2), slot + chunk * slots)

    def mate_keys(p, shape):
        mate = lax.broadcasted_iota(I32, shape, 0)
        return expert_key({**me, OUT[p][2]: mate // 2}, lax.rem(mate, 2), 0)

    tok, far, sends, arrivals, outputs = each('tok'), each('far'), each('send'), each('arrive'), each('output')
    middles, results, sums, others = each('middle'), each('result'), each('sum'), each('other')
    widths = [hi - lo for lo, hi in parts]


    band = min(32, tokens)

    def bands(body):
        lax.fori_loop(0, tokens // band, lambda i, c: (body(pl.ds(pl.multiple_of(i * band, band), band)), c)[1], 0)

    def one_row(scale):
        lines = scale[...].astype(F32)
        return jnp.concatenate([lines[i : i + 1, :] for i in range(lines.shape[0])], axis=1)

    def norm_both(here):
        normed = rms_rows(r.hidden[here, :], one_row(r.moe_scale))
        for p, (lo, hi) in enumerate(parts):
            tok[p][me[OUT[p][0]], here, :] = normed[:, lo:hi]
        r.rows[here, :] = rms_rows(r.hidden[here, :], one_row(r.attn_scale))

    bands(norm_both)
    keys_t = r.ids_t[...] * capacity + r.slots_t[...]
    for p in range(3):
        r.all_keys[p, me[OUT[p][1]], me[OUT[p][0]]] = keys_t
    pairs = ((r.gate_hbm, r.gate), (r.up_hbm, r.up), (r.down_hbm, r.down))
    loads = [pltpu.make_async_copy(src, dst, r.weight_sem.at[i]) for i, (src, dst) in enumerate(pairs)]
    for load in loads:
        load.start()

    half = tokens // 2
    halves = (pl.ds(0, half), pl.ds(half, half))

    def neighbour(axis, k):
        return lax.rem(me[axis] + side - strides[k], side)

    def send_far(p, n):
        near, axis, _ = OUT[p]
        d = lax.rem(me[near] + order[n], side)
        for k, stride in enumerate(strides):
            remote(
                tok[p].at[d], far[p].at[me[axis], d], r.far_send.at[p], r.far_recv.at[p, k, n], axis_peer(axis, stride)
            ).start()

    def pass_far(n):
        for k, stride in enumerate(strides):
            for p in range(3):
                near, axis, _ = OUT[p]
                d = lax.rem(me[near] + order[n], side)
                wait_bytes(tok[p].at[0], r.far_recv.at[p, k, n])
                if relay:
                    block = far[p].at[neighbour(axis, k), d, halves[k]]
                    remote(block, block, r.far_send.at[p], r.far_half.at[p, k, n], axis_peer(axis, stride)).start()

    for k, stride in enumerate(strides):
        for p in range(3):
            axis = OUT[p][0]
            block = tok[p].at[me[axis]]
            remote(block, block, r.tok_send.at[p], r.tok_recv.at[p, k], axis_peer(axis, stride)).start()
    for p in range(3):
        send_far(p, 0)
    for offset in range(1, side):
        for p in range(3):
            axis = OUT[p][0]
            keys = r.all_keys.at[p, me[OUT[p][1]], me[axis]]
            remote(keys, keys, r.key_send.at[p], r.key_recv.at[p], axis_peer(axis, offset)).start()


    ring = r.ring
    ring_sem = r.ring_sem

    def stream(n_steps, group, source, body):
        ahead = RING // group * group - group

        def copy(i, s):
            slot = lax.rem(i * group + s, RING // group * group)
            return pltpu.make_async_copy(source(i, s), ring.at[slot], ring_sem.at[slot])

        for i in range(min(ahead // group, n_steps)):
            for s in range(group):
                copy(i, s).start()

        def step(i, carry):
            @pl.when(i + ahead // group < n_steps)
            def _():
                for s in range(group):
                    copy(i + ahead // group, s).start()

            for s in range(group):
                copy(i, s).wait()
            body(i, [ring.at[lax.rem(i * group + s, RING // group * group)] for s in range(group)])
            return carry

        lax.fori_loop(0, n_steps, step, 0)

    def col_tile(i):
        return pl.ds(pl.multiple_of(i * TILE, TILE), TILE)

    def turned(y):
        return y * r.cos[...] + pltpu.roll(y, head_dim // 2, 1) * r.sin[...]

    def project(weight, out, rotary):
        def body(i, tiles):
            y = dot(r.rows[...], tiles[0][...])
            if rotary:
                y = jnp.concatenate([turned(y[:, lo : lo + head_dim]) for lo in range(0, TILE, head_dim)], axis=1)
            out[:, col_tile(i)] = y.astype(BF16)

        stream(weight.shape[1] // TILE, 1, lambda i, s: weight.at[:, col_tile(i)], body)

    project(r.w_query, r.query, True)
    project(r.w_key, r.key, True)
    project(r.w_value, r.value, False)


    logits = sum(dot(tok[p][me[OUT[p][0]]], r.w_router[lo:hi, :]) for p, (lo, hi) in enumerate(parts))
    top_k = r.ids_t.shape[0]
    gap = jnp.zeros((128 - 3 * top_k, tokens), F32)
    blank = jnp.zeros((top_k, tokens), F32)
    info = jnp.concatenate([keys_t.astype(F32), blank, r.ids_t[...].astype(F32), gap], axis=0).T
    lane = lax.broadcasted_iota(I32, logits.shape, 1).astype(F32)
    picked = [
        jnp.sum(jnp.where(lane == info[:, 2 * top_k + j : 2 * top_k + j + 1], logits, 0.0), axis=1, keepdims=True)
        for j in range(top_k)
    ]
    peak = functools.reduce(jnp.maximum, picked)
    powers = [jnp.exp(v - peak) for v in picked]
    norm = functools.reduce(jnp.add, powers)
    lane = lax.broadcasted_iota(I32, info.shape, 1)
    for j in range(top_k):
        info = jnp.where(lane == top_k + j, powers[j] / norm, info)
    r.my_gates[...] = info.T[0 : 2 * top_k, :]
    for p in range(3):
        r.line_gates[p, me[BACK[p][2]]] = r.my_gates[...]


    for k, stride in enumerate(strides):
        for p in range(3):
            axis = OUT[p][0]
            wait_bytes(tok[p].at[0], r.tok_recv.at[p, k])
            if relay:
                block = tok[p].at[neighbour(axis, k), halves[k]]
                remote(block, block, r.tok_send.at[p], r.tok_half.at[p, k], axis_peer(axis, stride)).start()
            send_far(p, 1 + k)
    pass_far(0)
    if relay:
        for p in range(3):
            for k in range(2):
                wait_bytes(tok[p].at[0, halves[k]], r.tok_half.at[p, k])
            send_far(p, 3)
    for p in range(3):
        wait_bytes(r.all_keys.at[p, 0, pl.ds(0, side - 1)], r.key_recv.at[p])
        for offset in range(1, side):
            keys = r.all_keys.at[p, me[OUT[p][1]]]
            remote(
                keys, keys, r.far_key_send.at[p], r.far_key_recv.at[p, offset - 1], axis_peer(OUT[p][1], offset)
            ).start()
    for offset in range(1, side):
        for p in range(3):
            axis = BACK[p][2]
            remote(
                r.my_gates, r.line_gates.at[p, me[axis]], r.gate_send.at[p], r.gate_recv.at[p], axis_peer(axis, offset)
            ).start()


    n_heads = r.query.shape[1] // head_dim
    per_key = r.query.shape[1] // r.key.shape[1]
    causal = lax.broadcasted_iota(I32, (tokens, tokens), 0) >= lax.broadcasted_iota(I32, (tokens, tokens), 1)

    def one_head(h, carry):
        cols = pl.ds(pl.multiple_of(h * head_dim, head_dim), head_dim)
        key_cols = pl.ds(pl.multiple_of(h // per_key * head_dim, head_dim), head_dim)
        scores = lax.dot_general(
            r.query[:, cols], r.key[:, key_cols], (((1,), (1,)), ((), ())), preferred_element_type=F32
        )
        scores = jnp.where(causal, scores * head_dim ** -0.5, -jnp.inf)
        power = jnp.exp(scores - jnp.max(scores, axis=1, keepdims=True))
        prob = (power / jnp.sum(power, axis=1, keepdims=True)).astype(BF16)
        r.query[:, cols] = dot(prob, r.value[:, key_cols]).astype(BF16)
        return carry


    stage = r.stage
    blocks = N_CHUNKS * mates
    out_mate = [me[OUT[p][2]] * 2 + me['c'] for p in range(3)]
    back_mate = [me[BACK[p][0]] * 2 + me['c'] for p in range(3)]

    def pick_rows(p, i, d, slot, source):
        keys = r.all_keys[p, i, d]
        first = mate_keys(p, (mates, tokens))
        held = jnp.full((mates, tokens), -1, I32)
        for j in range(top_k):
            slot_there = keys[j : j + 1, :] - first
            mine = jnp.logical_and(slot_there >= 0, slot_there < capacity)
            held = jnp.where(mine, slot_there, held)
        row_slot = lax.broadcasted_iota(I32, (capacity, tokens), 0)
        for mate in range(mates):
            pick = jnp.where(row_slot == held[mate : mate + 1, :], 1.0, 0.0).astype(BF16)
            for chunk in range(N_CHUNKS):
                at = (chunk * mates + mate) * slots
                r.split[at : at + slots, 0:tokens] = pick[chunk * slots : (chunk + 1) * slots, :]
        for lo, n in steps(widths[p], TILE):
            found = dot(r.split[0 : blocks * slots, 0:tokens], source[:, lo : lo + n]).astype(BF16)
            stage[slot, 0:blocks, :, lo : lo + n] = found.reshape(blocks, slots, n)

    def flush(p, i, d, slot):
        a, b = ordered({OUT[p][1]: i, OUT[p][0]: d})
        return pltpu.make_async_copy(
            stage.at[slot, pl.ds(0, blocks), :, pl.ds(0, widths[p])],
            sends[p].at[pl.ds(0, blocks), a, b],
            r.stage_sem.at[slot],
        )

    def keep(p, i, d, slot, chunk):
        spot = {**me, OUT[p][1]: i, OUT[p][0]: d}
        return pltpu.make_async_copy(
            stage.at[slot, chunk * mates + out_mate[p], :, pl.ds(0, widths[p])],
            arrivals[p].at[(chunk,) + ordered(spot)],
            r.keep_sem.at[slot, chunk],
        )

    def send_rows(p, chunk, i):
        near, far_axis, axis = OUT[p]
        free = (near,) if i is not None else (near, far_axis)
        a, b = ordered({far_axis: pl.ds(0, side) if i is None else i, near: pl.ds(0, side)})
        group_place = me if i is None else {**me, far_axis: i}

        def one_mate(offset, c):
            place = mate_peer(axis, offset)
            remote(
                sends[p].at[chunk * mates + place[axis] * 2 + place['c'], a, b],
                rows_of(arrivals[p], p, chunk, group_place, free),
                r.go_send.at[chunk, p],
                r.go_recv.at[chunk, p],
                place,
            ).start()
            return c

        lax.fori_loop(1, mates, one_mate, 0)

    def pick_group(offset):
        for p in range(3):
            i = lax.rem(me[OUT[p][1]] + side - offset, side)
            if offset:
                wait_bytes(r.all_keys.at[p, 0], r.far_key_recv.at[p, offset - 1])
            if relay and offset == 2:
                for n in range(side):
                    for k in range(2):
                        wait_bytes(tok[p].at[0, halves[k]], r.far_half.at[p, k, n])

            def load(d, slot):
                return pltpu.make_async_copy(
                    far[p].at[i, d], r.source.at[slot, :, pl.ds(0, widths[p])], r.source_sem.at[slot]
                )

            if offset:
                load(0, 0).start()

            def one_source(d, c):
                slot = lax.rem(d, 2)
                if offset:

                    @pl.when(d + 1 < side)
                    def _():
                        load(d + 1, 1 - slot).start()

                    load(d, slot).wait()

                @pl.when(d >= 2)
                def _():
                    flush(p, i, d - 2, slot).wait()
                    for chunk in range(N_CHUNKS):
                        keep(p, i, d - 2, slot, chunk).wait()

                pick_rows(p, i, d, slot, r.source.at[slot] if offset else tok[p].at[d])
                flush(p, i, d, slot).start()
                for chunk in range(N_CHUNKS):
                    keep(p, i, d, slot, chunk).start()
                return c

            lax.fori_loop(0, side, one_source, 0)
            for d in range(side - 2, side):
                flush(p, i, d, d % 2).wait()
                for chunk in range(N_CHUNKS):
                    keep(p, i, d, d % 2, chunk).wait()
            if offset:
                send_rows(p, 0, i)

    def heads(part, n_parts):
        lax.fori_loop(n_heads * part // n_parts, n_heads * (part + 1) // n_parts, one_head, 0)

    pick_group(0)
    for n in range(1, side):
        pass_far(n)
        heads(n - 1, side - 1)
    for p in range(3):
        send_rows(p, 0, me[OUT[p][1]])
    for offset in (1, 3, 2) if relay else (1,):
        pick_group(offset)
    for chunk in range(1, N_CHUNKS):
        for p in range(3):
            send_rows(p, chunk, None)


    out_split = n_heads * head_dim // model

    def out_body(i, tiles):
        total = r.hidden[:, col_tile(i)].astype(F32)
        attended = dot(r.query[:, 0:model], tiles[0][...])
        for s in range(1, out_split):
            attended += dot(r.query[:, s * model : (s + 1) * model], tiles[s][...])
        r.attended[:, col_tile(i)] = (total + attended).astype(BF16)

    stream(model // TILE, out_split, lambda i, s: r.w_out.at[pl.ds(s * model, model), col_tile(i)], out_body)

    def norm_attended(here):
        r.rows[here, :] = rms_rows(r.attended[here, :], one_row(r.ffn_scale))

    bands(norm_attended)

    def act_body(i, tiles):
        z = dot(r.rows[...], tiles[0][...])
        u = dot(r.rows[...], tiles[1][...])
        r.act[:, col_tile(i)] = (jax.nn.silu(z) * u).astype(BF16)

    ff_dim = r.ffn_gate.shape[1]
    stream(
        ff_dim // TILE, 2, lambda i, s: (r.ffn_gate, r.ffn_up)[s].at[:, col_tile(i)], act_body
    )
    down_split = ff_dim // model

    def down_body(i, tiles):
        total = dot(r.act[:, 0:model], tiles[0][...])
        for s in range(1, down_split):
            total += dot(r.act[:, s * model : (s + 1) * model], tiles[s][...])
        r.dense[:, col_tile(i)] = r.attended[:, col_tile(i)].astype(F32) + total

    stream(model // TILE, down_split, lambda i, s: r.ffn_down.at[pl.ds(s * model, model), col_tile(i)], down_body)


    for load in loads:
        load.wait()
    x_buf, y_buf, hidden_buf = r.x_buf, r.y_buf, r.hidden_buf
    group = x_buf.shape[1:-1]
    rows = math.prod(group)
    width = hidden_buf.shape[1]

    def fetch(chunk, y, slot):
        return [
            pltpu.make_async_copy(
                arrivals[p].at[chunk, y], x_buf.at[slot, :, :, :, :, pl.ds(lo, hi - lo)], r.in_sem.at[slot, p]
            )
            for p, (lo, hi) in enumerate(parts)
        ]

    def put(chunk, y, slot):
        return [
            pltpu.make_async_copy(
                y_buf.at[slot, :, :, :, :, pl.ds(lo, hi - lo)], outputs[p].at[chunk, y], r.out_sem.at[slot, p]
            )
            for p, (lo, hi) in enumerate(parts)
        ]

    def keep_own(chunk, y, slot, p):
        lo, hi = parts[p]
        free = BACK[p][1:]
        spot = [pl.ds(0, side) if axis in free else me[axis] for axis in ROW_AXES[1:]]
        mine = pltpu.make_async_copy(
            y_buf.at[tuple([slot] + spot + [pl.ds(0, slots), pl.ds(lo, hi - lo)])],
            middles[p].at[
                (chunk,) + ordered({axis: y if axis == 'y' else pl.ds(0, side) for axis in free}) + (back_mate[p],)
            ],
            r.own_sem.at[slot, p],
        )
        return mine, (None if 'y' in free else y == me['y'])

    def start_put(chunk, y, slot):
        for copy in put(chunk, y, slot):
            copy.start()
        for p in range(3):
            copy, when = keep_own(chunk, y, slot, p)
            if when is None:
                copy.start()
            else:
                pl.when(when)(copy.start)

    def wait_put(chunk, y, slot):
        for copy in put(chunk, y, slot):
            copy.wait()
        for p in range(3):
            copy, when = keep_own(chunk, y, slot, p)
            if when is None:
                copy.wait()
            else:
                pl.when(when)(copy.wait)

    def expert_chunk(chunk):
        for p in range(3):
            wait_bytes(sends[p].at[pl.ds(0, mates - 1)], r.go_recv.at[chunk, p])
        for copy in fetch(chunk, 0, 0):
            copy.start()

        def one_tile(y, c):
            slot = lax.rem(y, 2)

            @pl.when(y + 1 < side)
            def _():
                for copy in fetch(chunk, y + 1, 1 - slot):
                    copy.start()

            for copy in fetch(chunk, y, slot):
                copy.wait()

            @pl.when(y >= 2)
            def _():
                wait_put(chunk, y - 2, slot)

            for lo in range(0, width, f_chunk):
                cols = slice(lo, lo + f_chunk)
                z = dot(x_buf[slot].reshape(rows, model), r.gate[:, cols])
                u = dot(x_buf[slot].reshape(rows, model), r.up[:, cols])
                hidden_buf[:, cols] = (jax.nn.silu(z) * u).astype(BF16)
            for lo in range(0, model, d_chunk):
                cols = slice(lo, lo + d_chunk)
                y_rows = dot(hidden_buf[...], r.down[:, cols]).astype(BF16)
                y_buf[slot, :, :, :, :, cols] = y_rows.reshape(group + (d_chunk,))
            start_put(chunk, y, slot)
            return c

        lax.fori_loop(0, side, one_tile, 0)
        for y in range(side - 2, side):
            wait_put(chunk, y, y % 2)

        def one_mate(offset, c):
            for p in range(3):
                place = mate_peer(BACK[p][0], offset)
                remote(
                    rows_of(outputs[p], p, chunk, place, BACK[p][1:]),
                    middles[p].at[chunk, pl.ds(0, side), pl.ds(0, side), back_mate[p]],
                    r.back_send.at[chunk, p],
                    r.back_recv.at[chunk, p],
                    place,
                ).start()
            return c

        lax.fori_loop(1, mates, one_mate, 0)

    def middle_rows(p, chunk, i, d):
        return middles[p].at[(chunk,) + ordered({BACK[p][1]: i, BACK[p][2]: d})]

    def pass_on(chunk):
        for p in range(3):
            wait_bytes(middles[p].at[chunk, pl.ds(0, side), pl.ds(0, side), pl.ds(0, mates - 1)], r.back_recv.at[chunk, p])
            for offset in range(1, side):
                axis = BACK[p][1]
                place = axis_peer(axis, offset)
                remote(
                    middle_rows(p, chunk, place[axis], pl.ds(0, side)),
                    results[p].at[chunk, pl.ds(0, side), me[axis]],
                    r.home_send.at[chunk, p],
                    r.home_recv.at[chunk, p],
                    place,
                ).start()


    split = r.split
    lanes = min(128, rows_block)

    def weigh_chunk(chunk, carry):
        @pl.when(chunk == 1)
        def _():
            pass_on(N_CHUNKS - 1)

        for p in range(3):
            wait_bytes(results[p].at[chunk, pl.ds(0, side), pl.ds(0, side - 1)], r.home_recv.at[chunk, p])

        def source_of(p, n):
            ahead = 2 * side - 2 - 2 * n + 3 * (n // 2) if relay else 1 - n
            return lax.rem(me[BACK[p][2]] + ahead, side)

        def load(p, n, slot):
            copies = []
            for offset in range(side):
                i, d = lax.rem(me[BACK[p][1]] + offset, side), source_of(p, n)
                copies.append(
                    pltpu.make_async_copy(
                        results[p].at[chunk, d, i] if offset else middle_rows(p, chunk, i, d),
                        stage.at[slot, pl.ds(i * mates, mates), :, pl.ds(0, widths[p])],
                        r.load_sem.at[slot, offset],
                    )
                )
            return copies

        for copy in load(0, 0, 0):
            copy.start()

        def one_source(n, c):
            for p in range(3):
                d = source_of(p, n)
                slot = lax.rem(n + p, 2)

                @pl.when(n + p // 2 < side)
                def _():
                    for copy in load((p + 1) % 3, n + p // 2, 1 - slot):
                        copy.start()

                held = plane_keys(p, (1, rows_block), chunk).astype(F32)
                info = r.line_info[p, d]
                keys = [jnp.broadcast_to(info[:, j : j + 1], (tokens, lanes)) for j in range(top_k)]
                gates = [jnp.broadcast_to(info[:, top_k + j : top_k + j + 1], (tokens, lanes)) for j in range(top_k)]
                for lo in range(0, rows_block, lanes):
                    here = held[:, lo : lo + lanes]
                    weight = jnp.zeros((tokens, lanes), F32)
                    for j in range(top_k):
                        weight = jnp.where(here == keys[j], gates[j], weight)
                    high = weight.astype(BF16)
                    rest = weight - high.astype(F32)
                    middle = rest.astype(BF16)
                    low = (rest - middle.astype(F32)).astype(BF16)
                    split[0:tokens, lo : lo + lanes] = high
                    split[tokens : 2 * tokens, lo : lo + lanes] = middle
                    split[2 * tokens : 3 * tokens, lo : lo + lanes] = low
                for copy in load(p, n, slot):
                    copy.wait()
                for lo, size in steps(widths[p], TILE):
                    y = stage[slot, 0:members, :, lo : lo + size].reshape(rows_block, size)
                    both = dot(split[...], y)
                    total = both[0:tokens] + (both[tokens : 2 * tokens] + both[2 * tokens : 3 * tokens])

                    @pl.when(chunk == 0)
                    def _():
                        sums[p][d, :, lo : lo + size] = total

                    @pl.when(chunk > 0)
                    def _():
                        sums[p][d, :, lo : lo + size] += total

                last = chunk == N_CHUNKS - 1
                axis = BACK[p][2]

                @pl.when(jnp.logical_and(last, n == 0))
                def _():
                    for k, stride in enumerate(strides):
                        part, spot, arrived = sums[p].at[d], others[p].at[0], r.sum_recv.at[p, 0]
                        if relay:
                            part = sums[p].at[d, halves[k]]
                            spot, arrived = others[p].at[2, halves[k]], r.sum_half.at[p, k]
                        remote(part, spot, r.sum_send.at[p], arrived, axis_peer(axis, stride)).start()

                for k in range(2 if relay else 0):

                    @pl.when(jnp.logical_and(last, n == 2 + k))
                    def _():
                        wait_bytes(others[p].at[2, halves[k]], r.sum_half.at[p, k])
                        sums[p][d, halves[k], :] += others[p][2, halves[k], :]
                        remote(
                            sums[p].at[d], others[p].at[k], r.sum_send.at[p], r.sum_recv.at[p, k], axis_peer(axis, strides[k])
                        ).start()

            return c

        return lax.fori_loop(0, side, one_source, carry)


    def experts_and_back(chunk, carry):
        expert_chunk(chunk)
        pl.when(chunk >= 1)(lambda: pass_on(chunk - 1))
        return carry

    lax.fori_loop(0, N_CHUNKS, experts_and_back, 0)
    gap = jnp.zeros((128 - 2 * top_k, tokens), F32)
    for p in range(3):
        wait_bytes(r.line_gates.at[p, pl.ds(0, side - 1)], r.gate_recv.at[p])
        for d in range(side):
            r.line_info[p, d] = jnp.concatenate([r.line_gates[p, d], gap], axis=0).T
    lax.fori_loop(0, N_CHUNKS, weigh_chunk, 0)
    for p, (lo, hi) in enumerate(parts):
        for k in range(len(strides)):
            wait_bytes(others[p].at[k], r.sum_recv.at[p, k])

        def finish(here):
            moe = sums[p][me[BACK[p][2]], here, :]
            for k in range(len(strides)):
                moe += others[p][k, here, :]
            r.out[here, lo:hi] = (r.dense[here, lo:hi] + moe).astype(BF16)

        bands(finish)


    for p in range(3):
        wait_bytes(tok[p].at[pl.ds(0, side - 1)], r.tok_send.at[p])
        wait_bytes(r.all_keys.at[p, 0, pl.ds(0, side - 1)], r.key_send.at[p])
        wait_bytes(far[p].at[pl.ds(0, side - 1)], r.far_send.at[p])
        wait_bytes(r.all_keys.at[p, pl.ds(0, side - 1)], r.far_key_send.at[p])
        wait_bytes(r.line_gates.at[p, pl.ds(0, side - 1)], r.gate_send.at[p])
        wait_bytes(others[p], r.sum_send.at[p])
        for chunk in range(N_CHUNKS):
            wait_bytes(sends[p].at[pl.ds(0, mates - 1)], r.go_send.at[chunk, p])
            wait_bytes(middles[p].at[chunk, pl.ds(0, side), pl.ds(0, side), pl.ds(0, mates - 1)], r.back_send.at[chunk, p])
            wait_bytes(results[p].at[chunk, pl.ds(0, side), pl.ds(0, side - 1)], r.home_send.at[chunk, p])


def layer_pair(small, large, side, capacity, head_dim):
    tokens, model = small['hidden'].shape
    top_k, width = small['ids_t'].shape[0], large['gate_hbm'].shape[1]
    key_dim, ff_dim = large['w_key'].shape[1], large['ffn_gate'].shape[1]
    parts = column_parts(model)
    widths = [hi - lo for lo, hi in parts]
    slots, members, mates = capacity // N_CHUNKS, side * side * 2, side * 2
    group = (side, 2, side, slots)
    rows = math.prod(group)
    sds, vmem = jax.ShapeDtypeStruct, pltpu.VMEM
    dma = lambda *shape: pltpu.SemaphoreType.DMA(shape)
    outs = dict(out=sds((tokens, model), BF16))
    scratch = dict(
        rows=vmem((tokens, model), BF16),
        query=vmem((tokens, large['w_query'].shape[1]), BF16),
        key=vmem((tokens, key_dim), BF16),
        value=vmem((tokens, key_dim), BF16),
        attended=vmem((tokens, model), BF16),
        act=vmem((tokens, ff_dim), BF16),
        dense=vmem((tokens, model), F32),
        ring=vmem((RING, model, TILE), BF16),
        all_keys=vmem((3, side, side, top_k, tokens), I32),
        my_gates=vmem((2 * top_k, tokens), F32),
        line_gates=vmem((3, side, 2 * top_k, tokens), F32),
        line_info=vmem((3, side, tokens, 128), F32),
        source=vmem((2, tokens, max(widths)), BF16),
        stage=vmem((2, max(members, N_CHUNKS * mates), slots, max(widths)), BF16),
        split=vmem((3 * tokens, members * slots), BF16),
        gate=vmem((model, width), BF16),
        up=vmem((model, width), BF16),
        down=vmem((width, model), BF16),
        x_buf=vmem((2,) + group + (model,), BF16),
        y_buf=vmem((2,) + group + (model,), BF16),
        hidden_buf=vmem((rows, width), BF16),
        weight_sem=dma(3),
        ring_sem=dma(RING),
        source_sem=dma(2),
        stage_sem=dma(2),
        keep_sem=dma(2, N_CHUNKS),
        in_sem=dma(2, 3),
        out_sem=dma(2, 3),
        own_sem=dma(2, 3),
        load_sem=dma(2, side),
        tok_send=dma(3),
        tok_recv=dma(3, 2),
        tok_half=dma(3, 2),
        key_send=dma(3),
        key_recv=dma(3),
        far_send=dma(3),
        far_recv=dma(3, 2, side),
        far_half=dma(3, 2, side),
        far_key_send=dma(3),
        far_key_recv=dma(3, side - 1),
        gate_send=dma(3),
        gate_recv=dma(3),
        sum_send=dma(3),
        sum_recv=dma(3, 2),
        sum_half=dma(3, 2),
        go_send=dma(N_CHUNKS, 3),
        go_recv=dma(N_CHUNKS, 3),
        back_send=dma(N_CHUNKS, 3),
        back_recv=dma(N_CHUNKS, 3),
        home_send=dma(N_CHUNKS, 3),
        home_recv=dma(N_CHUNKS, 3),
    )
    for p, w in enumerate(widths):
        there = sds((N_CHUNKS, side, side, 2, side, slots, w), BF16)
        outs['far' + str(p)] = sds((side, side, tokens, w), BF16)
        outs['send' + str(p)] = sds((N_CHUNKS * mates, side, side, slots, w), BF16)
        outs['arrive' + str(p)] = there
        outs['output' + str(p)] = there
        outs['middle' + str(p)] = sds((N_CHUNKS, side, side, mates, slots, w), BF16)
        outs['result' + str(p)] = sds((N_CHUNKS, side, side, mates, slots, w), BF16)
        scratch['tok' + str(p)] = vmem((side, tokens, w), BF16)
        scratch['sum' + str(p)] = vmem((side, tokens, w), F32)
        scratch['other' + str(p)] = vmem((side - 1, tokens, w), F32)
    anywhere = pl.BlockSpec(memory_space=pl.ANY)
    local = pl.BlockSpec(memory_space=pltpu.VMEM)
    n_rows = members * side * capacity
    return pl.pallas_call(
        functools.partial(
            kernel,
            names=tuple(small) + tuple(large) + tuple(outs) + tuple(scratch),
            side=side,
            parts=parts,
            capacity=capacity,
            head_dim=head_dim,
            f_chunk=min(256, width),
            d_chunk=min(512, model),
        ),
        out_shape=list(outs.values()),
        in_specs=[local] * len(small) + [anywhere] * len(large),
        out_specs=[local] + [anywhere] * (len(outs) - 1),
        scratch_shapes=list(scratch.values()),
        compiler_params=pltpu.CompilerParams(has_side_effects=True, vmem_limit_bytes=67043328),
        cost_estimate=pl.CostEstimate(flops=6 * n_rows * model * width, bytes_accessed=8 * n_rows * model, transcendentals=0),
    )(*small.values(), *large.values())[0]


def solution(mesh):
    group_size = mesh.shape['ep']
    side = torus_side(group_size)
    torus = jax.sharding.Mesh(mesh.devices.reshape(side, side, side, 2), AXES)
    row_spec = P(AXES, None, None)
    vec_spec = P(None)
    mat_spec = P(None, None)
    cube_spec = P(None, None, None)
    expert_spec = P(AXES, None, None)

    def per_device(hidden, expert_ids, slot_ids, attn_norm, w_query, w_key, w_value, w_out, ffn_norm, ffn_gate, ffn_up, ffn_down, moe_norm, w_router, exp_gate, exp_up, exp_down):
        n_seqs, tokens, model = hidden.shape
        assert n_seqs == 1 and exp_gate.shape[0] == 1
        n_heads, head_dim = w_out.shape[0], w_out.shape[1]
        top_k = expert_ids.shape[2]
        capacity = CAP_FACTOR * tokens * top_k // group_size
        inv_freq = np.float32(ROPE_BASE) ** (np.float32(-2.0) * np.arange(head_dim // 2, dtype=np.float32) / head_dim)
        angles = np.arange(tokens, dtype=np.float32)[:, None] * inv_freq[None, :]
        cos, sin = np.cos(angles), np.sin(angles)
        small = dict(
            hidden=hidden[0],
            attn_scale=attn_norm.reshape(-1, 128),
            moe_scale=moe_norm.reshape(-1, 128),
            ffn_scale=ffn_norm.reshape(-1, 128),
            ids_t=expert_ids[0].T,
            slots_t=slot_ids[0].T,
            w_router=w_router,
            cos=np.concatenate([cos, cos], axis=1).astype(np.float32),
            sin=np.concatenate([-sin, sin], axis=1).astype(np.float32),
        )
        large = dict(
            w_query=w_query,
            w_key=w_key,
            w_value=w_value,
            w_out=w_out.reshape(n_heads * head_dim, model),
            ffn_gate=ffn_gate,
            ffn_up=ffn_up,
            ffn_down=ffn_down,
            gate_hbm=exp_gate[0],
            up_hbm=exp_up[0],
            down_hbm=exp_down[0],
        )
        return layer_pair(small, large, side, capacity, head_dim).reshape(hidden.shape)

    return jax.shard_map(per_device, mesh=torus, in_specs=(row_spec, row_spec, row_spec, vec_spec, mat_spec, mat_spec, mat_spec, cube_spec, vec_spec, mat_spec, mat_spec, mat_spec, vec_spec, mat_spec, expert_spec, expert_spec, expert_spec), out_specs=row_spec, check_vma=False)
```

```python
import functools
import math
import types

import jax
import jax.numpy as jnp
import numpy as np
from jax import lax
from jax.experimental import pallas as pl
from jax.experimental.pallas import tpu as pltpu
from jax.sharding import PartitionSpec as P

RMS_EPS = 1e-6
ROPE_BASE = 10000.0
CAP_FACTOR = 3
N_CHUNKS = 3
RING = 6
TILE = 256
MESH = pl.DeviceIdType.MESH

BF16, F32, I32 = jnp.bfloat16, jnp.float32, jnp.int32

AXES = ('z', 'y', 'x', 'c')
OUT = (('z', 'y', 'x'), ('x', 'z', 'y'), ('y', 'x', 'z'))
BACK = (('y', 'z', 'x'), ('z', 'x', 'y'), ('x', 'y', 'z'))
ROW_AXES = ('y', 'x', 'c', 'z')


def torus_side(n_devices):
    side = round((n_devices // 2) ** (1 / 3))
    assert side ** 3 * 2 == n_devices
    return side


def column_parts(model):
    lanes = model // 128
    first = -(-lanes // 3)
    second = -(-(lanes - first) // 2)
    ends = (0, first * 128, (first + second) * 128, model)
    return tuple((ends[p], ends[p + 1]) for p in range(3))


def steps(total, size):
    return [(lo, min(size, total - lo)) for lo in range(0, total, size)]


def rms_rows(rows, scale):
    as_float = rows.astype(F32)
    inv_rms = lax.rsqrt(jnp.mean(as_float * as_float, axis=-1, keepdims=True) + RMS_EPS)
    return (as_float * inv_rms * scale.astype(F32)).astype(BF16)


def dot(a, b):
    return jnp.dot(a, b, preferred_element_type=F32)


def kernel(*refs, names, side, parts, capacity, head_dim, f_chunk, d_chunk):
    r = types.SimpleNamespace(**dict(zip(names, refs)))
    each = lambda name: [getattr(r, name + str(p)) for p in range(3)]
    slots = capacity // N_CHUNKS
    members = side * side * 2
    mates = side * 2
    assert side in (2, 4)
    relay = side == 4
    strides = (1, side - 1) if relay else (1,)
    order = (0, side - 1, 1, 2) if relay else (0, 1)
    rows_block = members * slots
    tokens, model = r.hidden.shape
    me = {axis: lax.axis_index(axis) for axis in AXES}


    def rows_of(ref, p, chunk, place, free):
        spot = [pl.ds(0, side) if axis in free else place[axis] for axis in ROW_AXES]
        return ref.at[tuple([chunk] + spot)]

    def ordered(where):
        return tuple(where[axis] for axis in ROW_AXES if axis in where)

    def device(place):
        return tuple(place[axis] for axis in AXES)

    def axis_peer(axis, offset):
        return {**me, axis: lax.rem(me[axis] + offset, side)}

    def mate_peer(axis, offset):
        return {
            **me,
            axis: lax.rem(me[axis] + offset // 2, side),
            'c': lax.rem(me['c'] + lax.rem(offset, 2), 2),
        }

    def remote(src, dst, send_sem, recv_sem, place):
        return pltpu.make_async_remote_copy(
            src_ref=src, dst_ref=dst, send_sem=send_sem, recv_sem=recv_sem, device_id=device(place), device_id_type=MESH
        )

    def wait_bytes(ref, sem):
        pltpu.make_async_copy(ref, ref, sem).wait()

    def expert_key(place, core, slot):
        return (((place['z'] * side + place['y']) * side + place['x']) * 2 + core) * capacity + slot

    def plane_keys(p, shape):
        first, second, _ = BACK[p]
        which = lax.broadcasted_iota(I32, shape, 0)
        pair = which // 2
        place = {**me, second: pair // side, first: lax.rem(pair, side)}
        return expert_key(place, lax.rem(which, 2), 0)

    def mate_keys(p, shape):
        mate = lax.broadcasted_iota(I32, shape, 0)
        return expert_key({**me, OUT[p][2]: mate // 2}, lax.rem(mate, 2), 0)

    tok, far, sends, arrivals, outputs = each('tok'), each('far'), each('send'), each('arrive'), each('output')
    middles, results, sums, others = each('middle'), each('result'), each('sum'), each('other')
    widths = [hi - lo for lo, hi in parts]


    band = min(32, tokens)

    def bands(body):
        lax.fori_loop(0, tokens // band, lambda i, c: (body(pl.ds(pl.multiple_of(i * band, band), band)), c)[1], 0)

    def one_row(scale):
        lines = scale[...].astype(F32)
        return jnp.concatenate([lines[i : i + 1, :] for i in range(lines.shape[0])], axis=1)

    def norm_both(here):
        normed = rms_rows(r.hidden[here, :], one_row(r.moe_scale))
        for p, (lo, hi) in enumerate(parts):
            tok[p][me[OUT[p][0]], here, :] = normed[:, lo:hi]
        r.rows[here, :] = rms_rows(r.hidden[here, :], one_row(r.attn_scale))

    bands(norm_both)
    keys_t = r.ids_t[...] * capacity + r.slots_t[...]
    for p in range(3):
        r.all_keys[p, me[OUT[p][1]], me[OUT[p][0]]] = keys_t
    pairs = ((r.gate_hbm, r.gate), (r.up_hbm, r.up), (r.down_hbm, r.down))
    loads = [pltpu.make_async_copy(src, dst, r.weight_sem.at[i]) for i, (src, dst) in enumerate(pairs)]
    for load in loads:
        load.start()

    half = tokens // 2
    halves = (pl.ds(0, half), pl.ds(half, half))

    def neighbour(axis, k):
        return lax.rem(me[axis] + side - strides[k], side)

    def send_far(p, n):
        near, axis, _ = OUT[p]
        d = lax.rem(me[near] + order[n], side)
        for k, stride in enumerate(strides):
            remote(
                tok[p].at[d], far[p].at[me[axis], d], r.far_send.at[p], r.far_recv.at[p, k, n], axis_peer(axis, stride)
            ).start()

    def pass_far(n):
        for k, stride in enumerate(strides):
            for p in range(3):
                near, axis, _ = OUT[p]
                d = lax.rem(me[near] + order[n], side)
                wait_bytes(tok[p].at[0], r.far_recv.at[p, k, n])
                if relay:
                    block = far[p].at[neighbour(axis, k), d, halves[k]]
                    remote(block, block, r.far_send.at[p], r.far_half.at[p, k, n], axis_peer(axis, stride)).start()

    for k, stride in enumerate(strides):
        for p in range(3):
            axis = OUT[p][0]
            block = tok[p].at[me[axis]]
            remote(block, block, r.tok_send.at[p], r.tok_recv.at[p, k], axis_peer(axis, stride)).start()
    for p in range(3):
        send_far(p, 0)
    for offset in range(1, side):
        for p in range(3):
            axis = OUT[p][0]
            keys = r.all_keys.at[p, me[OUT[p][1]], me[axis]]
            remote(keys, keys, r.key_send.at[p], r.key_recv.at[p], axis_peer(axis, offset)).start()


    ring = r.ring
    ring_sem = r.ring_sem

    def stream(n_steps, group, source, body):
        ahead = RING // group * group - group

        def copy(i, s):
            slot = lax.rem(i * group + s, RING // group * group)
            return pltpu.make_async_copy(source(i, s), ring.at[slot], ring_sem.at[slot])

        for i in range(min(ahead // group, n_steps)):
            for s in range(group):
                copy(i, s).start()

        def step(i, carry):
            @pl.when(i + ahead // group < n_steps)
            def _():
                for s in range(group):
                    copy(i + ahead // group, s).start()

            for s in range(group):
                copy(i, s).wait()
            body(i, [ring.at[lax.rem(i * group + s, RING // group * group)] for s in range(group)])
            return carry

        lax.fori_loop(0, n_steps, step, 0)

    def col_tile(i):
        return pl.ds(pl.multiple_of(i * TILE, TILE), TILE)

    def turned(y):
        return y * r.cos[...] + pltpu.roll(y, head_dim // 2, 1) * r.sin[...]

    def project(weight, out, rotary):
        def body(i, tiles):
            y = dot(r.rows[...], tiles[0][...])
            if rotary:
                y = jnp.concatenate([turned(y[:, lo : lo + head_dim]) for lo in range(0, TILE, head_dim)], axis=1)
            out[:, col_tile(i)] = y.astype(BF16)

        stream(weight.shape[1] // TILE, 1, lambda i, s: weight.at[:, col_tile(i)], body)

    project(r.w_query, r.query, True)
    project(r.w_key, r.key, True)
    project(r.w_value, r.value, False)


    logits = sum(dot(tok[p][me[OUT[p][0]]], r.w_router[lo:hi, :]) for p, (lo, hi) in enumerate(parts))
    top_k = r.ids_t.shape[0]
    gap = jnp.zeros((128 - 3 * top_k, tokens), F32)
    blank = jnp.zeros((top_k, tokens), F32)
    info = jnp.concatenate([keys_t.astype(F32), blank, r.ids_t[...].astype(F32), gap], axis=0).T
    lane = lax.broadcasted_iota(I32, logits.shape, 1).astype(F32)
    picked = [
        jnp.sum(jnp.where(lane == info[:, 2 * top_k + j : 2 * top_k + j + 1], logits, 0.0), axis=1, keepdims=True)
        for j in range(top_k)
    ]
    peak = functools.reduce(jnp.maximum, picked)
    powers = [jnp.exp(v - peak) for v in picked]
    norm = functools.reduce(jnp.add, powers)
    lane = lax.broadcasted_iota(I32, info.shape, 1)
    for j in range(top_k):
        info = jnp.where(lane == top_k + j, powers[j] / norm, info)
    r.my_gates[...] = info.T[0 : 2 * top_k, :]
    for p in range(3):
        r.line_gates[p, me[BACK[p][2]]] = r.my_gates[...]


    for k, stride in enumerate(strides):
        for p in range(3):
            axis = OUT[p][0]
            wait_bytes(tok[p].at[0], r.tok_recv.at[p, k])
            if relay:
                block = tok[p].at[neighbour(axis, k), halves[k]]
                remote(block, block, r.tok_send.at[p], r.tok_half.at[p, k], axis_peer(axis, stride)).start()
            send_far(p, 1 + k)
    pass_far(0)
    if relay:
        for p in range(3):
            for k in range(2):
                wait_bytes(tok[p].at[0, halves[k]], r.tok_half.at[p, k])
            send_far(p, 3)
    for p in range(3):
        wait_bytes(r.all_keys.at[p, 0, pl.ds(0, side - 1)], r.key_recv.at[p])
        for offset in range(1, side):
            keys = r.all_keys.at[p, me[OUT[p][1]]]
            remote(
                keys, keys, r.far_key_send.at[p], r.far_key_recv.at[p, offset - 1], axis_peer(OUT[p][1], offset)
            ).start()
    for offset in range(1, side):
        for p in range(3):
            axis = BACK[p][2]
            remote(
                r.my_gates, r.line_gates.at[p, me[axis]], r.gate_send.at[p], r.gate_recv.at[p], axis_peer(axis, offset)
            ).start()


    n_heads = r.query.shape[1] // head_dim
    per_key = r.query.shape[1] // r.key.shape[1]
    causal = lax.broadcasted_iota(I32, (tokens, tokens), 0) >= lax.broadcasted_iota(I32, (tokens, tokens), 1)

    def one_head(h, carry):
        cols = pl.ds(pl.multiple_of(h * head_dim, head_dim), head_dim)
        key_cols = pl.ds(pl.multiple_of(h // per_key * head_dim, head_dim), head_dim)
        scores = lax.dot_general(
            r.query[:, cols], r.key[:, key_cols], (((1,), (1,)), ((), ())), preferred_element_type=F32
        )
        scores = jnp.where(causal, scores * head_dim ** -0.5, -jnp.inf)
        power = jnp.exp(scores - jnp.max(scores, axis=1, keepdims=True))
        prob = (power / jnp.sum(power, axis=1, keepdims=True)).astype(BF16)
        r.query[:, cols] = dot(prob, r.value[:, key_cols]).astype(BF16)
        return carry


    stage = r.stage
    blocks = N_CHUNKS * mates
    out_mate = [me[OUT[p][2]] * 2 + me['c'] for p in range(3)]
    back_mate = [me[BACK[p][0]] * 2 + me['c'] for p in range(3)]

    def pick_rows(p, i, d, slot, source):
        keys = r.all_keys[p, i, d]
        first = mate_keys(p, (mates, tokens))
        held = jnp.full((mates, tokens), -1, I32)
        for j in range(top_k):
            slot_there = keys[j : j + 1, :] - first
            mine = jnp.logical_and(slot_there >= 0, slot_there < capacity)
            held = jnp.where(mine, slot_there, held)
        row_slot = lax.broadcasted_iota(I32, (capacity, tokens), 0)
        for mate in range(mates):
            pick = jnp.where(row_slot == held[mate : mate + 1, :], 1.0, 0.0).astype(BF16)
            for chunk in range(N_CHUNKS):
                at = (chunk * mates + mate) * slots
                r.split[at : at + slots, 0:tokens] = pick[chunk * slots : (chunk + 1) * slots, :]
        for lo, n in steps(widths[p], TILE):
            found = dot(r.split[0 : blocks * slots, 0:tokens], source[:, lo : lo + n]).astype(BF16)
            stage[slot, 0:blocks, :, lo : lo + n] = found.reshape(blocks, slots, n)

    def flush(p, i, d, slot):
        a, b = ordered({OUT[p][1]: i, OUT[p][0]: d})
        return pltpu.make_async_copy(
            stage.at[slot, pl.ds(0, blocks), :, pl.ds(0, widths[p])],
            sends[p].at[pl.ds(0, blocks), a, b],
            r.stage_sem.at[slot],
        )

    def keep(p, i, d, slot, chunk):
        spot = {**me, OUT[p][1]: i, OUT[p][0]: d}
        return pltpu.make_async_copy(
            stage.at[slot, chunk * mates + out_mate[p], :, pl.ds(0, widths[p])],
            arrivals[p].at[(chunk,) + ordered(spot)],
            r.keep_sem.at[slot, chunk],
        )

    def send_rows(p, chunk, i):
        near, far_axis, axis = OUT[p]
        free = (near,) if i is not None else (near, far_axis)
        a, b = ordered({far_axis: pl.ds(0, side) if i is None else i, near: pl.ds(0, side)})
        group_place = me if i is None else {**me, far_axis: i}

        def one_mate(offset, c):
            place = mate_peer(axis, offset)
            remote(
                sends[p].at[chunk * mates + place[axis] * 2 + place['c'], a, b],
                rows_of(arrivals[p], p, chunk, group_place, free),
                r.go_send.at[chunk, p],
                r.go_recv.at[chunk, p],
                place,
            ).start()
            return c

        lax.fori_loop(1, mates, one_mate, 0)

    def pick_group(offset):
        for p in range(3):
            i = lax.rem(me[OUT[p][1]] + side - offset, side)
            if offset:
                wait_bytes(r.all_keys.at[p, 0], r.far_key_recv.at[p, offset - 1])
            if relay and offset == 2:
                for n in range(side):
                    for k in range(2):
                        wait_bytes(tok[p].at[0, halves[k]], r.far_half.at[p, k, n])

            def load(d, slot):
                return pltpu.make_async_copy(
                    far[p].at[i, d], r.source.at[slot, :, pl.ds(0, widths[p])], r.source_sem.at[slot]
                )

            if offset:
                load(0, 0).start()

            def one_source(d, c):
                slot = lax.rem(d, 2)
                if offset:

                    @pl.when(d + 1 < side)
                    def _():
                        load(d + 1, 1 - slot).start()

                    load(d, slot).wait()

                @pl.when(d >= 2)
                def _():
                    flush(p, i, d - 2, slot).wait()
                    for chunk in range(N_CHUNKS):
                        keep(p, i, d - 2, slot, chunk).wait()

                pick_rows(p, i, d, slot, r.source.at[slot] if offset else tok[p].at[d])
                flush(p, i, d, slot).start()
                for chunk in range(N_CHUNKS):
                    keep(p, i, d, slot, chunk).start()
                return c

            lax.fori_loop(0, side, one_source, 0)
            for d in range(side - 2, side):
                flush(p, i, d, d % 2).wait()
                for chunk in range(N_CHUNKS):
                    keep(p, i, d, d % 2, chunk).wait()
            if offset:
                send_rows(p, 0, i)

    def heads(part, n_parts):
        lax.fori_loop(n_heads * part // n_parts, n_heads * (part + 1) // n_parts, one_head, 0)

    pick_group(0)
    for n in range(1, side):
        pass_far(n)
        heads(n - 1, side - 1)
    for p in range(3):
        send_rows(p, 0, me[OUT[p][1]])
    for offset in (1, 3, 2) if relay else (1,):
        pick_group(offset)
    for chunk in range(1, N_CHUNKS):
        for p in range(3):
            send_rows(p, chunk, None)


    out_split = n_heads * head_dim // model

    def out_body(i, tiles):
        total = r.hidden[:, col_tile(i)].astype(F32)
        attended = dot(r.query[:, 0:model], tiles[0][...])
        for s in range(1, out_split):
            attended += dot(r.query[:, s * model : (s + 1) * model], tiles[s][...])
        r.attended[:, col_tile(i)] = (total + attended).astype(BF16)

    stream(model // TILE, out_split, lambda i, s: r.w_out.at[pl.ds(s * model, model), col_tile(i)], out_body)

    def norm_attended(here):
        r.rows[here, :] = rms_rows(r.attended[here, :], one_row(r.ffn_scale))

    bands(norm_attended)

    def act_body(i, tiles):
        z = dot(r.rows[...], tiles[0][...])
        u = dot(r.rows[...], tiles[1][...])
        r.act[:, col_tile(i)] = (jax.nn.silu(z) * u).astype(BF16)

    ff_dim = r.ffn_gate.shape[1]
    stream(
        ff_dim // TILE, 2, lambda i, s: (r.ffn_gate, r.ffn_up)[s].at[:, col_tile(i)], act_body
    )
    down_split = ff_dim // model

    def down_body(i, tiles):
        total = dot(r.act[:, 0:model], tiles[0][...])
        for s in range(1, down_split):
            total += dot(r.act[:, s * model : (s + 1) * model], tiles[s][...])
        r.dense[:, col_tile(i)] = r.attended[:, col_tile(i)].astype(F32) + total

    stream(model // TILE, down_split, lambda i, s: r.ffn_down.at[pl.ds(s * model, model), col_tile(i)], down_body)


    for load in loads:
        load.wait()
    x_buf, y_buf, hidden_buf = r.x_buf, r.y_buf, r.hidden_buf
    group = x_buf.shape[1:-1]
    rows = math.prod(group)
    width = hidden_buf.shape[1]

    def fetch(chunk, y, slot):
        return [
            pltpu.make_async_copy(
                arrivals[p].at[chunk, y], x_buf.at[slot, :, :, :, :, pl.ds(lo, hi - lo)], r.in_sem.at[slot, p]
            )
            for p, (lo, hi) in enumerate(parts)
        ]

    def put(chunk, y, slot):
        return [
            pltpu.make_async_copy(
                y_buf.at[slot, :, :, :, :, pl.ds(lo, hi - lo)], outputs[p].at[chunk, y], r.out_sem.at[slot, p]
            )
            for p, (lo, hi) in enumerate(parts)
        ]

    def keep_own(chunk, y, slot, p):
        lo, hi = parts[p]
        free = BACK[p][1:]
        spot = [pl.ds(0, side) if axis in free else me[axis] for axis in ROW_AXES[1:]]
        mine = pltpu.make_async_copy(
            y_buf.at[tuple([slot] + spot + [pl.ds(0, slots), pl.ds(lo, hi - lo)])],
            middles[p].at[
                (chunk,) + ordered({axis: y if axis == 'y' else pl.ds(0, side) for axis in free}) + (back_mate[p],)
            ],
            r.own_sem.at[slot, p],
        )
        return mine, (None if 'y' in free else y == me['y'])

    def start_put(chunk, y, slot):
        for copy in put(chunk, y, slot):
            copy.start()
        for p in range(3):
            copy, when = keep_own(chunk, y, slot, p)
            if when is None:
                copy.start()
            else:
                pl.when(when)(copy.start)

    def wait_put(chunk, y, slot):
        for copy in put(chunk, y, slot):
            copy.wait()
        for p in range(3):
            copy, when = keep_own(chunk, y, slot, p)
            if when is None:
                copy.wait()
            else:
                pl.when(when)(copy.wait)

    def expert_chunk(chunk):
        for p in range(3):
            wait_bytes(sends[p].at[pl.ds(0, mates - 1)], r.go_recv.at[chunk, p])
        for copy in fetch(chunk, 0, 0):
            copy.start()

        def one_tile(y, c):
            slot = lax.rem(y, 2)

            @pl.when(y + 1 < side)
            def _():
                for copy in fetch(chunk, y + 1, 1 - slot):
                    copy.start()

            for copy in fetch(chunk, y, slot):
                copy.wait()

            @pl.when(y >= 2)
            def _():
                wait_put(chunk, y - 2, slot)

            for lo in range(0, width, f_chunk):
                cols = slice(lo, lo + f_chunk)
                z = dot(x_buf[slot].reshape(rows, model), r.gate[:, cols])
                u = dot(x_buf[slot].reshape(rows, model), r.up[:, cols])
                hidden_buf[:, cols] = (jax.nn.silu(z) * u).astype(BF16)
            for lo in range(0, model, d_chunk):
                cols = slice(lo, lo + d_chunk)
                y_rows = dot(hidden_buf[...], r.down[:, cols]).astype(BF16)
                y_buf[slot, :, :, :, :, cols] = y_rows.reshape(group + (d_chunk,))
            start_put(chunk, y, slot)
            return c

        lax.fori_loop(0, side, one_tile, 0)
        for y in range(side - 2, side):
            wait_put(chunk, y, y % 2)

        def one_mate(offset, c):
            for p in range(3):
                place = mate_peer(BACK[p][0], offset)
                remote(
                    rows_of(outputs[p], p, chunk, place, BACK[p][1:]),
                    middles[p].at[chunk, pl.ds(0, side), pl.ds(0, side), back_mate[p]],
                    r.back_send.at[chunk, p],
                    r.back_recv.at[chunk, p],
                    place,
                ).start()
            return c

        lax.fori_loop(1, mates, one_mate, 0)

    def middle_rows(p, chunk, i, d):
        return middles[p].at[(chunk,) + ordered({BACK[p][1]: i, BACK[p][2]: d})]

    def pass_on(chunk):
        for p in range(3):
            wait_bytes(middles[p].at[chunk, pl.ds(0, side), pl.ds(0, side), pl.ds(0, mates - 1)], r.back_recv.at[chunk, p])
            for offset in range(1, side):
                axis = BACK[p][1]
                place = axis_peer(axis, offset)
                remote(
                    middle_rows(p, chunk, place[axis], pl.ds(0, side)),
                    results[p].at[chunk, pl.ds(0, side), me[axis]],
                    r.home_send.at[chunk, p],
                    r.home_recv.at[chunk, p],
                    place,
                ).start()


    split = r.split
    lanes = min(128, rows_block)

    def weigh_chunk(chunk, carry):
        @pl.when(chunk == 1)
        def _():
            pass_on(N_CHUNKS - 1)

        for p in range(3):
            wait_bytes(results[p].at[chunk, pl.ds(0, side), pl.ds(0, side - 1)], r.home_recv.at[chunk, p])

        def source_of(p, n):
            ahead = 2 * side - 2 - 2 * n + 3 * (n // 2) if relay else 1 - n
            return lax.rem(me[BACK[p][2]] + ahead, side)

        def load(p, n, slot):
            copies = []
            for offset in range(side):
                i, d = lax.rem(me[BACK[p][1]] + offset, side), source_of(p, n)
                copies.append(
                    pltpu.make_async_copy(
                        results[p].at[chunk, d, i] if offset else middle_rows(p, chunk, i, d),
                        stage.at[slot, pl.ds(i * mates, mates), :, pl.ds(0, widths[p])],
                        r.load_sem.at[slot, offset],
                    )
                )
            return copies

        for copy in load(0, 0, 0):
            copy.start()

        def one_source(n, c):
            for p in range(3):
                d = source_of(p, n)
                slot = lax.rem(n + p, 2)

                @pl.when(n + p // 2 < side)
                def _():
                    for copy in load((p + 1) % 3, n + p // 2, 1 - slot):
                        copy.start()

                lane = lax.broadcasted_iota(I32, (1, lanes), 1)
                wanted = (lax.rem(lane, slots) + chunk * slots).astype(F32)
                for lo in range(0, rows_block, lanes):
                    which = jnp.broadcast_to(lane // slots + lo // slots, (tokens, lanes))
                    take = functools.partial(jnp.take_along_axis, indices=which, axis=1, mode='promise_in_bounds')
                    weight = jnp.where(take(r.held[p, d]) == wanted, take(r.gates[p, d]), 0.0)
                    high = weight.astype(BF16)
                    rest = weight - high.astype(F32)
                    middle = rest.astype(BF16)
                    low = (rest - middle.astype(F32)).astype(BF16)
                    split[0:tokens, lo : lo + lanes] = high
                    split[tokens : 2 * tokens, lo : lo + lanes] = middle
                    split[2 * tokens : 3 * tokens, lo : lo + lanes] = low
                for copy in load(p, n, slot):
                    copy.wait()
                for lo, size in steps(widths[p], TILE):
                    y = stage[slot, 0:members, :, lo : lo + size].reshape(rows_block, size)
                    both = dot(split[...], y)
                    total = both[0:tokens] + (both[tokens : 2 * tokens] + both[2 * tokens : 3 * tokens])

                    @pl.when(chunk == 0)
                    def _():
                        sums[p][d, :, lo : lo + size] = total

                    @pl.when(chunk > 0)
                    def _():
                        sums[p][d, :, lo : lo + size] += total

                last = chunk == N_CHUNKS - 1
                axis = BACK[p][2]

                @pl.when(jnp.logical_and(last, n == 0))
                def _():
                    for k, stride in enumerate(strides):
                        part, spot, arrived = sums[p].at[d], others[p].at[0], r.sum_recv.at[p, 0]
                        if relay:
                            part = sums[p].at[d, halves[k]]
                            spot, arrived = others[p].at[2, halves[k]], r.sum_half.at[p, k]
                        remote(part, spot, r.sum_send.at[p], arrived, axis_peer(axis, stride)).start()

                for k in range(2 if relay else 0):

                    @pl.when(jnp.logical_and(last, n == 2 + k))
                    def _():
                        wait_bytes(others[p].at[2, halves[k]], r.sum_half.at[p, k])
                        sums[p][d, halves[k], :] += others[p][2, halves[k], :]
                        remote(
                            sums[p].at[d], others[p].at[k], r.sum_send.at[p], r.sum_recv.at[p, k], axis_peer(axis, strides[k])
                        ).start()

            return c

        return lax.fori_loop(0, side, one_source, carry)


    def experts_and_back(chunk, carry):
        expert_chunk(chunk)
        pl.when(chunk >= 1)(lambda: pass_on(chunk - 1))
        return carry

    lax.fori_loop(0, N_CHUNKS, experts_and_back, 0)
    gap = jnp.zeros((128 - members, tokens), F32)
    for p in range(3):
        wait_bytes(r.line_gates.at[p, pl.ds(0, side - 1)], r.gate_recv.at[p])
        first = plane_keys(p, (members, tokens)).astype(F32)

        def spread(d, c):
            info = r.line_gates[p, d]
            held, gate = jnp.full((members, tokens), -1.0, F32), jnp.zeros((members, tokens), F32)
            for j in range(top_k):
                there = info[j : j + 1, :] - first
                mine = jnp.logical_and(there >= 0, there < capacity)
                held = jnp.where(mine, there, held)
                gate = jnp.where(mine, info[top_k + j : top_k + j + 1, :], gate)
            r.held[p, d] = jnp.concatenate([held, gap], axis=0).T
            r.gates[p, d] = jnp.concatenate([gate, gap], axis=0).T
            return c

        lax.fori_loop(0, side, spread, 0)
    lax.fori_loop(0, N_CHUNKS, weigh_chunk, 0)
    for p, (lo, hi) in enumerate(parts):
        for k in range(len(strides)):
            wait_bytes(others[p].at[k], r.sum_recv.at[p, k])

        def finish(here):
            moe = sums[p][me[BACK[p][2]], here, :]
            for k in range(len(strides)):
                moe += others[p][k, here, :]
            r.out[here, lo:hi] = (r.dense[here, lo:hi] + moe).astype(BF16)

        bands(finish)


    for p in range(3):
        wait_bytes(tok[p].at[pl.ds(0, side - 1)], r.tok_send.at[p])
        wait_bytes(r.all_keys.at[p, 0, pl.ds(0, side - 1)], r.key_send.at[p])
        wait_bytes(far[p].at[pl.ds(0, side - 1)], r.far_send.at[p])
        wait_bytes(r.all_keys.at[p, pl.ds(0, side - 1)], r.far_key_send.at[p])
        wait_bytes(r.line_gates.at[p, pl.ds(0, side - 1)], r.gate_send.at[p])
        wait_bytes(others[p], r.sum_send.at[p])
        for chunk in range(N_CHUNKS):
            wait_bytes(sends[p].at[pl.ds(0, mates - 1)], r.go_send.at[chunk, p])
            wait_bytes(middles[p].at[chunk, pl.ds(0, side), pl.ds(0, side), pl.ds(0, mates - 1)], r.back_send.at[chunk, p])
            wait_bytes(results[p].at[chunk, pl.ds(0, side), pl.ds(0, side - 1)], r.home_send.at[chunk, p])


def layer_pair(small, large, side, capacity, head_dim):
    tokens, model = small['hidden'].shape
    top_k, width = small['ids_t'].shape[0], large['gate_hbm'].shape[1]
    key_dim, ff_dim = large['w_key'].shape[1], large['ffn_gate'].shape[1]
    parts = column_parts(model)
    widths = [hi - lo for lo, hi in parts]
    slots, members, mates = capacity // N_CHUNKS, side * side * 2, side * 2
    group = (side, 2, side, slots)
    rows = math.prod(group)
    sds, vmem = jax.ShapeDtypeStruct, pltpu.VMEM
    dma = lambda *shape: pltpu.SemaphoreType.DMA(shape)
    outs = dict(out=sds((tokens, model), BF16))
    scratch = dict(
        rows=vmem((tokens, model), BF16),
        query=vmem((tokens, large['w_query'].shape[1]), BF16),
        key=vmem((tokens, key_dim), BF16),
        value=vmem((tokens, key_dim), BF16),
        attended=vmem((tokens, model), BF16),
        act=vmem((tokens, ff_dim), BF16),
        dense=vmem((tokens, model), F32),
        ring=vmem((RING, model, TILE), BF16),
        all_keys=vmem((3, side, side, top_k, tokens), I32),
        my_gates=vmem((2 * top_k, tokens), F32),
        line_gates=vmem((3, side, 2 * top_k, tokens), F32),
        held=vmem((3, side, tokens, 128), F32),
        gates=vmem((3, side, tokens, 128), F32),
        source=vmem((2, tokens, max(widths)), BF16),
        stage=vmem((2, max(members, N_CHUNKS * mates), slots, max(widths)), BF16),
        split=vmem((3 * tokens, members * slots), BF16),
        gate=vmem((model, width), BF16),
        up=vmem((model, width), BF16),
        down=vmem((width, model), BF16),
        x_buf=vmem((2,) + group + (model,), BF16),
        y_buf=vmem((2,) + group + (model,), BF16),
        hidden_buf=vmem((rows, width), BF16),
        weight_sem=dma(3),
        ring_sem=dma(RING),
        source_sem=dma(2),
        stage_sem=dma(2),
        keep_sem=dma(2, N_CHUNKS),
        in_sem=dma(2, 3),
        out_sem=dma(2, 3),
        own_sem=dma(2, 3),
        load_sem=dma(2, side),
        tok_send=dma(3),
        tok_recv=dma(3, 2),
        tok_half=dma(3, 2),
        key_send=dma(3),
        key_recv=dma(3),
        far_send=dma(3),
        far_recv=dma(3, 2, side),
        far_half=dma(3, 2, side),
        far_key_send=dma(3),
        far_key_recv=dma(3, side - 1),
        gate_send=dma(3),
        gate_recv=dma(3),
        sum_send=dma(3),
        sum_recv=dma(3, 2),
        sum_half=dma(3, 2),
        go_send=dma(N_CHUNKS, 3),
        go_recv=dma(N_CHUNKS, 3),
        back_send=dma(N_CHUNKS, 3),
        back_recv=dma(N_CHUNKS, 3),
        home_send=dma(N_CHUNKS, 3),
        home_recv=dma(N_CHUNKS, 3),
    )
    for p, w in enumerate(widths):
        there = sds((N_CHUNKS, side, side, 2, side, slots, w), BF16)
        outs['far' + str(p)] = sds((side, side, tokens, w), BF16)
        outs['send' + str(p)] = sds((N_CHUNKS * mates, side, side, slots, w), BF16)
        outs['arrive' + str(p)] = there
        outs['output' + str(p)] = there
        outs['middle' + str(p)] = sds((N_CHUNKS, side, side, mates, slots, w), BF16)
        outs['result' + str(p)] = sds((N_CHUNKS, side, side, mates, slots, w), BF16)
        scratch['tok' + str(p)] = vmem((side, tokens, w), BF16)
        scratch['sum' + str(p)] = vmem((side, tokens, w), F32)
        scratch['other' + str(p)] = vmem((side - 1, tokens, w), F32)
    anywhere = pl.BlockSpec(memory_space=pl.ANY)
    local = pl.BlockSpec(memory_space=pltpu.VMEM)
    n_rows = members * side * capacity
    return pl.pallas_call(
        functools.partial(
            kernel,
            names=tuple(small) + tuple(large) + tuple(outs) + tuple(scratch),
            side=side,
            parts=parts,
            capacity=capacity,
            head_dim=head_dim,
            f_chunk=min(256, width),
            d_chunk=min(512, model),
        ),
        out_shape=list(outs.values()),
        in_specs=[local] * len(small) + [anywhere] * len(large),
        out_specs=[local] + [anywhere] * (len(outs) - 1),
        scratch_shapes=list(scratch.values()),
        compiler_params=pltpu.CompilerParams(has_side_effects=True, vmem_limit_bytes=67043328),
        cost_estimate=pl.CostEstimate(flops=6 * n_rows * model * width, bytes_accessed=8 * n_rows * model, transcendentals=0),
    )(*small.values(), *large.values())[0]


def solution(mesh):
    group_size = mesh.shape['ep']
    side = torus_side(group_size)
    torus = jax.sharding.Mesh(mesh.devices.reshape(side, side, side, 2), AXES)
    row_spec = P(AXES, None, None)
    vec_spec = P(None)
    mat_spec = P(None, None)
    cube_spec = P(None, None, None)
    expert_spec = P(AXES, None, None)

    def per_device(hidden, expert_ids, slot_ids, attn_norm, w_query, w_key, w_value, w_out, ffn_norm, ffn_gate, ffn_up, ffn_down, moe_norm, w_router, exp_gate, exp_up, exp_down):
        n_seqs, tokens, model = hidden.shape
        assert n_seqs == 1 and exp_gate.shape[0] == 1
        n_heads, head_dim = w_out.shape[0], w_out.shape[1]
        top_k = expert_ids.shape[2]
        capacity = CAP_FACTOR * tokens * top_k // group_size
        inv_freq = np.float32(ROPE_BASE) ** (np.float32(-2.0) * np.arange(head_dim // 2, dtype=np.float32) / head_dim)
        angles = np.arange(tokens, dtype=np.float32)[:, None] * inv_freq[None, :]
        cos, sin = np.cos(angles), np.sin(angles)
        small = dict(
            hidden=hidden[0],
            attn_scale=attn_norm.reshape(-1, 128),
            moe_scale=moe_norm.reshape(-1, 128),
            ffn_scale=ffn_norm.reshape(-1, 128),
            ids_t=expert_ids[0].T,
            slots_t=slot_ids[0].T,
            w_router=w_router,
            cos=np.concatenate([cos, cos], axis=1).astype(np.float32),
            sin=np.concatenate([-sin, sin], axis=1).astype(np.float32),
        )
        large = dict(
            w_query=w_query,
            w_key=w_key,
            w_value=w_value,
            w_out=w_out.reshape(n_heads * head_dim, model),
            ffn_gate=ffn_gate,
            ffn_up=ffn_up,
            ffn_down=ffn_down,
            gate_hbm=exp_gate[0],
            up_hbm=exp_up[0],
            down_hbm=exp_down[0],
        )
        return layer_pair(small, large, side, capacity, head_dim).reshape(hidden.shape)

    return jax.shard_map(per_device, mesh=torus, in_specs=(row_spec, row_spec, row_spec, vec_spec, mat_spec, mat_spec, mat_spec, cube_spec, vec_spec, mat_spec, mat_spec, mat_spec, vec_spec, mat_spec, expert_spec, expert_spec, expert_spec), out_specs=row_spec, check_vma=False)
```

```python
import functools
import math
import types

import jax
import jax.numpy as jnp
import numpy as np
from jax import lax
from jax.experimental import pallas as pl
from jax.experimental.pallas import tpu as pltpu
from jax.sharding import PartitionSpec as P

RMS_EPS = 1e-6
ROPE_BASE = 10000.0
CAP_FACTOR = 3
N_CHUNKS = 3
RING = 6
TILE = 256
MESH = pl.DeviceIdType.MESH

BF16, F32, I32 = jnp.bfloat16, jnp.float32, jnp.int32

AXES = ('z', 'y', 'x', 'c')
OUT = (('z', 'y', 'x'), ('x', 'z', 'y'), ('y', 'x', 'z'))
BACK = (('y', 'z', 'x'), ('z', 'x', 'y'), ('x', 'y', 'z'))
ROW_AXES = ('y', 'x', 'c', 'z')


def torus_side(n_devices):
    side = round((n_devices // 2) ** (1 / 3))
    assert side ** 3 * 2 == n_devices
    return side


def column_parts(model):
    lanes = model // 128
    first = -(-lanes // 3)
    second = -(-(lanes - first) // 2)
    ends = (0, first * 128, (first + second) * 128, model)
    return tuple((ends[p], ends[p + 1]) for p in range(3))


def steps(total, size):
    return [(lo, min(size, total - lo)) for lo in range(0, total, size)]


def rms_rows(rows, scale):
    as_float = rows.astype(F32)
    inv_rms = lax.rsqrt(jnp.mean(as_float * as_float, axis=-1, keepdims=True) + RMS_EPS)
    return (as_float * inv_rms * scale.astype(F32)).astype(BF16)


def dot(a, b):
    return jnp.dot(a, b, preferred_element_type=F32)


def kernel(*refs, names, side, parts, capacity, head_dim, f_chunk, d_chunk):
    r = types.SimpleNamespace(**dict(zip(names, refs)))
    each = lambda name: [getattr(r, name + str(p)) for p in range(3)]
    slots = capacity // N_CHUNKS
    members = side * side * 2
    mates = side * 2
    assert side in (2, 4)
    relay = side == 4
    strides = (1, side - 1) if relay else (1,)
    order = (0, side - 1, 1, 2) if relay else (0, 1)
    rows_block = members * slots
    tokens, model = r.hidden.shape
    me = {axis: lax.axis_index(axis) for axis in AXES}


    def rows_of(ref, p, chunk, place, free):
        spot = [pl.ds(0, side) if axis in free else place[axis] for axis in ROW_AXES]
        return ref.at[tuple([chunk] + spot)]

    def ordered(where):
        return tuple(where[axis] for axis in ROW_AXES if axis in where)

    def device(place):
        return tuple(place[axis] for axis in AXES)

    def axis_peer(axis, offset):
        return {**me, axis: lax.rem(me[axis] + offset, side)}

    def mate_peer(axis, offset):
        return {
            **me,
            axis: lax.rem(me[axis] + offset // 2, side),
            'c': lax.rem(me['c'] + lax.rem(offset, 2), 2),
        }

    def remote(src, dst, send_sem, recv_sem, place):
        return pltpu.make_async_remote_copy(
            src_ref=src, dst_ref=dst, send_sem=send_sem, recv_sem=recv_sem, device_id=device(place), device_id_type=MESH
        )

    def wait_bytes(ref, sem):
        pltpu.make_async_copy(ref, ref, sem).wait()

    def expert_key(place, core, slot):
        return (((place['z'] * side + place['y']) * side + place['x']) * 2 + core) * capacity + slot

    def plane_keys(p, shape):
        first, second, _ = BACK[p]
        which = lax.broadcasted_iota(I32, shape, 0)
        pair = which // 2
        place = {**me, second: pair // side, first: lax.rem(pair, side)}
        return expert_key(place, lax.rem(which, 2), 0)

    def mate_keys(p, shape):
        mate = lax.broadcasted_iota(I32, shape, 0)
        return expert_key({**me, OUT[p][2]: mate // 2}, lax.rem(mate, 2), 0)

    tok, far, sends, arrivals, outputs = each('tok'), each('far'), each('send'), each('arrive'), each('output')
    middles, results, sums, others = each('middle'), each('result'), each('sum'), each('other')
    widths = [hi - lo for lo, hi in parts]


    band = min(32, tokens)

    def bands(body):
        lax.fori_loop(0, tokens // band, lambda i, c: (body(pl.ds(pl.multiple_of(i * band, band), band)), c)[1], 0)

    def one_row(scale):
        lines = scale[...].astype(F32)
        return jnp.concatenate([lines[i : i + 1, :] for i in range(lines.shape[0])], axis=1)

    def norm_both(here):
        normed = rms_rows(r.hidden[here, :], one_row(r.moe_scale))
        for p, (lo, hi) in enumerate(parts):
            tok[p][me[OUT[p][0]], here, :] = normed[:, lo:hi]
        r.rows[here, :] = rms_rows(r.hidden[here, :], one_row(r.attn_scale))

    bands(norm_both)
    keys_t = r.ids_t[...] * capacity + r.slots_t[...]
    for p in range(3):
        r.all_keys[p, me[OUT[p][1]], me[OUT[p][0]]] = keys_t
    pairs = ((r.gate_hbm, r.gate), (r.up_hbm, r.up), (r.down_hbm, r.down))
    loads = [pltpu.make_async_copy(src, dst, r.weight_sem.at[i]) for i, (src, dst) in enumerate(pairs)]
    for load in loads:
        load.start()

    half = tokens // 2
    halves = (pl.ds(0, half), pl.ds(half, half))

    def neighbour(axis, k):
        return lax.rem(me[axis] + side - strides[k], side)

    def send_far(p, n):
        near, axis, _ = OUT[p]
        d = lax.rem(me[near] + order[n], side)
        for k, stride in enumerate(strides):
            remote(
                tok[p].at[d], far[p].at[me[axis], d], r.far_send.at[p], r.far_recv.at[p, k, n], axis_peer(axis, stride)
            ).start()

    def pass_far(n):
        for k, stride in enumerate(strides):
            for p in range(3):
                near, axis, _ = OUT[p]
                d = lax.rem(me[near] + order[n], side)
                wait_bytes(tok[p].at[0], r.far_recv.at[p, k, n])
                if relay:
                    block = far[p].at[neighbour(axis, k), d, halves[k]]
                    remote(block, block, r.far_send.at[p], r.far_half.at[p, k, n], axis_peer(axis, stride)).start()

    for k, stride in enumerate(strides):
        for p in range(3):
            axis = OUT[p][0]
            block = tok[p].at[me[axis]]
            remote(block, block, r.tok_send.at[p], r.tok_recv.at[p, k], axis_peer(axis, stride)).start()
    for p in range(3):
        send_far(p, 0)
    for offset in range(1, side):
        for p in range(3):
            axis = OUT[p][0]
            keys = r.all_keys.at[p, me[OUT[p][1]], me[axis]]
            remote(keys, keys, r.key_send.at[p], r.key_recv.at[p], axis_peer(axis, offset)).start()


    ring = r.ring
    ring_sem = r.ring_sem

    def stream(n_steps, group, source, body):
        ahead = RING // group * group - group

        def copy(i, s):
            slot = lax.rem(i * group + s, RING // group * group)
            return pltpu.make_async_copy(source(i, s), ring.at[slot], ring_sem.at[slot])

        for i in range(min(ahead // group, n_steps)):
            for s in range(group):
                copy(i, s).start()

        def step(i, carry):
            @pl.when(i + ahead // group < n_steps)
            def _():
                for s in range(group):
                    copy(i + ahead // group, s).start()

            for s in range(group):
                copy(i, s).wait()
            body(i, [ring.at[lax.rem(i * group + s, RING // group * group)] for s in range(group)])
            return carry

        lax.fori_loop(0, n_steps, step, 0)

    def col_tile(i):
        return pl.ds(pl.multiple_of(i * TILE, TILE), TILE)

    def turned(y):
        return y * r.cos[...] + pltpu.roll(y, head_dim // 2, 1) * r.sin[...]

    def project(weight, out, rotary):
        def body(i, tiles):
            y = dot(r.rows[...], tiles[0][...])
            if rotary:
                y = jnp.concatenate([turned(y[:, lo : lo + head_dim]) for lo in range(0, TILE, head_dim)], axis=1)
            out[:, col_tile(i)] = y.astype(BF16)

        stream(weight.shape[1] // TILE, 1, lambda i, s: weight.at[:, col_tile(i)], body)

    project(r.w_query, r.query, True)
    project(r.w_key, r.key, True)
    project(r.w_value, r.value, False)


    logits = sum(dot(tok[p][me[OUT[p][0]]], r.w_router[lo:hi, :]) for p, (lo, hi) in enumerate(parts))
    top_k = r.ids_t.shape[0]
    gap = jnp.zeros((128 - 3 * top_k, tokens), F32)
    blank = jnp.zeros((top_k, tokens), F32)
    info = jnp.concatenate([keys_t.astype(F32), blank, r.ids_t[...].astype(F32), gap], axis=0).T
    lane = lax.broadcasted_iota(I32, logits.shape, 1).astype(F32)
    picked = [
        jnp.sum(jnp.where(lane == info[:, 2 * top_k + j : 2 * top_k + j + 1], logits, 0.0), axis=1, keepdims=True)
        for j in range(top_k)
    ]
    peak = functools.reduce(jnp.maximum, picked)
    powers = [jnp.exp(v - peak) for v in picked]
    norm = functools.reduce(jnp.add, powers)
    lane = lax.broadcasted_iota(I32, info.shape, 1)
    for j in range(top_k):
        info = jnp.where(lane == top_k + j, powers[j] / norm, info)
    r.my_gates[...] = info.T[0 : 2 * top_k, :]
    for p in range(3):
        r.line_gates[p, me[BACK[p][2]]] = r.my_gates[...]


    for k, stride in enumerate(strides):
        for p in range(3):
            axis = OUT[p][0]
            wait_bytes(tok[p].at[0], r.tok_recv.at[p, k])
            if relay:
                block = tok[p].at[neighbour(axis, k), halves[k]]
                remote(block, block, r.tok_send.at[p], r.tok_half.at[p, k], axis_peer(axis, stride)).start()
            send_far(p, 1 + k)
    pass_far(0)
    if relay:
        for p in range(3):
            for k in range(2):
                wait_bytes(tok[p].at[0, halves[k]], r.tok_half.at[p, k])
            send_far(p, 3)
    for p in range(3):
        wait_bytes(r.all_keys.at[p, 0, pl.ds(0, side - 1)], r.key_recv.at[p])
        for offset in range(1, side):
            keys = r.all_keys.at[p, me[OUT[p][1]]]
            remote(
                keys, keys, r.far_key_send.at[p], r.far_key_recv.at[p, offset - 1], axis_peer(OUT[p][1], offset)
            ).start()
    for offset in range(1, side):
        for p in range(3):
            axis = BACK[p][2]
            remote(
                r.my_gates, r.line_gates.at[p, me[axis]], r.gate_send.at[p], r.gate_recv.at[p], axis_peer(axis, offset)
            ).start()


    n_heads = r.query.shape[1] // head_dim
    per_key = r.query.shape[1] // r.key.shape[1]
    causal = lax.broadcasted_iota(I32, (tokens, tokens), 0) >= lax.broadcasted_iota(I32, (tokens, tokens), 1)

    def one_head(h, carry):
        cols = pl.ds(pl.multiple_of(h * head_dim, head_dim), head_dim)
        key_cols = pl.ds(pl.multiple_of(h // per_key * head_dim, head_dim), head_dim)
        scores = lax.dot_general(
            r.query[:, cols], r.key[:, key_cols], (((1,), (1,)), ((), ())), preferred_element_type=F32
        )
        scores = jnp.where(causal, scores * head_dim ** -0.5, -jnp.inf)
        power = jnp.exp(scores - jnp.max(scores, axis=1, keepdims=True))
        prob = (power / jnp.sum(power, axis=1, keepdims=True)).astype(BF16)
        r.query[:, cols] = dot(prob, r.value[:, key_cols]).astype(BF16)
        return carry


    stage = r.stage
    blocks = N_CHUNKS * mates
    out_mate = [me[OUT[p][2]] * 2 + me['c'] for p in range(3)]
    back_mate = [me[BACK[p][0]] * 2 + me['c'] for p in range(3)]

    def pick_rows(p, i, d, slot, source):
        keys = r.all_keys[p, i, d]
        first = mate_keys(p, (mates, tokens))
        held = jnp.full((mates, tokens), -1, I32)
        for j in range(top_k):
            slot_there = keys[j : j + 1, :] - first
            mine = jnp.logical_and(slot_there >= 0, slot_there < capacity)
            held = jnp.where(mine, slot_there, held)
        row_slot = lax.broadcasted_iota(I32, (capacity, tokens), 0)
        for mate in range(mates):
            pick = jnp.where(row_slot == held[mate : mate + 1, :], 1.0, 0.0).astype(BF16)
            for chunk in range(N_CHUNKS):
                at = (chunk * mates + mate) * slots
                r.split[at : at + slots, 0:tokens] = pick[chunk * slots : (chunk + 1) * slots, :]
        for lo, n in steps(widths[p], TILE):
            found = dot(r.split[0 : blocks * slots, 0:tokens], source[:, lo : lo + n]).astype(BF16)
            stage[slot, 0:blocks, :, lo : lo + n] = found.reshape(blocks, slots, n)

    def flush(p, i, d, slot):
        a, b = ordered({OUT[p][1]: i, OUT[p][0]: d})
        return pltpu.make_async_copy(
            stage.at[slot, pl.ds(0, blocks), :, pl.ds(0, widths[p])],
            sends[p].at[pl.ds(0, blocks), a, b],
            r.stage_sem.at[slot],
        )

    def keep(p, i, d, slot, chunk):
        spot = {**me, OUT[p][1]: i, OUT[p][0]: d}
        return pltpu.make_async_copy(
            stage.at[slot, chunk * mates + out_mate[p], :, pl.ds(0, widths[p])],
            arrivals[p].at[(chunk,) + ordered(spot)],
            r.keep_sem.at[slot, chunk],
        )

    def send_rows(p, chunk, i):
        near, far_axis, axis = OUT[p]
        free = (near,) if i is not None else (near, far_axis)
        a, b = ordered({far_axis: pl.ds(0, side) if i is None else i, near: pl.ds(0, side)})
        group_place = me if i is None else {**me, far_axis: i}

        def one_mate(offset, c):
            place = mate_peer(axis, offset)
            remote(
                sends[p].at[chunk * mates + place[axis] * 2 + place['c'], a, b],
                rows_of(arrivals[p], p, chunk, group_place, free),
                r.go_send.at[chunk, p],
                r.go_recv.at[chunk, p],
                place,
            ).start()
            return c

        lax.fori_loop(1, mates, one_mate, 0)

    def pick_group(offset):
        for p in range(3):
            i = lax.rem(me[OUT[p][1]] + side - offset, side)
            if offset:
                wait_bytes(r.all_keys.at[p, 0], r.far_key_recv.at[p, offset - 1])
            if relay and offset == 2:
                for n in range(side):
                    for k in range(2):
                        wait_bytes(tok[p].at[0, halves[k]], r.far_half.at[p, k, n])

            def load(d, slot):
                return pltpu.make_async_copy(
                    far[p].at[i, d], r.source.at[slot, :, pl.ds(0, widths[p])], r.source_sem.at[slot]
                )

            if offset:
                load(0, 0).start()

            def one_source(d, c):
                slot = lax.rem(d, 2)
                if offset:

                    @pl.when(d + 1 < side)
                    def _():
                        load(d + 1, 1 - slot).start()

                    load(d, slot).wait()

                @pl.when(d >= 2)
                def _():
                    flush(p, i, d - 2, slot).wait()
                    for chunk in range(N_CHUNKS):
                        keep(p, i, d - 2, slot, chunk).wait()

                pick_rows(p, i, d, slot, r.source.at[slot] if offset else tok[p].at[d])
                flush(p, i, d, slot).start()
                for chunk in range(N_CHUNKS):
                    keep(p, i, d, slot, chunk).start()
                return c

            lax.fori_loop(0, side, one_source, 0)
            for d in range(side - 2, side):
                flush(p, i, d, d % 2).wait()
                for chunk in range(N_CHUNKS):
                    keep(p, i, d, d % 2, chunk).wait()
            if offset:
                send_rows(p, 0, i)

    def heads(part, n_parts):
        lax.fori_loop(n_heads * part // n_parts, n_heads * (part + 1) // n_parts, one_head, 0)

    pick_group(0)
    for n in range(1, side):
        pass_far(n)
        heads(n - 1, side - 1)
    for p in range(3):
        send_rows(p, 0, me[OUT[p][1]])
    for offset in (1, 3, 2) if relay else (1,):
        pick_group(offset)
    for chunk in range(1, N_CHUNKS):
        for p in range(3):
            send_rows(p, chunk, None)


    out_split = n_heads * head_dim // model

    def out_body(i, tiles):
        total = r.hidden[:, col_tile(i)].astype(F32)
        attended = dot(r.query[:, 0:model], tiles[0][...])
        for s in range(1, out_split):
            attended += dot(r.query[:, s * model : (s + 1) * model], tiles[s][...])
        r.attended[:, col_tile(i)] = (total + attended).astype(BF16)

    stream(model // TILE, out_split, lambda i, s: r.w_out.at[pl.ds(s * model, model), col_tile(i)], out_body)

    def norm_attended(here):
        r.rows[here, :] = rms_rows(r.attended[here, :], one_row(r.ffn_scale))

    bands(norm_attended)

    def act_body(i, tiles):
        z = dot(r.rows[...], tiles[0][...])
        u = dot(r.rows[...], tiles[1][...])
        r.act[:, col_tile(i)] = (jax.nn.silu(z) * u).astype(BF16)

    ff_dim = r.ffn_gate.shape[1]
    stream(
        ff_dim // TILE, 2, lambda i, s: (r.ffn_gate, r.ffn_up)[s].at[:, col_tile(i)], act_body
    )
    down_split = ff_dim // model

    def down_body(i, tiles):
        total = dot(r.act[:, 0:model], tiles[0][...])
        for s in range(1, down_split):
            total += dot(r.act[:, s * model : (s + 1) * model], tiles[s][...])
        r.dense[:, col_tile(i)] = r.attended[:, col_tile(i)].astype(F32) + total

    stream(model // TILE, down_split, lambda i, s: r.ffn_down.at[pl.ds(s * model, model), col_tile(i)], down_body)


    for load in loads:
        load.wait()
    x_buf, y_buf, hidden_buf = r.x_buf, r.y_buf, r.hidden_buf
    group = x_buf.shape[1:-1]
    rows = math.prod(group)
    width = hidden_buf.shape[1]

    def fetch(chunk, y, slot):
        return [
            pltpu.make_async_copy(
                arrivals[p].at[chunk, y], x_buf.at[slot, :, :, :, :, pl.ds(lo, hi - lo)], r.in_sem.at[slot, p]
            )
            for p, (lo, hi) in enumerate(parts)
        ]

    def put(chunk, y, slot):
        return [
            pltpu.make_async_copy(
                y_buf.at[slot, :, :, :, :, pl.ds(lo, hi - lo)], outputs[p].at[chunk, y], r.out_sem.at[slot, p]
            )
            for p, (lo, hi) in enumerate(parts)
        ]

    def keep_own(chunk, y, slot, p):
        lo, hi = parts[p]
        free = BACK[p][1:]
        spot = [pl.ds(0, side) if axis in free else me[axis] for axis in ROW_AXES[1:]]
        mine = pltpu.make_async_copy(
            y_buf.at[tuple([slot] + spot + [pl.ds(0, slots), pl.ds(lo, hi - lo)])],
            middles[p].at[
                (chunk,) + ordered({axis: y if axis == 'y' else pl.ds(0, side) for axis in free}) + (back_mate[p],)
            ],
            r.own_sem.at[slot, p],
        )
        return mine, (None if 'y' in free else y == me['y'])

    def start_put(chunk, y, slot):
        for copy in put(chunk, y, slot):
            copy.start()
        for p in range(3):
            copy, when = keep_own(chunk, y, slot, p)
            if when is None:
                copy.start()
            else:
                pl.when(when)(copy.start)

    def wait_put(chunk, y, slot):
        for copy in put(chunk, y, slot):
            copy.wait()
        for p in range(3):
            copy, when = keep_own(chunk, y, slot, p)
            if when is None:
                copy.wait()
            else:
                pl.when(when)(copy.wait)

    def expert_chunk(chunk):
        for p in range(3):
            wait_bytes(sends[p].at[pl.ds(0, mates - 1)], r.go_recv.at[chunk, p])
        for copy in fetch(chunk, 0, 0):
            copy.start()

        def one_tile(y, c):
            slot = lax.rem(y, 2)

            @pl.when(y + 1 < side)
            def _():
                for copy in fetch(chunk, y + 1, 1 - slot):
                    copy.start()

            for copy in fetch(chunk, y, slot):
                copy.wait()

            @pl.when(y >= 2)
            def _():
                wait_put(chunk, y - 2, slot)

            for lo in range(0, width, f_chunk):
                cols = slice(lo, lo + f_chunk)
                z = dot(x_buf[slot].reshape(rows, model), r.gate[:, cols])
                u = dot(x_buf[slot].reshape(rows, model), r.up[:, cols])
                hidden_buf[:, cols] = (jax.nn.silu(z) * u).astype(BF16)
            for lo in range(0, model, d_chunk):
                cols = slice(lo, lo + d_chunk)
                y_rows = dot(hidden_buf[...], r.down[:, cols]).astype(BF16)
                y_buf[slot, :, :, :, :, cols] = y_rows.reshape(group + (d_chunk,))
            start_put(chunk, y, slot)
            return c

        lax.fori_loop(0, side, one_tile, 0)
        for y in range(side - 2, side):
            wait_put(chunk, y, y % 2)

        def one_mate(offset, c):
            for p in range(3):
                place = mate_peer(BACK[p][0], offset)
                remote(
                    rows_of(outputs[p], p, chunk, place, BACK[p][1:]),
                    middles[p].at[chunk, pl.ds(0, side), pl.ds(0, side), back_mate[p]],
                    r.back_send.at[chunk, p],
                    r.back_recv.at[chunk, p],
                    place,
                ).start()
            return c

        lax.fori_loop(1, mates, one_mate, 0)

    def middle_rows(p, chunk, i, d):
        return middles[p].at[(chunk,) + ordered({BACK[p][1]: i, BACK[p][2]: d})]

    def pass_on(chunk):
        for p in range(3):
            wait_bytes(middles[p].at[chunk, pl.ds(0, side), pl.ds(0, side), pl.ds(0, mates - 1)], r.back_recv.at[chunk, p])
            for offset in range(1, side):
                axis = BACK[p][1]
                place = axis_peer(axis, offset)
                remote(
                    middle_rows(p, chunk, place[axis], pl.ds(0, side)),
                    results[p].at[chunk, pl.ds(0, side), me[axis]],
                    r.home_send.at[chunk, p],
                    r.home_recv.at[chunk, p],
                    place,
                ).start()


    split = r.split
    lanes = min(128, rows_block)

    def weigh_chunk(chunk, carry):
        for p in range(3):
            wait_bytes(results[p].at[chunk, pl.ds(0, side), pl.ds(0, side - 1)], r.home_recv.at[chunk, p])

        def source_of(p, n):
            ahead = 2 * side - 2 - 2 * n + 3 * (n // 2) if relay else 1 - n
            return lax.rem(me[BACK[p][2]] + ahead, side)

        def load(p, n, slot):
            copies = []
            for offset in range(side):
                i, d = lax.rem(me[BACK[p][1]] + offset, side), source_of(p, n)
                copies.append(
                    pltpu.make_async_copy(
                        results[p].at[chunk, d, i] if offset else middle_rows(p, chunk, i, d),
                        stage.at[slot, pl.ds(i * mates, mates), :, pl.ds(0, widths[p])],
                        r.load_sem.at[slot, offset],
                    )
                )
            return copies

        for copy in load(0, 0, 0):
            copy.start()

        def one_source(n, c):
            for p in range(3):
                d = source_of(p, n)
                slot = lax.rem(n + p, 2)

                @pl.when(n + p // 2 < side)
                def _():
                    for copy in load((p + 1) % 3, n + p // 2, 1 - slot):
                        copy.start()

                lane = lax.broadcasted_iota(I32, (1, lanes), 1)
                wanted = (lax.rem(lane, slots) + chunk * slots).astype(F32)
                for lo in range(0, rows_block, lanes):
                    which = jnp.broadcast_to(lane // slots + lo // slots, (tokens, lanes))
                    take = functools.partial(jnp.take_along_axis, indices=which, axis=1, mode='promise_in_bounds')
                    weight = jnp.where(take(r.held[p, d]) == wanted, take(r.gates[p, d]), 0.0)
                    high = weight.astype(BF16)
                    rest = weight - high.astype(F32)
                    middle = rest.astype(BF16)
                    low = (rest - middle.astype(F32)).astype(BF16)
                    split[0:tokens, lo : lo + lanes] = high
                    split[tokens : 2 * tokens, lo : lo + lanes] = middle
                    split[2 * tokens : 3 * tokens, lo : lo + lanes] = low
                for copy in load(p, n, slot):
                    copy.wait()
                for lo, size in steps(widths[p], TILE):
                    y = stage[slot, 0:members, :, lo : lo + size].reshape(rows_block, size)
                    both = dot(split[...], y)
                    total = both[0:tokens] + (both[tokens : 2 * tokens] + both[2 * tokens : 3 * tokens])

                    @pl.when(chunk == 0)
                    def _():
                        sums[p][d, :, lo : lo + size] = total

                    @pl.when(chunk > 0)
                    def _():
                        sums[p][d, :, lo : lo + size] += total

                last = chunk == N_CHUNKS - 1
                axis = BACK[p][2]

                @pl.when(jnp.logical_and(last, n == 0))
                def _():
                    for k, stride in enumerate(strides):
                        part, spot, arrived = sums[p].at[d], others[p].at[0], r.sum_recv.at[p, 0]
                        if relay:
                            part = sums[p].at[d, halves[k]]
                            spot, arrived = others[p].at[2, halves[k]], r.sum_half.at[p, k]
                        remote(part, spot, r.sum_send.at[p], arrived, axis_peer(axis, stride)).start()

                for k in range(2 if relay else 0):

                    @pl.when(jnp.logical_and(last, n == 2 + k))
                    def _():
                        wait_bytes(others[p].at[2, halves[k]], r.sum_half.at[p, k])
                        sums[p][d, halves[k], :] += others[p][2, halves[k], :]
                        remote(
                            sums[p].at[d], others[p].at[k], r.sum_send.at[p], r.sum_recv.at[p, k], axis_peer(axis, strides[k])
                        ).start()

            return c

        return lax.fori_loop(0, side, one_source, carry)


    def one_by_one(step):
        lax.fori_loop(0, N_CHUNKS, lambda chunk, c: (step(chunk), c)[1], 0)

    one_by_one(expert_chunk)
    one_by_one(pass_on)
    gap = jnp.zeros((128 - members, tokens), F32)
    for p in range(3):
        wait_bytes(r.line_gates.at[p, pl.ds(0, side - 1)], r.gate_recv.at[p])
        first = plane_keys(p, (members, tokens)).astype(F32)

        def spread(d, c):
            info = r.line_gates[p, d]
            held, gate = jnp.full((members, tokens), -1.0, F32), jnp.zeros((members, tokens), F32)
            for j in range(top_k):
                there = info[j : j + 1, :] - first
                mine = jnp.logical_and(there >= 0, there < capacity)
                held = jnp.where(mine, there, held)
                gate = jnp.where(mine, info[top_k + j : top_k + j + 1, :], gate)
            r.held[p, d] = jnp.concatenate([held, gap], axis=0).T
            r.gates[p, d] = jnp.concatenate([gate, gap], axis=0).T
            return c

        lax.fori_loop(0, side, spread, 0)
    lax.fori_loop(0, N_CHUNKS, weigh_chunk, 0)
    for p, (lo, hi) in enumerate(parts):
        for k in range(len(strides)):
            wait_bytes(others[p].at[k], r.sum_recv.at[p, k])

        def finish(here):
            moe = sums[p][me[BACK[p][2]], here, :]
            for k in range(len(strides)):
                moe += others[p][k, here, :]
            r.out[here, lo:hi] = (r.dense[here, lo:hi] + moe).astype(BF16)

        bands(finish)


    for p in range(3):
        wait_bytes(tok[p].at[pl.ds(0, side - 1)], r.tok_send.at[p])
        wait_bytes(r.all_keys.at[p, 0, pl.ds(0, side - 1)], r.key_send.at[p])
        wait_bytes(far[p].at[pl.ds(0, side - 1)], r.far_send.at[p])
        wait_bytes(r.all_keys.at[p, pl.ds(0, side - 1)], r.far_key_send.at[p])
        wait_bytes(r.line_gates.at[p, pl.ds(0, side - 1)], r.gate_send.at[p])
        wait_bytes(others[p], r.sum_send.at[p])
        for chunk in range(N_CHUNKS):
            wait_bytes(sends[p].at[pl.ds(0, mates - 1)], r.go_send.at[chunk, p])
            wait_bytes(middles[p].at[chunk, pl.ds(0, side), pl.ds(0, side), pl.ds(0, mates - 1)], r.back_send.at[chunk, p])
            wait_bytes(results[p].at[chunk, pl.ds(0, side), pl.ds(0, side - 1)], r.home_send.at[chunk, p])


def layer_pair(small, large, side, capacity, head_dim):
    tokens, model = small['hidden'].shape
    top_k, width = small['ids_t'].shape[0], large['gate_hbm'].shape[1]
    key_dim, ff_dim = large['w_key'].shape[1], large['ffn_gate'].shape[1]
    parts = column_parts(model)
    widths = [hi - lo for lo, hi in parts]
    slots, members, mates = capacity // N_CHUNKS, side * side * 2, side * 2
    group = (side, 2, side, slots)
    rows = math.prod(group)
    sds, vmem = jax.ShapeDtypeStruct, pltpu.VMEM
    dma = lambda *shape: pltpu.SemaphoreType.DMA(shape)
    outs = dict(out=sds((tokens, model), BF16))
    scratch = dict(
        rows=vmem((tokens, model), BF16),
        query=vmem((tokens, large['w_query'].shape[1]), BF16),
        key=vmem((tokens, key_dim), BF16),
        value=vmem((tokens, key_dim), BF16),
        attended=vmem((tokens, model), BF16),
        act=vmem((tokens, ff_dim), BF16),
        dense=vmem((tokens, model), F32),
        ring=vmem((RING, model, TILE), BF16),
        all_keys=vmem((3, side, side, top_k, tokens), I32),
        my_gates=vmem((2 * top_k, tokens), F32),
        line_gates=vmem((3, side, 2 * top_k, tokens), F32),
        held=vmem((3, side, tokens, 128), F32),
        gates=vmem((3, side, tokens, 128), F32),
        source=vmem((2, tokens, max(widths)), BF16),
        stage=vmem((2, max(members, N_CHUNKS * mates), slots, max(widths)), BF16),
        split=vmem((3 * tokens, members * slots), BF16),
        gate=vmem((model, width), BF16),
        up=vmem((model, width), BF16),
        down=vmem((width, model), BF16),
        x_buf=vmem((2,) + group + (model,), BF16),
        y_buf=vmem((2,) + group + (model,), BF16),
        hidden_buf=vmem((rows, width), BF16),
        weight_sem=dma(3),
        ring_sem=dma(RING),
        source_sem=dma(2),
        stage_sem=dma(2),
        keep_sem=dma(2, N_CHUNKS),
        in_sem=dma(2, 3),
        out_sem=dma(2, 3),
        own_sem=dma(2, 3),
        load_sem=dma(2, side),
        tok_send=dma(3),
        tok_recv=dma(3, 2),
        tok_half=dma(3, 2),
        key_send=dma(3),
        key_recv=dma(3),
        far_send=dma(3),
        far_recv=dma(3, 2, side),
        far_half=dma(3, 2, side),
        far_key_send=dma(3),
        far_key_recv=dma(3, side - 1),
        gate_send=dma(3),
        gate_recv=dma(3),
        sum_send=dma(3),
        sum_recv=dma(3, 2),
        sum_half=dma(3, 2),
        go_send=dma(N_CHUNKS, 3),
        go_recv=dma(N_CHUNKS, 3),
        back_send=dma(N_CHUNKS, 3),
        back_recv=dma(N_CHUNKS, 3),
        home_send=dma(N_CHUNKS, 3),
        home_recv=dma(N_CHUNKS, 3),
    )
    for p, w in enumerate(widths):
        there = sds((N_CHUNKS, side, side, 2, side, slots, w), BF16)
        outs['far' + str(p)] = sds((side, side, tokens, w), BF16)
        outs['send' + str(p)] = sds((N_CHUNKS * mates, side, side, slots, w), BF16)
        outs['arrive' + str(p)] = there
        outs['output' + str(p)] = there
        outs['middle' + str(p)] = sds((N_CHUNKS, side, side, mates, slots, w), BF16)
        outs['result' + str(p)] = sds((N_CHUNKS, side, side, mates, slots, w), BF16)
        scratch['tok' + str(p)] = vmem((side, tokens, w), BF16)
        scratch['sum' + str(p)] = vmem((side, tokens, w), F32)
        scratch['other' + str(p)] = vmem((side - 1, tokens, w), F32)
    anywhere = pl.BlockSpec(memory_space=pl.ANY)
    local = pl.BlockSpec(memory_space=pltpu.VMEM)
    n_rows = members * side * capacity
    return pl.pallas_call(
        functools.partial(
            kernel,
            names=tuple(small) + tuple(large) + tuple(outs) + tuple(scratch),
            side=side,
            parts=parts,
            capacity=capacity,
            head_dim=head_dim,
            f_chunk=min(256, width),
            d_chunk=min(512, model),
        ),
        out_shape=list(outs.values()),
        in_specs=[local] * len(small) + [anywhere] * len(large),
        out_specs=[local] + [anywhere] * (len(outs) - 1),
        scratch_shapes=list(scratch.values()),
        compiler_params=pltpu.CompilerParams(has_side_effects=True, vmem_limit_bytes=67043328),
        cost_estimate=pl.CostEstimate(flops=6 * n_rows * model * width, bytes_accessed=8 * n_rows * model, transcendentals=0),
    )(*small.values(), *large.values())[0]


def solution(mesh):
    group_size = mesh.shape['ep']
    side = torus_side(group_size)
    torus = jax.sharding.Mesh(mesh.devices.reshape(side, side, side, 2), AXES)
    row_spec = P(AXES, None, None)
    vec_spec = P(None)
    mat_spec = P(None, None)
    cube_spec = P(None, None, None)
    expert_spec = P(AXES, None, None)

    def per_device(hidden, expert_ids, slot_ids, attn_norm, w_query, w_key, w_value, w_out, ffn_norm, ffn_gate, ffn_up, ffn_down, moe_norm, w_router, exp_gate, exp_up, exp_down):
        n_seqs, tokens, model = hidden.shape
        assert n_seqs == 1 and exp_gate.shape[0] == 1
        n_heads, head_dim = w_out.shape[0], w_out.shape[1]
        top_k = expert_ids.shape[2]
        capacity = CAP_FACTOR * tokens * top_k // group_size
        inv_freq = np.float32(ROPE_BASE) ** (np.float32(-2.0) * np.arange(head_dim // 2, dtype=np.float32) / head_dim)
        angles = np.arange(tokens, dtype=np.float32)[:, None] * inv_freq[None, :]
        cos, sin = np.cos(angles), np.sin(angles)
        small = dict(
            hidden=hidden[0],
            attn_scale=attn_norm.reshape(-1, 128),
            moe_scale=moe_norm.reshape(-1, 128),
            ffn_scale=ffn_norm.reshape(-1, 128),
            ids_t=expert_ids[0].T,
            slots_t=slot_ids[0].T,
            w_router=w_router,
            cos=np.concatenate([cos, cos], axis=1).astype(np.float32),
            sin=np.concatenate([-sin, sin], axis=1).astype(np.float32),
        )
        large = dict(
            w_query=w_query,
            w_key=w_key,
            w_value=w_value,
            w_out=w_out.reshape(n_heads * head_dim, model),
            ffn_gate=ffn_gate,
            ffn_up=ffn_up,
            ffn_down=ffn_down,
            gate_hbm=exp_gate[0],
            up_hbm=exp_up[0],
            down_hbm=exp_down[0],
        )
        return layer_pair(small, large, side, capacity, head_dim).reshape(hidden.shape)

    return jax.shard_map(per_device, mesh=torus, in_specs=(row_spec, row_spec, row_spec, vec_spec, mat_spec, mat_spec, mat_spec, cube_spec, vec_spec, mat_spec, mat_spec, mat_spec, vec_spec, mat_spec, expert_spec, expert_spec, expert_spec), out_specs=row_spec, check_vma=False)
```

```python
import functools
import math
import types

import jax
import jax.numpy as jnp
import numpy as np
from jax import lax
from jax.experimental import pallas as pl
from jax.experimental.pallas import tpu as pltpu
from jax.sharding import PartitionSpec as P

RMS_EPS = 1e-6
ROPE_BASE = 10000.0
CAP_FACTOR = 3
N_CHUNKS = 3
RING = 6
TILE = 256
MESH = pl.DeviceIdType.MESH

BF16, F32, I32 = jnp.bfloat16, jnp.float32, jnp.int32

AXES = ('z', 'y', 'x', 'c')
OUT = (('z', 'y', 'x'), ('x', 'z', 'y'), ('y', 'x', 'z'))
BACK = (('y', 'z', 'x'), ('z', 'x', 'y'), ('x', 'y', 'z'))
ROW_AXES = ('y', 'x', 'c', 'z')


def torus_side(n_devices):
    side = round((n_devices // 2) ** (1 / 3))
    assert side ** 3 * 2 == n_devices
    return side


def column_parts(model):
    lanes = model // 128
    first = -(-lanes // 3)
    second = -(-(lanes - first) // 2)
    ends = (0, first * 128, (first + second) * 128, model)
    return tuple((ends[p], ends[p + 1]) for p in range(3))


def steps(total, size):
    return [(lo, min(size, total - lo)) for lo in range(0, total, size)]


def rms_rows(rows, scale):
    as_float = rows.astype(F32)
    inv_rms = lax.rsqrt(jnp.mean(as_float * as_float, axis=-1, keepdims=True) + RMS_EPS)
    return (as_float * inv_rms * scale.astype(F32)).astype(BF16)


def dot(a, b):
    return jnp.dot(a, b, preferred_element_type=F32)


def kernel(*refs, names, side, parts, capacity, head_dim, f_chunk, d_chunk):
    r = types.SimpleNamespace(**dict(zip(names, refs)))
    each = lambda name: [getattr(r, name + str(p)) for p in range(3)]
    slots = capacity // N_CHUNKS
    members = side * side * 2
    mates = side * 2
    assert side in (2, 4)
    relay = side == 4
    strides = (1, side - 1) if relay else (1,)
    order = (0, side - 1, 1, 2) if relay else (0, 1)
    rows_block = members * slots
    tokens, model = r.hidden.shape
    me = {axis: lax.axis_index(axis) for axis in AXES}


    def rows_of(ref, p, chunk, place, free):
        spot = [pl.ds(0, side) if axis in free else place[axis] for axis in ROW_AXES]
        return ref.at[tuple([chunk] + spot)]

    def ordered(where):
        return tuple(where[axis] for axis in ROW_AXES if axis in where)

    def device(place):
        return tuple(place[axis] for axis in AXES)

    def axis_peer(axis, offset):
        return {**me, axis: lax.rem(me[axis] + offset, side)}

    def mate_peer(axis, offset):
        return {
            **me,
            axis: lax.rem(me[axis] + offset // 2, side),
            'c': lax.rem(me['c'] + lax.rem(offset, 2), 2),
        }

    def remote(src, dst, send_sem, recv_sem, place):
        return pltpu.make_async_remote_copy(
            src_ref=src, dst_ref=dst, send_sem=send_sem, recv_sem=recv_sem, device_id=device(place), device_id_type=MESH
        )

    def wait_bytes(ref, sem):
        pltpu.make_async_copy(ref, ref, sem).wait()

    def expert_key(place, core, slot):
        return (((place['z'] * side + place['y']) * side + place['x']) * 2 + core) * capacity + slot

    def plane_keys(p, shape):
        first, second, _ = BACK[p]
        which = lax.broadcasted_iota(I32, shape, 0)
        pair = which // 2
        place = {**me, second: pair // side, first: lax.rem(pair, side)}
        return expert_key(place, lax.rem(which, 2), 0)

    def mate_keys(p, shape):
        mate = lax.broadcasted_iota(I32, shape, 0)
        return expert_key({**me, OUT[p][2]: mate // 2}, lax.rem(mate, 2), 0)

    tok, far, sends, arrivals, outputs = each('tok'), each('far'), each('send'), each('arrive'), each('output')
    middles, results, sums, others = each('middle'), each('result'), each('sum'), each('other')
    widths = [hi - lo for lo, hi in parts]


    band = min(32, tokens)

    def bands(body):
        lax.fori_loop(0, tokens // band, lambda i, c: (body(pl.ds(pl.multiple_of(i * band, band), band)), c)[1], 0)

    def one_row(scale):
        lines = scale[...].astype(F32)
        return jnp.concatenate([lines[i : i + 1, :] for i in range(lines.shape[0])], axis=1)

    def norm_both(here):
        normed = rms_rows(r.hidden[here, :], one_row(r.moe_scale))
        for p, (lo, hi) in enumerate(parts):
            tok[p][me[OUT[p][0]], here, :] = normed[:, lo:hi]
        r.rows[here, :] = rms_rows(r.hidden[here, :], one_row(r.attn_scale))

    bands(norm_both)
    keys_t = r.ids_t[...] * capacity + r.slots_t[...]
    for p in range(3):
        r.all_keys[p, me[OUT[p][1]], me[OUT[p][0]]] = keys_t
    pairs = ((r.gate_hbm, r.gate), (r.up_hbm, r.up), (r.down_hbm, r.down))
    loads = [pltpu.make_async_copy(src, dst, r.weight_sem.at[i]) for i, (src, dst) in enumerate(pairs)]
    for load in loads:
        load.start()

    half = tokens // 2
    halves = (pl.ds(0, half), pl.ds(half, half))

    def neighbour(axis, k):
        return lax.rem(me[axis] + side - strides[k], side)

    def send_far(p, n):
        near, axis, _ = OUT[p]
        d = lax.rem(me[near] + order[n], side)
        for k, stride in enumerate(strides):
            remote(
                tok[p].at[d], far[p].at[me[axis], d], r.far_send.at[p], r.far_recv.at[p, k, n], axis_peer(axis, stride)
            ).start()

    def pass_far(n):
        for k, stride in enumerate(strides):
            for p in range(3):
                near, axis, _ = OUT[p]
                d = lax.rem(me[near] + order[n], side)
                wait_bytes(tok[p].at[0], r.far_recv.at[p, k, n])
                if relay:
                    block = far[p].at[neighbour(axis, k), d, halves[k]]
                    remote(block, block, r.far_send.at[p], r.far_half.at[p, k, n], axis_peer(axis, stride)).start()

    for k, stride in enumerate(strides):
        for p in range(3):
            axis = OUT[p][0]
            block = tok[p].at[me[axis]]
            remote(block, block, r.tok_send.at[p], r.tok_recv.at[p, k], axis_peer(axis, stride)).start()
    for p in range(3):
        send_far(p, 0)
    for offset in range(1, side):
        for p in range(3):
            axis = OUT[p][0]
            keys = r.all_keys.at[p, me[OUT[p][1]], me[axis]]
            remote(keys, keys, r.key_send.at[p], r.key_recv.at[p], axis_peer(axis, offset)).start()


    ring = r.ring
    ring_sem = r.ring_sem

    def stream(n_steps, group, source, body):
        ahead = RING // group * group - group

        def copy(i, s):
            slot = lax.rem(i * group + s, RING // group * group)
            return pltpu.make_async_copy(source(i, s), ring.at[slot], ring_sem.at[slot])

        for i in range(min(ahead // group, n_steps)):
            for s in range(group):
                copy(i, s).start()

        def step(i, carry):
            @pl.when(i + ahead // group < n_steps)
            def _():
                for s in range(group):
                    copy(i + ahead // group, s).start()

            for s in range(group):
                copy(i, s).wait()
            body(i, [ring.at[lax.rem(i * group + s, RING // group * group)] for s in range(group)])
            return carry

        lax.fori_loop(0, n_steps, step, 0)

    def col_tile(i):
        return pl.ds(pl.multiple_of(i * TILE, TILE), TILE)

    def turned(y):
        return y * r.cos[...] + pltpu.roll(y, head_dim // 2, 1) * r.sin[...]

    def project(weight, out, rotary):
        def body(i, tiles):
            y = dot(r.rows[...], tiles[0][...])
            if rotary:
                y = jnp.concatenate([turned(y[:, lo : lo + head_dim]) for lo in range(0, TILE, head_dim)], axis=1)
            out[:, col_tile(i)] = y.astype(BF16)

        stream(weight.shape[1] // TILE, 1, lambda i, s: weight.at[:, col_tile(i)], body)

    project(r.w_query, r.query, True)
    project(r.w_key, r.key, True)
    project(r.w_value, r.value, False)


    logits = sum(dot(tok[p][me[OUT[p][0]]], r.w_router[lo:hi, :]) for p, (lo, hi) in enumerate(parts))
    top_k = r.ids_t.shape[0]
    gap = jnp.zeros((128 - 3 * top_k, tokens), F32)
    blank = jnp.zeros((top_k, tokens), F32)
    info = jnp.concatenate([keys_t.astype(F32), blank, r.ids_t[...].astype(F32), gap], axis=0).T
    lane = lax.broadcasted_iota(I32, logits.shape, 1).astype(F32)
    picked = [
        jnp.sum(jnp.where(lane == info[:, 2 * top_k + j : 2 * top_k + j + 1], logits, 0.0), axis=1, keepdims=True)
        for j in range(top_k)
    ]
    peak = functools.reduce(jnp.maximum, picked)
    powers = [jnp.exp(v - peak) for v in picked]
    norm = functools.reduce(jnp.add, powers)
    lane = lax.broadcasted_iota(I32, info.shape, 1)
    for j in range(top_k):
        info = jnp.where(lane == top_k + j, powers[j] / norm, info)
    r.my_gates[...] = info.T[0 : 2 * top_k, :]
    for p in range(3):
        r.line_gates[p, me[BACK[p][2]]] = r.my_gates[...]


    for k, stride in enumerate(strides):
        for p in range(3):
            axis = OUT[p][0]
            wait_bytes(tok[p].at[0], r.tok_recv.at[p, k])
            if relay:
                block = tok[p].at[neighbour(axis, k), halves[k]]
                remote(block, block, r.tok_send.at[p], r.tok_half.at[p, k], axis_peer(axis, stride)).start()
            send_far(p, 1 + k)
    pass_far(0)
    if relay:
        for p in range(3):
            for k in range(2):
                wait_bytes(tok[p].at[0, halves[k]], r.tok_half.at[p, k])
            send_far(p, 3)
    for p in range(3):
        wait_bytes(r.all_keys.at[p, 0, pl.ds(0, side - 1)], r.key_recv.at[p])
        for offset in range(1, side):
            keys = r.all_keys.at[p, me[OUT[p][1]]]
            remote(
                keys, keys, r.far_key_send.at[p], r.far_key_recv.at[p, offset - 1], axis_peer(OUT[p][1], offset)
            ).start()
    for offset in range(1, side):
        for p in range(3):
            axis = BACK[p][2]
            remote(
                r.my_gates, r.line_gates.at[p, me[axis]], r.gate_send.at[p], r.gate_recv.at[p], axis_peer(axis, offset)
            ).start()


    n_heads = r.query.shape[1] // head_dim
    per_key = r.query.shape[1] // r.key.shape[1]
    causal = lax.broadcasted_iota(I32, (tokens, tokens), 0) >= lax.broadcasted_iota(I32, (tokens, tokens), 1)

    def one_head(h, carry):
        cols = pl.ds(pl.multiple_of(h * head_dim, head_dim), head_dim)
        key_cols = pl.ds(pl.multiple_of(h // per_key * head_dim, head_dim), head_dim)
        scores = lax.dot_general(
            r.query[:, cols], r.key[:, key_cols], (((1,), (1,)), ((), ())), preferred_element_type=F32
        )
        scores = jnp.where(causal, scores * head_dim ** -0.5, -jnp.inf)
        power = jnp.exp(scores - jnp.max(scores, axis=1, keepdims=True))
        prob = (power / jnp.sum(power, axis=1, keepdims=True)).astype(BF16)
        r.query[:, cols] = dot(prob, r.value[:, key_cols]).astype(BF16)
        return carry


    stage = r.stage
    blocks = N_CHUNKS * mates
    out_mate = [me[OUT[p][2]] * 2 + me['c'] for p in range(3)]
    back_mate = [me[BACK[p][0]] * 2 + me['c'] for p in range(3)]

    def pick_rows(p, i, d, slot, source):
        keys = r.all_keys[p, i, d]
        first = mate_keys(p, (mates, tokens))
        held = jnp.full((mates, tokens), -1, I32)
        for j in range(top_k):
            slot_there = keys[j : j + 1, :] - first
            mine = jnp.logical_and(slot_there >= 0, slot_there < capacity)
            held = jnp.where(mine, slot_there, held)
        row_slot = lax.broadcasted_iota(I32, (capacity, tokens), 0)
        for mate in range(mates):
            pick = jnp.where(row_slot == held[mate : mate + 1, :], 1.0, 0.0).astype(BF16)
            for chunk in range(N_CHUNKS):
                at = (chunk * mates + mate) * slots
                r.split[at : at + slots, 0:tokens] = pick[chunk * slots : (chunk + 1) * slots, :]
        for lo, n in steps(widths[p], TILE):
            found = dot(r.split[0 : blocks * slots, 0:tokens], source[:, lo : lo + n]).astype(BF16)
            stage[slot, 0:blocks, :, lo : lo + n] = found.reshape(blocks, slots, n)

    def flush(p, i, d, slot):
        a, b = ordered({OUT[p][1]: i, OUT[p][0]: d})
        return pltpu.make_async_copy(
            stage.at[slot, pl.ds(0, blocks), :, pl.ds(0, widths[p])],
            sends[p].at[pl.ds(0, blocks), a, b],
            r.stage_sem.at[slot],
        )

    def keep(p, i, d, slot, chunk):
        spot = {**me, OUT[p][1]: i, OUT[p][0]: d}
        return pltpu.make_async_copy(
            stage.at[slot, chunk * mates + out_mate[p], :, pl.ds(0, widths[p])],
            arrivals[p].at[(chunk,) + ordered(spot)],
            r.keep_sem.at[slot, chunk],
        )

    def send_rows(p, chunk, first, count):
        near, far_axis, axis = OUT[p]
        groups = pl.ds(first, count)
        a, b = ordered({far_axis: groups, near: pl.ds(0, side)})

        def one_mate(offset, c):
            place = mate_peer(axis, offset)
            remote(
                sends[p].at[chunk * mates + place[axis] * 2 + place['c'], a, b],
                rows_of(arrivals[p], p, chunk, {**me, far_axis: groups}, (near,)),
                r.go_send.at[chunk, p],
                r.go_recv.at[chunk, p],
                place,
            ).start()
            return c

        lax.fori_loop(1, mates, one_mate, 0)

    def pick_group(offset):
        for p in range(3):
            i = lax.rem(me[OUT[p][1]] + side - offset, side)
            if offset:
                wait_bytes(r.all_keys.at[p, 0], r.far_key_recv.at[p, offset - 1])
            if relay and offset == 2:
                for n in range(side):
                    for k in range(2):
                        wait_bytes(tok[p].at[0, halves[k]], r.far_half.at[p, k, n])

            def load(d, slot):
                return pltpu.make_async_copy(
                    far[p].at[i, d], r.source.at[slot, :, pl.ds(0, widths[p])], r.source_sem.at[slot]
                )

            if offset:
                load(0, 0).start()

            def one_source(d, c):
                slot = lax.rem(d, 2)
                if offset:

                    @pl.when(d + 1 < side)
                    def _():
                        load(d + 1, 1 - slot).start()

                    load(d, slot).wait()

                @pl.when(d >= 2)
                def _():
                    flush(p, i, d - 2, slot).wait()
                    for chunk in range(N_CHUNKS):
                        keep(p, i, d - 2, slot, chunk).wait()

                pick_rows(p, i, d, slot, r.source.at[slot] if offset else tok[p].at[d])
                flush(p, i, d, slot).start()
                for chunk in range(N_CHUNKS):
                    keep(p, i, d, slot, chunk).start()
                return c

            lax.fori_loop(0, side, one_source, 0)
            for d in range(side - 2, side):
                flush(p, i, d, d % 2).wait()
                for chunk in range(N_CHUNKS):
                    keep(p, i, d, d % 2, chunk).wait()

    def heads(part, n_parts):
        lax.fori_loop(n_heads * part // n_parts, n_heads * (part + 1) // n_parts, one_head, 0)

    pick_group(0)
    for n in range(1, side):
        pass_far(n)
        heads(n - 1, side - 1)
    for offset in (1, 3) if relay else (1,):
        pick_group(offset)
    pair = [me[OUT[p][1]] // 2 * 2 for p in range(3)]
    for p in range(3):
        send_rows(p, 0, pair[p], 2)
    if relay:
        pick_group(2)
        for p in range(3):
            send_rows(p, 0, 2 - pair[p], 2)
    for chunk in range(1, N_CHUNKS):
        for p in range(3):
            send_rows(p, chunk, 0, side)


    out_split = n_heads * head_dim // model

    def out_body(i, tiles):
        total = r.hidden[:, col_tile(i)].astype(F32)
        attended = dot(r.query[:, 0:model], tiles[0][...])
        for s in range(1, out_split):
            attended += dot(r.query[:, s * model : (s + 1) * model], tiles[s][...])
        r.attended[:, col_tile(i)] = (total + attended).astype(BF16)

    stream(model // TILE, out_split, lambda i, s: r.w_out.at[pl.ds(s * model, model), col_tile(i)], out_body)

    def norm_attended(here):
        r.rows[here, :] = rms_rows(r.attended[here, :], one_row(r.ffn_scale))

    bands(norm_attended)

    def act_body(i, tiles):
        z = dot(r.rows[...], tiles[0][...])
        u = dot(r.rows[...], tiles[1][...])
        r.act[:, col_tile(i)] = (jax.nn.silu(z) * u).astype(BF16)

    ff_dim = r.ffn_gate.shape[1]
    stream(
        ff_dim // TILE, 2, lambda i, s: (r.ffn_gate, r.ffn_up)[s].at[:, col_tile(i)], act_body
    )
    down_split = ff_dim // model

    def down_body(i, tiles):
        total = dot(r.act[:, 0:model], tiles[0][...])
        for s in range(1, down_split):
            total += dot(r.act[:, s * model : (s + 1) * model], tiles[s][...])
        r.dense[:, col_tile(i)] = r.attended[:, col_tile(i)].astype(F32) + total

    stream(model // TILE, down_split, lambda i, s: r.ffn_down.at[pl.ds(s * model, model), col_tile(i)], down_body)


    for load in loads:
        load.wait()
    x_buf, y_buf, hidden_buf = r.x_buf, r.y_buf, r.hidden_buf
    group = x_buf.shape[1:-1]
    rows = math.prod(group)
    width = hidden_buf.shape[1]

    def fetch(chunk, y, slot):
        return [
            pltpu.make_async_copy(
                arrivals[p].at[chunk, y], x_buf.at[slot, :, :, :, :, pl.ds(lo, hi - lo)], r.in_sem.at[slot, p]
            )
            for p, (lo, hi) in enumerate(parts)
        ]

    def put(chunk, y, slot):
        return [
            pltpu.make_async_copy(
                y_buf.at[slot, :, :, :, :, pl.ds(lo, hi - lo)], outputs[p].at[chunk, y], r.out_sem.at[slot, p]
            )
            for p, (lo, hi) in enumerate(parts)
        ]

    def keep_own(chunk, y, slot, p):
        lo, hi = parts[p]
        free = BACK[p][1:]
        spot = [pl.ds(0, side) if axis in free else me[axis] for axis in ROW_AXES[1:]]
        mine = pltpu.make_async_copy(
            y_buf.at[tuple([slot] + spot + [pl.ds(0, slots), pl.ds(lo, hi - lo)])],
            middles[p].at[
                (chunk,) + ordered({axis: y if axis == 'y' else pl.ds(0, side) for axis in free}) + (back_mate[p],)
            ],
            r.own_sem.at[slot, p],
        )
        return mine, (None if 'y' in free else y == me['y'])

    def start_put(chunk, y, slot):
        for copy in put(chunk, y, slot):
            copy.start()
        for p in range(3):
            copy, when = keep_own(chunk, y, slot, p)
            if when is None:
                copy.start()
            else:
                pl.when(when)(copy.start)

    def wait_put(chunk, y, slot):
        for copy in put(chunk, y, slot):
            copy.wait()
        for p in range(3):
            copy, when = keep_own(chunk, y, slot, p)
            if when is None:
                copy.wait()
            else:
                pl.when(when)(copy.wait)

    def expert_chunk(chunk):
        for p in range(3):
            wait_bytes(sends[p].at[pl.ds(0, mates - 1)], r.go_recv.at[chunk, p])
        for copy in fetch(chunk, 0, 0):
            copy.start()

        def one_tile(y, c):
            slot = lax.rem(y, 2)

            @pl.when(y + 1 < side)
            def _():
                for copy in fetch(chunk, y + 1, 1 - slot):
                    copy.start()

            for copy in fetch(chunk, y, slot):
                copy.wait()

            @pl.when(y >= 2)
            def _():
                wait_put(chunk, y - 2, slot)

            for lo in range(0, width, f_chunk):
                cols = slice(lo, lo + f_chunk)
                z = dot(x_buf[slot].reshape(rows, model), r.gate[:, cols])
                u = dot(x_buf[slot].reshape(rows, model), r.up[:, cols])
                hidden_buf[:, cols] = (jax.nn.silu(z) * u).astype(BF16)
            for lo in range(0, model, d_chunk):
                cols = slice(lo, lo + d_chunk)
                y_rows = dot(hidden_buf[...], r.down[:, cols]).astype(BF16)
                y_buf[slot, :, :, :, :, cols] = y_rows.reshape(group + (d_chunk,))
            start_put(chunk, y, slot)
            return c

        lax.fori_loop(0, side, one_tile, 0)
        for y in range(side - 2, side):
            wait_put(chunk, y, y % 2)

        def one_mate(offset, c):
            for p in range(3):
                place = mate_peer(BACK[p][0], offset)
                remote(
                    rows_of(outputs[p], p, chunk, place, BACK[p][1:]),
                    middles[p].at[chunk, pl.ds(0, side), pl.ds(0, side), back_mate[p]],
                    r.back_send.at[chunk, p],
                    r.back_recv.at[chunk, p],
                    place,
                ).start()
            return c

        lax.fori_loop(1, mates, one_mate, 0)

    def middle_rows(p, chunk, i, d):
        return middles[p].at[(chunk,) + ordered({BACK[p][1]: i, BACK[p][2]: d})]

    def pass_on(chunk):
        for p in range(3):
            wait_bytes(middles[p].at[chunk, pl.ds(0, side), pl.ds(0, side), pl.ds(0, mates - 1)], r.back_recv.at[chunk, p])
            for offset in range(1, side):
                axis = BACK[p][1]
                place = axis_peer(axis, offset)
                remote(
                    middle_rows(p, chunk, place[axis], pl.ds(0, side)),
                    results[p].at[chunk, pl.ds(0, side), me[axis]],
                    r.home_send.at[chunk, p],
                    r.home_recv.at[chunk, p],
                    place,
                ).start()


    split = r.split
    lanes = min(128, rows_block)

    def weigh_chunk(chunk, carry):
        for p in range(3):
            wait_bytes(results[p].at[chunk, pl.ds(0, side), pl.ds(0, side - 1)], r.home_recv.at[chunk, p])

        def source_of(p, n):
            ahead = 2 * side - 2 - 2 * n + 3 * (n // 2) if relay else 1 - n
            return lax.rem(me[BACK[p][2]] + ahead, side)

        def load(p, n, slot):
            copies = []
            for offset in range(side):
                i, d = lax.rem(me[BACK[p][1]] + offset, side), source_of(p, n)
                copies.append(
                    pltpu.make_async_copy(
                        results[p].at[chunk, d, i] if offset else middle_rows(p, chunk, i, d),
                        stage.at[slot, pl.ds(i * mates, mates), :, pl.ds(0, widths[p])],
                        r.load_sem.at[slot, offset],
                    )
                )
            return copies

        for copy in load(0, 0, 0):
            copy.start()

        def one_source(n, c):
            for p in range(3):
                d = source_of(p, n)
                slot = lax.rem(n + p, 2)

                @pl.when(n + p // 2 < side)
                def _():
                    for copy in load((p + 1) % 3, n + p // 2, 1 - slot):
                        copy.start()

                lane = lax.broadcasted_iota(I32, (1, lanes), 1)
                wanted = (lax.rem(lane, slots) + chunk * slots).astype(F32)
                for lo in range(0, rows_block, lanes):
                    which = jnp.broadcast_to(lane // slots + lo // slots, (tokens, lanes))
                    take = functools.partial(jnp.take_along_axis, indices=which, axis=1, mode='promise_in_bounds')
                    weight = jnp.where(take(r.held[p, d]) == wanted, take(r.gates[p, d]), 0.0)
                    high = weight.astype(BF16)
                    rest = weight - high.astype(F32)
                    middle = rest.astype(BF16)
                    low = (rest - middle.astype(F32)).astype(BF16)
                    split[0:tokens, lo : lo + lanes] = high
                    split[tokens : 2 * tokens, lo : lo + lanes] = middle
                    split[2 * tokens : 3 * tokens, lo : lo + lanes] = low
                for copy in load(p, n, slot):
                    copy.wait()
                for lo, size in steps(widths[p], TILE):
                    y = stage[slot, 0:members, :, lo : lo + size].reshape(rows_block, size)
                    both = dot(split[...], y)
                    total = both[0:tokens] + (both[tokens : 2 * tokens] + both[2 * tokens : 3 * tokens])

                    @pl.when(chunk == 0)
                    def _():
                        sums[p][d, :, lo : lo + size] = total

                    @pl.when(chunk > 0)
                    def _():
                        sums[p][d, :, lo : lo + size] += total

                last = chunk == N_CHUNKS - 1
                axis = BACK[p][2]

                @pl.when(jnp.logical_and(last, n == 0))
                def _():
                    for k, stride in enumerate(strides):
                        part, spot, arrived = sums[p].at[d], others[p].at[0], r.sum_recv.at[p, 0]
                        if relay:
                            part = sums[p].at[d, halves[k]]
                            spot, arrived = others[p].at[2, halves[k]], r.sum_half.at[p, k]
                        remote(part, spot, r.sum_send.at[p], arrived, axis_peer(axis, stride)).start()

                for k in range(2 if relay else 0):

                    @pl.when(jnp.logical_and(last, n == 2 + k))
                    def _():
                        wait_bytes(others[p].at[2, halves[k]], r.sum_half.at[p, k])
                        sums[p][d, halves[k], :] += others[p][2, halves[k], :]
                        remote(
                            sums[p].at[d], others[p].at[k], r.sum_send.at[p], r.sum_recv.at[p, k], axis_peer(axis, strides[k])
                        ).start()

            return c

        return lax.fori_loop(0, side, one_source, carry)


    def one_by_one(step):
        lax.fori_loop(0, N_CHUNKS, lambda chunk, c: (step(chunk), c)[1], 0)

    one_by_one(expert_chunk)
    one_by_one(pass_on)
    gap = jnp.zeros((128 - members, tokens), F32)
    for p in range(3):
        wait_bytes(r.line_gates.at[p, pl.ds(0, side - 1)], r.gate_recv.at[p])
        first = plane_keys(p, (members, tokens)).astype(F32)

        def spread(d, c):
            info = r.line_gates[p, d]
            held, gate = jnp.full((members, tokens), -1.0, F32), jnp.zeros((members, tokens), F32)
            for j in range(top_k):
                there = info[j : j + 1, :] - first
                mine = jnp.logical_and(there >= 0, there < capacity)
                held = jnp.where(mine, there, held)
                gate = jnp.where(mine, info[top_k + j : top_k + j + 1, :], gate)
            r.held[p, d] = jnp.concatenate([held, gap], axis=0).T
            r.gates[p, d] = jnp.concatenate([gate, gap], axis=0).T
            return c

        lax.fori_loop(0, side, spread, 0)
    lax.fori_loop(0, N_CHUNKS, weigh_chunk, 0)
    for p, (lo, hi) in enumerate(parts):
        for k in range(len(strides)):
            wait_bytes(others[p].at[k], r.sum_recv.at[p, k])

        def finish(here):
            moe = sums[p][me[BACK[p][2]], here, :]
            for k in range(len(strides)):
                moe += others[p][k, here, :]
            r.out[here, lo:hi] = (r.dense[here, lo:hi] + moe).astype(BF16)

        bands(finish)


    for p in range(3):
        wait_bytes(tok[p].at[pl.ds(0, side - 1)], r.tok_send.at[p])
        wait_bytes(r.all_keys.at[p, 0, pl.ds(0, side - 1)], r.key_send.at[p])
        wait_bytes(far[p].at[pl.ds(0, side - 1)], r.far_send.at[p])
        wait_bytes(r.all_keys.at[p, pl.ds(0, side - 1)], r.far_key_send.at[p])
        wait_bytes(r.line_gates.at[p, pl.ds(0, side - 1)], r.gate_send.at[p])
        wait_bytes(others[p], r.sum_send.at[p])
        for chunk in range(N_CHUNKS):
            wait_bytes(sends[p].at[pl.ds(0, mates - 1)], r.go_send.at[chunk, p])
            wait_bytes(middles[p].at[chunk, pl.ds(0, side), pl.ds(0, side), pl.ds(0, mates - 1)], r.back_send.at[chunk, p])
            wait_bytes(results[p].at[chunk, pl.ds(0, side), pl.ds(0, side - 1)], r.home_send.at[chunk, p])


def layer_pair(small, large, side, capacity, head_dim):
    tokens, model = small['hidden'].shape
    top_k, width = small['ids_t'].shape[0], large['gate_hbm'].shape[1]
    key_dim, ff_dim = large['w_key'].shape[1], large['ffn_gate'].shape[1]
    parts = column_parts(model)
    widths = [hi - lo for lo, hi in parts]
    slots, members, mates = capacity // N_CHUNKS, side * side * 2, side * 2
    group = (side, 2, side, slots)
    rows = math.prod(group)
    sds, vmem = jax.ShapeDtypeStruct, pltpu.VMEM
    dma = lambda *shape: pltpu.SemaphoreType.DMA(shape)
    outs = dict(out=sds((tokens, model), BF16))
    scratch = dict(
        rows=vmem((tokens, model), BF16),
        query=vmem((tokens, large['w_query'].shape[1]), BF16),
        key=vmem((tokens, key_dim), BF16),
        value=vmem((tokens, key_dim), BF16),
        attended=vmem((tokens, model), BF16),
        act=vmem((tokens, ff_dim), BF16),
        dense=vmem((tokens, model), F32),
        ring=vmem((RING, model, TILE), BF16),
        all_keys=vmem((3, side, side, top_k, tokens), I32),
        my_gates=vmem((2 * top_k, tokens), F32),
        line_gates=vmem((3, side, 2 * top_k, tokens), F32),
        held=vmem((3, side, tokens, 128), F32),
        gates=vmem((3, side, tokens, 128), F32),
        source=vmem((2, tokens, max(widths)), BF16),
        stage=vmem((2, max(members, N_CHUNKS * mates), slots, max(widths)), BF16),
        split=vmem((3 * tokens, members * slots), BF16),
        gate=vmem((model, width), BF16),
        up=vmem((model, width), BF16),
        down=vmem((width, model), BF16),
        x_buf=vmem((2,) + group + (model,), BF16),
        y_buf=vmem((2,) + group + (model,), BF16),
        hidden_buf=vmem((rows, width), BF16),
        weight_sem=dma(3),
        ring_sem=dma(RING),
        source_sem=dma(2),
        stage_sem=dma(2),
        keep_sem=dma(2, N_CHUNKS),
        in_sem=dma(2, 3),
        out_sem=dma(2, 3),
        own_sem=dma(2, 3),
        load_sem=dma(2, side),
        tok_send=dma(3),
        tok_recv=dma(3, 2),
        tok_half=dma(3, 2),
        key_send=dma(3),
        key_recv=dma(3),
        far_send=dma(3),
        far_recv=dma(3, 2, side),
        far_half=dma(3, 2, side),
        far_key_send=dma(3),
        far_key_recv=dma(3, side - 1),
        gate_send=dma(3),
        gate_recv=dma(3),
        sum_send=dma(3),
        sum_recv=dma(3, 2),
        sum_half=dma(3, 2),
        go_send=dma(N_CHUNKS, 3),
        go_recv=dma(N_CHUNKS, 3),
        back_send=dma(N_CHUNKS, 3),
        back_recv=dma(N_CHUNKS, 3),
        home_send=dma(N_CHUNKS, 3),
        home_recv=dma(N_CHUNKS, 3),
    )
    for p, w in enumerate(widths):
        there = sds((N_CHUNKS, side, side, 2, side, slots, w), BF16)
        outs['far' + str(p)] = sds((side, side, tokens, w), BF16)
        outs['send' + str(p)] = sds((N_CHUNKS * mates, side, side, slots, w), BF16)
        outs['arrive' + str(p)] = there
        outs['output' + str(p)] = there
        outs['middle' + str(p)] = sds((N_CHUNKS, side, side, mates, slots, w), BF16)
        outs['result' + str(p)] = sds((N_CHUNKS, side, side, mates, slots, w), BF16)
        scratch['tok' + str(p)] = vmem((side, tokens, w), BF16)
        scratch['sum' + str(p)] = vmem((side, tokens, w), F32)
        scratch['other' + str(p)] = vmem((side - 1, tokens, w), F32)
    anywhere = pl.BlockSpec(memory_space=pl.ANY)
    local = pl.BlockSpec(memory_space=pltpu.VMEM)
    n_rows = members * side * capacity
    return pl.pallas_call(
        functools.partial(
            kernel,
            names=tuple(small) + tuple(large) + tuple(outs) + tuple(scratch),
            side=side,
            parts=parts,
            capacity=capacity,
            head_dim=head_dim,
            f_chunk=min(256, width),
            d_chunk=min(512, model),
        ),
        out_shape=list(outs.values()),
        in_specs=[local] * len(small) + [anywhere] * len(large),
        out_specs=[local] + [anywhere] * (len(outs) - 1),
        scratch_shapes=list(scratch.values()),
        compiler_params=pltpu.CompilerParams(has_side_effects=True, vmem_limit_bytes=67043328),
        cost_estimate=pl.CostEstimate(flops=6 * n_rows * model * width, bytes_accessed=8 * n_rows * model, transcendentals=0),
    )(*small.values(), *large.values())[0]


def solution(mesh):
    group_size = mesh.shape['ep']
    side = torus_side(group_size)
    torus = jax.sharding.Mesh(mesh.devices.reshape(side, side, side, 2), AXES)
    row_spec = P(AXES, None, None)
    vec_spec = P(None)
    mat_spec = P(None, None)
    cube_spec = P(None, None, None)
    expert_spec = P(AXES, None, None)

    def per_device(hidden, expert_ids, slot_ids, attn_norm, w_query, w_key, w_value, w_out, ffn_norm, ffn_gate, ffn_up, ffn_down, moe_norm, w_router, exp_gate, exp_up, exp_down):
        n_seqs, tokens, model = hidden.shape
        assert n_seqs == 1 and exp_gate.shape[0] == 1
        n_heads, head_dim = w_out.shape[0], w_out.shape[1]
        top_k = expert_ids.shape[2]
        capacity = CAP_FACTOR * tokens * top_k // group_size
        inv_freq = np.float32(ROPE_BASE) ** (np.float32(-2.0) * np.arange(head_dim // 2, dtype=np.float32) / head_dim)
        angles = np.arange(tokens, dtype=np.float32)[:, None] * inv_freq[None, :]
        cos, sin = np.cos(angles), np.sin(angles)
        small = dict(
            hidden=hidden[0],
            attn_scale=attn_norm.reshape(-1, 128),
            moe_scale=moe_norm.reshape(-1, 128),
            ffn_scale=ffn_norm.reshape(-1, 128),
            ids_t=expert_ids[0].T,
            slots_t=slot_ids[0].T,
            w_router=w_router,
            cos=np.concatenate([cos, cos], axis=1).astype(np.float32),
            sin=np.concatenate([-sin, sin], axis=1).astype(np.float32),
        )
        large = dict(
            w_query=w_query,
            w_key=w_key,
            w_value=w_value,
            w_out=w_out.reshape(n_heads * head_dim, model),
            ffn_gate=ffn_gate,
            ffn_up=ffn_up,
            ffn_down=ffn_down,
            gate_hbm=exp_gate[0],
            up_hbm=exp_up[0],
            down_hbm=exp_down[0],
        )
        return layer_pair(small, large, side, capacity, head_dim).reshape(hidden.shape)

    return jax.shard_map(per_device, mesh=torus, in_specs=(row_spec, row_spec, row_spec, vec_spec, mat_spec, mat_spec, mat_spec, cube_spec, vec_spec, mat_spec, mat_spec, mat_spec, vec_spec, mat_spec, expert_spec, expert_spec, expert_spec), out_specs=row_spec, check_vma=False)
```

```python
import functools
import math
import types

import jax
import jax.numpy as jnp
import numpy as np
from jax import lax
from jax.experimental import pallas as pl
from jax.experimental.pallas import tpu as pltpu
from jax.sharding import PartitionSpec as P

RMS_EPS = 1e-6
ROPE_BASE = 10000.0
CAP_FACTOR = 3
N_CHUNKS = 3
RING = 6
TILE = 256
MESH = pl.DeviceIdType.MESH

BF16, F32, I32 = jnp.bfloat16, jnp.float32, jnp.int32

AXES = ('z', 'y', 'x', 'c')
OUT = (('z', 'y', 'x'), ('x', 'z', 'y'), ('y', 'x', 'z'))
BACK = (('y', 'z', 'x'), ('z', 'x', 'y'), ('x', 'y', 'z'))
ROW_AXES = ('y', 'x', 'c', 'z')


def torus_side(n_devices):
    side = round((n_devices // 2) ** (1 / 3))
    assert side ** 3 * 2 == n_devices
    return side


def column_parts(model):
    lanes = model // 128
    first = -(-lanes // 3)
    second = -(-(lanes - first) // 2)
    ends = (0, first * 128, (first + second) * 128, model)
    return tuple((ends[p], ends[p + 1]) for p in range(3))


def steps(total, size):
    return [(lo, min(size, total - lo)) for lo in range(0, total, size)]


def rms_rows(rows, scale):
    as_float = rows.astype(F32)
    inv_rms = lax.rsqrt(jnp.mean(as_float * as_float, axis=-1, keepdims=True) + RMS_EPS)
    return (as_float * inv_rms * scale.astype(F32)).astype(BF16)


def dot(a, b):
    return jnp.dot(a, b, preferred_element_type=F32)


def kernel(*refs, names, side, parts, capacity, head_dim, f_chunk, d_chunk):
    r = types.SimpleNamespace(**dict(zip(names, refs)))
    each = lambda name: [getattr(r, name + str(p)) for p in range(3)]
    slots = capacity // N_CHUNKS
    members = side * side * 2
    mates = side * 2
    assert side in (2, 4)
    relay = side == 4
    strides = (1, side - 1) if relay else (1,)

    def order(n):
        return 3 * n - 5 * (n // 2) - 2 * (n // 3) if relay else n

    rows_block = members * slots
    tokens, model = r.hidden.shape
    me = {axis: lax.axis_index(axis) for axis in AXES}


    def rows_of(ref, p, chunk, place, free):
        spot = [pl.ds(0, side) if axis in free else place[axis] for axis in ROW_AXES]
        return ref.at[tuple([chunk] + spot)]

    def ordered(where):
        return tuple(where[axis] for axis in ROW_AXES if axis in where)

    def device(place):
        return tuple(place[axis] for axis in AXES)

    def axis_peer(axis, offset):
        return {**me, axis: lax.rem(me[axis] + offset, side)}

    def mate_peer(axis, offset):
        return {
            **me,
            axis: lax.rem(me[axis] + offset // 2, side),
            'c': lax.rem(me['c'] + lax.rem(offset, 2), 2),
        }

    def remote(src, dst, send_sem, recv_sem, place):
        return pltpu.make_async_remote_copy(
            src_ref=src, dst_ref=dst, send_sem=send_sem, recv_sem=recv_sem, device_id=device(place), device_id_type=MESH
        )

    def wait_bytes(ref, sem):
        pltpu.make_async_copy(ref, ref, sem).wait()

    def expert_key(place, core, slot):
        return (((place['z'] * side + place['y']) * side + place['x']) * 2 + core) * capacity + slot

    def plane_keys(p, shape):
        first, second, _ = BACK[p]
        which = lax.broadcasted_iota(I32, shape, 0)
        pair = which // 2
        place = {**me, second: pair // side, first: lax.rem(pair, side)}
        return expert_key(place, lax.rem(which, 2), 0)

    def mate_keys(p, shape):
        mate = lax.broadcasted_iota(I32, shape, 0)
        return expert_key({**me, OUT[p][2]: mate // 2}, lax.rem(mate, 2), 0)

    tok, far, sends, arrivals, outputs = each('tok'), each('far'), each('send'), each('arrive'), each('output')
    middles, results, sums, others = each('middle'), each('result'), each('sum'), each('other')
    widths = [hi - lo for lo, hi in parts]


    band = min(32, tokens)

    def bands(body):
        lax.fori_loop(0, tokens // band, lambda i, c: (body(pl.ds(pl.multiple_of(i * band, band), band)), c)[1], 0)

    def one_row(scale):
        lines = scale[...].astype(F32)
        return jnp.concatenate([lines[i : i + 1, :] for i in range(lines.shape[0])], axis=1)

    def norm_both(here):
        normed = rms_rows(r.hidden[here, :], one_row(r.moe_scale))
        for p, (lo, hi) in enumerate(parts):
            tok[p][me[OUT[p][0]], here, :] = normed[:, lo:hi]
        r.rows[here, :] = rms_rows(r.hidden[here, :], one_row(r.attn_scale))

    bands(norm_both)
    keys_t = r.ids_t[...] * capacity + r.slots_t[...]
    for p in range(3):
        r.all_keys[p, me[OUT[p][1]], me[OUT[p][0]]] = keys_t
    pairs = ((r.gate_hbm, r.gate), (r.up_hbm, r.up), (r.down_hbm, r.down))
    loads = [pltpu.make_async_copy(src, dst, r.weight_sem.at[i]) for i, (src, dst) in enumerate(pairs)]
    for load in loads:
        load.start()

    half = tokens // 2
    halves = (pl.ds(0, half), pl.ds(half, half))

    def neighbour(axis, k):
        return lax.rem(me[axis] + side - strides[k], side)

    def send_far(p, n):
        near, axis, _ = OUT[p]
        d = lax.rem(me[near] + order(n), side)
        for k, stride in enumerate(strides):
            remote(
                tok[p].at[d], far[p].at[me[axis], d], r.far_send.at[p], r.far_recv.at[p, k, n], axis_peer(axis, stride)
            ).start()

    def pass_far(n):
        for k, stride in enumerate(strides):
            for p in range(3):
                near, axis, _ = OUT[p]
                d = lax.rem(me[near] + order(n), side)
                wait_bytes(tok[p].at[0], r.far_recv.at[p, k, n])
                if relay:
                    block = far[p].at[neighbour(axis, k), d, halves[k]]
                    remote(block, block, r.far_send.at[p], r.far_half.at[p, k, n], axis_peer(axis, stride)).start()

    for k, stride in enumerate(strides):
        for p in range(3):
            axis = OUT[p][0]
            block = tok[p].at[me[axis]]
            remote(block, block, r.tok_send.at[p], r.tok_recv.at[p, k], axis_peer(axis, stride)).start()
    for p in range(3):
        send_far(p, 0)
    for offset in range(1, side):
        for p in range(3):
            axis = OUT[p][0]
            keys = r.all_keys.at[p, me[OUT[p][1]], me[axis]]
            remote(keys, keys, r.key_send.at[p], r.key_recv.at[p], axis_peer(axis, offset)).start()


    ring = r.ring
    ring_sem = r.ring_sem

    def stream(n_steps, group, source, body):
        ahead = RING // group * group - group

        def copy(i, s):
            slot = lax.rem(i * group + s, RING // group * group)
            return pltpu.make_async_copy(source(i, s), ring.at[slot], ring_sem.at[slot])

        for i in range(min(ahead // group, n_steps)):
            for s in range(group):
                copy(i, s).start()

        def step(i, carry):
            @pl.when(i + ahead // group < n_steps)
            def _():
                for s in range(group):
                    copy(i + ahead // group, s).start()

            for s in range(group):
                copy(i, s).wait()
            body(i, [ring.at[lax.rem(i * group + s, RING // group * group)] for s in range(group)])
            return carry

        lax.fori_loop(0, n_steps, step, 0)

    def col_tile(i):
        return pl.ds(pl.multiple_of(i * TILE, TILE), TILE)

    def turned(y):
        return y * r.cos[...] + pltpu.roll(y, head_dim // 2, 1) * r.sin[...]

    def project(weight, out, rotary):
        def body(i, tiles):
            y = dot(r.rows[...], tiles[0][...])
            if rotary:
                y = jnp.concatenate([turned(y[:, lo : lo + head_dim]) for lo in range(0, TILE, head_dim)], axis=1)
            out[:, col_tile(i)] = y.astype(BF16)

        stream(weight.shape[1] // TILE, 1, lambda i, s: weight.at[:, col_tile(i)], body)

    project(r.w_query, r.query, True)
    project(r.w_key, r.key, True)
    project(r.w_value, r.value, False)


    logits = sum(dot(tok[p][me[OUT[p][0]]], r.w_router[lo:hi, :]) for p, (lo, hi) in enumerate(parts))
    top_k = r.ids_t.shape[0]
    gap = jnp.zeros((128 - 3 * top_k, tokens), F32)
    blank = jnp.zeros((top_k, tokens), F32)
    info = jnp.concatenate([keys_t.astype(F32), blank, r.ids_t[...].astype(F32), gap], axis=0).T
    lane = lax.broadcasted_iota(I32, logits.shape, 1).astype(F32)
    picked = [
        jnp.sum(jnp.where(lane == info[:, 2 * top_k + j : 2 * top_k + j + 1], logits, 0.0), axis=1, keepdims=True)
        for j in range(top_k)
    ]
    peak = functools.reduce(jnp.maximum, picked)
    powers = [jnp.exp(v - peak) for v in picked]
    norm = functools.reduce(jnp.add, powers)
    lane = lax.broadcasted_iota(I32, info.shape, 1)
    for j in range(top_k):
        info = jnp.where(lane == top_k + j, powers[j] / norm, info)
    r.my_gates[...] = info.T[0 : 2 * top_k, :]
    for p in range(3):
        r.line_gates[p, me[BACK[p][2]]] = r.my_gates[...]


    for k, stride in enumerate(strides):
        for p in range(3):
            axis = OUT[p][0]
            wait_bytes(tok[p].at[0], r.tok_recv.at[p, k])
            if relay:
                block = tok[p].at[neighbour(axis, k), halves[k]]
                remote(block, block, r.tok_send.at[p], r.tok_half.at[p, k], axis_peer(axis, stride)).start()
            send_far(p, 1 + k)
    if relay:
        for p in range(3):
            for k in range(2):
                wait_bytes(tok[p].at[0, halves[k]], r.tok_half.at[p, k])
            send_far(p, 3)
    for p in range(3):
        wait_bytes(r.all_keys.at[p, 0, pl.ds(0, side - 1)], r.key_recv.at[p])
        for offset in range(1, side):
            keys = r.all_keys.at[p, me[OUT[p][1]]]
            remote(
                keys, keys, r.far_key_send.at[p], r.far_key_recv.at[p, offset - 1], axis_peer(OUT[p][1], offset)
            ).start()
    for offset in range(1, side):
        for p in range(3):
            axis = BACK[p][2]
            remote(
                r.my_gates, r.line_gates.at[p, me[axis]], r.gate_send.at[p], r.gate_recv.at[p], axis_peer(axis, offset)
            ).start()


    n_heads = r.query.shape[1] // head_dim
    per_key = r.query.shape[1] // r.key.shape[1]
    causal = lax.broadcasted_iota(I32, (tokens, tokens), 0) >= lax.broadcasted_iota(I32, (tokens, tokens), 1)

    def one_head(h, carry):
        cols = pl.ds(pl.multiple_of(h * head_dim, head_dim), head_dim)
        key_cols = pl.ds(pl.multiple_of(h // per_key * head_dim, head_dim), head_dim)
        scores = lax.dot_general(
            r.query[:, cols], r.key[:, key_cols], (((1,), (1,)), ((), ())), preferred_element_type=F32
        )
        scores = jnp.where(causal, scores * head_dim ** -0.5, -jnp.inf)
        power = jnp.exp(scores - jnp.max(scores, axis=1, keepdims=True))
        prob = (power / jnp.sum(power, axis=1, keepdims=True)).astype(BF16)
        r.query[:, cols] = dot(prob, r.value[:, key_cols]).astype(BF16)
        return carry


    stage = r.stage
    blocks = N_CHUNKS * mates
    out_mate = [me[OUT[p][2]] * 2 + me['c'] for p in range(3)]
    back_mate = [me[BACK[p][0]] * 2 + me['c'] for p in range(3)]

    def pick_rows(p, i, d, source):
        keys = r.all_keys[p, i, d]
        first = mate_keys(p, (mates, tokens))
        held = jnp.full((mates, tokens), -1, I32)
        for j in range(top_k):
            slot_there = keys[j : j + 1, :] - first
            mine = jnp.logical_and(slot_there >= 0, slot_there < capacity)
            held = jnp.where(mine, slot_there, held)
        row_slot = lax.broadcasted_iota(I32, (capacity, tokens), 0)
        for mate in range(mates):
            pick = jnp.where(row_slot == held[mate : mate + 1, :], 1.0, 0.0).astype(BF16)
            for chunk in range(N_CHUNKS):
                at = (chunk * mates + mate) * slots
                r.split[at : at + slots, 0:tokens] = pick[chunk * slots : (chunk + 1) * slots, :]
        for lo, n in steps(widths[p], TILE):
            found = dot(r.split[0 : blocks * slots, 0:tokens], source[:, lo : lo + n]).astype(BF16)
            stage[p * blocks : (p + 1) * blocks, :, lo : lo + n] = found.reshape(blocks, slots, n)

    def flush(p, i, d):
        a, b = ordered({OUT[p][1]: i, OUT[p][0]: d})
        return pltpu.make_async_copy(
            stage.at[pl.ds(p * blocks, blocks), :, pl.ds(0, widths[p])],
            sends[p].at[pl.ds(0, blocks), a, b],
            r.stage_sem.at[p],
        )

    def keep(p, i, d, chunk):
        spot = {**me, OUT[p][1]: i, OUT[p][0]: d}
        return pltpu.make_async_copy(
            stage.at[p * blocks + chunk * mates + out_mate[p], :, pl.ds(0, widths[p])],
            arrivals[p].at[(chunk,) + ordered(spot)],
            r.keep_sem.at[p, chunk],
        )

    def wait_staged(p):
        flush(p, 0, 0).wait()
        for chunk in range(N_CHUNKS):
            keep(p, 0, 0, chunk).wait()

    def pick_one(p, i, d, source):
        pick_rows(p, i, d, source)
        flush(p, i, d).start()
        for chunk in range(N_CHUNKS):
            keep(p, i, d, chunk).start()

    def send_rows(p, chunk, i):
        near, far_axis, axis = OUT[p]
        free = (near,) if i is not None else (near, far_axis)
        a, b = ordered({far_axis: pl.ds(0, side) if i is None else i, near: pl.ds(0, side)})
        group_place = me if i is None else {**me, far_axis: i}

        def one_mate(offset, c):
            place = mate_peer(axis, offset)
            remote(
                sends[p].at[chunk * mates + place[axis] * 2 + place['c'], a, b],
                rows_of(arrivals[p], p, chunk, group_place, free),
                r.go_send.at[chunk, p],
                r.go_recv.at[chunk, p],
                place,
            ).start()
            return c

        lax.fori_loop(1, mates, one_mate, 0)

    def heads(part, n_parts):
        lax.fori_loop(n_heads * part // n_parts, n_heads * (part + 1) // n_parts, one_head, 0)

    def own_line(d, c):
        for p in range(3):
            pl.when(d >= 1)(functools.partial(wait_staged, p))
            pick_one(p, me[OUT[p][1]], d, tok[p].at[d])
        return c

    def load_far(p, k, i, n):
        d = lax.rem(me[OUT[p][0]] + order(n), side)
        copy = pltpu.make_async_copy(
            far[p].at[i, d], r.source.at[p, :, pl.ds(0, widths[p])], r.source_sem.at[p]
        )
        return copy, d

    def pick_far(k, n, place, first):
        for p in range(3):
            i = place(OUT[p][1])
            copy, d = load_far(p, k, i, n)
            copy.wait()
            if first is None:
                wait_staged(p)
            else:
                pl.when(jnp.logical_not(first))(functools.partial(wait_staged, p))
            pick_one(p, i, d, r.source.at[p])

    def neighbours(n, c):
        heads(n, side)
        pass_far(n)
        for k in range(len(strides)):
            for p in range(3):
                load_far(p, k, neighbour(OUT[p][1], k), n)[0].start()
            pick_far(k, n, functools.partial(neighbour, k=k), None)
        return c

    def opposite(n, c):
        for p in range(3):
            for k in range(2):
                wait_bytes(tok[p].at[0, halves[k]], r.far_half.at[p, k, n])
            load_far(p, 0, opposite_of(OUT[p][1]), n)[0].start()
        pick_far(0, n, opposite_of, n == 0)
        return c

    def opposite_of(axis):
        return lax.rem(me[axis] + 2, side)

    lax.fori_loop(0, side, own_line, 0)
    for p in range(3):
        for offset in range(1, side):
            wait_bytes(r.all_keys.at[p, 0], r.far_key_recv.at[p, offset - 1])
    lax.fori_loop(0, side, neighbours, 0)
    for p in range(3):
        wait_staged(p)
    for p in range(3):
        send_rows(p, 0, me[OUT[p][1]])
    for k in range(len(strides)):
        for p in range(3):
            send_rows(p, 0, neighbour(OUT[p][1], k))
    if relay:
        lax.fori_loop(0, side, opposite, 0)
        for p in range(3):
            wait_staged(p)
            send_rows(p, 0, opposite_of(OUT[p][1]))
    for chunk in range(1, N_CHUNKS):
        for p in range(3):
            send_rows(p, chunk, None)


    out_split = n_heads * head_dim // model

    def out_body(i, tiles):
        total = r.hidden[:, col_tile(i)].astype(F32)
        attended = dot(r.query[:, 0:model], tiles[0][...])
        for s in range(1, out_split):
            attended += dot(r.query[:, s * model : (s + 1) * model], tiles[s][...])
        r.attended[:, col_tile(i)] = (total + attended).astype(BF16)

    stream(model // TILE, out_split, lambda i, s: r.w_out.at[pl.ds(s * model, model), col_tile(i)], out_body)

    def norm_attended(here):
        r.rows[here, :] = rms_rows(r.attended[here, :], one_row(r.ffn_scale))

    bands(norm_attended)

    def act_body(i, tiles):
        z = dot(r.rows[...], tiles[0][...])
        u = dot(r.rows[...], tiles[1][...])
        r.act[:, col_tile(i)] = (jax.nn.silu(z) * u).astype(BF16)

    ff_dim = r.ffn_gate.shape[1]
    stream(
        ff_dim // TILE, 2, lambda i, s: (r.ffn_gate, r.ffn_up)[s].at[:, col_tile(i)], act_body
    )
    down_split = ff_dim // model

    def down_body(i, tiles):
        total = dot(r.act[:, 0:model], tiles[0][...])
        for s in range(1, down_split):
            total += dot(r.act[:, s * model : (s + 1) * model], tiles[s][...])
        r.dense[:, col_tile(i)] = r.attended[:, col_tile(i)].astype(F32) + total

    stream(model // TILE, down_split, lambda i, s: r.ffn_down.at[pl.ds(s * model, model), col_tile(i)], down_body)


    for load in loads:
        load.wait()
    x_buf, y_buf, hidden_buf = r.x_buf, r.y_buf, r.hidden_buf
    group = x_buf.shape[1:-1]
    rows = math.prod(group)
    width = hidden_buf.shape[1]

    def fetch(chunk, y, slot):
        return [
            pltpu.make_async_copy(
                arrivals[p].at[chunk, y], x_buf.at[slot, :, :, :, :, pl.ds(lo, hi - lo)], r.in_sem.at[slot, p]
            )
            for p, (lo, hi) in enumerate(parts)
        ]

    def put(chunk, y, slot):
        return [
            pltpu.make_async_copy(
                y_buf.at[slot, :, :, :, :, pl.ds(lo, hi - lo)], outputs[p].at[chunk, y], r.out_sem.at[slot, p]
            )
            for p, (lo, hi) in enumerate(parts)
        ]

    def keep_own(chunk, y, slot, p):
        lo, hi = parts[p]
        free = BACK[p][1:]
        spot = [pl.ds(0, side) if axis in free else me[axis] for axis in ROW_AXES[1:]]
        mine = pltpu.make_async_copy(
            y_buf.at[tuple([slot] + spot + [pl.ds(0, slots), pl.ds(lo, hi - lo)])],
            middles[p].at[
                (chunk,) + ordered({axis: y if axis == 'y' else pl.ds(0, side) for axis in free}) + (back_mate[p],)
            ],
            r.own_sem.at[slot, p],
        )
        return mine, (None if 'y' in free else y == me['y'])

    def start_put(chunk, y, slot):
        for copy in put(chunk, y, slot):
            copy.start()
        for p in range(3):
            copy, when = keep_own(chunk, y, slot, p)
            if when is None:
                copy.start()
            else:
                pl.when(when)(copy.start)

    def wait_put(chunk, y, slot):
        for copy in put(chunk, y, slot):
            copy.wait()
        for p in range(3):
            copy, when = keep_own(chunk, y, slot, p)
            if when is None:
                copy.wait()
            else:
                pl.when(when)(copy.wait)

    def expert_chunk(chunk):
        for p in range(3):
            wait_bytes(sends[p].at[pl.ds(0, mates - 1)], r.go_recv.at[chunk, p])
        for copy in fetch(chunk, 0, 0):
            copy.start()

        def one_tile(y, c):
            slot = lax.rem(y, 2)

            @pl.when(y + 1 < side)
            def _():
                for copy in fetch(chunk, y + 1, 1 - slot):
                    copy.start()

            for copy in fetch(chunk, y, slot):
                copy.wait()

            @pl.when(y >= 2)
            def _():
                wait_put(chunk, y - 2, slot)

            for lo in range(0, width, f_chunk):
                cols = slice(lo, lo + f_chunk)
                z = dot(x_buf[slot].reshape(rows, model), r.gate[:, cols])
                u = dot(x_buf[slot].reshape(rows, model), r.up[:, cols])
                hidden_buf[:, cols] = (jax.nn.silu(z) * u).astype(BF16)
            for lo in range(0, model, d_chunk):
                cols = slice(lo, lo + d_chunk)
                y_rows = dot(hidden_buf[...], r.down[:, cols]).astype(BF16)
                y_buf[slot, :, :, :, :, cols] = y_rows.reshape(group + (d_chunk,))
            start_put(chunk, y, slot)
            return c

        lax.fori_loop(0, side, one_tile, 0)
        for y in range(side - 2, side):
            wait_put(chunk, y, y % 2)

        def one_mate(offset, c):
            for p in range(3):
                place = mate_peer(BACK[p][0], offset)
                remote(
                    rows_of(outputs[p], p, chunk, place, BACK[p][1:]),
                    middles[p].at[chunk, pl.ds(0, side), pl.ds(0, side), back_mate[p]],
                    r.back_send.at[chunk, p],
                    r.back_recv.at[chunk, p],
                    place,
                ).start()
            return c

        lax.fori_loop(1, mates, one_mate, 0)

    def middle_rows(p, chunk, i, d):
        return middles[p].at[(chunk,) + ordered({BACK[p][1]: i, BACK[p][2]: d})]

    def pass_on(chunk):
        for p in range(3):
            wait_bytes(middles[p].at[chunk, pl.ds(0, side), pl.ds(0, side), pl.ds(0, mates - 1)], r.back_recv.at[chunk, p])
            for offset in range(1, side):
                axis = BACK[p][1]
                place = axis_peer(axis, offset)
                remote(
                    middle_rows(p, chunk, place[axis], pl.ds(0, side)),
                    results[p].at[chunk, pl.ds(0, side), me[axis]],
                    r.home_send.at[chunk, p],
                    r.home_recv.at[chunk, p],
                    place,
                ).start()


    split = r.split
    lanes = min(128, rows_block)

    def weigh_chunk(chunk, carry):
        for p in range(3):
            wait_bytes(results[p].at[chunk, pl.ds(0, side), pl.ds(0, side - 1)], r.home_recv.at[chunk, p])

        def source_of(p, n):
            ahead = 2 * side - 2 - 2 * n + 3 * (n // 2) if relay else 1 - n
            return lax.rem(me[BACK[p][2]] + ahead, side)

        def load(p, n, slot):
            copies = []
            for offset in range(side):
                i, d = lax.rem(me[BACK[p][1]] + offset, side), source_of(p, n)
                copies.append(
                    pltpu.make_async_copy(
                        results[p].at[chunk, d, i] if offset else middle_rows(p, chunk, i, d),
                        stage.at[pl.ds(slot * members + i * mates, mates), :, pl.ds(0, widths[p])],
                        r.load_sem.at[slot, offset],
                    )
                )
            return copies

        for copy in load(0, 0, 0):
            copy.start()

        def one_source(n, c):
            for p in range(3):
                d = source_of(p, n)
                slot = lax.rem(n + p, 2)

                @pl.when(n + p // 2 < side)
                def _():
                    for copy in load((p + 1) % 3, n + p // 2, 1 - slot):
                        copy.start()

                lane = lax.broadcasted_iota(I32, (1, lanes), 1)
                wanted = (lax.rem(lane, slots) + chunk * slots).astype(F32)
                for lo in range(0, rows_block, lanes):
                    which = jnp.broadcast_to(lane // slots + lo // slots, (tokens, lanes))
                    take = functools.partial(jnp.take_along_axis, indices=which, axis=1, mode='promise_in_bounds')
                    weight = jnp.where(take(r.held[p, d]) == wanted, take(r.gates[p, d]), 0.0)
                    high = weight.astype(BF16)
                    rest = weight - high.astype(F32)
                    middle = rest.astype(BF16)
                    low = (rest - middle.astype(F32)).astype(BF16)
                    split[0:tokens, lo : lo + lanes] = high
                    split[tokens : 2 * tokens, lo : lo + lanes] = middle
                    split[2 * tokens : 3 * tokens, lo : lo + lanes] = low
                for copy in load(p, n, slot):
                    copy.wait()
                for lo, size in steps(widths[p], TILE):
                    y = stage[pl.ds(slot * members, members), :, lo : lo + size].reshape(rows_block, size)
                    both = dot(split[...], y)
                    total = both[0:tokens] + (both[tokens : 2 * tokens] + both[2 * tokens : 3 * tokens])

                    @pl.when(chunk == 0)
                    def _():
                        sums[p][d, :, lo : lo + size] = total

                    @pl.when(chunk > 0)
                    def _():
                        sums[p][d, :, lo : lo + size] += total

                last = chunk == N_CHUNKS - 1
                axis = BACK[p][2]

                @pl.when(jnp.logical_and(last, n == 0))
                def _():
                    for k, stride in enumerate(strides):
                        part, spot, arrived = sums[p].at[d], others[p].at[0], r.sum_recv.at[p, 0]
                        if relay:
                            part = sums[p].at[d, halves[k]]
                            spot, arrived = others[p].at[2, halves[k]], r.sum_half.at[p, k]
                        remote(part, spot, r.sum_send.at[p], arrived, axis_peer(axis, stride)).start()

                for k in range(2 if relay else 0):

                    @pl.when(jnp.logical_and(last, n == 2 + k))
                    def _():
                        wait_bytes(others[p].at[2, halves[k]], r.sum_half.at[p, k])
                        sums[p][d, halves[k], :] += others[p][2, halves[k], :]
                        remote(
                            sums[p].at[d], others[p].at[k], r.sum_send.at[p], r.sum_recv.at[p, k], axis_peer(axis, strides[k])
                        ).start()

            return c

        return lax.fori_loop(0, side, one_source, carry)


    def one_by_one(step):
        lax.fori_loop(0, N_CHUNKS, lambda chunk, c: (step(chunk), c)[1], 0)

    one_by_one(expert_chunk)
    one_by_one(pass_on)
    gap = jnp.zeros((128 - members, tokens), F32)
    for p in range(3):
        wait_bytes(r.line_gates.at[p, pl.ds(0, side - 1)], r.gate_recv.at[p])
        first = plane_keys(p, (members, tokens)).astype(F32)

        def spread(d, c):
            info = r.line_gates[p, d]
            held, gate = jnp.full((members, tokens), -1.0, F32), jnp.zeros((members, tokens), F32)
            for j in range(top_k):
                there = info[j : j + 1, :] - first
                mine = jnp.logical_and(there >= 0, there < capacity)
                held = jnp.where(mine, there, held)
                gate = jnp.where(mine, info[top_k + j : top_k + j + 1, :], gate)
            r.held[p, d] = jnp.concatenate([held, gap], axis=0).T
            r.gates[p, d] = jnp.concatenate([gate, gap], axis=0).T
            return c

        lax.fori_loop(0, side, spread, 0)
    lax.fori_loop(0, N_CHUNKS, weigh_chunk, 0)
    for p, (lo, hi) in enumerate(parts):
        for k in range(len(strides)):
            wait_bytes(others[p].at[k], r.sum_recv.at[p, k])

        def finish(here):
            moe = sums[p][me[BACK[p][2]], here, :]
            for k in range(len(strides)):
                moe += others[p][k, here, :]
            r.out[here, lo:hi] = (r.dense[here, lo:hi] + moe).astype(BF16)

        bands(finish)


    for p in range(3):
        wait_bytes(tok[p].at[pl.ds(0, side - 1)], r.tok_send.at[p])
        wait_bytes(r.all_keys.at[p, 0, pl.ds(0, side - 1)], r.key_send.at[p])
        wait_bytes(far[p].at[pl.ds(0, side - 1)], r.far_send.at[p])
        wait_bytes(r.all_keys.at[p, pl.ds(0, side - 1)], r.far_key_send.at[p])
        wait_bytes(r.line_gates.at[p, pl.ds(0, side - 1)], r.gate_send.at[p])
        wait_bytes(others[p], r.sum_send.at[p])
        for chunk in range(N_CHUNKS):
            wait_bytes(sends[p].at[pl.ds(0, mates - 1)], r.go_send.at[chunk, p])
            wait_bytes(middles[p].at[chunk, pl.ds(0, side), pl.ds(0, side), pl.ds(0, mates - 1)], r.back_send.at[chunk, p])
            wait_bytes(results[p].at[chunk, pl.ds(0, side), pl.ds(0, side - 1)], r.home_send.at[chunk, p])


def layer_pair(small, large, side, capacity, head_dim):
    tokens, model = small['hidden'].shape
    top_k, width = small['ids_t'].shape[0], large['gate_hbm'].shape[1]
    key_dim, ff_dim = large['w_key'].shape[1], large['ffn_gate'].shape[1]
    parts = column_parts(model)
    widths = [hi - lo for lo, hi in parts]
    slots, members, mates = capacity // N_CHUNKS, side * side * 2, side * 2
    group = (side, 2, side, slots)
    rows = math.prod(group)
    sds, vmem = jax.ShapeDtypeStruct, pltpu.VMEM
    dma = lambda *shape: pltpu.SemaphoreType.DMA(shape)
    outs = dict(out=sds((tokens, model), BF16))
    scratch = dict(
        rows=vmem((tokens, model), BF16),
        query=vmem((tokens, large['w_query'].shape[1]), BF16),
        key=vmem((tokens, key_dim), BF16),
        value=vmem((tokens, key_dim), BF16),
        attended=vmem((tokens, model), BF16),
        act=vmem((tokens, ff_dim), BF16),
        dense=vmem((tokens, model), F32),
        ring=vmem((RING, model, TILE), BF16),
        all_keys=vmem((3, side, side, top_k, tokens), I32),
        my_gates=vmem((2 * top_k, tokens), F32),
        line_gates=vmem((3, side, 2 * top_k, tokens), F32),
        held=vmem((3, side, tokens, 128), F32),
        gates=vmem((3, side, tokens, 128), F32),
        source=vmem((3, tokens, max(widths)), BF16),
        stage=vmem((max(2 * members, 3 * N_CHUNKS * mates), slots, max(widths)), BF16),
        split=vmem((3 * tokens, members * slots), BF16),
        gate=vmem((model, width), BF16),
        up=vmem((model, width), BF16),
        down=vmem((width, model), BF16),
        x_buf=vmem((2,) + group + (model,), BF16),
        y_buf=vmem((2,) + group + (model,), BF16),
        hidden_buf=vmem((rows, width), BF16),
        weight_sem=dma(3),
        ring_sem=dma(RING),
        source_sem=dma(3),
        stage_sem=dma(3),
        keep_sem=dma(3, N_CHUNKS),
        in_sem=dma(2, 3),
        out_sem=dma(2, 3),
        own_sem=dma(2, 3),
        load_sem=dma(2, side),
        tok_send=dma(3),
        tok_recv=dma(3, 2),
        tok_half=dma(3, 2),
        key_send=dma(3),
        key_recv=dma(3),
        far_send=dma(3),
        far_recv=dma(3, 2, side),
        far_half=dma(3, 2, side),
        far_key_send=dma(3),
        far_key_recv=dma(3, side - 1),
        gate_send=dma(3),
        gate_recv=dma(3),
        sum_send=dma(3),
        sum_recv=dma(3, 2),
        sum_half=dma(3, 2),
        go_send=dma(N_CHUNKS, 3),
        go_recv=dma(N_CHUNKS, 3),
        back_send=dma(N_CHUNKS, 3),
        back_recv=dma(N_CHUNKS, 3),
        home_send=dma(N_CHUNKS, 3),
        home_recv=dma(N_CHUNKS, 3),
    )
    for p, w in enumerate(widths):
        there = sds((N_CHUNKS, side, side, 2, side, slots, w), BF16)
        outs['far' + str(p)] = sds((side, side, tokens, w), BF16)
        outs['send' + str(p)] = sds((N_CHUNKS * mates, side, side, slots, w), BF16)
        outs['arrive' + str(p)] = there
        outs['output' + str(p)] = there
        outs['middle' + str(p)] = sds((N_CHUNKS, side, side, mates, slots, w), BF16)
        outs['result' + str(p)] = sds((N_CHUNKS, side, side, mates, slots, w), BF16)
        scratch['tok' + str(p)] = vmem((side, tokens, w), BF16)
        scratch['sum' + str(p)] = vmem((side, tokens, w), F32)
        scratch['other' + str(p)] = vmem((side - 1, tokens, w), F32)
    anywhere = pl.BlockSpec(memory_space=pl.ANY)
    local = pl.BlockSpec(memory_space=pltpu.VMEM)
    n_rows = members * side * capacity
    return pl.pallas_call(
        functools.partial(
            kernel,
            names=tuple(small) + tuple(large) + tuple(outs) + tuple(scratch),
            side=side,
            parts=parts,
            capacity=capacity,
            head_dim=head_dim,
            f_chunk=min(256, width),
            d_chunk=min(512, model),
        ),
        out_shape=list(outs.values()),
        in_specs=[local] * len(small) + [anywhere] * len(large),
        out_specs=[local] + [anywhere] * (len(outs) - 1),
        scratch_shapes=list(scratch.values()),
        compiler_params=pltpu.CompilerParams(has_side_effects=True, vmem_limit_bytes=67043328),
        cost_estimate=pl.CostEstimate(flops=6 * n_rows * model * width, bytes_accessed=8 * n_rows * model, transcendentals=0),
    )(*small.values(), *large.values())[0]


def solution(mesh):
    group_size = mesh.shape['ep']
    side = torus_side(group_size)
    torus = jax.sharding.Mesh(mesh.devices.reshape(side, side, side, 2), AXES)
    row_spec = P(AXES, None, None)
    vec_spec = P(None)
    mat_spec = P(None, None)
    cube_spec = P(None, None, None)
    expert_spec = P(AXES, None, None)

    def per_device(hidden, expert_ids, slot_ids, attn_norm, w_query, w_key, w_value, w_out, ffn_norm, ffn_gate, ffn_up, ffn_down, moe_norm, w_router, exp_gate, exp_up, exp_down):
        n_seqs, tokens, model = hidden.shape
        assert n_seqs == 1 and exp_gate.shape[0] == 1
        n_heads, head_dim = w_out.shape[0], w_out.shape[1]
        top_k = expert_ids.shape[2]
        capacity = CAP_FACTOR * tokens * top_k // group_size
        inv_freq = np.float32(ROPE_BASE) ** (np.float32(-2.0) * np.arange(head_dim // 2, dtype=np.float32) / head_dim)
        angles = np.arange(tokens, dtype=np.float32)[:, None] * inv_freq[None, :]
        cos, sin = np.cos(angles), np.sin(angles)
        small = dict(
            hidden=hidden[0],
            attn_scale=attn_norm.reshape(-1, 128),
            moe_scale=moe_norm.reshape(-1, 128),
            ffn_scale=ffn_norm.reshape(-1, 128),
            ids_t=expert_ids[0].T,
            slots_t=slot_ids[0].T,
            w_router=w_router,
            cos=np.concatenate([cos, cos], axis=1).astype(np.float32),
            sin=np.concatenate([-sin, sin], axis=1).astype(np.float32),
        )
        large = dict(
            w_query=w_query,
            w_key=w_key,
            w_value=w_value,
            w_out=w_out.reshape(n_heads * head_dim, model),
            ffn_gate=ffn_gate,
            ffn_up=ffn_up,
            ffn_down=ffn_down,
            gate_hbm=exp_gate[0],
            up_hbm=exp_up[0],
            down_hbm=exp_down[0],
        )
        return layer_pair(small, large, side, capacity, head_dim).reshape(hidden.shape)

    return jax.shard_map(per_device, mesh=torus, in_specs=(row_spec, row_spec, row_spec, vec_spec, mat_spec, mat_spec, mat_spec, cube_spec, vec_spec, mat_spec, mat_spec, mat_spec, vec_spec, mat_spec, expert_spec, expert_spec, expert_spec), out_specs=row_spec, check_vma=False)
```

```python
import functools
import math
import types

import jax
import jax.numpy as jnp
import numpy as np
from jax import lax
from jax.experimental import pallas as pl
from jax.experimental.pallas import tpu as pltpu
from jax.sharding import PartitionSpec as P

RMS_EPS = 1e-6
ROPE_BASE = 10000.0
CAP_FACTOR = 3
N_CHUNKS = 3
RING = 6
TILE = 256
MESH = pl.DeviceIdType.MESH

BF16, F32, I32 = jnp.bfloat16, jnp.float32, jnp.int32

AXES = ('z', 'y', 'x', 'c')
OUT = (('z', 'y', 'x'), ('x', 'z', 'y'), ('y', 'x', 'z'))
BACK = (('y', 'z', 'x'), ('z', 'x', 'y'), ('x', 'y', 'z'))
ROW_AXES = ('y', 'x', 'c', 'z')


def torus_side(n_devices):
    side = round((n_devices // 2) ** (1 / 3))
    assert side ** 3 * 2 == n_devices
    return side


def column_parts(model):
    lanes = model // 128
    first = -(-lanes // 3)
    second = -(-(lanes - first) // 2)
    ends = (0, first * 128, (first + second) * 128, model)
    return tuple((ends[p], ends[p + 1]) for p in range(3))


def steps(total, size):
    return [(lo, min(size, total - lo)) for lo in range(0, total, size)]


def rms_rows(rows, scale):
    as_float = rows.astype(F32)
    inv_rms = lax.rsqrt(jnp.mean(as_float * as_float, axis=-1, keepdims=True) + RMS_EPS)
    return (as_float * inv_rms * scale.astype(F32)).astype(BF16)


def dot(a, b):
    return jnp.dot(a, b, preferred_element_type=F32)


def kernel(*refs, names, side, parts, capacity, head_dim, f_chunk, d_chunk):
    r = types.SimpleNamespace(**dict(zip(names, refs)))
    each = lambda name: [getattr(r, name + str(p)) for p in range(3)]
    slots = capacity // N_CHUNKS
    members = side * side * 2
    mates = side * 2
    assert side in (2, 4)
    relay = side == 4
    strides = (1, side - 1) if relay else (1,)
    order = (0, side - 1, 1, 2) if relay else (0, 1)
    rows_block = members * slots
    tokens, model = r.hidden.shape
    me = {axis: lax.axis_index(axis) for axis in AXES}


    def rows_of(ref, p, chunk, place, free):
        spot = [pl.ds(0, side) if axis in free else place[axis] for axis in ROW_AXES]
        return ref.at[tuple([chunk] + spot)]

    def ordered(where):
        return tuple(where[axis] for axis in ROW_AXES if axis in where)

    def device(place):
        return tuple(place[axis] for axis in AXES)

    def axis_peer(axis, offset):
        return {**me, axis: lax.rem(me[axis] + offset, side)}

    def mate_peer(axis, offset):
        return {
            **me,
            axis: lax.rem(me[axis] + offset // 2, side),
            'c': lax.rem(me['c'] + lax.rem(offset, 2), 2),
        }

    def remote(src, dst, send_sem, recv_sem, place):
        return pltpu.make_async_remote_copy(
            src_ref=src, dst_ref=dst, send_sem=send_sem, recv_sem=recv_sem, device_id=device(place), device_id_type=MESH
        )

    def wait_bytes(ref, sem):
        pltpu.make_async_copy(ref, ref, sem).wait()

    def expert_key(place, core, slot):
        return (((place['z'] * side + place['y']) * side + place['x']) * 2 + core) * capacity + slot

    def plane_keys(p, shape):
        first, second, _ = BACK[p]
        which = lax.broadcasted_iota(I32, shape, 0)
        pair = which // 2
        place = {**me, second: pair // side, first: lax.rem(pair, side)}
        return expert_key(place, lax.rem(which, 2), 0)

    def mate_keys(p, shape):
        mate = lax.broadcasted_iota(I32, shape, 0)
        return expert_key({**me, OUT[p][2]: mate // 2}, lax.rem(mate, 2), 0)

    tok, far, sends, arrivals, outputs = each('tok'), each('far'), each('send'), each('arrive'), each('output')
    middles, results, sums, others = each('middle'), each('result'), each('sum'), each('other')
    widths = [hi - lo for lo, hi in parts]


    band = min(32, tokens)

    def bands(body):
        lax.fori_loop(0, tokens // band, lambda i, c: (body(pl.ds(pl.multiple_of(i * band, band), band)), c)[1], 0)

    def one_row(scale):
        lines = scale[...].astype(F32)
        return jnp.concatenate([lines[i : i + 1, :] for i in range(lines.shape[0])], axis=1)

    def norm_both(here):
        normed = rms_rows(r.hidden[here, :], one_row(r.moe_scale))
        for p, (lo, hi) in enumerate(parts):
            tok[p][me[OUT[p][0]], here, :] = normed[:, lo:hi]
        r.rows[here, :] = rms_rows(r.hidden[here, :], one_row(r.attn_scale))

    bands(norm_both)
    keys_t = r.ids_t[...] * capacity + r.slots_t[...]
    for p in range(3):
        r.all_keys[p, me[OUT[p][1]], me[OUT[p][0]]] = keys_t
    pairs = ((r.gate_hbm, r.gate), (r.up_hbm, r.up), (r.down_hbm, r.down))
    loads = [pltpu.make_async_copy(src, dst, r.weight_sem.at[i]) for i, (src, dst) in enumerate(pairs)]
    for load in loads:
        load.start()

    half = tokens // 2
    halves = (pl.ds(0, half), pl.ds(half, half))

    def neighbour(axis, k):
        return lax.rem(me[axis] + side - strides[k], side)

    def send_far(p, n):
        near, axis, _ = OUT[p]
        d = lax.rem(me[near] + order[n], side)
        for k, stride in enumerate(strides):
            remote(
                tok[p].at[d], far[p].at[me[axis], d], r.far_send.at[p], r.far_recv.at[p, k, n], axis_peer(axis, stride)
            ).start()

    def pass_far(n):
        for k, stride in enumerate(strides):
            for p in range(3):
                near, axis, _ = OUT[p]
                d = lax.rem(me[near] + order[n], side)
                wait_bytes(tok[p].at[0], r.far_recv.at[p, k, n])
                if relay:
                    block = far[p].at[neighbour(axis, k), d, halves[k]]
                    remote(block, block, r.far_send.at[p], r.far_half.at[p, k, n], axis_peer(axis, stride)).start()

    for k, stride in enumerate(strides):
        for p in range(3):
            axis = OUT[p][0]
            block = tok[p].at[me[axis]]
            remote(block, block, r.tok_send.at[p], r.tok_recv.at[p, k], axis_peer(axis, stride)).start()
    for p in range(3):
        send_far(p, 0)
    for offset in range(1, side):
        for p in range(3):
            axis = OUT[p][0]
            keys = r.all_keys.at[p, me[OUT[p][1]], me[axis]]
            remote(keys, keys, r.key_send.at[p], r.key_recv.at[p], axis_peer(axis, offset)).start()


    ring = r.ring
    ring_sem = r.ring_sem

    def stream(n_steps, group, source, body):
        ahead = RING // group * group - group

        def copy(i, s):
            slot = lax.rem(i * group + s, RING // group * group)
            return pltpu.make_async_copy(source(i, s), ring.at[slot], ring_sem.at[slot])

        for i in range(min(ahead // group, n_steps)):
            for s in range(group):
                copy(i, s).start()

        def step(i, carry):
            @pl.when(i + ahead // group < n_steps)
            def _():
                for s in range(group):
                    copy(i + ahead // group, s).start()

            for s in range(group):
                copy(i, s).wait()
            body(i, [ring.at[lax.rem(i * group + s, RING // group * group)] for s in range(group)])
            return carry

        lax.fori_loop(0, n_steps, step, 0)

    def col_tile(i):
        return pl.ds(pl.multiple_of(i * TILE, TILE), TILE)

    def turned(y):
        return y * r.cos[...] + pltpu.roll(y, head_dim // 2, 1) * r.sin[...]

    def project(weight, out, rotary):
        def body(i, tiles):
            y = dot(r.rows[...], tiles[0][...])
            if rotary:
                y = jnp.concatenate([turned(y[:, lo : lo + head_dim]) for lo in range(0, TILE, head_dim)], axis=1)
            out[:, col_tile(i)] = y.astype(BF16)

        stream(weight.shape[1] // TILE, 1, lambda i, s: weight.at[:, col_tile(i)], body)

    project(r.w_query, r.query, True)
    project(r.w_key, r.key, True)
    project(r.w_value, r.value, False)


    logits = sum(dot(tok[p][me[OUT[p][0]]], r.w_router[lo:hi, :]) for p, (lo, hi) in enumerate(parts))
    top_k = r.ids_t.shape[0]
    gap = jnp.zeros((128 - 3 * top_k, tokens), F32)
    blank = jnp.zeros((top_k, tokens), F32)
    info = jnp.concatenate([keys_t.astype(F32), blank, r.ids_t[...].astype(F32), gap], axis=0).T
    lane = lax.broadcasted_iota(I32, logits.shape, 1).astype(F32)
    picked = [
        jnp.sum(jnp.where(lane == info[:, 2 * top_k + j : 2 * top_k + j + 1], logits, 0.0), axis=1, keepdims=True)
        for j in range(top_k)
    ]
    peak = functools.reduce(jnp.maximum, picked)
    powers = [jnp.exp(v - peak) for v in picked]
    norm = functools.reduce(jnp.add, powers)
    lane = lax.broadcasted_iota(I32, info.shape, 1)
    for j in range(top_k):
        info = jnp.where(lane == top_k + j, powers[j] / norm, info)
    r.my_gates[...] = info.T[0 : 2 * top_k, :]
    for p in range(3):
        r.line_gates[p, me[BACK[p][2]]] = r.my_gates[...]


    for k, stride in enumerate(strides):
        for p in range(3):
            axis = OUT[p][0]
            wait_bytes(tok[p].at[0], r.tok_recv.at[p, k])
            if relay:
                block = tok[p].at[neighbour(axis, k), halves[k]]
                remote(block, block, r.tok_send.at[p], r.tok_half.at[p, k], axis_peer(axis, stride)).start()
            send_far(p, 1 + k)
    pass_far(0)
    if relay:
        for p in range(3):
            for k in range(2):
                wait_bytes(tok[p].at[0, halves[k]], r.tok_half.at[p, k])
            send_far(p, 3)
    for p in range(3):
        wait_bytes(r.all_keys.at[p, 0, pl.ds(0, side - 1)], r.key_recv.at[p])
        for offset in range(1, side):
            keys = r.all_keys.at[p, me[OUT[p][1]]]
            remote(
                keys, keys, r.far_key_send.at[p], r.far_key_recv.at[p, offset - 1], axis_peer(OUT[p][1], offset)
            ).start()
    for offset in range(1, side):
        for p in range(3):
            axis = BACK[p][2]
            remote(
                r.my_gates, r.line_gates.at[p, me[axis]], r.gate_send.at[p], r.gate_recv.at[p], axis_peer(axis, offset)
            ).start()


    n_heads = r.query.shape[1] // head_dim
    per_key = r.query.shape[1] // r.key.shape[1]
    causal = lax.broadcasted_iota(I32, (tokens, tokens), 0) >= lax.broadcasted_iota(I32, (tokens, tokens), 1)

    def one_head(h, carry):
        cols = pl.ds(pl.multiple_of(h * head_dim, head_dim), head_dim)
        key_cols = pl.ds(pl.multiple_of(h // per_key * head_dim, head_dim), head_dim)
        scores = lax.dot_general(
            r.query[:, cols], r.key[:, key_cols], (((1,), (1,)), ((), ())), preferred_element_type=F32
        )
        scores = jnp.where(causal, scores * head_dim ** -0.5, -jnp.inf)
        power = jnp.exp(scores - jnp.max(scores, axis=1, keepdims=True))
        prob = (power / jnp.sum(power, axis=1, keepdims=True)).astype(BF16)
        r.query[:, cols] = dot(prob, r.value[:, key_cols]).astype(BF16)
        return carry


    stage = r.stage
    blocks = N_CHUNKS * mates
    out_mate = [me[OUT[p][2]] * 2 + me['c'] for p in range(3)]
    back_mate = [me[BACK[p][0]] * 2 + me['c'] for p in range(3)]

    def pick_rows(p, i, d, slot, source):
        keys = r.all_keys[p, i, d]
        first = mate_keys(p, (mates, tokens))
        held = jnp.full((mates, tokens), -1, I32)
        for j in range(top_k):
            slot_there = keys[j : j + 1, :] - first
            mine = jnp.logical_and(slot_there >= 0, slot_there < capacity)
            held = jnp.where(mine, slot_there, held)
        row_slot = lax.broadcasted_iota(I32, (capacity, tokens), 0)
        for mate in range(mates):
            pick = jnp.where(row_slot == held[mate : mate + 1, :], 1.0, 0.0).astype(BF16)
            for chunk in range(N_CHUNKS):
                at = (chunk * mates + mate) * slots
                r.split[at : at + slots, 0:tokens] = pick[chunk * slots : (chunk + 1) * slots, :]
        for lo, n in steps(widths[p], TILE):
            found = dot(r.split[0 : blocks * slots, 0:tokens], source[:, lo : lo + n]).astype(BF16)
            stage[slot, 0:blocks, :, lo : lo + n] = found.reshape(blocks, slots, n)

    def flush(p, i, d, slot):
        a, b = ordered({OUT[p][1]: i, OUT[p][0]: d})
        return pltpu.make_async_copy(
            stage.at[slot, pl.ds(0, blocks), :, pl.ds(0, widths[p])],
            sends[p].at[pl.ds(0, blocks), a, b],
            r.stage_sem.at[slot],
        )

    def keep(p, i, d, slot, chunk):
        spot = {**me, OUT[p][1]: i, OUT[p][0]: d}
        return pltpu.make_async_copy(
            stage.at[slot, chunk * mates + out_mate[p], :, pl.ds(0, widths[p])],
            arrivals[p].at[(chunk,) + ordered(spot)],
            r.keep_sem.at[slot, chunk],
        )

    def send_rows(p, chunk, i):
        near, far_axis, axis = OUT[p]
        free = (near,) if i is not None else (near, far_axis)
        a, b = ordered({far_axis: pl.ds(0, side) if i is None else i, near: pl.ds(0, side)})
        group_place = me if i is None else {**me, far_axis: i}

        def one_mate(offset, c):
            place = mate_peer(axis, offset)
            remote(
                sends[p].at[chunk * mates + place[axis] * 2 + place['c'], a, b],
                rows_of(arrivals[p], p, chunk, group_place, free),
                r.go_send.at[chunk, p],
                r.go_recv.at[chunk, p],
                place,
            ).start()
            return c

        lax.fori_loop(1, mates, one_mate, 0)

    def pick_group(offset):
        for p in range(3):
            i = lax.rem(me[OUT[p][1]] + side - offset, side)
            if offset:
                wait_bytes(r.all_keys.at[p, 0], r.far_key_recv.at[p, offset - 1])
            if relay and offset == 2:
                for n in range(side):
                    for k in range(2):
                        wait_bytes(tok[p].at[0, halves[k]], r.far_half.at[p, k, n])

            def load(d, slot):
                return pltpu.make_async_copy(
                    far[p].at[i, d], r.source.at[slot, :, pl.ds(0, widths[p])], r.source_sem.at[slot]
                )

            if offset:
                load(0, 0).start()

            def one_source(d, c):
                slot = lax.rem(d, 2)
                if offset:

                    @pl.when(d + 1 < side)
                    def _():
                        load(d + 1, 1 - slot).start()

                    load(d, slot).wait()

                @pl.when(d >= 2)
                def _():
                    flush(p, i, d - 2, slot).wait()
                    for chunk in range(N_CHUNKS):
                        keep(p, i, d - 2, slot, chunk).wait()

                pick_rows(p, i, d, slot, r.source.at[slot] if offset else tok[p].at[d])
                flush(p, i, d, slot).start()
                for chunk in range(N_CHUNKS):
                    keep(p, i, d, slot, chunk).start()
                return c

            lax.fori_loop(0, side, one_source, 0)
            for d in range(side - 2, side):
                flush(p, i, d, d % 2).wait()
                for chunk in range(N_CHUNKS):
                    keep(p, i, d, d % 2, chunk).wait()
            if offset:
                send_rows(p, 0, i)

    def heads(part, n_parts):
        lax.fori_loop(n_heads * part // n_parts, n_heads * (part + 1) // n_parts, one_head, 0)

    pick_group(0)
    for n in range(1, side):
        heads(n - 1, side - 1)
        pass_far(n)
    for p in range(3):
        send_rows(p, 0, me[OUT[p][1]])
    for offset in (1, 3, 2) if relay else (1,):
        pick_group(offset)
    for chunk in range(1, N_CHUNKS):
        for p in range(3):
            send_rows(p, chunk, None)


    out_split = n_heads * head_dim // model

    def out_body(i, tiles):
        total = r.hidden[:, col_tile(i)].astype(F32)
        attended = dot(r.query[:, 0:model], tiles[0][...])
        for s in range(1, out_split):
            attended += dot(r.query[:, s * model : (s + 1) * model], tiles[s][...])
        r.attended[:, col_tile(i)] = (total + attended).astype(BF16)

    stream(model // TILE, out_split, lambda i, s: r.w_out.at[pl.ds(s * model, model), col_tile(i)], out_body)

    def norm_attended(here):
        r.rows[here, :] = rms_rows(r.attended[here, :], one_row(r.ffn_scale))

    bands(norm_attended)

    def act_body(i, tiles):
        z = dot(r.rows[...], tiles[0][...])
        u = dot(r.rows[...], tiles[1][...])
        r.act[:, col_tile(i)] = (jax.nn.silu(z) * u).astype(BF16)

    ff_dim = r.ffn_gate.shape[1]
    stream(
        ff_dim // TILE, 2, lambda i, s: (r.ffn_gate, r.ffn_up)[s].at[:, col_tile(i)], act_body
    )
    down_split = ff_dim // model

    def down_body(i, tiles):
        total = dot(r.act[:, 0:model], tiles[0][...])
        for s in range(1, down_split):
            total += dot(r.act[:, s * model : (s + 1) * model], tiles[s][...])
        r.dense[:, col_tile(i)] = r.attended[:, col_tile(i)].astype(F32) + total

    stream(model // TILE, down_split, lambda i, s: r.ffn_down.at[pl.ds(s * model, model), col_tile(i)], down_body)


    for load in loads:
        load.wait()
    x_buf, y_buf, hidden_buf = r.x_buf, r.y_buf, r.hidden_buf
    group = x_buf.shape[1:-1]
    rows = math.prod(group)
    width = hidden_buf.shape[1]

    def fetch(chunk, y, slot):
        return [
            pltpu.make_async_copy(
                arrivals[p].at[chunk, y], x_buf.at[slot, :, :, :, :, pl.ds(lo, hi - lo)], r.in_sem.at[slot, p]
            )
            for p, (lo, hi) in enumerate(parts)
        ]

    def put(chunk, y, slot):
        return [
            pltpu.make_async_copy(
                y_buf.at[slot, :, :, :, :, pl.ds(lo, hi - lo)], outputs[p].at[chunk, y], r.out_sem.at[slot, p]
            )
            for p, (lo, hi) in enumerate(parts)
        ]

    def keep_own(chunk, y, slot, p):
        lo, hi = parts[p]
        free = BACK[p][1:]
        spot = [pl.ds(0, side) if axis in free else me[axis] for axis in ROW_AXES[1:]]
        mine = pltpu.make_async_copy(
            y_buf.at[tuple([slot] + spot + [pl.ds(0, slots), pl.ds(lo, hi - lo)])],
            middles[p].at[
                (chunk,) + ordered({axis: y if axis == 'y' else pl.ds(0, side) for axis in free}) + (back_mate[p],)
            ],
            r.own_sem.at[slot, p],
        )
        return mine, (None if 'y' in free else y == me['y'])

    def start_put(chunk, y, slot):
        for copy in put(chunk, y, slot):
            copy.start()
        for p in range(3):
            copy, when = keep_own(chunk, y, slot, p)
            if when is None:
                copy.start()
            else:
                pl.when(when)(copy.start)

    def wait_put(chunk, y, slot):
        for copy in put(chunk, y, slot):
            copy.wait()
        for p in range(3):
            copy, when = keep_own(chunk, y, slot, p)
            if when is None:
                copy.wait()
            else:
                pl.when(when)(copy.wait)

    def expert_chunk(chunk):
        for p in range(3):
            wait_bytes(sends[p].at[pl.ds(0, mates - 1)], r.go_recv.at[chunk, p])
        for copy in fetch(chunk, 0, 0):
            copy.start()

        def one_tile(y, c):
            slot = lax.rem(y, 2)

            @pl.when(y + 1 < side)
            def _():
                for copy in fetch(chunk, y + 1, 1 - slot):
                    copy.start()

            for copy in fetch(chunk, y, slot):
                copy.wait()

            @pl.when(y >= 2)
            def _():
                wait_put(chunk, y - 2, slot)

            for lo in range(0, width, f_chunk):
                cols = slice(lo, lo + f_chunk)
                z = dot(x_buf[slot].reshape(rows, model), r.gate[:, cols])
                u = dot(x_buf[slot].reshape(rows, model), r.up[:, cols])
                hidden_buf[:, cols] = (jax.nn.silu(z) * u).astype(BF16)
            for lo in range(0, model, d_chunk):
                cols = slice(lo, lo + d_chunk)
                y_rows = dot(hidden_buf[...], r.down[:, cols]).astype(BF16)
                y_buf[slot, :, :, :, :, cols] = y_rows.reshape(group + (d_chunk,))
            start_put(chunk, y, slot)
            return c

        lax.fori_loop(0, side, one_tile, 0)
        for y in range(side - 2, side):
            wait_put(chunk, y, y % 2)

        def one_mate(offset, c):
            for p in range(3):
                place = mate_peer(BACK[p][0], offset)
                remote(
                    rows_of(outputs[p], p, chunk, place, BACK[p][1:]),
                    middles[p].at[chunk, pl.ds(0, side), pl.ds(0, side), back_mate[p]],
                    r.back_send.at[chunk, p],
                    r.back_recv.at[chunk, p],
                    place,
                ).start()
            return c

        lax.fori_loop(1, mates, one_mate, 0)

    def middle_rows(p, chunk, i, d):
        return middles[p].at[(chunk,) + ordered({BACK[p][1]: i, BACK[p][2]: d})]

    def pass_on(chunk):
        for p in range(3):
            wait_bytes(middles[p].at[chunk, pl.ds(0, side), pl.ds(0, side), pl.ds(0, mates - 1)], r.back_recv.at[chunk, p])
            for offset in range(1, side):
                axis = BACK[p][1]
                place = axis_peer(axis, offset)
                remote(
                    middle_rows(p, chunk, place[axis], pl.ds(0, side)),
                    results[p].at[chunk, pl.ds(0, side), me[axis]],
                    r.home_send.at[chunk, p],
                    r.home_recv.at[chunk, p],
                    place,
                ).start()


    split = r.split
    lanes = min(128, rows_block)

    def weigh_chunk(chunk, carry):
        for p in range(3):
            wait_bytes(results[p].at[chunk, pl.ds(0, side), pl.ds(0, side - 1)], r.home_recv.at[chunk, p])

        def source_of(p, n):
            ahead = 2 * side - 2 - 2 * n + 3 * (n // 2) if relay else 1 - n
            return lax.rem(me[BACK[p][2]] + ahead, side)

        def load(p, n, slot):
            copies = []
            for offset in range(side):
                i, d = lax.rem(me[BACK[p][1]] + offset, side), source_of(p, n)
                copies.append(
                    pltpu.make_async_copy(
                        results[p].at[chunk, d, i] if offset else middle_rows(p, chunk, i, d),
                        stage.at[slot, pl.ds(i * mates, mates), :, pl.ds(0, widths[p])],
                        r.load_sem.at[slot, offset],
                    )
                )
            return copies

        for copy in load(0, 0, 0):
            copy.start()

        def one_source(n, c):
            for p in range(3):
                d = source_of(p, n)
                slot = lax.rem(n + p, 2)

                @pl.when(n + p // 2 < side)
                def _():
                    for copy in load((p + 1) % 3, n + p // 2, 1 - slot):
                        copy.start()

                lane = lax.broadcasted_iota(I32, (1, lanes), 1)
                wanted = (lax.rem(lane, slots) + chunk * slots).astype(F32)
                for lo in range(0, rows_block, lanes):
                    which = jnp.broadcast_to(lane // slots + lo // slots, (tokens, lanes))
                    take = functools.partial(jnp.take_along_axis, indices=which, axis=1, mode='promise_in_bounds')
                    weight = jnp.where(take(r.held[p, d]) == wanted, take(r.gates[p, d]), 0.0)
                    high = weight.astype(BF16)
                    rest = weight - high.astype(F32)
                    middle = rest.astype(BF16)
                    low = (rest - middle.astype(F32)).astype(BF16)
                    split[0:tokens, lo : lo + lanes] = high
                    split[tokens : 2 * tokens, lo : lo + lanes] = middle
                    split[2 * tokens : 3 * tokens, lo : lo + lanes] = low
                for copy in load(p, n, slot):
                    copy.wait()
                for lo, size in steps(widths[p], TILE):
                    y = stage[slot, 0:members, :, lo : lo + size].reshape(rows_block, size)
                    both = dot(split[...], y)
                    total = both[0:tokens] + (both[tokens : 2 * tokens] + both[2 * tokens : 3 * tokens])

                    @pl.when(chunk == 0)
                    def _():
                        sums[p][d, :, lo : lo + size] = total

                    @pl.when(chunk > 0)
                    def _():
                        sums[p][d, :, lo : lo + size] += total

                last = chunk == N_CHUNKS - 1
                axis = BACK[p][2]

                @pl.when(jnp.logical_and(last, n == 0))
                def _():
                    for k, stride in enumerate(strides):
                        part, spot, arrived = sums[p].at[d], others[p].at[0], r.sum_recv.at[p, 0]
                        if relay:
                            part = sums[p].at[d, halves[k]]
                            spot, arrived = others[p].at[2, halves[k]], r.sum_half.at[p, k]
                        remote(part, spot, r.sum_send.at[p], arrived, axis_peer(axis, stride)).start()

                for k in range(2 if relay else 0):

                    @pl.when(jnp.logical_and(last, n == 2 + k))
                    def _():
                        wait_bytes(others[p].at[2, halves[k]], r.sum_half.at[p, k])
                        sums[p][d, halves[k], :] += others[p][2, halves[k], :]
                        remote(
                            sums[p].at[d], others[p].at[k], r.sum_send.at[p], r.sum_recv.at[p, k], axis_peer(axis, strides[k])
                        ).start()

            return c

        return lax.fori_loop(0, side, one_source, carry)


    def one_by_one(step):
        lax.fori_loop(0, N_CHUNKS, lambda chunk, c: (step(chunk), c)[1], 0)

    one_by_one(expert_chunk)
    one_by_one(pass_on)
    gap = jnp.zeros((128 - members, tokens), F32)
    for p in range(3):
        wait_bytes(r.line_gates.at[p, pl.ds(0, side - 1)], r.gate_recv.at[p])
        first = plane_keys(p, (members, tokens)).astype(F32)

        def spread(d, c):
            info = r.line_gates[p, d]
            held, gate = jnp.full((members, tokens), -1.0, F32), jnp.zeros((members, tokens), F32)
            for j in range(top_k):
                there = info[j : j + 1, :] - first
                mine = jnp.logical_and(there >= 0, there < capacity)
                held = jnp.where(mine, there, held)
                gate = jnp.where(mine, info[top_k + j : top_k + j + 1, :], gate)
            r.held[p, d] = jnp.concatenate([held, gap], axis=0).T
            r.gates[p, d] = jnp.concatenate([gate, gap], axis=0).T
            return c

        lax.fori_loop(0, side, spread, 0)
    lax.fori_loop(0, N_CHUNKS, weigh_chunk, 0)
    for p, (lo, hi) in enumerate(parts):
        for k in range(len(strides)):
            wait_bytes(others[p].at[k], r.sum_recv.at[p, k])

        def finish(here):
            moe = sums[p][me[BACK[p][2]], here, :]
            for k in range(len(strides)):
                moe += others[p][k, here, :]
            r.out[here, lo:hi] = (r.dense[here, lo:hi] + moe).astype(BF16)

        bands(finish)


    for p in range(3):
        wait_bytes(tok[p].at[pl.ds(0, side - 1)], r.tok_send.at[p])
        wait_bytes(r.all_keys.at[p, 0, pl.ds(0, side - 1)], r.key_send.at[p])
        wait_bytes(far[p].at[pl.ds(0, side - 1)], r.far_send.at[p])
        wait_bytes(r.all_keys.at[p, pl.ds(0, side - 1)], r.far_key_send.at[p])
        wait_bytes(r.line_gates.at[p, pl.ds(0, side - 1)], r.gate_send.at[p])
        wait_bytes(others[p], r.sum_send.at[p])
        for chunk in range(N_CHUNKS):
            wait_bytes(sends[p].at[pl.ds(0, mates - 1)], r.go_send.at[chunk, p])
            wait_bytes(middles[p].at[chunk, pl.ds(0, side), pl.ds(0, side), pl.ds(0, mates - 1)], r.back_send.at[chunk, p])
            wait_bytes(results[p].at[chunk, pl.ds(0, side), pl.ds(0, side - 1)], r.home_send.at[chunk, p])


def layer_pair(small, large, side, capacity, head_dim):
    tokens, model = small['hidden'].shape
    top_k, width = small['ids_t'].shape[0], large['gate_hbm'].shape[1]
    key_dim, ff_dim = large['w_key'].shape[1], large['ffn_gate'].shape[1]
    parts = column_parts(model)
    widths = [hi - lo for lo, hi in parts]
    slots, members, mates = capacity // N_CHUNKS, side * side * 2, side * 2
    group = (side, 2, side, slots)
    rows = math.prod(group)
    sds, vmem = jax.ShapeDtypeStruct, pltpu.VMEM
    dma = lambda *shape: pltpu.SemaphoreType.DMA(shape)
    outs = dict(out=sds((tokens, model), BF16))
    scratch = dict(
        rows=vmem((tokens, model), BF16),
        query=vmem((tokens, large['w_query'].shape[1]), BF16),
        key=vmem((tokens, key_dim), BF16),
        value=vmem((tokens, key_dim), BF16),
        attended=vmem((tokens, model), BF16),
        act=vmem((tokens, ff_dim), BF16),
        dense=vmem((tokens, model), F32),
        ring=vmem((RING, model, TILE), BF16),
        all_keys=vmem((3, side, side, top_k, tokens), I32),
        my_gates=vmem((2 * top_k, tokens), F32),
        line_gates=vmem((3, side, 2 * top_k, tokens), F32),
        held=vmem((3, side, tokens, 128), F32),
        gates=vmem((3, side, tokens, 128), F32),
        source=vmem((2, tokens, max(widths)), BF16),
        stage=vmem((2, max(members, N_CHUNKS * mates), slots, max(widths)), BF16),
        split=vmem((3 * tokens, members * slots), BF16),
        gate=vmem((model, width), BF16),
        up=vmem((model, width), BF16),
        down=vmem((width, model), BF16),
        x_buf=vmem((2,) + group + (model,), BF16),
        y_buf=vmem((2,) + group + (model,), BF16),
        hidden_buf=vmem((rows, width), BF16),
        weight_sem=dma(3),
        ring_sem=dma(RING),
        source_sem=dma(2),
        stage_sem=dma(2),
        keep_sem=dma(2, N_CHUNKS),
        in_sem=dma(2, 3),
        out_sem=dma(2, 3),
        own_sem=dma(2, 3),
        load_sem=dma(2, side),
        tok_send=dma(3),
        tok_recv=dma(3, 2),
        tok_half=dma(3, 2),
        key_send=dma(3),
        key_recv=dma(3),
        far_send=dma(3),
        far_recv=dma(3, 2, side),
        far_half=dma(3, 2, side),
        far_key_send=dma(3),
        far_key_recv=dma(3, side - 1),
        gate_send=dma(3),
        gate_recv=dma(3),
        sum_send=dma(3),
        sum_recv=dma(3, 2),
        sum_half=dma(3, 2),
        go_send=dma(N_CHUNKS, 3),
        go_recv=dma(N_CHUNKS, 3),
        back_send=dma(N_CHUNKS, 3),
        back_recv=dma(N_CHUNKS, 3),
        home_send=dma(N_CHUNKS, 3),
        home_recv=dma(N_CHUNKS, 3),
    )
    for p, w in enumerate(widths):
        there = sds((N_CHUNKS, side, side, 2, side, slots, w), BF16)
        outs['far' + str(p)] = sds((side, side, tokens, w), BF16)
        outs['send' + str(p)] = sds((N_CHUNKS * mates, side, side, slots, w), BF16)
        outs['arrive' + str(p)] = there
        outs['output' + str(p)] = there
        outs['middle' + str(p)] = sds((N_CHUNKS, side, side, mates, slots, w), BF16)
        outs['result' + str(p)] = sds((N_CHUNKS, side, side, mates, slots, w), BF16)
        scratch['tok' + str(p)] = vmem((side, tokens, w), BF16)
        scratch['sum' + str(p)] = vmem((side, tokens, w), F32)
        scratch['other' + str(p)] = vmem((side - 1, tokens, w), F32)
    anywhere = pl.BlockSpec(memory_space=pl.ANY)
    local = pl.BlockSpec(memory_space=pltpu.VMEM)
    n_rows = members * side * capacity
    return pl.pallas_call(
        functools.partial(
            kernel,
            names=tuple(small) + tuple(large) + tuple(outs) + tuple(scratch),
            side=side,
            parts=parts,
            capacity=capacity,
            head_dim=head_dim,
            f_chunk=min(256, width),
            d_chunk=min(512, model),
        ),
        out_shape=list(outs.values()),
        in_specs=[local] * len(small) + [anywhere] * len(large),
        out_specs=[local] + [anywhere] * (len(outs) - 1),
        scratch_shapes=list(scratch.values()),
        compiler_params=pltpu.CompilerParams(has_side_effects=True, vmem_limit_bytes=67043328),
        cost_estimate=pl.CostEstimate(flops=6 * n_rows * model * width, bytes_accessed=8 * n_rows * model, transcendentals=0),
    )(*small.values(), *large.values())[0]


def solution(mesh):
    group_size = mesh.shape['ep']
    side = torus_side(group_size)
    torus = jax.sharding.Mesh(mesh.devices.reshape(side, side, side, 2), AXES)
    row_spec = P(AXES, None, None)
    vec_spec = P(None)
    mat_spec = P(None, None)
    cube_spec = P(None, None, None)
    expert_spec = P(AXES, None, None)

    def per_device(hidden, expert_ids, slot_ids, attn_norm, w_query, w_key, w_value, w_out, ffn_norm, ffn_gate, ffn_up, ffn_down, moe_norm, w_router, exp_gate, exp_up, exp_down):
        n_seqs, tokens, model = hidden.shape
        assert n_seqs == 1 and exp_gate.shape[0] == 1
        n_heads, head_dim = w_out.shape[0], w_out.shape[1]
        top_k = expert_ids.shape[2]
        capacity = CAP_FACTOR * tokens * top_k // group_size
        inv_freq = np.float32(ROPE_BASE) ** (np.float32(-2.0) * np.arange(head_dim // 2, dtype=np.float32) / head_dim)
        angles = np.arange(tokens, dtype=np.float32)[:, None] * inv_freq[None, :]
        cos, sin = np.cos(angles), np.sin(angles)
        small = dict(
            hidden=hidden[0],
            attn_scale=attn_norm.reshape(-1, 128),
            moe_scale=moe_norm.reshape(-1, 128),
            ffn_scale=ffn_norm.reshape(-1, 128),
            ids_t=expert_ids[0].T,
            slots_t=slot_ids[0].T,
            w_router=w_router,
            cos=np.concatenate([cos, cos], axis=1).astype(np.float32),
            sin=np.concatenate([-sin, sin], axis=1).astype(np.float32),
        )
        large = dict(
            w_query=w_query,
            w_key=w_key,
            w_value=w_value,
            w_out=w_out.reshape(n_heads * head_dim, model),
            ffn_gate=ffn_gate,
            ffn_up=ffn_up,
            ffn_down=ffn_down,
            gate_hbm=exp_gate[0],
            up_hbm=exp_up[0],
            down_hbm=exp_down[0],
        )
        return layer_pair(small, large, side, capacity, head_dim).reshape(hidden.shape)

    return jax.shard_map(per_device, mesh=torus, in_specs=(row_spec, row_spec, row_spec, vec_spec, mat_spec, mat_spec, mat_spec, cube_spec, vec_spec, mat_spec, mat_spec, mat_spec, vec_spec, mat_spec, expert_spec, expert_spec, expert_spec), out_specs=row_spec, check_vma=False)
```
